32 devices in a mesh: member: 2 (over x), lat: 16 (over z, y, core).
Axes of the slice: x: 2, y: 2, z: 4, core: 2. Of those that a mesh axis runs over, the one named last changes fastest.
Arguments:
- field_in: float32 [24, 128, 128, 256], P('member', None, 'lat'), parts along dimension 0
- grad_out: float32 [24, 128, 128, 256], P('member', None, 'lat'), parts along dimension 0
- p_fwd: float32 [128, 128, 128], replicated
- p_inv: float32 [128, 128, 128], replicated
- w_mix: float32 [128, 128, 128, 2], replicated
Outputs:
- output 1: float32 [24, 128, 128, 256], P('member', None, 'lat'), parts along dimension 0
- output 2: float32 [256, 128, 128, 2], P('member'), parts along dimension 0
There are 2 independent parts. The reference program is written for one: setup_inputs(seed, part) draws one part's arguments, and reference() takes and returns one part's arrays. A program takes and returns all parts, laid end to end along the dimension named above; an argument that names none is the same for every part.
All inputs are finite; a program needn't handle non-finite values.
Results may differ from the reference program's by a relative error of at most 0.00656154.
Values are sent between devices in bfloat16 or wider.
A program may use at most 1 GiB of HBM per device.

```python
import math
import jax
import jax.numpy as jnp
from jax import lax

BATCH = 12
CHANNELS = 128
NLAT = 128

NLON = 2 * NLAT


def setup_inputs(seed: int = 0, part: int = 0) -> dict:
    part_key = jax.random.fold_in(jax.random.key(seed), part)
    key_field, key_grad = jax.random.split(part_key, 2)
    key_fwd, key_inv, key_mix = jax.random.split(jax.random.key(seed + 1), 3)
    field_in = jax.random.normal(key_field, (BATCH, CHANNELS, NLAT, NLON), jnp.float32)
    grad_out = jax.random.normal(key_grad, (BATCH, CHANNELS, NLAT, NLON), jnp.float32)
    wave_num = jnp.arange(NLAT)[:, None, None]
    degree = jnp.arange(NLAT)[None, :, None]
    lower_tri = (degree >= wave_num).astype(jnp.float32)
    fwd_scale = lower_tri / math.sqrt(NLAT)
    inv_scale = lower_tri / jnp.sqrt((NLAT - wave_num).astype(jnp.float32))
    p_fwd = jax.random.normal(key_fwd, (NLAT, NLAT, NLAT), jnp.float32) * fwd_scale
    p_inv = jax.random.normal(key_inv, (NLAT, NLAT, NLAT), jnp.float32) * inv_scale
    w_mix = jax.random.normal(key_mix, (NLAT, CHANNELS, CHANNELS, 2), jnp.float32) / math.sqrt(2 * CHANNELS)
    return {'field_in': field_in, 'grad_out': grad_out, 'p_fwd': p_fwd, 'p_inv': p_inv, 'w_mix': w_mix}


def to_bf16(values):
    return values.astype(jnp.bfloat16).astype(jnp.float32)


def gelu_grad(values):
    cumulative = 0.5 * (1.0 + lax.erf(values * math.sqrt(0.5)))
    density = jnp.exp(-0.5 * values * values) / math.sqrt(2.0 * math.pi)
    return cumulative + values * density


def mix_matrix(w_mix):
    w_real = w_mix[..., 0]
    w_imag = w_mix[..., 1]
    upper_half = jnp.stack([w_real, -w_imag], axis=-1)
    lower_half = jnp.stack([w_imag, w_real], axis=-1)
    return jnp.stack([upper_half, lower_half], axis=2)


def analysis(values, mode_gains):
    spectrum = jnp.fft.rfft(values, axis=-1)[..., :NLAT] * mode_gains
    return jnp.stack([spectrum.real, spectrum.imag], axis=-2)


def synthesis(spec_pair, mode_gains):
    complex_spec = lax.complex(spec_pair[..., 0, :], spec_pair[..., 1, :]) * mode_gains
    padded = jnp.pad(complex_spec, [(0, 0)] * (complex_spec.ndim - 1) + [(0, NLON // 2 + 1 - NLAT)])
    return jnp.fft.irfft(padded, n=NLON, axis=-1)


def reference(field_in, grad_out, p_fwd, p_inv, w_mix):
    root_lon = math.sqrt(NLON)
    is_mean = jnp.arange(NLAT) == 0
    pw_half = to_bf16(p_fwd)
    pi_half = to_bf16(p_inv)
    w_big = to_bf16(mix_matrix(w_mix))
    four_lat = to_bf16(analysis(field_in, 1.0 / root_lon))
    coeffs = to_bf16(jnp.einsum('mlt,bctrm->bclrm', pw_half, four_lat))
    mixed_coef = to_bf16(jnp.einsum('losir,bilrm->bolsm', w_big, coeffs))
    back_lat = to_bf16(jnp.einsum('mlt,bclrm->bctrm', pi_half, mixed_coef))
    hidden = synthesis(back_lat, root_lon)
    grad_hidden = grad_out * gelu_grad(hidden)
    grad_back = to_bf16(analysis(grad_hidden, jnp.where(is_mean, 1.0, 2.0) / root_lon))
    grad_mixed = to_bf16(jnp.einsum('mlt,bctrm->bclrm', pi_half, grad_back))
    grad_big = jnp.einsum('bolsm,bilrm->losir', grad_mixed, coeffs)
    grad_coef = to_bf16(jnp.einsum('losir,bolsm->bilrm', w_big, grad_mixed))
    grad_four = to_bf16(jnp.einsum('mlt,bclrm->bctrm', pw_half, grad_coef))
    grad_field = grad_out + synthesis(grad_four, jnp.where(is_mean, 1.0, 0.5) * root_lon)
    grad_wmix = jnp.stack([grad_big[:, :, 0, :, 0] + grad_big[:, :, 1, :, 1], grad_big[:, :, 1, :, 0] - grad_big[:, :, 0, :, 1]], axis=-1)
    return grad_field, grad_wmix
```

```python
import functools
import math

import jax
import jax.numpy as jnp
import numpy as np
from jax import lax
from jax.experimental import pallas as pl
from jax.experimental.pallas import tpu as pltpu
from jax.sharding import PartitionSpec as P

MESH = pl.DeviceIdType.MESH
LANES = 128
SLOTS = 3
VMEM_LIMIT = 60 * 1024 * 1024
F32 = jnp.float32
BF16 = jnp.bfloat16

NN = (((1,), (0,)), ((), ()))
NT = (((1,), (1,)), ((), ()))
TN = (((0,), (0,)), ((), ()))


def dot(lhs, rhs, dims):
    return lax.dot_general(lhs, rhs, dims, preferred_element_type=F32)


def split_halves(values):
    high = values.astype(BF16)
    low = (values - high.astype(F32)).astype(BF16)
    return high, low


def dft_tables(group, m_local, lon_count):
    owner, slot, part = np.meshgrid(np.arange(group), np.arange(m_local), np.arange(2), indexing='ij')
    wave = (slot * group + owner).reshape(-1)
    part = part.reshape(-1)
    phase = 2.0 * np.pi * ((wave[:, None] * np.arange(lon_count)[None, :]) % lon_count) / lon_count
    base = np.where(part[:, None] == 0, np.cos(phase), -np.sin(phase)) / math.sqrt(lon_count)
    gains = np.where(wave == 0, 1.0, 2.0)[:, None]
    return base.astype(np.float32), (base * gains).astype(np.float32)


def two_halves(table):
    high = jnp.asarray(table).astype(BF16)
    low = (jnp.asarray(table) - high.astype(F32)).astype(BF16)
    return jnp.stack([high, low])


class Halves:
    def __init__(self, whole, b, halves, slot, sem, outward=False):
        self.copies = []
        for half in range(halves.shape[1]):
            ends = whole.at[b, :, pl.ds(half * LANES, LANES)], halves.at[slot, half]
            source, target = ends[::-1] if outward else ends
            self.copies.append(pltpu.make_async_copy(source, target, sem.at[slot, half]))

    def start(self):
        for copy in self.copies:
            copy.start()

    def wait(self):
        for copy in self.copies:
            copy.wait()


def read_row(halves, slot, t, channels, rows_local):
    at = pl.ds(t, channels, stride=rows_local)
    return jnp.concatenate([halves[slot, half, at, :] for half in range(halves.shape[1])], axis=1)


def write_row(halves, slot, t, channels, rows_local, values):
    at = pl.ds(t, channels, stride=rows_local)
    for half in range(halves.shape[1]):
        halves[slot, half, at, :] = values[:, half * LANES:(half + 1) * LANES]


class Exchange:
    def __init__(self, me, group, batch, send, recv, send_sem, recv_sem):
        self.me, self.group, self.batch = me, group, batch
        self.send, self.recv, self.send_sem, self.recv_sem = send, recv, send_sem, recv_sem

    def all_copies(self, b):
        slot = lax.rem(b, SLOTS)
        others = pl.ds(0, self.group - 1)
        return pltpu.make_async_remote_copy(
            self.send.at[slot, others], self.recv.at[b, others], self.send_sem.at[slot], self.recv_sem.at[b],
            device_id={'lat': lax.rem(self.me + 1, self.group)}, device_id_type=MESH)

    def reserve(self, b):
        @pl.when(b >= SLOTS)
        def _():
            self.all_copies(b - SLOTS).wait_send()

    def start(self, b):
        slot = lax.rem(b, SLOTS)
        self.recv[b, self.me] = self.send[slot, self.me]

        @pl.loop(1, self.group)
        def _(step):
            target = lax.rem(self.me + step, self.group)
            pltpu.make_async_remote_copy(
                self.send.at[slot, target], self.recv.at[b, self.me], self.send_sem.at[slot], self.recv_sem.at[b],
                device_id={'lat': target}, device_id_type=MESH).start()

    def arrive(self, b):
        self.all_copies(b).wait_recv()

    def drain(self):
        for b in range(max(0, self.batch - SLOTS), self.batch):
            self.all_copies(b).wait_send()


def enter(me, group):
    barrier = pltpu.get_barrier_semaphore()

    @pl.loop(1, group)
    def _(step):
        pl.semaphore_signal(barrier, inc=1, device_id={'lat': lax.rem(me + step, group)}, device_id_type=MESH)

    pl.semaphore_wait(barrier, group - 1)


def load_legendre(me, group, table_hbm, stage, sem):
    m_local = stage.shape[0]
    copies = [pltpu.make_async_copy(table_hbm.at[slot * group + me], stage.at[slot], sem) for slot in range(m_local)]
    for copy in copies:
        copy.start()
    pltpu.make_async_copy(table_hbm.at[pl.ds(0, m_local)], stage, sem).wait()


def expand_rows(stage, expanded, rows_local):
    m_local, degrees, lats = stage.shape
    row = lax.broadcasted_iota(jnp.int32, (lats, 2 * lats), 0)
    col = lax.broadcasted_iota(jnp.int32, (lats, 2 * lats), 1)
    source = col // (2 * rows_local)
    inner = col % (2 * rows_local)
    for part in range(2):
        pick = (row == source * rows_local + inner - part * rows_local) & (inner // rows_local == part)
        pick = pick.astype(F32).astype(BF16)
        for slot in range(m_local):
            expanded[slot, pl.ds(part * degrees, degrees), :] = dot(stage[slot].astype(BF16), pick, NN).astype(BF16)


def flip_rows(stage, flipped):
    for slot in range(stage.shape[0]):
        flipped[slot] = stage[slot].T.astype(BF16)


def analyse(values_at, table, turn, rows_local):
    modes = table.shape[1]
    for t in range(0, rows_local, 2):
        pair = jnp.concatenate([values_at(t), values_at(t + 1)], axis=0)
        high, low = split_halves(pair)
        out = dot(table[0], high, NT) + dot(table[0], low, NT) + dot(table[1], high, NT)
        channels = out.shape[1] // 2
        turn[pl.ds(t, modes, stride=rows_local), :] = out[:, :channels]
        turn[pl.ds(t + 1, modes, stride=rows_local), :] = out[:, channels:]


def pack_blocks(turn, send, slot):
    group, rows, lanes = send.shape[1:]
    for d in range(group):
        send[slot, d] = turn[pl.ds(d * rows, rows), :].astype(BF16)


def unpack_blocks(recv, b, turn):
    group, rows, lanes = recv.shape[1:]
    for d in range(group):
        turn[pl.ds(d * rows, rows), :] = recv[b, d].astype(F32)


def synthesise(turn, t, table, rows_local):
    modes = table.shape[1]
    spec = turn[pl.ds(t, modes, stride=rows_local), :].astype(BF16)
    return dot(spec, table[0], TN) + dot(spec, table[1], TN)


def legendre_forward(recv, b, expanded, out, rows_local):
    m_local = expanded.shape[0]
    degrees = expanded.shape[1] // 2
    group, _, lanes = recv.shape[1:]
    tile = 2 * rows_local
    for slot in range(m_local):
        rows = recv[b, :, pl.ds(slot * tile, tile), :].reshape(group * tile, lanes)
        res = dot(expanded[slot], rows, NN)
        for part in range(2):
            out[part, pl.ds(slot, degrees, stride=m_local), :] = res[part * degrees:(part + 1) * degrees]


def legendre_inverse(coef, flipped, send, slot_out, rows_local):
    m_local, lats, degrees = flipped.shape
    group = lats // rows_local
    tile = 2 * rows_local
    for slot in range(m_local):
        parts = [coef.at[part][pl.ds(slot, degrees, stride=m_local), :].astype(BF16) for part in range(2)]
        res = dot(flipped[slot], jnp.concatenate(parts, axis=1), NN)
        lanes = res.shape[1] // 2
        blocks = [res[:, part * lanes:(part + 1) * lanes].reshape(group, rows_local, lanes) for part in range(2)]
        send[slot_out, :, pl.ds(slot * tile, tile), :] = jnp.concatenate(blocks, axis=1).astype(BF16)


def gelu_slope(values):
    cumulative = 0.5 * (1.0 + lax.erf(values * math.sqrt(0.5)))
    density = jnp.exp(-0.5 * values * values) * (1.0 / math.sqrt(2.0 * math.pi))
    return cumulative + values * density


def mix_block(w_block):
    half = w_block.shape[0] // 2
    w_real = w_block[pl.ds(0, half, stride=2), :]
    w_imag = w_block[pl.ds(1, half, stride=2), :]
    top = jnp.concatenate([w_real, -w_imag], axis=1)
    bottom = jnp.concatenate([w_imag, w_real], axis=1)
    return jnp.concatenate([top, bottom], axis=0).astype(BF16)


def rows_of_degree(block, inner, m_local):
    batch = block.shape[0]
    lanes = block.shape[-1]
    parts = [block[:, part, pl.ds(inner * m_local, m_local), :].reshape(batch * m_local, lanes) for part in range(2)]
    return jnp.concatenate(parts, axis=1).astype(BF16)


def first_kernel(group, rows_local, field, table, p_fwd, coef_out, field_buf, stage, expanded, turn, send, recv,
                 coef_buf, in_sem, out_sem, p_sem, send_sem, recv_sem):
    me = lax.axis_index('lat')
    batch = field.shape[0]
    channels = field.shape[1] // rows_local

    def fetch(b):
        return Halves(field, b, field_buf, lax.rem(b, 2), in_sem)

    def put(b):
        return pltpu.make_async_copy(coef_buf.at[lax.rem(b, 2)], coef_out.at[b], out_sem.at[lax.rem(b, 2)])

    fetch(0).start()
    enter(me, group)
    swap = Exchange(me, group, batch, send, recv, send_sem, recv_sem)
    lag = 2

    def body(i, carry):
        @pl.when(i < batch)
        def _():
            @pl.when(i + 1 < batch)
            def _():
                fetch(i + 1).start()

            fetch(i).wait()
            half = lax.rem(i, 2)
            analyse(lambda t: read_row(field_buf, half, t, channels, rows_local), table, turn, rows_local)
            swap.reserve(i)
            pack_blocks(turn, send, lax.rem(i, SLOTS))
            swap.start(i)

        @pl.when(i == 0)
        def _():
            load_legendre(me, group, p_fwd, stage, p_sem)
            expand_rows(stage, expanded, rows_local)

        @pl.when(i >= lag)
        def _():
            b = i - lag
            swap.arrive(b)

            @pl.when(b >= 2)
            def _():
                put(b - 2).wait()

            legendre_forward(recv, b, expanded, coef_buf.at[lax.rem(b, 2)], rows_local)
            put(b).start()

        return carry

    lax.fori_loop(0, batch + lag, body, 0)
    swap.drain()
    put(batch - 2).wait()
    put(batch - 1).wait()


def mix_loop(w_hbm, in_hbms, bufs, w_buf, w_sem, in_sems, blocks, step):
    per = w_buf.shape[1]

    def copies(k):
        slot = lax.rem(k, 2)
        out = [pltpu.make_async_copy(w_hbm.at[pl.ds(k * per, per)], w_buf.at[slot], w_sem.at[slot])]
        for src, buf, sem in zip(in_hbms, bufs, in_sems):
            rows = buf.shape[3]
            out.append(pltpu.make_async_copy(src.at[:, :, pl.ds(k * rows, rows), :], buf.at[slot], sem.at[slot]))
        return out

    for copy in copies(0):
        copy.start()

    def body(k, carry):
        @pl.when(k + 1 < blocks)
        def _():
            for copy in copies(k + 1):
                copy.start()

        for copy in copies(k):
            copy.wait()
        step(k, lax.rem(k, 2))
        return carry

    lax.fori_loop(0, blocks, body, 0)


def second_kernel(group, rows_local, coef, w_mix, p_inv, table, grad, mixed_out, w_buf, coef_blk, mixed, stage, flipped,
                  expanded, turn, grad_buf, out_buf, send_a, recv_a, send_b, recv_b, w_sem, c_sem, in_sem, out_sem, p_sem,
                  send_a_sem, recv_a_sem, send_b_sem, recv_b_sem):
    me = lax.axis_index('lat')
    batch = grad.shape[0]
    channels = grad.shape[1] // rows_local
    m_local = stage.shape[0]
    per = w_buf.shape[1]
    degrees = stage.shape[1]

    def fetch(b):
        return Halves(grad, b, grad_buf, lax.rem(b, 2), in_sem)

    def put(b):
        return pltpu.make_async_copy(out_buf.at[lax.rem(b, 2)], mixed_out.at[b], out_sem.at[lax.rem(b, 2)])

    fetch(0).start()
    load_legendre(me, group, p_inv, stage, p_sem)
    flip_rows(stage, flipped)
    expand_rows(stage, expanded, rows_local)

    def mix(k, slot):
        for inner in range(per):
            rows = rows_of_degree(coef_blk.at[slot], inner, m_local)
            res = dot(rows, mix_block(w_buf.at[slot, inner]), NT)
            at = pl.ds(pl.multiple_of((k * per + inner) * m_local, m_local), m_local)
            for part in range(2):
                lanes = res.shape[1] // 2
                mixed[:, part, at, :] = res[:, part * lanes:(part + 1) * lanes].reshape(batch, m_local, lanes)

    mix_loop(w_mix, [coef], [coef_blk], w_buf, w_sem, [c_sem], degrees // per, mix)

    enter(me, group)
    swap_a = Exchange(me, group, batch, send_a, recv_a, send_a_sem, recv_a_sem)
    swap_b = Exchange(me, group, batch, send_b, recv_b, send_b_sem, recv_b_sem)
    lag = 2

    def body(i, carry):
        @pl.when(i < batch)
        def _():
            swap_a.reserve(i)
            legendre_inverse(mixed.at[i], flipped, send_a, lax.rem(i, SLOTS), rows_local)
            swap_a.start(i)

        @pl.when((i >= lag) & (i < batch + lag))
        def _():
            b = i - lag
            half = lax.rem(b, 2)

            @pl.when(b + 1 < batch)
            def _():
                fetch(b + 1).start()

            fetch(b).wait()
            swap_a.arrive(b)
            unpack_blocks(recv_a, b, turn)
            for t in range(rows_local):
                slope = gelu_slope(synthesise(turn, t, table, rows_local))
                given = read_row(grad_buf, half, t, channels, rows_local)
                write_row(grad_buf, half, t, channels, rows_local, given * slope)
            analyse(lambda t: read_row(grad_buf, half, t, channels, rows_local), table, turn, rows_local)
            swap_b.reserve(b)
            pack_blocks(turn, send_b, lax.rem(b, SLOTS))
            swap_b.start(b)

        @pl.when(i >= 2 * lag)
        def _():
            b = i - 2 * lag
            swap_b.arrive(b)

            @pl.when(b >= 2)
            def _():
                put(b - 2).wait()

            legendre_forward(recv_b, b, expanded, out_buf.at[lax.rem(b, 2)], rows_local)
            put(b).start()

        return carry

    lax.fori_loop(0, batch + 2 * lag, body, 0)
    swap_a.drain()
    swap_b.drain()
    put(batch - 2).wait()
    put(batch - 1).wait()


def weight_kernel(mixed, coef, w_mix, grad_w, back, w_buf, mixed_blk, coef_blk, gw_buf, back_buf, w_sem, m_sem, c_sem,
                  gw_sem, back_sem):
    per = w_buf.shape[1]
    batch = mixed.shape[0]
    degrees = w_mix.shape[0]
    m_local = mixed.shape[2] // degrees
    blocks = degrees // per

    def puts(k):
        slot = lax.rem(k, 2)
        rows = per * m_local
        return [pltpu.make_async_copy(gw_buf.at[slot], grad_w.at[pl.ds(k * per, per)], gw_sem.at[slot]),
                pltpu.make_async_copy(back_buf.at[slot], back.at[:, :, pl.ds(k * rows, rows), :], back_sem.at[slot])]

    def step(k, slot):
        @pl.when(k >= 2)
        def _():
            for copy in puts(k - 2):
                copy.wait()

        for inner in range(per):
            rows = rows_of_degree(mixed_blk.at[slot], inner, m_local)
            keep = rows_of_degree(coef_blk.at[slot], inner, m_local)
            res = dot(rows, mix_block(w_buf.at[slot, inner]), NN)
            at = pl.ds(inner * m_local, m_local)
            half = res.shape[1] // 2
            for part in range(2):
                back_buf[slot, :, part, at, :] = res[:, part * half:(part + 1) * half].reshape(batch, m_local, half)
            big = dot(rows, keep, TN)
            gw_buf[slot, inner, pl.ds(0, half, stride=2), :] = big[:half, :half] + big[half:, half:]
            gw_buf[slot, inner, pl.ds(1, half, stride=2), :] = big[half:, :half] - big[:half, half:]
        for copy in puts(k):
            copy.start()

    mix_loop(w_mix, [mixed, coef], [mixed_blk, coef_blk], w_buf, w_sem, [m_sem, c_sem], blocks, step)
    for k in (blocks - 2, blocks - 1):
        for copy in puts(k):
            copy.wait()


def last_kernel(group, rows_local, back, p_fwd, table, grad, field_out, back_buf, stage, flipped, turn, grad_buf, send, recv,
                b_sem, in_sem, out_sem, p_sem, send_sem, recv_sem):
    me = lax.axis_index('lat')
    batch = grad.shape[0]
    channels = grad.shape[1] // rows_local
    ring = grad_buf.shape[0]

    def fetch_back(b):
        return pltpu.make_async_copy(back.at[b], back_buf.at[lax.rem(b, 2)], b_sem.at[lax.rem(b, 2)])

    def fetch(b):
        return Halves(grad, b, grad_buf, lax.rem(b, ring), in_sem)

    def put(b):
        return Halves(field_out, b, grad_buf, lax.rem(b, ring), out_sem, outward=True)

    fetch_back(0).start()
    fetch(0).start()
    load_legendre(me, group, p_fwd, stage, p_sem)
    flip_rows(stage, flipped)
    enter(me, group)
    swap = Exchange(me, group, batch, send, recv, send_sem, recv_sem)
    lag = 2

    def body(i, carry):
        @pl.when(i < batch)
        def _():
            @pl.when(i + 1 < batch)
            def _():
                fetch_back(i + 1).start()

            fetch_back(i).wait()
            swap.reserve(i)
            legendre_inverse(back_buf.at[lax.rem(i, 2)], flipped, send, lax.rem(i, SLOTS), rows_local)
            swap.start(i)

        @pl.when(i >= lag)
        def _():
            b = i - lag
            half = lax.rem(b, ring)

            @pl.when(b >= ring - 1)
            def _():
                put(b - ring + 1).wait()

            @pl.when(b + 1 < batch)
            def _():
                fetch(b + 1).start()

            fetch(b).wait()
            swap.arrive(b)
            unpack_blocks(recv, b, turn)
            for t in range(rows_local):
                added = synthesise(turn, t, table, rows_local)
                given = read_row(grad_buf, half, t, channels, rows_local)
                write_row(grad_buf, half, t, channels, rows_local, given + added)
            put(b).start()

        return carry

    lax.fori_loop(0, batch + lag, body, 0)
    swap.drain()
    for b in range(batch - ring + 1, batch):
        put(b).wait()


def any_specs(n):
    return [pl.BlockSpec(memory_space=pl.ANY)] * n


def params(collective_id=None):
    if collective_id is None:
        return pltpu.CompilerParams(vmem_limit_bytes=VMEM_LIMIT)
    return pltpu.CompilerParams(collective_id=collective_id, has_side_effects=True, vmem_limit_bytes=VMEM_LIMIT)


def solution(mesh):
    group = mesh.shape['lat']
    field_spec = P('member', None, 'lat', None)

    def local_step(field_loc, grad_loc, p_fwd, p_inv, w_mix):
        batch, channels, rows_local, lon_count = field_loc.shape
        degrees, lats = p_fwd.shape[1:]
        m_local = p_fwd.shape[0] // group
        modes = group * m_local * 2
        base, gained = (two_halves(table) for table in dft_tables(group, m_local, lon_count))
        field = field_loc.reshape(batch, channels * rows_local, lon_count)
        grad = grad_loc.reshape(batch, channels * rows_local, lon_count)
        w_rows = jnp.swapaxes(w_mix, 2, 3).reshape(degrees, channels * 2, channels)
        dma, vmem = pltpu.SemaphoreType.DMA, pltpu.VMEM
        block_rows = m_local * 2 * rows_local
        coef_shape = (batch, 2, degrees * m_local, channels)
        send_t = vmem((SLOTS, group, block_rows, channels), BF16)
        recv_t = vmem((batch, group, block_rows, channels), BF16)
        turn_t = vmem((modes * rows_local, channels), F32)
        stage_t = vmem((m_local, degrees, lats), F32)
        expanded_t = vmem((m_local, 2 * degrees, 2 * lats), BF16)
        flipped_t = vmem((m_local, lats, degrees), BF16)
        pair_t = vmem((2, 2, degrees * m_local, channels), F32)
        field_t = vmem((2, lon_count // LANES, channels * rows_local, LANES), F32)
        table_spec = pl.BlockSpec(memory_space=pltpu.VMEM)
        any_spec = pl.BlockSpec(memory_space=pl.ANY)
        per = 8

        coef = pl.pallas_call(
            functools.partial(first_kernel, group, rows_local), name='first',
            out_shape=jax.ShapeDtypeStruct(coef_shape, F32),
            in_specs=[any_spec, table_spec, any_spec], out_specs=any_spec,
            scratch_shapes=[field_t, stage_t, expanded_t, turn_t, send_t, recv_t, pair_t, dma((2, 2)), dma((2,)), dma(()),
                            dma((SLOTS,)), dma((batch,))],
            compiler_params=params(0))(field, base, p_fwd)

        blk_t = vmem((2, batch, 2, per * m_local, channels), F32)
        w_t = vmem((2, per, channels * 2, channels), F32)
        mixed = pl.pallas_call(
            functools.partial(second_kernel, group, rows_local), name='second',
            out_shape=jax.ShapeDtypeStruct(coef_shape, F32),
            in_specs=[any_spec, any_spec, any_spec, table_spec, any_spec], out_specs=any_spec,
            scratch_shapes=[w_t, blk_t, vmem(coef_shape, F32), stage_t, flipped_t, expanded_t, turn_t, field_t, pair_t,
                            send_t, recv_t, send_t, recv_t, dma((2,)), dma((2,)), dma((2, 2)), dma((2,)), dma(()),
                            dma((SLOTS,)), dma((batch,)), dma((SLOTS,)), dma((batch,))],
            compiler_params=params(1))(coef, w_rows, p_inv, gained, grad)

        gw_part, back = pl.pallas_call(
            weight_kernel, name='weight',
            out_shape=[jax.ShapeDtypeStruct(w_rows.shape, F32), jax.ShapeDtypeStruct(coef_shape, F32)],
            in_specs=[any_spec] * 3, out_specs=[any_spec] * 2,
            scratch_shapes=[w_t, blk_t, blk_t, w_t, blk_t, dma((2,)), dma((2,)), dma((2,)), dma((2,)), dma((2,))],
            compiler_params=params())(mixed, coef, w_rows)
        gw_total = lax.psum(gw_part, 'lat')

        field_out = pl.pallas_call(
            functools.partial(last_kernel, group, rows_local), name='last',
            out_shape=jax.ShapeDtypeStruct(grad.shape, F32),
            in_specs=[any_spec, any_spec, table_spec, any_spec], out_specs=any_spec,
            scratch_shapes=[pair_t, stage_t, flipped_t, turn_t, vmem((3, lon_count // LANES, channels * rows_local, LANES), F32), send_t,
                            recv_t, dma((2,)), dma((3, 2)), dma((3, 2)), dma(()), dma((SLOTS,)), dma((batch,))],
            compiler_params=params(2))(back, p_fwd, base, grad)

        grad_wmix = jnp.swapaxes(gw_total.reshape(degrees, channels, 2, channels), 2, 3)
        return field_out.reshape(grad_loc.shape), grad_wmix

    return jax.shard_map(local_step, mesh=mesh, in_specs=(field_spec, field_spec, P(), P(), P()),
                         out_specs=(field_spec, P('member', None, None, None)), check_vma=False)
```

```python
import functools
import math

import jax
import jax.numpy as jnp
import numpy as np
from jax import lax
from jax.experimental import pallas as pl
from jax.experimental.pallas import tpu as pltpu
from jax.sharding import PartitionSpec as P

MESH = pl.DeviceIdType.MESH
LANES = 128
SLOTS = 3
VMEM_LIMIT = 60 * 1024 * 1024
F32 = jnp.float32
BF16 = jnp.bfloat16

NN = (((1,), (0,)), ((), ()))
NT = (((1,), (1,)), ((), ()))
TN = (((0,), (0,)), ((), ()))


def dot(lhs, rhs, dims):
    return lax.dot_general(lhs, rhs, dims, preferred_element_type=F32)


def split_halves(values):
    high = values.astype(BF16)
    low = (values - high.astype(F32)).astype(BF16)
    return high, low


def dft_tables(group, m_local, lon_count):
    owner, slot, part = np.meshgrid(np.arange(group), np.arange(m_local), np.arange(2), indexing='ij')
    wave = (slot * group + owner).reshape(-1)
    part = part.reshape(-1)
    phase = 2.0 * np.pi * ((wave[:, None] * np.arange(lon_count)[None, :]) % lon_count) / lon_count
    base = np.where(part[:, None] == 0, np.cos(phase), -np.sin(phase)) / math.sqrt(lon_count)
    gains = np.where(wave == 0, 1.0, 2.0)[:, None]
    return base.astype(np.float32), (base * gains).astype(np.float32)


def two_halves(table):
    high = jnp.asarray(table).astype(BF16)
    low = (jnp.asarray(table) - high.astype(F32)).astype(BF16)
    return jnp.stack([high, low])


class Halves:
    def __init__(self, whole, b, halves, slot, sem, outward=False):
        self.copies = []
        for half in range(halves.shape[1]):
            ends = whole.at[b, :, pl.ds(half * LANES, LANES)], halves.at[slot, half]
            source, target = ends[::-1] if outward else ends
            self.copies.append(pltpu.make_async_copy(source, target, sem.at[slot, half]))

    def start(self):
        for copy in self.copies:
            copy.start()

    def wait(self):
        for copy in self.copies:
            copy.wait()


def read_row(halves, slot, t, channels, rows_local):
    at = pl.ds(t, channels, stride=rows_local)
    return jnp.concatenate([halves[slot, half, at, :] for half in range(halves.shape[1])], axis=1)


def write_row(halves, slot, t, channels, rows_local, values):
    at = pl.ds(t, channels, stride=rows_local)
    for half in range(halves.shape[1]):
        halves[slot, half, at, :] = values[:, half * LANES:(half + 1) * LANES]


class Exchange:
    def __init__(self, me, group, batch, send, recv, send_sem, recv_sem):
        self.me, self.group, self.batch = me, group, batch
        self.send, self.recv, self.send_sem, self.recv_sem = send, recv, send_sem, recv_sem

    def all_copies(self, b):
        slot = lax.rem(b, SLOTS)
        others = pl.ds(0, self.group - 1)
        return pltpu.make_async_remote_copy(
            self.send.at[slot, others], self.recv.at[b, others], self.send_sem.at[slot], self.recv_sem.at[b],
            device_id={'lat': lax.rem(self.me + 1, self.group)}, device_id_type=MESH)

    def reserve(self, b):
        @pl.when(b >= SLOTS)
        def _():
            self.all_copies(b - SLOTS).wait_send()

    def start(self, b):
        slot = lax.rem(b, SLOTS)
        self.recv[b, self.me] = self.send[slot, self.me]

        @pl.loop(1, self.group)
        def _(step):
            target = lax.rem(self.me + step, self.group)
            pltpu.make_async_remote_copy(
                self.send.at[slot, target], self.recv.at[b, self.me], self.send_sem.at[slot], self.recv_sem.at[b],
                device_id={'lat': target}, device_id_type=MESH).start()

    def arrive(self, b):
        self.all_copies(b).wait_recv()

    def drain(self):
        for b in range(max(0, self.batch - SLOTS), self.batch):
            self.all_copies(b).wait_send()


def enter(me, group):
    barrier = pltpu.get_barrier_semaphore()

    @pl.loop(1, group)
    def _(step):
        pl.semaphore_signal(barrier, inc=1, device_id={'lat': lax.rem(me + step, group)}, device_id_type=MESH)

    pl.semaphore_wait(barrier, group - 1)


def load_legendre(me, group, table_hbm, stage, sem):
    m_local = stage.shape[0]
    copies = [pltpu.make_async_copy(table_hbm.at[slot * group + me], stage.at[slot], sem) for slot in range(m_local)]
    for copy in copies:
        copy.start()
    pltpu.make_async_copy(table_hbm.at[pl.ds(0, m_local)], stage, sem).wait()


def expand_rows(stage, expanded, rows_local):
    m_local, degrees, lats = stage.shape
    row = lax.broadcasted_iota(jnp.int32, (lats, 2 * lats), 0)
    col = lax.broadcasted_iota(jnp.int32, (lats, 2 * lats), 1)
    source = col // (2 * rows_local)
    inner = col % (2 * rows_local)
    for part in range(2):
        pick = (row == source * rows_local + inner - part * rows_local) & (inner // rows_local == part)
        pick = pick.astype(F32).astype(BF16)
        for slot in range(m_local):
            expanded[slot, pl.ds(part * degrees, degrees), :] = dot(stage[slot].astype(BF16), pick, NN).astype(BF16)


def flip_rows(stage, flipped):
    for slot in range(stage.shape[0]):
        flipped[slot] = stage[slot].T.astype(BF16)


def analyse(values_at, table, turn, rows_local):
    modes = table.shape[1]
    for t in range(0, rows_local, 2):
        pair = jnp.concatenate([values_at(t), values_at(t + 1)], axis=0)
        high, low = split_halves(pair)
        out = dot(table[0], high, NT) + dot(table[0], low, NT) + dot(table[1], high, NT)
        channels = out.shape[1] // 2
        turn[pl.ds(t, modes, stride=rows_local), :] = out[:, :channels]
        turn[pl.ds(t + 1, modes, stride=rows_local), :] = out[:, channels:]


def pack_blocks(turn, send, slot):
    group, rows, lanes = send.shape[1:]
    for d in range(group):
        send[slot, d] = turn[pl.ds(d * rows, rows), :].astype(BF16)


def unpack_blocks(recv, b, turn):
    group, rows, lanes = recv.shape[1:]
    for d in range(group):
        turn[pl.ds(d * rows, rows), :] = recv[b, d].astype(F32)


def synthesise(turn, t, table, rows_local):
    modes = table.shape[1]
    spec = turn[pl.ds(t, modes, stride=rows_local), :].astype(BF16)
    return dot(spec, table[0], TN) + dot(spec, table[1], TN)


def legendre_forward(recv, b, expanded, out, rows_local):
    m_local = expanded.shape[0]
    degrees = expanded.shape[1] // 2
    group, _, lanes = recv.shape[1:]
    tile = 2 * rows_local
    for slot in range(m_local):
        rows = recv[b, :, pl.ds(slot * tile, tile), :].reshape(group * tile, lanes)
        res = dot(expanded[slot], rows, NN)
        for part in range(2):
            out[part, pl.ds(slot, degrees, stride=m_local), :] = res[part * degrees:(part + 1) * degrees]


def legendre_inverse(coef, flipped, send, slot_out, rows_local):
    m_local, lats, degrees = flipped.shape
    group = lats // rows_local
    tile = 2 * rows_local
    for slot in range(m_local):
        parts = [coef.at[part][pl.ds(slot, degrees, stride=m_local), :].astype(BF16) for part in range(2)]
        res = dot(flipped[slot], jnp.concatenate(parts, axis=1), NN)
        lanes = res.shape[1] // 2
        blocks = [res[:, part * lanes:(part + 1) * lanes].reshape(group, rows_local, lanes) for part in range(2)]
        send[slot_out, :, pl.ds(slot * tile, tile), :] = jnp.concatenate(blocks, axis=1).astype(BF16)


def gelu_slope(values):
    cumulative = 0.5 * (1.0 + lax.erf(values * math.sqrt(0.5)))
    density = jnp.exp(-0.5 * values * values) * (1.0 / math.sqrt(2.0 * math.pi))
    return cumulative + values * density


def mix_block(w_block):
    half = w_block.shape[0] // 2
    w_real = w_block[pl.ds(0, half, stride=2), :]
    w_imag = w_block[pl.ds(1, half, stride=2), :]
    top = jnp.concatenate([w_real, -w_imag], axis=1)
    bottom = jnp.concatenate([w_imag, w_real], axis=1)
    return jnp.concatenate([top, bottom], axis=0).astype(BF16)


def rows_of_degree(block, inner, m_local):
    batch = block.shape[0]
    lanes = block.shape[-1]
    parts = [block[:, part, pl.ds(inner * m_local, m_local), :].reshape(batch * m_local, lanes) for part in range(2)]
    return jnp.concatenate(parts, axis=1).astype(BF16)


def first_kernel(group, rows_local, field, table, p_fwd, coef_out, field_buf, stage, expanded, turn, send, recv,
                 coef_buf, in_sem, out_sem, p_sem, send_sem, recv_sem):
    me = lax.axis_index('lat')
    batch = field.shape[0]
    channels = field.shape[1] // rows_local

    def fetch(b):
        return Halves(field, b, field_buf, lax.rem(b, 2), in_sem)

    def put(b):
        return pltpu.make_async_copy(coef_buf.at[lax.rem(b, 2)], coef_out.at[b], out_sem.at[lax.rem(b, 2)])

    fetch(0).start()
    enter(me, group)
    swap = Exchange(me, group, batch, send, recv, send_sem, recv_sem)
    lag = 2

    def body(i, carry):
        @pl.when(i < batch)
        def _():
            @pl.when(i + 1 < batch)
            def _():
                fetch(i + 1).start()

            fetch(i).wait()
            half = lax.rem(i, 2)
            analyse(lambda t: read_row(field_buf, half, t, channels, rows_local), table, turn, rows_local)
            swap.reserve(i)
            pack_blocks(turn, send, lax.rem(i, SLOTS))
            swap.start(i)

        @pl.when(i == 0)
        def _():
            load_legendre(me, group, p_fwd, stage, p_sem)
            expand_rows(stage, expanded, rows_local)

        @pl.when(i >= lag)
        def _():
            b = i - lag
            swap.arrive(b)

            @pl.when(b >= 2)
            def _():
                put(b - 2).wait()

            legendre_forward(recv, b, expanded, coef_buf.at[lax.rem(b, 2)], rows_local)
            put(b).start()

        return carry

    lax.fori_loop(0, batch + lag, body, 0)
    swap.drain()
    put(batch - 2).wait()
    put(batch - 1).wait()


def mix_loop(w_hbm, in_hbms, bufs, w_buf, w_sem, in_sems, blocks, step):
    per = w_buf.shape[1]

    def copies(k):
        slot = lax.rem(k, 2)
        out = [pltpu.make_async_copy(w_hbm.at[pl.ds(k * per, per)], w_buf.at[slot], w_sem.at[slot])]
        for src, buf, sem in zip(in_hbms, bufs, in_sems):
            rows = buf.shape[3]
            out.append(pltpu.make_async_copy(src.at[:, :, pl.ds(k * rows, rows), :], buf.at[slot], sem.at[slot]))
        return out

    for copy in copies(0):
        copy.start()

    def body(k, carry):
        @pl.when(k + 1 < blocks)
        def _():
            for copy in copies(k + 1):
                copy.start()

        for copy in copies(k):
            copy.wait()
        step(k, lax.rem(k, 2))
        return carry

    lax.fori_loop(0, blocks, body, 0)


def second_kernel(group, rows_local, coef, w_mix, p_inv, table, grad, mixed_out, w_buf, coef_blk, mixed, stage, flipped,
                  expanded, turn, grad_buf, out_buf, send_a, recv_a, send_b, recv_b, w_sem, c_sem, in_sem, out_sem, p_sem,
                  send_a_sem, recv_a_sem, send_b_sem, recv_b_sem):
    me = lax.axis_index('lat')
    batch = grad.shape[0]
    channels = grad.shape[1] // rows_local
    m_local = stage.shape[0]
    per = w_buf.shape[1]
    degrees = stage.shape[1]

    def fetch(b):
        return Halves(grad, b, grad_buf, lax.rem(b, 2), in_sem)

    def put(b):
        return pltpu.make_async_copy(out_buf.at[lax.rem(b, 2)], mixed_out.at[b], out_sem.at[lax.rem(b, 2)])

    fetch(0).start()
    load_legendre(me, group, p_inv, stage, p_sem)
    flip_rows(stage, flipped)
    expand_rows(stage, expanded, rows_local)

    def mix(k, slot):
        for inner in range(per):
            rows = rows_of_degree(coef_blk.at[slot], inner, m_local)
            res = dot(rows, mix_block(w_buf.at[slot, inner]), NT)
            at = pl.ds(pl.multiple_of((k * per + inner) * m_local, m_local), m_local)
            for part in range(2):
                lanes = res.shape[1] // 2
                mixed[:, part, at, :] = res[:, part * lanes:(part + 1) * lanes].reshape(batch, m_local, lanes)

    mix_loop(w_mix, [coef], [coef_blk], w_buf, w_sem, [c_sem], degrees // per, mix)

    enter(me, group)
    swap_a = Exchange(me, group, batch, send_a, recv_a, send_a_sem, recv_a_sem)
    swap_b = Exchange(me, group, batch, send_b, recv_b, send_b_sem, recv_b_sem)
    lag = 2

    def body(i, carry):
        @pl.when(i < batch)
        def _():
            swap_a.reserve(i)
            legendre_inverse(mixed.at[i], flipped, send_a, lax.rem(i, SLOTS), rows_local)
            swap_a.start(i)

        @pl.when((i >= lag) & (i < batch + lag))
        def _():
            b = i - lag
            half = lax.rem(b, 2)

            @pl.when(b + 1 < batch)
            def _():
                fetch(b + 1).start()

            fetch(b).wait()
            swap_a.arrive(b)
            unpack_blocks(recv_a, b, turn)
            for t in range(rows_local):
                slope = gelu_slope(synthesise(turn, t, table, rows_local))
                given = read_row(grad_buf, half, t, channels, rows_local)
                write_row(grad_buf, half, t, channels, rows_local, given * slope)
            analyse(lambda t: read_row(grad_buf, half, t, channels, rows_local), table, turn, rows_local)
            swap_b.reserve(b)
            pack_blocks(turn, send_b, lax.rem(b, SLOTS))
            swap_b.start(b)

        @pl.when(i >= 2 * lag)
        def _():
            b = i - 2 * lag
            swap_b.arrive(b)

            @pl.when(b >= 2)
            def _():
                put(b - 2).wait()

            legendre_forward(recv_b, b, expanded, out_buf.at[lax.rem(b, 2)], rows_local)
            put(b).start()

        return carry

    lax.fori_loop(0, batch + 2 * lag, body, 0)
    swap_a.drain()
    swap_b.drain()
    put(batch - 2).wait()
    put(batch - 1).wait()


class WeightSum:
    def __init__(self, me, ring, sums, got, out, sems):
        self.ring, self.sums, self.got, self.out, self.sems = ring, sums, got, out, sems
        self.me = me
        self.core, self.y = lax.rem(me, 2), lax.rem(me // 2, 2)
        self.near, self.far = lax.rem(me // 4, 2), me // 8
        self.quarter = sums.shape[1]
        self.rows = sums.shape[2] // 2
        self.degree = self.y * (self.quarter // 2) + self.near

    def peer(self, phase):
        step = (1, 2, 4, 8)[phase]
        bit = (self.core, self.y, self.near, self.far)[phase]
        return {'lat': self.me + step - 2 * step * bit}

    def remote(self, phase, k, source, target, back):
        return pltpu.make_async_remote_copy(source, target, self.sems.at[back, 0, phase, k], self.sems.at[back, 1, phase, k],
                                            device_id=self.peer(phase), device_id_type=MESH)

    def halving(self, phase, k):
        if phase == 0:
            source, target = self.ring.at[lax.rem(k, self.ring.shape[0]), 1 - self.core], self.sums.at[k]
        elif phase == 1:
            half = self.quarter // 2
            source, target = self.sums.at[k, pl.ds((1 - self.y) * half, half)], self.got[0].at[k]
        elif phase == 2:
            source, target = self.sums.at[k, self.y * (self.quarter // 2) + 1 - self.near], self.got[1].at[k]
        else:
            at = pl.ds(pl.multiple_of((1 - self.far) * self.rows, self.rows), self.rows)
            source, target = self.sums.at[k, self.degree, at], self.got[2].at[k]
        return self.remote(phase, k, source, target, 0)

    def absorb(self, phase, k):
        self.halving(phase, k).wait()
        if phase == 0:
            self.sums[k] = self.sums[k] + self.ring[lax.rem(k, self.ring.shape[0]), self.core]
        elif phase == 1:
            half = self.quarter // 2
            at = pl.ds(self.y * half, half)
            self.sums[k, at] = self.sums[k, at] + self.got[0][k]
        elif phase == 2:
            self.sums[k, self.degree] = self.sums[k, self.degree] + self.got[1][k]
        else:
            at = self.last_rows()
            self.sums[k, self.degree, at] = self.sums[k, self.degree, at] + self.got[2][k]

    def last_rows(self):
        return pl.ds(pl.multiple_of(self.far * self.rows, self.rows), self.rows)

    def reduce_step(self, phase, k):
        self.absorb(phase - 1, k)
        if phase < 4:
            self.halving(phase, k).start()
        else:
            self.settle(k).start()
            self.doubling(3, k).start()

    def settle(self, k):
        at = self.last_rows()
        degree = k * 2 * self.quarter + self.core * self.quarter + self.degree
        return pltpu.make_async_copy(self.sums.at[k, self.degree, at], self.out.at[degree, at], self.sems.at[1, 2, 0, k])

    def doubling(self, phase, k):
        base = k * 2 * self.quarter + self.core * self.quarter
        if phase == 3:
            at = self.last_rows()
            return self.remote(3, k, self.sums.at[k, self.degree, at], self.out.at[base + self.degree, at], 1)
        if phase == 2:
            span = pl.ds(base + self.degree, 1)
        elif phase == 1:
            half = self.quarter // 2
            span = pl.ds(base + self.y * half, half)
        else:
            span = pl.ds(base, self.quarter)
        return self.remote(phase, k, self.out.at[span], self.out.at[span], 1)

    def gather_step(self, phase, k):
        if phase == 2:
            self.settle(k).wait()
        self.doubling(phase + 1, k).wait()
        if phase >= 0:
            self.doubling(phase, k).start()


def third_kernel(group, rows_local, mixed, coef, w_mix, p_fwd, table, grad, field_out, grad_w, w_buf, mixed_blk, coef_blk, ring,
                 sums, got_a, got_b, got_c, back, stage, flipped, turn, grad_buf, send, recv, w_sem, m_sem, c_sem, gw_sem,
                 in_sem, out_sem, p_sem, send_sem, recv_sem):
    me = lax.axis_index('lat')
    batch = grad.shape[0]
    channels = grad.shape[1] // rows_local
    depth = grad_buf.shape[0]
    per = w_buf.shape[1]
    degrees = w_mix.shape[0]
    m_local = stage.shape[0]
    blocks = degrees // per

    def fetch(b):
        return Halves(grad, b, grad_buf, lax.rem(b, depth), in_sem)

    def put(b):
        return Halves(field_out, b, grad_buf, lax.rem(b, depth), out_sem, outward=True)

    enter(me, group)
    total = WeightSum(me, ring, sums, (got_a, got_b, got_c), grad_w, gw_sem)
    swap = Exchange(me, group, batch, send, recv, send_sem, recv_sem)

    def weigh(k, slot):
        place = lax.rem(k, ring.shape[0])
        for inner in range(per):
            rows = rows_of_degree(mixed_blk.at[slot], inner, m_local)
            keep = rows_of_degree(coef_blk.at[slot], inner, m_local)
            res = dot(rows, mix_block(w_buf.at[slot, inner]), NN)
            at = pl.ds(pl.multiple_of((k * per + inner) * m_local, m_local), m_local)
            half = res.shape[1] // 2
            for part in range(2):
                back[:, part, at, :] = res[:, part * half:(part + 1) * half].reshape(batch, m_local, half)
            big = dot(rows, keep, TN)
            side, spot = inner // (per // 2), inner % (per // 2)
            ring[place, side, spot, pl.ds(0, half, stride=2), :] = big[:half, :half] + big[half:, half:]
            ring[place, side, spot, pl.ds(1, half, stride=2), :] = big[half:, :half] - big[:half, half:]
        total.halving(0, k).start()

        @pl.when(k >= 2)
        def _():
            total.reduce_step(1, k - 2)

    mix_loop(w_mix, [mixed, coef], [mixed_blk, coef_blk], w_buf, w_sem, [m_sem, c_sem], blocks, weigh)
    fetch(0).start()
    total.reduce_step(1, blocks - 2)
    total.reduce_step(1, blocks - 1)
    load_legendre(me, group, p_fwd, stage, p_sem)
    flip_rows(stage, flipped)
    lag = 2
    width = 2

    def body(i, carry):
        @pl.when(i < batch)
        def _():
            swap.reserve(i)
            legendre_inverse(back.at[i], flipped, send, lax.rem(i, SLOTS), rows_local)
            swap.start(i)

        steps = [(total.reduce_step, p) for p in (2, 3, 4)] + [(total.gather_step, p) for p in (2, 1, 0, -1)]
        for late, (step, phase) in enumerate(steps):
            for j in range(width):
                k = (i - late) * width + j

                @pl.when((k >= 0) & (k < blocks))
                def _():
                    step(phase, k)

        @pl.when((i >= lag) & (i < batch + lag))
        def _():
            b = i - lag
            half = lax.rem(b, depth)

            @pl.when(b >= depth - 1)
            def _():
                put(b - depth + 1).wait()

            @pl.when(b + 1 < batch)
            def _():
                fetch(b + 1).start()

            fetch(b).wait()
            swap.arrive(b)
            unpack_blocks(recv, b, turn)
            for t in range(rows_local):
                added = synthesise(turn, t, table, rows_local)
                given = read_row(grad_buf, half, t, channels, rows_local)
                write_row(grad_buf, half, t, channels, rows_local, given + added)
            put(b).start()

        return carry

    lax.fori_loop(0, max(batch + lag, blocks // width + 6), body, 0)
    swap.drain()
    for b in range(batch - depth + 1, batch):
        put(b).wait()


def any_specs(n):
    return [pl.BlockSpec(memory_space=pl.ANY)] * n


def params(collective_id=None):
    if collective_id is None:
        return pltpu.CompilerParams(vmem_limit_bytes=VMEM_LIMIT)
    return pltpu.CompilerParams(collective_id=collective_id, has_side_effects=True, vmem_limit_bytes=VMEM_LIMIT)


def solution(mesh):
    group = mesh.shape['lat']
    field_spec = P('member', None, 'lat', None)

    def local_step(field_loc, grad_loc, p_fwd, p_inv, w_mix):
        batch, channels, rows_local, lon_count = field_loc.shape
        degrees, lats = p_fwd.shape[1:]
        m_local = p_fwd.shape[0] // group
        modes = group * m_local * 2
        base, gained = (two_halves(table) for table in dft_tables(group, m_local, lon_count))
        field = field_loc.reshape(batch, channels * rows_local, lon_count)
        grad = grad_loc.reshape(batch, channels * rows_local, lon_count)
        w_rows = jnp.swapaxes(w_mix, 2, 3).reshape(degrees, channels * 2, channels)
        dma, vmem = pltpu.SemaphoreType.DMA, pltpu.VMEM
        block_rows = m_local * 2 * rows_local
        coef_shape = (batch, 2, degrees * m_local, channels)
        send_t = vmem((SLOTS, group, block_rows, channels), BF16)
        recv_t = vmem((batch, group, block_rows, channels), BF16)
        turn_t = vmem((modes * rows_local, channels), F32)
        stage_t = vmem((m_local, degrees, lats), F32)
        expanded_t = vmem((m_local, 2 * degrees, 2 * lats), BF16)
        flipped_t = vmem((m_local, lats, degrees), BF16)
        pair_t = vmem((2, 2, degrees * m_local, channels), F32)
        field_t = vmem((2, lon_count // LANES, channels * rows_local, LANES), F32)
        table_spec = pl.BlockSpec(memory_space=pltpu.VMEM)
        any_spec = pl.BlockSpec(memory_space=pl.ANY)
        per = 8

        coef = pl.pallas_call(
            functools.partial(first_kernel, group, rows_local), name='first',
            out_shape=jax.ShapeDtypeStruct(coef_shape, F32),
            in_specs=[any_spec, table_spec, any_spec], out_specs=any_spec,
            scratch_shapes=[field_t, stage_t, expanded_t, turn_t, send_t, recv_t, pair_t, dma((2, 2)), dma((2,)), dma(()),
                            dma((SLOTS,)), dma((batch,))],
            compiler_params=params(0))(field, base, p_fwd)

        blk_t = vmem((2, batch, 2, per * m_local, channels), F32)
        w_t = vmem((2, per, channels * 2, channels), F32)
        mixed = pl.pallas_call(
            functools.partial(second_kernel, group, rows_local), name='second',
            out_shape=jax.ShapeDtypeStruct(coef_shape, F32),
            in_specs=[any_spec, any_spec, any_spec, table_spec, any_spec], out_specs=any_spec,
            scratch_shapes=[w_t, blk_t, vmem(coef_shape, F32), stage_t, flipped_t, expanded_t, turn_t, field_t, pair_t,
                            send_t, recv_t, send_t, recv_t, dma((2,)), dma((2,)), dma((2, 2)), dma((2,)), dma(()),
                            dma((SLOTS,)), dma((batch,)), dma((SLOTS,)), dma((batch,))],
            compiler_params=params(1))(coef, w_rows, p_inv, gained, grad)

        blocks = degrees // per
        field_out, gw_total = pl.pallas_call(
            functools.partial(third_kernel, group, rows_local), name='third',
            out_shape=[jax.ShapeDtypeStruct(grad.shape, F32), jax.ShapeDtypeStruct(w_rows.shape, F32)],
            in_specs=[any_spec] * 4 + [table_spec, any_spec], out_specs=[any_spec] * 2,
            scratch_shapes=[w_t, blk_t, blk_t, vmem((4, 2, per // 2, channels * 2, channels), F32),
                            vmem((blocks, per // 2, channels * 2, channels), F32),
                            vmem((blocks, per // 4, channels * 2, channels), F32),
                            vmem((blocks, channels * 2, channels), F32), vmem((blocks, channels, channels), F32),
                            vmem(coef_shape, F32), stage_t, flipped_t, turn_t,
                            vmem((3, lon_count // LANES, channels * rows_local, LANES), F32), send_t, recv_t,
                            dma((2,)), dma((2,)), dma((2,)), dma((2, 3, 4, blocks)), dma((3, 2)), dma((3, 2)), dma(()),
                            dma((SLOTS,)), dma((batch,))],
            compiler_params=params(2))(mixed, coef, w_rows, p_fwd, base, grad)

        grad_wmix = jnp.swapaxes(gw_total.reshape(degrees, channels, 2, channels), 2, 3)
        return field_out.reshape(grad_loc.shape), grad_wmix

    return jax.shard_map(local_step, mesh=mesh, in_specs=(field_spec, field_spec, P(), P(), P()),
                         out_specs=(field_spec, P('member', None, None, None)), check_vma=False)
```

```python
import functools
import math

import jax
import jax.numpy as jnp
import numpy as np
from jax import lax
from jax.experimental import pallas as pl
from jax.experimental.pallas import tpu as pltpu
from jax.sharding import PartitionSpec as P

MESH = pl.DeviceIdType.MESH
LANES = 128
SLOTS = 3
VMEM_LIMIT = 60 * 1024 * 1024
F32 = jnp.float32
BF16 = jnp.bfloat16

NN = (((1,), (0,)), ((), ()))
NT = (((1,), (1,)), ((), ()))
TN = (((0,), (0,)), ((), ()))


def dot(lhs, rhs, dims):
    return lax.dot_general(lhs, rhs, dims, preferred_element_type=F32)


def split_halves(values):
    high = values.astype(BF16)
    low = (values - high.astype(F32)).astype(BF16)
    return high, low


def dft_tables(group, m_local, lon_count):
    owner, slot, part = np.meshgrid(np.arange(group), np.arange(m_local), np.arange(2), indexing='ij')
    wave = (slot * group + owner).reshape(-1)
    part = part.reshape(-1)
    phase = 2.0 * np.pi * ((wave[:, None] * np.arange(lon_count)[None, :]) % lon_count) / lon_count
    base = np.where(part[:, None] == 0, np.cos(phase), -np.sin(phase)) / math.sqrt(lon_count)
    gains = np.where(wave == 0, 1.0, 2.0)[:, None]
    return base.astype(np.float32), (base * gains).astype(np.float32)


def two_halves(table):
    high = jnp.asarray(table).astype(BF16)
    low = (jnp.asarray(table) - high.astype(F32)).astype(BF16)
    return jnp.stack([high, low])


class Halves:
    def __init__(self, whole, b, halves, slot, sem, outward=False):
        self.copies = []
        for half in range(halves.shape[1]):
            ends = whole.at[b, :, pl.ds(half * LANES, LANES)], halves.at[slot, half]
            source, target = ends[::-1] if outward else ends
            self.copies.append(pltpu.make_async_copy(source, target, sem.at[slot, half]))

    def start(self):
        for copy in self.copies:
            copy.start()

    def wait(self):
        for copy in self.copies:
            copy.wait()


def read_row(halves, slot, t, channels, rows_local):
    at = pl.ds(t, channels, stride=rows_local)
    return jnp.concatenate([halves[slot, half, at, :] for half in range(halves.shape[1])], axis=1)


def write_row(halves, slot, t, channels, rows_local, values):
    at = pl.ds(t, channels, stride=rows_local)
    for half in range(halves.shape[1]):
        halves[slot, half, at, :] = values[:, half * LANES:(half + 1) * LANES]


class Exchange:
    def __init__(self, me, group, batch, send, recv, send_sem, recv_sem):
        self.me, self.group, self.batch = me, group, batch
        self.send, self.recv, self.send_sem, self.recv_sem = send, recv, send_sem, recv_sem

    def all_copies(self, b):
        slot = lax.rem(b, SLOTS)
        others = pl.ds(0, self.group - 1)
        return pltpu.make_async_remote_copy(
            self.send.at[slot, others], self.recv.at[b, others], self.send_sem.at[slot], self.recv_sem.at[b],
            device_id={'lat': lax.rem(self.me + 1, self.group)}, device_id_type=MESH)

    def reserve(self, b):
        @pl.when(b >= SLOTS)
        def _():
            self.all_copies(b - SLOTS).wait_send()

    def start(self, b):
        slot = lax.rem(b, SLOTS)
        self.recv[b, self.me] = self.send[slot, self.me]

        @pl.loop(1, self.group)
        def _(step):
            target = lax.rem(self.me + step, self.group)
            pltpu.make_async_remote_copy(
                self.send.at[slot, target], self.recv.at[b, self.me], self.send_sem.at[slot], self.recv_sem.at[b],
                device_id={'lat': target}, device_id_type=MESH).start()

    def arrive(self, b):
        self.all_copies(b).wait_recv()

    def drain(self):
        for b in range(max(0, self.batch - SLOTS), self.batch):
            self.all_copies(b).wait_send()


def enter(me, group):
    barrier = pltpu.get_barrier_semaphore()

    @pl.loop(1, group)
    def _(step):
        pl.semaphore_signal(barrier, inc=1, device_id={'lat': lax.rem(me + step, group)}, device_id_type=MESH)

    pl.semaphore_wait(barrier, group - 1)


def load_legendre(me, group, table_hbm, stage, sem):
    m_local = stage.shape[0]
    copies = [pltpu.make_async_copy(table_hbm.at[slot * group + me], stage.at[slot], sem) for slot in range(m_local)]
    for copy in copies:
        copy.start()
    pltpu.make_async_copy(table_hbm.at[pl.ds(0, m_local)], stage, sem).wait()


def expand_rows(stage, expanded, rows_local):
    m_local, degrees, lats = stage.shape
    row = lax.broadcasted_iota(jnp.int32, (lats, 2 * lats), 0)
    col = lax.broadcasted_iota(jnp.int32, (lats, 2 * lats), 1)
    source = col // (2 * rows_local)
    inner = col % (2 * rows_local)
    for part in range(2):
        pick = (row == source * rows_local + inner - part * rows_local) & (inner // rows_local == part)
        pick = pick.astype(F32).astype(BF16)
        for slot in range(m_local):
            expanded[slot, pl.ds(part * degrees, degrees), :] = dot(stage[slot].astype(BF16), pick, NN).astype(BF16)


def flip_rows(stage, flipped):
    for slot in range(stage.shape[0]):
        flipped[slot] = stage[slot].T.astype(BF16)


def analyse(values_at, table, turn, rows_local):
    modes = table.shape[1]
    for t in range(0, rows_local, 2):
        pair = jnp.concatenate([values_at(t), values_at(t + 1)], axis=0)
        high, low = split_halves(pair)
        out = dot(table[0], high, NT) + dot(table[0], low, NT) + dot(table[1], high, NT)
        channels = out.shape[1] // 2
        turn[pl.ds(t, modes, stride=rows_local), :] = out[:, :channels]
        turn[pl.ds(t + 1, modes, stride=rows_local), :] = out[:, channels:]


def pack_blocks(turn, send, slot):
    group, rows, lanes = send.shape[1:]
    for d in range(group):
        send[slot, d] = turn[pl.ds(d * rows, rows), :].astype(BF16)


def unpack_blocks(recv, b, turn):
    group, rows, lanes = recv.shape[1:]
    for d in range(group):
        turn[pl.ds(d * rows, rows), :] = recv[b, d].astype(F32)


def synthesise(turn, t, table, rows_local):
    modes = table.shape[1]
    spec = turn[pl.ds(t, modes, stride=rows_local), :].astype(BF16)
    return dot(spec, table[0], TN) + dot(spec, table[1], TN)


def legendre_forward(recv, b, expanded, out, rows_local):
    m_local = expanded.shape[0]
    degrees = expanded.shape[1] // 2
    group, _, lanes = recv.shape[1:]
    tile = 2 * rows_local
    for slot in range(m_local):
        rows = recv[b, :, pl.ds(slot * tile, tile), :].reshape(group * tile, lanes)
        res = dot(expanded[slot], rows, NN)
        for part in range(2):
            out[part, pl.ds(slot, degrees, stride=m_local), :] = res[part * degrees:(part + 1) * degrees]


def legendre_inverse(coef, flipped, send, slot_out, rows_local):
    m_local, lats, degrees = flipped.shape
    group = lats // rows_local
    tile = 2 * rows_local
    for slot in range(m_local):
        parts = [coef.at[part][pl.ds(slot, degrees, stride=m_local), :].astype(BF16) for part in range(2)]
        res = dot(flipped[slot], jnp.concatenate(parts, axis=1), NN)
        lanes = res.shape[1] // 2
        blocks = [res[:, part * lanes:(part + 1) * lanes].reshape(group, rows_local, lanes) for part in range(2)]
        send[slot_out, :, pl.ds(slot * tile, tile), :] = jnp.concatenate(blocks, axis=1).astype(BF16)


def gelu_slope(values):
    cumulative = 0.5 * (1.0 + lax.erf(values * math.sqrt(0.5)))
    density = jnp.exp(-0.5 * values * values) * (1.0 / math.sqrt(2.0 * math.pi))
    return cumulative + values * density


def mix_block(w_block):
    half = w_block.shape[0] // 2
    w_real = w_block[pl.ds(0, half, stride=2), :]
    w_imag = w_block[pl.ds(1, half, stride=2), :]
    top = jnp.concatenate([w_real, -w_imag], axis=1)
    bottom = jnp.concatenate([w_imag, w_real], axis=1)
    return jnp.concatenate([top, bottom], axis=0).astype(BF16)


def rows_of_degree(block, inner, m_local):
    batch = block.shape[0]
    lanes = block.shape[-1]
    parts = [block[:, part, pl.ds(inner * m_local, m_local), :].reshape(batch * m_local, lanes) for part in range(2)]
    return jnp.concatenate(parts, axis=1).astype(BF16)


def first_kernel(group, rows_local, field, table, p_fwd, coef_out, field_buf, stage, expanded, turn, send, recv,
                 coef_buf, in_sem, out_sem, p_sem, send_sem, recv_sem):
    me = lax.axis_index('lat')
    batch = field.shape[0]
    channels = field.shape[1] // rows_local

    def fetch(b):
        return Halves(field, b, field_buf, lax.rem(b, 2), in_sem)

    def put(b):
        return pltpu.make_async_copy(coef_buf.at[lax.rem(b, 2)], coef_out.at[b], out_sem.at[lax.rem(b, 2)])

    fetch(0).start()
    enter(me, group)
    swap = Exchange(me, group, batch, send, recv, send_sem, recv_sem)
    lag = 2

    def body(i, carry):
        @pl.when(i < batch)
        def _():
            @pl.when(i + 1 < batch)
            def _():
                fetch(i + 1).start()

            fetch(i).wait()
            half = lax.rem(i, 2)
            analyse(lambda t: read_row(field_buf, half, t, channels, rows_local), table, turn, rows_local)
            swap.reserve(i)
            pack_blocks(turn, send, lax.rem(i, SLOTS))
            swap.start(i)

        @pl.when(i == 0)
        def _():
            load_legendre(me, group, p_fwd, stage, p_sem)
            expand_rows(stage, expanded, rows_local)

        @pl.when(i >= lag)
        def _():
            b = i - lag
            swap.arrive(b)

            @pl.when(b >= 2)
            def _():
                put(b - 2).wait()

            legendre_forward(recv, b, expanded, coef_buf.at[lax.rem(b, 2)], rows_local)
            put(b).start()

        return carry

    lax.fori_loop(0, batch + lag, body, 0)
    swap.drain()
    put(batch - 2).wait()
    put(batch - 1).wait()


def mix_loop(w_hbm, in_hbms, bufs, w_buf, w_sem, in_sems, blocks, step):
    per = w_buf.shape[1]

    def copies(k):
        slot = lax.rem(k, 2)
        out = [pltpu.make_async_copy(w_hbm.at[pl.ds(k * per, per)], w_buf.at[slot], w_sem.at[slot])]
        for src, buf, sem in zip(in_hbms, bufs, in_sems):
            rows = buf.shape[3]
            out.append(pltpu.make_async_copy(src.at[:, :, pl.ds(k * rows, rows), :], buf.at[slot], sem.at[slot]))
        return out

    for copy in copies(0):
        copy.start()

    def body(k, carry):
        @pl.when(k + 1 < blocks)
        def _():
            for copy in copies(k + 1):
                copy.start()

        for copy in copies(k):
            copy.wait()
        step(k, lax.rem(k, 2))
        return carry

    lax.fori_loop(0, blocks, body, 0)


def second_kernel(group, rows_local, coef, w_mix, p_inv, table, grad, mixed_out, w_buf, coef_blk, mixed, stage, flipped,
                  expanded, turn, grad_buf, out_buf, send_a, recv_a, send_b, recv_b, w_sem, c_sem, in_sem, out_sem, p_sem,
                  send_a_sem, recv_a_sem, send_b_sem, recv_b_sem):
    me = lax.axis_index('lat')
    batch = grad.shape[0]
    channels = grad.shape[1] // rows_local
    m_local = stage.shape[0]
    per = w_buf.shape[1]
    degrees = stage.shape[1]

    def fetch(b):
        return Halves(grad, b, grad_buf, lax.rem(b, 2), in_sem)

    def put(b):
        return pltpu.make_async_copy(out_buf.at[lax.rem(b, 2)], mixed_out.at[b], out_sem.at[lax.rem(b, 2)])

    fetch(0).start()
    load_legendre(me, group, p_inv, stage, p_sem)
    flip_rows(stage, flipped)
    expand_rows(stage, expanded, rows_local)

    def mix(k, slot):
        for inner in range(per):
            rows = rows_of_degree(coef_blk.at[slot], inner, m_local)
            res = dot(rows, mix_block(w_buf.at[slot, inner]), NT)
            at = pl.ds(pl.multiple_of((k * per + inner) * m_local, m_local), m_local)
            for part in range(2):
                lanes = res.shape[1] // 2
                mixed[:, part, at, :] = res[:, part * lanes:(part + 1) * lanes].reshape(batch, m_local, lanes)

    mix_loop(w_mix, [coef], [coef_blk], w_buf, w_sem, [c_sem], degrees // per, mix)

    enter(me, group)
    swap_a = Exchange(me, group, batch, send_a, recv_a, send_a_sem, recv_a_sem)
    swap_b = Exchange(me, group, batch, send_b, recv_b, send_b_sem, recv_b_sem)
    lag = 2

    def body(i, carry):
        @pl.when(i < batch)
        def _():
            swap_a.reserve(i)
            legendre_inverse(mixed.at[i], flipped, send_a, lax.rem(i, SLOTS), rows_local)
            swap_a.start(i)

        @pl.when((i >= lag) & (i < batch + lag))
        def _():
            b = i - lag
            half = lax.rem(b, 2)

            @pl.when(b + 1 < batch)
            def _():
                fetch(b + 1).start()

            fetch(b).wait()
            swap_a.arrive(b)
            unpack_blocks(recv_a, b, turn)
            for t in range(rows_local):
                slope = gelu_slope(synthesise(turn, t, table, rows_local))
                given = read_row(grad_buf, half, t, channels, rows_local)
                write_row(grad_buf, half, t, channels, rows_local, given * slope)
            analyse(lambda t: read_row(grad_buf, half, t, channels, rows_local), table, turn, rows_local)
            swap_b.reserve(b)
            pack_blocks(turn, send_b, lax.rem(b, SLOTS))
            swap_b.start(b)

        @pl.when(i >= 2 * lag)
        def _():
            b = i - 2 * lag
            swap_b.arrive(b)

            @pl.when(b >= 2)
            def _():
                put(b - 2).wait()

            legendre_forward(recv_b, b, expanded, out_buf.at[lax.rem(b, 2)], rows_local)
            put(b).start()

        return carry

    lax.fori_loop(0, batch + 2 * lag, body, 0)
    swap_a.drain()
    swap_b.drain()
    put(batch - 2).wait()
    put(batch - 1).wait()


class WeightSum:
    def __init__(self, me, ring, sums, got, out, sems):
        self.ring, self.sums, self.got, self.out, self.sems = ring, sums, got, out, sems
        self.me = me
        self.core, self.y = lax.rem(me, 2), lax.rem(me // 2, 2)
        self.near, self.far = lax.rem(me // 4, 2), me // 8
        self.quarter = sums.shape[1]
        self.rows = sums.shape[2] // 2
        self.degree = self.y * (self.quarter // 2) + self.near

    def peer(self, phase):
        step = (1, 2, 4, 8)[phase]
        bit = (self.core, self.y, self.near, self.far)[phase]
        return {'lat': self.me + step - 2 * step * bit}

    def remote(self, phase, k, source, target, back):
        return pltpu.make_async_remote_copy(source, target, self.sems.at[back, 0, phase, k], self.sems.at[back, 1, phase, k],
                                            device_id=self.peer(phase), device_id_type=MESH)

    def halving(self, phase, k):
        if phase == 0:
            source, target = self.ring.at[lax.rem(k, self.ring.shape[0]), 1 - self.core], self.sums.at[k]
        elif phase == 1:
            half = self.quarter // 2
            source, target = self.sums.at[k, pl.ds((1 - self.y) * half, half)], self.got[0].at[k]
        elif phase == 2:
            source, target = self.sums.at[k, self.y * (self.quarter // 2) + 1 - self.near], self.got[1].at[k]
        else:
            at = pl.ds(pl.multiple_of((1 - self.far) * self.rows, self.rows), self.rows)
            source, target = self.sums.at[k, self.degree, at], self.got[2].at[k]
        return self.remote(phase, k, source, target, 0)

    def absorb(self, phase, k):
        self.halving(phase, k).wait()
        if phase == 0:
            self.sums[k] = self.sums[k] + self.ring[lax.rem(k, self.ring.shape[0]), self.core]
        elif phase == 1:
            half = self.quarter // 2
            at = pl.ds(self.y * half, half)
            self.sums[k, at] = self.sums[k, at] + self.got[0][k]
        elif phase == 2:
            self.sums[k, self.degree] = self.sums[k, self.degree] + self.got[1][k]
        else:
            at = self.last_rows()
            self.sums[k, self.degree, at] = self.sums[k, self.degree, at] + self.got[2][k]

    def last_rows(self):
        return pl.ds(pl.multiple_of(self.far * self.rows, self.rows), self.rows)

    def reduce_step(self, phase, k):
        self.absorb(phase - 1, k)
        if phase < 4:
            self.halving(phase, k).start()
        else:
            self.settle(k).start()
            self.doubling(3, k).start()

    def settle(self, k):
        at = self.last_rows()
        degree = k * 2 * self.quarter + self.core * self.quarter + self.degree
        return pltpu.make_async_copy(self.sums.at[k, self.degree, at], self.out.at[degree, at], self.sems.at[1, 2, 0, k])

    def doubling(self, phase, k):
        base = k * 2 * self.quarter + self.core * self.quarter
        if phase == 3:
            at = self.last_rows()
            return self.remote(3, k, self.sums.at[k, self.degree, at], self.out.at[base + self.degree, at], 1)
        if phase == 2:
            span = pl.ds(base + self.degree, 1)
        elif phase == 1:
            half = self.quarter // 2
            span = pl.ds(base + self.y * half, half)
        else:
            span = pl.ds(base, self.quarter)
        return self.remote(phase, k, self.out.at[span], self.out.at[span], 1)

    def gather_step(self, phase, k):
        if phase == 2:
            self.settle(k).wait()
        self.doubling(phase + 1, k).wait()
        if phase >= 0:
            self.doubling(phase, k).start()


def third_kernel(group, rows_local, mixed, coef, w_mix, p_fwd, table, grad, field_out, grad_w, w_buf, mixed_blk, coef_blk, ring,
                 sums, got_a, got_b, got_c, back, stage, flipped, turn, grad_buf, send, recv, w_sem, m_sem, c_sem, gw_sem,
                 in_sem, out_sem, p_sem, send_sem, recv_sem):
    me = lax.axis_index('lat')
    batch = grad.shape[0]
    channels = grad.shape[1] // rows_local
    depth = grad_buf.shape[0]
    per = w_buf.shape[1]
    degrees = w_mix.shape[0]
    m_local = stage.shape[0]
    blocks = degrees // per

    def fetch(b):
        return Halves(grad, b, grad_buf, lax.rem(b, depth), in_sem)

    def put(b):
        return Halves(field_out, b, grad_buf, lax.rem(b, depth), out_sem, outward=True)

    enter(me, group)
    total = WeightSum(me, ring, sums, (got_a, got_b, got_c), grad_w, gw_sem)
    swap = Exchange(me, group, batch, send, recv, send_sem, recv_sem)

    early = 4

    def weigh(k, slot):
        place = lax.rem(k, ring.shape[0])
        for inner in range(per):
            rows = rows_of_degree(mixed_blk.at[slot], inner, m_local)
            keep = rows_of_degree(coef_blk.at[slot], inner, m_local)
            res = dot(rows, mix_block(w_buf.at[slot, inner]), NN)
            at = pl.ds(pl.multiple_of((k * per + inner) * m_local, m_local), m_local)
            half = res.shape[1] // 2
            for part in range(2):
                back[:, part, at, :] = res[:, part * half:(part + 1) * half].reshape(batch, m_local, half)
            big = dot(rows, keep, TN)
            side, spot = inner // (per // 2), inner % (per // 2)
            ring[place, side, spot, pl.ds(0, half, stride=2), :] = big[:half, :half] + big[half:, half:]
            ring[place, side, spot, pl.ds(1, half, stride=2), :] = big[half:, :half] - big[:half, half:]
        total.halving(0, k).start()

        @pl.when(k >= 2)
        def _():
            total.absorb(0, k - 2)

            @pl.when(k - 2 < early)
            def _():
                total.halving(1, k - 2).start()

    mix_loop(w_mix, [mixed, coef], [mixed_blk, coef_blk], w_buf, w_sem, [m_sem, c_sem], blocks, weigh)
    fetch(0).start()
    total.absorb(0, blocks - 2)
    total.absorb(0, blocks - 1)
    load_legendre(me, group, p_fwd, stage, p_sem)
    flip_rows(stage, flipped)
    lag = 2
    width = 2

    def body(i, carry):
        @pl.when(i < batch)
        def _():
            swap.reserve(i)
            legendre_inverse(back.at[i], flipped, send, lax.rem(i, SLOTS), rows_local)
            swap.start(i)

        for j in range(width):
            k = early + i * width + j

            @pl.when(k < blocks)
            def _():
                total.halving(1, k).start()

        steps = [(total.reduce_step, p) for p in (2, 3, 4)] + [(total.gather_step, p) for p in (2, 1, 0, -1)]
        for late, (step, phase) in enumerate(steps):
            for j in range(width):
                k = (i - late) * width + j

                @pl.when((k >= 0) & (k < blocks))
                def _():
                    step(phase, k)

        @pl.when((i >= lag) & (i < batch + lag))
        def _():
            b = i - lag
            half = lax.rem(b, depth)

            @pl.when(b >= depth - 1)
            def _():
                put(b - depth + 1).wait()

            @pl.when(b + 1 < batch)
            def _():
                fetch(b + 1).start()

            fetch(b).wait()
            swap.arrive(b)
            unpack_blocks(recv, b, turn)
            for t in range(rows_local):
                added = synthesise(turn, t, table, rows_local)
                given = read_row(grad_buf, half, t, channels, rows_local)
                write_row(grad_buf, half, t, channels, rows_local, given + added)
            put(b).start()

        return carry

    lax.fori_loop(0, max(batch + lag, blocks // width + 6), body, 0)
    swap.drain()
    for b in range(batch - depth + 1, batch):
        put(b).wait()


def any_specs(n):
    return [pl.BlockSpec(memory_space=pl.ANY)] * n


def params(collective_id=None):
    if collective_id is None:
        return pltpu.CompilerParams(vmem_limit_bytes=VMEM_LIMIT)
    return pltpu.CompilerParams(collective_id=collective_id, has_side_effects=True, vmem_limit_bytes=VMEM_LIMIT)


def solution(mesh):
    group = mesh.shape['lat']
    field_spec = P('member', None, 'lat', None)

    def local_step(field_loc, grad_loc, p_fwd, p_inv, w_mix):
        batch, channels, rows_local, lon_count = field_loc.shape
        degrees, lats = p_fwd.shape[1:]
        m_local = p_fwd.shape[0] // group
        modes = group * m_local * 2
        base, gained = (two_halves(table) for table in dft_tables(group, m_local, lon_count))
        field = field_loc.reshape(batch, channels * rows_local, lon_count)
        grad = grad_loc.reshape(batch, channels * rows_local, lon_count)
        w_rows = jnp.swapaxes(w_mix, 2, 3).reshape(degrees, channels * 2, channels)
        dma, vmem = pltpu.SemaphoreType.DMA, pltpu.VMEM
        block_rows = m_local * 2 * rows_local
        coef_shape = (batch, 2, degrees * m_local, channels)
        send_t = vmem((SLOTS, group, block_rows, channels), BF16)
        recv_t = vmem((batch, group, block_rows, channels), BF16)
        turn_t = vmem((modes * rows_local, channels), F32)
        stage_t = vmem((m_local, degrees, lats), F32)
        expanded_t = vmem((m_local, 2 * degrees, 2 * lats), BF16)
        flipped_t = vmem((m_local, lats, degrees), BF16)
        pair_t = vmem((2, 2, degrees * m_local, channels), F32)
        field_t = vmem((2, lon_count // LANES, channels * rows_local, LANES), F32)
        table_spec = pl.BlockSpec(memory_space=pltpu.VMEM)
        any_spec = pl.BlockSpec(memory_space=pl.ANY)
        per = 8

        coef = pl.pallas_call(
            functools.partial(first_kernel, group, rows_local), name='first',
            out_shape=jax.ShapeDtypeStruct(coef_shape, F32),
            in_specs=[any_spec, table_spec, any_spec], out_specs=any_spec,
            scratch_shapes=[field_t, stage_t, expanded_t, turn_t, send_t, recv_t, pair_t, dma((2, 2)), dma((2,)), dma(()),
                            dma((SLOTS,)), dma((batch,))],
            compiler_params=params(0))(field, base, p_fwd)

        blk_t = vmem((2, batch, 2, per * m_local, channels), F32)
        w_t = vmem((2, per, channels * 2, channels), F32)
        mixed = pl.pallas_call(
            functools.partial(second_kernel, group, rows_local), name='second',
            out_shape=jax.ShapeDtypeStruct(coef_shape, F32),
            in_specs=[any_spec, any_spec, any_spec, table_spec, any_spec], out_specs=any_spec,
            scratch_shapes=[w_t, blk_t, vmem(coef_shape, F32), stage_t, flipped_t, expanded_t, turn_t, field_t, pair_t,
                            send_t, recv_t, send_t, recv_t, dma((2,)), dma((2,)), dma((2, 2)), dma((2,)), dma(()),
                            dma((SLOTS,)), dma((batch,)), dma((SLOTS,)), dma((batch,))],
            compiler_params=params(1))(coef, w_rows, p_inv, gained, grad)

        blocks = degrees // per
        field_out, gw_total = pl.pallas_call(
            functools.partial(third_kernel, group, rows_local), name='third',
            out_shape=[jax.ShapeDtypeStruct(grad.shape, F32), jax.ShapeDtypeStruct(w_rows.shape, F32)],
            in_specs=[any_spec] * 4 + [table_spec, any_spec], out_specs=[any_spec] * 2,
            scratch_shapes=[w_t, blk_t, blk_t, vmem((4, 2, per // 2, channels * 2, channels), F32),
                            vmem((blocks, per // 2, channels * 2, channels), F32),
                            vmem((blocks, per // 4, channels * 2, channels), F32),
                            vmem((blocks, channels * 2, channels), F32), vmem((blocks, channels, channels), F32),
                            vmem(coef_shape, F32), stage_t, flipped_t, turn_t,
                            vmem((3, lon_count // LANES, channels * rows_local, LANES), F32), send_t, recv_t,
                            dma((2,)), dma((2,)), dma((2,)), dma((2, 3, 4, blocks)), dma((3, 2)), dma((3, 2)), dma(()),
                            dma((SLOTS,)), dma((batch,))],
            compiler_params=params(2))(mixed, coef, w_rows, p_fwd, base, grad)

        grad_wmix = jnp.swapaxes(gw_total.reshape(degrees, channels, 2, channels), 2, 3)
        return field_out.reshape(grad_loc.shape), grad_wmix

    return jax.shard_map(local_step, mesh=mesh, in_specs=(field_spec, field_spec, P(), P(), P()),
                         out_specs=(field_spec, P('member', None, None, None)), check_vma=False)
```

```python
import functools
import math

import jax
import jax.numpy as jnp
import numpy as np
from jax import lax
from jax.experimental import pallas as pl
from jax.experimental.pallas import tpu as pltpu
from jax.sharding import PartitionSpec as P

MESH = pl.DeviceIdType.MESH
LANES = 128
SLOTS = 3
VMEM_LIMIT = 60 * 1024 * 1024
F32 = jnp.float32
BF16 = jnp.bfloat16

NN = (((1,), (0,)), ((), ()))
NT = (((1,), (1,)), ((), ()))
TN = (((0,), (0,)), ((), ()))


def dot(lhs, rhs, dims):
    return lax.dot_general(lhs, rhs, dims, preferred_element_type=F32)


def split_halves(values):
    high = values.astype(BF16)
    low = (values - high.astype(F32)).astype(BF16)
    return high, low


def dft_tables(group, m_local, lon_count):
    owner, slot, part = np.meshgrid(np.arange(group), np.arange(m_local), np.arange(2), indexing='ij')
    wave = (slot * group + owner).reshape(-1)
    part = part.reshape(-1)
    phase = 2.0 * np.pi * ((wave[:, None] * np.arange(lon_count)[None, :]) % lon_count) / lon_count
    base = np.where(part[:, None] == 0, np.cos(phase), -np.sin(phase)) / math.sqrt(lon_count)
    gains = np.where(wave == 0, 1.0, 2.0)[:, None]
    return base.astype(np.float32), (base * gains).astype(np.float32)


def two_halves(table):
    high = jnp.asarray(table).astype(BF16)
    low = (jnp.asarray(table) - high.astype(F32)).astype(BF16)
    return jnp.stack([high, low])


class Halves:
    def __init__(self, whole, b, halves, slot, sem, outward=False):
        self.copies = []
        for half in range(halves.shape[1]):
            ends = whole.at[b, :, pl.ds(half * LANES, LANES)], halves.at[slot, half]
            source, target = ends[::-1] if outward else ends
            self.copies.append(pltpu.make_async_copy(source, target, sem.at[slot, half]))

    def start(self):
        for copy in self.copies:
            copy.start()

    def wait(self):
        for copy in self.copies:
            copy.wait()


def read_row(halves, slot, t, channels, rows_local):
    at = pl.ds(t, channels, stride=rows_local)
    return jnp.concatenate([halves[slot, half, at, :] for half in range(halves.shape[1])], axis=1)


def write_row(halves, slot, t, channels, rows_local, values):
    at = pl.ds(t, channels, stride=rows_local)
    for half in range(halves.shape[1]):
        halves[slot, half, at, :] = values[:, half * LANES:(half + 1) * LANES]


class Exchange:
    def __init__(self, me, group, batch, send, recv, send_sem, recv_sem):
        self.me, self.group, self.batch = me, group, batch
        self.send, self.recv, self.send_sem, self.recv_sem = send, recv, send_sem, recv_sem

    def all_copies(self, b):
        slot = lax.rem(b, SLOTS)
        others = pl.ds(0, self.group - 1)
        return pltpu.make_async_remote_copy(
            self.send.at[slot, others], self.recv.at[b, others], self.send_sem.at[slot], self.recv_sem.at[b],
            device_id={'lat': lax.rem(self.me + 1, self.group)}, device_id_type=MESH)

    def reserve(self, b):
        @pl.when(b >= SLOTS)
        def _():
            self.all_copies(b - SLOTS).wait_send()

    def start(self, b):
        slot = lax.rem(b, SLOTS)
        self.recv[b, self.me] = self.send[slot, self.me]

        @pl.loop(1, self.group)
        def _(step):
            target = lax.rem(self.me + step, self.group)
            pltpu.make_async_remote_copy(
                self.send.at[slot, target], self.recv.at[b, self.me], self.send_sem.at[slot], self.recv_sem.at[b],
                device_id={'lat': target}, device_id_type=MESH).start()

    def arrive(self, b):
        self.all_copies(b).wait_recv()

    def drain(self):
        for b in range(max(0, self.batch - SLOTS), self.batch):
            self.all_copies(b).wait_send()


class BridgedExchange:
    def __init__(self, me, group, batch, bufs, sems):
        self.me, self.group, self.batch = me, group, batch
        self.send, self.recv, self.bridge_send, self.bridge_recv, self.relay_send, self.flipped_far = bufs
        self.send_sem, self.recv_sem, self.bridge_send_sem, self.bridge_recv_sem, self.relay_send_sem, self.relay_recv_sem = sems
        self.half_size = group // 2
        self.half = me // self.half_size
        self.place = lax.rem(me, self.half_size)
        self.twin = self.half_size + me - 2 * self.half_size * self.half
        self.rows = self.send.shape[2]
        self.late_rows = self.relay_send.shape[2]
        self.early_rows = self.rows - self.late_rows
        self.tile = self.late_rows // self.flipped_far.shape[0]
        self.direct = self.early_rows // self.tile

    def copy(self, source, target, send_sem, recv_sem, device):
        return pltpu.make_async_remote_copy(source, target, send_sem, recv_sem, device_id={'lat': device},
                                            device_id_type=MESH)

    def all_direct(self, b):
        slot = lax.rem(b, SLOTS)
        count = (self.half_size - 1) * self.rows + self.half_size * self.early_rows
        span = pl.ds(0, count // self.rows)
        return self.copy(self.send.at[slot, span], self.recv.at[b, span], self.send_sem.at[slot], self.recv_sem.at[b], self.twin)

    def all_relayed(self, b):
        slot = lax.rem(b, SLOTS)
        span, part = pl.ds(0, self.half_size - 1), pl.ds(0, self.late_rows)
        return self.copy(self.relay_send.at[slot, span], self.recv.at[b, span, part], self.relay_send_sem.at[slot],
                         self.relay_recv_sem.at[b], self.twin)

    def bridge(self, b):
        slot = lax.rem(b, SLOTS)
        return self.copy(self.bridge_send.at[slot], self.bridge_recv.at[b], self.bridge_send_sem.at[slot],
                         self.bridge_recv_sem.at[b], self.twin)

    def reserve(self, b):
        @pl.when(b >= SLOTS)
        def _():
            self.all_direct(b - SLOTS).wait_send()
            self.bridge(b - SLOTS).wait_send()

    def start(self, b):
        slot = lax.rem(b, SLOTS)
        self.bridge(b).start()
        early = pl.ds(0, self.early_rows)

        @pl.loop(0, self.half_size)
        def _(step):
            target = (1 - self.half) * self.half_size + lax.rem(self.place + step, self.half_size)
            self.copy(self.send.at[slot, target, early], self.recv.at[b, self.me, early], self.send_sem.at[slot],
                      self.recv_sem.at[b], target).start()

        @pl.loop(1, self.half_size)
        def _(step):
            target = self.half * self.half_size + lax.rem(self.place + step, self.half_size)
            self.copy(self.send.at[slot, target], self.recv.at[b, self.me], self.send_sem.at[slot], self.recv_sem.at[b],
                      target).start()

        self.recv[b, self.me] = self.send[slot, self.me]

    def relay(self, b):
        slot = lax.rem(b, SLOTS)

        @pl.when(b >= SLOTS)
        def _():
            self.all_relayed(b - SLOTS).wait_send()

        self.bridge(b).wait_recv()
        lats, degrees = self.flipped_far.shape[1:]
        own = pl.ds(pl.multiple_of(self.half * (lats // 2), lats // 2), lats // 2)
        at = 0
        for late in range(self.flipped_far.shape[0]):
            first = (self.direct + late) * self.group
            count = degrees - first
            parts = []
            for part in range(2):
                rows = self.bridge_recv[b, part, pl.ds(at, count), :]
                parts.append(jnp.concatenate([jnp.zeros((first, rows.shape[1]), BF16), rows], axis=0))
            at += count
            res = dot(self.flipped_far[late, own, :], jnp.concatenate(parts, axis=1), NN)
            lanes = res.shape[1] // 2
            blocks = [res[:, part * lanes:(part + 1) * lanes].reshape(self.half_size, self.tile // 2, lanes) for part in range(2)]
            self.relay_send[slot, :, pl.ds(late * self.tile, self.tile), :] = jnp.concatenate(blocks, axis=1).astype(BF16)
        late_at = pl.ds(self.early_rows, self.late_rows)

        @pl.loop(1, self.half_size)
        def _(step):
            place = lax.rem(self.place + step, self.half_size)
            self.copy(self.relay_send.at[slot, place], self.recv.at[b, self.twin, late_at], self.relay_send_sem.at[slot],
                      self.relay_recv_sem.at[b], self.half * self.half_size + place).start()

        self.recv[b, self.twin, late_at] = self.relay_send[slot, self.place]

    def arrive(self, b):
        self.all_direct(b).wait_recv()
        self.all_relayed(b).wait_recv()

    def drain(self):
        for b in range(max(0, self.batch - SLOTS), self.batch):
            self.all_direct(b).wait_send()
            self.bridge(b).wait_send()
            self.all_relayed(b).wait_send()


def enter(me, group):
    barrier = pltpu.get_barrier_semaphore()

    @pl.loop(1, group)
    def _(step):
        pl.semaphore_signal(barrier, inc=1, device_id={'lat': lax.rem(me + step, group)}, device_id_type=MESH)

    pl.semaphore_wait(barrier, group - 1)


def load_legendre(me, group, table_hbm, stage, sem):
    m_local = stage.shape[0]
    copies = [pltpu.make_async_copy(table_hbm.at[slot * group + me], stage.at[slot], sem) for slot in range(m_local)]
    for copy in copies:
        copy.start()
    pltpu.make_async_copy(table_hbm.at[pl.ds(0, m_local)], stage, sem).wait()


def expand_rows(stage, expanded, rows_local):
    m_local, degrees, lats = stage.shape
    row = lax.broadcasted_iota(jnp.int32, (lats, 2 * lats), 0)
    col = lax.broadcasted_iota(jnp.int32, (lats, 2 * lats), 1)
    source = col // (2 * rows_local)
    inner = col % (2 * rows_local)
    for part in range(2):
        pick = (row == source * rows_local + inner - part * rows_local) & (inner // rows_local == part)
        pick = pick.astype(F32).astype(BF16)
        for slot in range(m_local):
            expanded[slot, pl.ds(part * degrees, degrees), :] = dot(stage[slot].astype(BF16), pick, NN).astype(BF16)


def flip_far(swap, table_hbm, stage, sem):
    late = swap.flipped_far.shape[0]
    copies = [pltpu.make_async_copy(table_hbm.at[(swap.direct + n) * swap.group + swap.twin], stage.at[n], sem) for n in range(late)]
    for copy in copies:
        copy.start()
    pltpu.make_async_copy(table_hbm.at[pl.ds(0, late)], stage.at[pl.ds(0, late)], sem).wait()
    for n in range(late):
        swap.flipped_far[n] = stage[n].T.astype(BF16)


def flip_rows(stage, flipped):
    for slot in range(stage.shape[0]):
        flipped[slot] = stage[slot].T.astype(BF16)


def analyse(values_at, table, turn, rows_local):
    modes = table.shape[1]
    for t in range(0, rows_local, 2):
        pair = jnp.concatenate([values_at(t), values_at(t + 1)], axis=0)
        high, low = split_halves(pair)
        out = dot(table[0], high, NT) + dot(table[0], low, NT) + dot(table[1], high, NT)
        channels = out.shape[1] // 2
        turn[pl.ds(t, modes, stride=rows_local), :] = out[:, :channels]
        turn[pl.ds(t + 1, modes, stride=rows_local), :] = out[:, channels:]


def pack_blocks(turn, send, slot):
    group, rows, lanes = send.shape[1:]
    for d in range(group):
        send[slot, d] = turn[pl.ds(d * rows, rows), :].astype(BF16)


def unpack_blocks(recv, b, turn):
    group, rows, lanes = recv.shape[1:]
    for d in range(group):
        turn[pl.ds(d * rows, rows), :] = recv[b, d].astype(F32)


def synthesise(turn, t, table, rows_local):
    modes = table.shape[1]
    spec = turn[pl.ds(t, modes, stride=rows_local), :].astype(BF16)
    return dot(spec, table[0], TN) + dot(spec, table[1], TN)


def legendre_forward(recv, b, expanded, out, rows_local):
    m_local = expanded.shape[0]
    degrees = expanded.shape[1] // 2
    group, _, lanes = recv.shape[1:]
    tile = 2 * rows_local
    for slot in range(m_local):
        rows = recv[b, :, pl.ds(slot * tile, tile), :].reshape(group * tile, lanes)
        res = dot(expanded[slot], rows, NN)
        for part in range(2):
            out[part, pl.ds(slot, degrees, stride=m_local), :] = res[part * degrees:(part + 1) * degrees]


def legendre_inverse(coef, flipped, swap, slot_out, rows_local):
    m_local, lats, degrees = flipped.shape
    send = swap.send
    at = 0
    group = lats // rows_local
    tile = 2 * rows_local
    for slot in range(m_local):
        parts = [coef.at[part][pl.ds(slot, degrees, stride=m_local), :].astype(BF16) for part in range(2)]
        if slot >= swap.direct:
            first = slot * group
            for part in range(2):
                swap.bridge_send[slot_out, part, pl.ds(at, degrees - first), :] = parts[part][first:]
            at += degrees - first
        res = dot(flipped[slot], jnp.concatenate(parts, axis=1), NN)
        lanes = res.shape[1] // 2
        blocks = [res[:, part * lanes:(part + 1) * lanes].reshape(group, rows_local, lanes) for part in range(2)]
        send[slot_out, :, pl.ds(slot * tile, tile), :] = jnp.concatenate(blocks, axis=1).astype(BF16)


def gelu_slope(values):
    cumulative = 0.5 * (1.0 + lax.erf(values * math.sqrt(0.5)))
    density = jnp.exp(-0.5 * values * values) * (1.0 / math.sqrt(2.0 * math.pi))
    return cumulative + values * density


def mix_block(w_block):
    half = w_block.shape[0] // 2
    w_real = w_block[pl.ds(0, half, stride=2), :]
    w_imag = w_block[pl.ds(1, half, stride=2), :]
    top = jnp.concatenate([w_real, -w_imag], axis=1)
    bottom = jnp.concatenate([w_imag, w_real], axis=1)
    return jnp.concatenate([top, bottom], axis=0).astype(BF16)


def rows_of_degree(block, inner, m_local):
    batch = block.shape[0]
    lanes = block.shape[-1]
    parts = [block[:, part, pl.ds(inner * m_local, m_local), :].reshape(batch * m_local, lanes) for part in range(2)]
    return jnp.concatenate(parts, axis=1).astype(BF16)


def first_kernel(group, rows_local, field, table, p_fwd, coef_out, field_buf, stage, expanded, turn, send, recv,
                 coef_buf, in_sem, out_sem, p_sem, send_sem, recv_sem):
    me = lax.axis_index('lat')
    batch = field.shape[0]
    channels = field.shape[1] // rows_local

    def fetch(b):
        return Halves(field, b, field_buf, lax.rem(b, 2), in_sem)

    def put(b):
        return pltpu.make_async_copy(coef_buf.at[lax.rem(b, 2)], coef_out.at[b], out_sem.at[lax.rem(b, 2)])

    fetch(0).start()
    enter(me, group)
    swap = Exchange(me, group, batch, send, recv, send_sem, recv_sem)
    lag = 2

    def body(i, carry):
        @pl.when(i < batch)
        def _():
            @pl.when(i + 1 < batch)
            def _():
                fetch(i + 1).start()

            fetch(i).wait()
            half = lax.rem(i, 2)
            analyse(lambda t: read_row(field_buf, half, t, channels, rows_local), table, turn, rows_local)
            swap.reserve(i)
            pack_blocks(turn, send, lax.rem(i, SLOTS))
            swap.start(i)

        @pl.when(i == 0)
        def _():
            load_legendre(me, group, p_fwd, stage, p_sem)
            expand_rows(stage, expanded, rows_local)

        @pl.when(i >= lag)
        def _():
            b = i - lag
            swap.arrive(b)

            @pl.when(b >= 2)
            def _():
                put(b - 2).wait()

            legendre_forward(recv, b, expanded, coef_buf.at[lax.rem(b, 2)], rows_local)
            put(b).start()

        return carry

    lax.fori_loop(0, batch + lag, body, 0)
    swap.drain()
    put(batch - 2).wait()
    put(batch - 1).wait()


def mix_loop(w_hbm, in_hbms, bufs, w_buf, w_sem, in_sems, blocks, step):
    per = w_buf.shape[1]

    def copies(k):
        slot = lax.rem(k, 2)
        out = [pltpu.make_async_copy(w_hbm.at[pl.ds(k * per, per)], w_buf.at[slot], w_sem.at[slot])]
        for src, buf, sem in zip(in_hbms, bufs, in_sems):
            rows = buf.shape[3]
            out.append(pltpu.make_async_copy(src.at[:, :, pl.ds(k * rows, rows), :], buf.at[slot], sem.at[slot]))
        return out

    for copy in copies(0):
        copy.start()

    def body(k, carry):
        @pl.when(k + 1 < blocks)
        def _():
            for copy in copies(k + 1):
                copy.start()

        for copy in copies(k):
            copy.wait()
        step(k, lax.rem(k, 2))
        return carry

    lax.fori_loop(0, blocks, body, 0)


def second_kernel(group, rows_local, coef, w_mix, p_inv, table, grad, mixed_out, w_buf, coef_blk, mixed, stage, flipped,
                  expanded, turn, grad_buf, out_buf, bridged, send_b, recv_b, w_sem, c_sem, in_sem, out_sem, p_sem,
                  bridged_sems, send_b_sem, recv_b_sem):
    me = lax.axis_index('lat')
    batch = grad.shape[0]
    channels = grad.shape[1] // rows_local
    m_local = stage.shape[0]
    per = w_buf.shape[1]
    degrees = stage.shape[1]

    def fetch(b):
        return Halves(grad, b, grad_buf, lax.rem(b, 2), in_sem)

    def put(b):
        return pltpu.make_async_copy(out_buf.at[lax.rem(b, 2)], mixed_out.at[b], out_sem.at[lax.rem(b, 2)])

    fetch(0).start()
    swap_a = BridgedExchange(me, group, batch, bridged, bridged_sems)
    load_legendre(me, group, p_inv, stage, p_sem)
    flip_rows(stage, flipped)
    expand_rows(stage, expanded, rows_local)
    flip_far(swap_a, p_inv, stage, p_sem)

    def mix(k, slot):
        for inner in range(per):
            rows = rows_of_degree(coef_blk.at[slot], inner, m_local)
            res = dot(rows, mix_block(w_buf.at[slot, inner]), NT)
            at = pl.ds(pl.multiple_of((k * per + inner) * m_local, m_local), m_local)
            for part in range(2):
                lanes = res.shape[1] // 2
                mixed[:, part, at, :] = res[:, part * lanes:(part + 1) * lanes].reshape(batch, m_local, lanes)

    mix_loop(w_mix, [coef], [coef_blk], w_buf, w_sem, [c_sem], degrees // per, mix)

    enter(me, group)
    swap_b = Exchange(me, group, batch, send_b, recv_b, send_b_sem, recv_b_sem)
    lag, lag_b = 2, 2

    def body(i, carry):
        @pl.when(i < batch)
        def _():
            swap_a.reserve(i)
            legendre_inverse(mixed.at[i], flipped, swap_a, lax.rem(i, SLOTS), rows_local)
            swap_a.start(i)

        @pl.when((i >= 1) & (i < batch + 1))
        def _():
            swap_a.relay(i - 1)

        @pl.when((i >= lag) & (i < batch + lag))
        def _():
            b = i - lag
            half = lax.rem(b, 2)

            @pl.when(b + 1 < batch)
            def _():
                fetch(b + 1).start()

            fetch(b).wait()
            swap_a.arrive(b)
            unpack_blocks(swap_a.recv, b, turn)
            for t in range(rows_local):
                slope = gelu_slope(synthesise(turn, t, table, rows_local))
                given = read_row(grad_buf, half, t, channels, rows_local)
                write_row(grad_buf, half, t, channels, rows_local, given * slope)
            analyse(lambda t: read_row(grad_buf, half, t, channels, rows_local), table, turn, rows_local)
            swap_b.reserve(b)
            pack_blocks(turn, send_b, lax.rem(b, SLOTS))
            swap_b.start(b)

        @pl.when(i >= lag + lag_b)
        def _():
            b = i - lag - lag_b
            swap_b.arrive(b)

            @pl.when(b >= 2)
            def _():
                put(b - 2).wait()

            legendre_forward(recv_b, b, expanded, out_buf.at[lax.rem(b, 2)], rows_local)
            put(b).start()

        return carry

    lax.fori_loop(0, batch + lag + lag_b, body, 0)
    swap_a.drain()
    swap_b.drain()
    put(batch - 2).wait()
    put(batch - 1).wait()


class WeightSum:
    def __init__(self, me, ring, sums, got, out, sems):
        self.ring, self.sums, self.got, self.out, self.sems = ring, sums, got, out, sems
        self.me = me
        self.core, self.y = lax.rem(me, 2), lax.rem(me // 2, 2)
        self.near, self.far = lax.rem(me // 4, 2), me // 8
        self.quarter = sums.shape[1]
        self.rows = sums.shape[2] // 2
        self.degree = self.y * (self.quarter // 2) + self.near

    def peer(self, phase):
        step = (1, 2, 4, 8)[phase]
        bit = (self.core, self.y, self.near, self.far)[phase]
        return {'lat': self.me + step - 2 * step * bit}

    def remote(self, phase, k, source, target, back):
        return pltpu.make_async_remote_copy(source, target, self.sems.at[back, 0, phase, k], self.sems.at[back, 1, phase, k],
                                            device_id=self.peer(phase), device_id_type=MESH)

    def halving(self, phase, k):
        if phase == 0:
            source, target = self.ring.at[lax.rem(k, self.ring.shape[0]), 1 - self.core], self.sums.at[k]
        elif phase == 1:
            half = self.quarter // 2
            source, target = self.sums.at[k, pl.ds((1 - self.y) * half, half)], self.got[0].at[k]
        elif phase == 2:
            source, target = self.sums.at[k, self.y * (self.quarter // 2) + 1 - self.near], self.got[1].at[k]
        else:
            at = pl.ds(pl.multiple_of((1 - self.far) * self.rows, self.rows), self.rows)
            source, target = self.sums.at[k, self.degree, at], self.got[2].at[k]
        return self.remote(phase, k, source, target, 0)

    def absorb(self, phase, k):
        self.halving(phase, k).wait()
        if phase == 0:
            self.sums[k] = self.sums[k] + self.ring[lax.rem(k, self.ring.shape[0]), self.core]
        elif phase == 1:
            half = self.quarter // 2
            at = pl.ds(self.y * half, half)
            self.sums[k, at] = self.sums[k, at] + self.got[0][k]
        elif phase == 2:
            self.sums[k, self.degree] = self.sums[k, self.degree] + self.got[1][k]
        else:
            at = self.last_rows()
            self.sums[k, self.degree, at] = self.sums[k, self.degree, at] + self.got[2][k]

    def last_rows(self):
        return pl.ds(pl.multiple_of(self.far * self.rows, self.rows), self.rows)

    def reduce_step(self, phase, k):
        self.absorb(phase - 1, k)
        if phase < 4:
            self.halving(phase, k).start()
        else:
            self.settle(k).start()
            self.doubling(3, k).start()

    def settle(self, k):
        at = self.last_rows()
        degree = k * 2 * self.quarter + self.core * self.quarter + self.degree
        return pltpu.make_async_copy(self.sums.at[k, self.degree, at], self.out.at[degree, at], self.sems.at[1, 2, 0, k])

    def doubling(self, phase, k):
        base = k * 2 * self.quarter + self.core * self.quarter
        if phase == 3:
            at = self.last_rows()
            return self.remote(3, k, self.sums.at[k, self.degree, at], self.out.at[base + self.degree, at], 1)
        if phase == 2:
            span = pl.ds(base + self.degree, 1)
        elif phase == 1:
            half = self.quarter // 2
            span = pl.ds(base + self.y * half, half)
        else:
            span = pl.ds(base, self.quarter)
        return self.remote(phase, k, self.out.at[span], self.out.at[span], 1)

    def gather_step(self, phase, k):
        if phase == 2:
            self.settle(k).wait()
        self.doubling(phase + 1, k).wait()
        if phase >= 0:
            self.doubling(phase, k).start()


def third_kernel(group, rows_local, mixed, coef, w_mix, p_fwd, table, grad, field_out, grad_w, w_buf, mixed_blk, coef_blk, ring,
                 sums, got_a, got_b, got_c, back, stage, flipped, turn, grad_buf, bridged, w_sem, m_sem, c_sem, gw_sem,
                 in_sem, out_sem, p_sem, bridged_sems):
    me = lax.axis_index('lat')
    batch = grad.shape[0]
    channels = grad.shape[1] // rows_local
    depth = grad_buf.shape[0]
    per = w_buf.shape[1]
    degrees = w_mix.shape[0]
    m_local = stage.shape[0]
    blocks = degrees // per

    def fetch(b):
        return Halves(grad, b, grad_buf, lax.rem(b, depth), in_sem)

    def put(b):
        return Halves(field_out, b, grad_buf, lax.rem(b, depth), out_sem, outward=True)

    enter(me, group)
    total = WeightSum(me, ring, sums, (got_a, got_b, got_c), grad_w, gw_sem)
    swap = BridgedExchange(me, group, batch, bridged, bridged_sems)

    early = 4

    def weigh(k, slot):
        place = lax.rem(k, ring.shape[0])
        for inner in range(per):
            rows = rows_of_degree(mixed_blk.at[slot], inner, m_local)
            keep = rows_of_degree(coef_blk.at[slot], inner, m_local)
            res = dot(rows, mix_block(w_buf.at[slot, inner]), NN)
            at = pl.ds(pl.multiple_of((k * per + inner) * m_local, m_local), m_local)
            half = res.shape[1] // 2
            for part in range(2):
                back[:, part, at, :] = res[:, part * half:(part + 1) * half].reshape(batch, m_local, half)
            big = dot(rows, keep, TN)
            side, spot = inner // (per // 2), inner % (per // 2)
            ring[place, side, spot, pl.ds(0, half, stride=2), :] = big[:half, :half] + big[half:, half:]
            ring[place, side, spot, pl.ds(1, half, stride=2), :] = big[half:, :half] - big[:half, half:]
        total.halving(0, k).start()

        @pl.when(k >= 2)
        def _():
            total.absorb(0, k - 2)

            @pl.when(k - 2 < early)
            def _():
                total.halving(1, k - 2).start()

    mix_loop(w_mix, [mixed, coef], [mixed_blk, coef_blk], w_buf, w_sem, [m_sem, c_sem], blocks, weigh)
    fetch(0).start()
    total.absorb(0, blocks - 2)
    total.absorb(0, blocks - 1)
    load_legendre(me, group, p_fwd, stage, p_sem)
    flip_rows(stage, flipped)
    flip_far(swap, p_fwd, stage, p_sem)
    lag = 2
    width = 2

    def body(i, carry):
        @pl.when(i < batch)
        def _():
            swap.reserve(i)
            legendre_inverse(back.at[i], flipped, swap, lax.rem(i, SLOTS), rows_local)
            swap.start(i)

        @pl.when((i >= 1) & (i < batch + 1))
        def _():
            swap.relay(i - 1)

        for j in range(width):
            k = early + i * width + j

            @pl.when(k < blocks)
            def _():
                total.halving(1, k).start()

        steps = [(total.reduce_step, p) for p in (2, 3, 4)] + [(total.gather_step, p) for p in (2, 1, 0, -1)]
        for late, (step, phase) in enumerate(steps):
            for j in range(width):
                k = (i - late) * width + j

                @pl.when((k >= 0) & (k < blocks))
                def _():
                    step(phase, k)

        @pl.when((i >= lag) & (i < batch + lag))
        def _():
            b = i - lag
            half = lax.rem(b, depth)

            @pl.when(b >= depth - 1)
            def _():
                put(b - depth + 1).wait()

            @pl.when(b + 1 < batch)
            def _():
                fetch(b + 1).start()

            fetch(b).wait()
            swap.arrive(b)
            unpack_blocks(swap.recv, b, turn)
            for t in range(rows_local):
                added = synthesise(turn, t, table, rows_local)
                given = read_row(grad_buf, half, t, channels, rows_local)
                write_row(grad_buf, half, t, channels, rows_local, given + added)
            put(b).start()

        return carry

    lax.fori_loop(0, max(batch + lag, blocks // width + 6), body, 0)
    swap.drain()
    for b in range(batch - depth + 1, batch):
        put(b).wait()


def any_specs(n):
    return [pl.BlockSpec(memory_space=pl.ANY)] * n


def params(collective_id=None):
    if collective_id is None:
        return pltpu.CompilerParams(vmem_limit_bytes=VMEM_LIMIT)
    return pltpu.CompilerParams(collective_id=collective_id, has_side_effects=True, vmem_limit_bytes=VMEM_LIMIT)


def solution(mesh):
    group = mesh.shape['lat']
    field_spec = P('member', None, 'lat', None)

    def local_step(field_loc, grad_loc, p_fwd, p_inv, w_mix):
        batch, channels, rows_local, lon_count = field_loc.shape
        degrees, lats = p_fwd.shape[1:]
        m_local = p_fwd.shape[0] // group
        modes = group * m_local * 2
        base, gained = (two_halves(table) for table in dft_tables(group, m_local, lon_count))
        field = field_loc.reshape(batch, channels * rows_local, lon_count)
        grad = grad_loc.reshape(batch, channels * rows_local, lon_count)
        w_rows = jnp.swapaxes(w_mix, 2, 3).reshape(degrees, channels * 2, channels)
        dma, vmem = pltpu.SemaphoreType.DMA, pltpu.VMEM
        block_rows = m_local * 2 * rows_local
        coef_shape = (batch, 2, degrees * m_local, channels)
        send_t = vmem((SLOTS, group, block_rows, channels), BF16)
        recv_t = vmem((batch, group, block_rows, channels), BF16)
        turn_t = vmem((modes * rows_local, channels), F32)
        stage_t = vmem((m_local, degrees, lats), F32)
        expanded_t = vmem((m_local, 2 * degrees, 2 * lats), BF16)
        flipped_t = vmem((m_local, lats, degrees), BF16)
        pair_t = vmem((2, 2, degrees * m_local, channels), F32)
        field_t = vmem((2, lon_count // LANES, channels * rows_local, LANES), F32)
        table_spec = pl.BlockSpec(memory_space=pltpu.VMEM)
        any_spec = pl.BlockSpec(memory_space=pl.ANY)
        per = 8
        late = sum(degrees - slot * group < lats // 2 for slot in range(m_local))
        far_rows = sum(degrees - slot * group for slot in range(m_local - late, m_local))
        late_rows = late * 2 * rows_local
        bridged_t = (send_t, recv_t, vmem((SLOTS, 2, far_rows, channels), BF16), vmem((batch, 2, far_rows, channels), BF16),
                     vmem((SLOTS, group // 2, late_rows, channels), BF16), vmem((late, lats, degrees), BF16))
        bridged_sems = (dma((SLOTS,)), dma((batch,))) * 3

        coef = pl.pallas_call(
            functools.partial(first_kernel, group, rows_local), name='first',
            out_shape=jax.ShapeDtypeStruct(coef_shape, F32),
            in_specs=[any_spec, table_spec, any_spec], out_specs=any_spec,
            scratch_shapes=[field_t, stage_t, expanded_t, turn_t, send_t, recv_t, pair_t, dma((2, 2)), dma((2,)), dma(()),
                            dma((SLOTS,)), dma((batch,))],
            compiler_params=params(0))(field, base, p_fwd)

        blk_t = vmem((2, batch, 2, per * m_local, channels), F32)
        w_t = vmem((2, per, channels * 2, channels), F32)
        mixed = pl.pallas_call(
            functools.partial(second_kernel, group, rows_local), name='second',
            out_shape=jax.ShapeDtypeStruct(coef_shape, F32),
            in_specs=[any_spec, any_spec, any_spec, table_spec, any_spec], out_specs=any_spec,
            scratch_shapes=[w_t, blk_t, vmem(coef_shape, F32), stage_t, flipped_t, expanded_t, turn_t, field_t, pair_t,
                            bridged_t, send_t, recv_t, dma((2,)), dma((2,)), dma((2, 2)), dma((2,)), dma(()),
                            bridged_sems, dma((SLOTS,)), dma((batch,))],
            compiler_params=params(1))(coef, w_rows, p_inv, gained, grad)

        blocks = degrees // per
        field_out, gw_total = pl.pallas_call(
            functools.partial(third_kernel, group, rows_local), name='third',
            out_shape=[jax.ShapeDtypeStruct(grad.shape, F32), jax.ShapeDtypeStruct(w_rows.shape, F32)],
            in_specs=[any_spec] * 4 + [table_spec, any_spec], out_specs=[any_spec] * 2,
            scratch_shapes=[w_t, blk_t, blk_t, vmem((4, 2, per // 2, channels * 2, channels), F32),
                            vmem((blocks, per // 2, channels * 2, channels), F32),
                            vmem((blocks, per // 4, channels * 2, channels), F32),
                            vmem((blocks, channels * 2, channels), F32), vmem((blocks, channels, channels), F32),
                            vmem(coef_shape, F32), stage_t, flipped_t, turn_t,
                            vmem((3, lon_count // LANES, channels * rows_local, LANES), F32), bridged_t,
                            dma((2,)), dma((2,)), dma((2,)), dma((2, 3, 4, blocks)), dma((3, 2)), dma((3, 2)), dma(()),
                            bridged_sems],
            compiler_params=params(2))(mixed, coef, w_rows, p_fwd, base, grad)

        grad_wmix = jnp.swapaxes(gw_total.reshape(degrees, channels, 2, channels), 2, 3)
        return field_out.reshape(grad_loc.shape), grad_wmix

    return jax.shard_map(local_step, mesh=mesh, in_specs=(field_spec, field_spec, P(), P(), P()),
                         out_specs=(field_spec, P('member', None, None, None)), check_vma=False)
```

```python
import functools
import math

import jax
import jax.numpy as jnp
import numpy as np
from jax import lax
from jax.experimental import pallas as pl
from jax.experimental.pallas import tpu as pltpu
from jax.sharding import PartitionSpec as P

MESH = pl.DeviceIdType.MESH
LANES = 128
SLOTS = 3
VMEM_LIMIT = 60 * 1024 * 1024
F32 = jnp.float32
BF16 = jnp.bfloat16

NN = (((1,), (0,)), ((), ()))
NT = (((1,), (1,)), ((), ()))
TN = (((0,), (0,)), ((), ()))


def dot(lhs, rhs, dims):
    return lax.dot_general(lhs, rhs, dims, preferred_element_type=F32)


def split_halves(values):
    high = values.astype(BF16)
    low = (values - high.astype(F32)).astype(BF16)
    return high, low


def dft_tables(group, m_local, lon_count):
    owner, slot, part = np.meshgrid(np.arange(group), np.arange(m_local), np.arange(2), indexing='ij')
    wave = (slot * group + owner).reshape(-1)
    part = part.reshape(-1)
    phase = 2.0 * np.pi * ((wave[:, None] * np.arange(lon_count)[None, :]) % lon_count) / lon_count
    base = np.where(part[:, None] == 0, np.cos(phase), -np.sin(phase)) / math.sqrt(lon_count)
    gains = np.where(wave == 0, 1.0, 2.0)[:, None]
    return base.astype(np.float32), (base * gains).astype(np.float32)


def two_halves(table):
    high = jnp.asarray(table).astype(BF16)
    low = (jnp.asarray(table) - high.astype(F32)).astype(BF16)
    return jnp.stack([high, low])


class Halves:
    def __init__(self, whole, b, halves, slot, sem, outward=False):
        self.copies = []
        for half in range(halves.shape[1]):
            ends = whole.at[b, :, pl.ds(half * LANES, LANES)], halves.at[slot, half]
            source, target = ends[::-1] if outward else ends
            self.copies.append(pltpu.make_async_copy(source, target, sem.at[slot, half]))

    def start(self):
        for copy in self.copies:
            copy.start()

    def wait(self):
        for copy in self.copies:
            copy.wait()


def read_row(halves, slot, t, channels, rows_local):
    at = pl.ds(t, channels, stride=rows_local)
    return jnp.concatenate([halves[slot, half, at, :] for half in range(halves.shape[1])], axis=1)


def write_row(halves, slot, t, channels, rows_local, values):
    at = pl.ds(t, channels, stride=rows_local)
    for half in range(halves.shape[1]):
        halves[slot, half, at, :] = values[:, half * LANES:(half + 1) * LANES]


class Exchange:
    def __init__(self, me, group, batch, send, recv, send_sem, recv_sem):
        self.me, self.group, self.batch = me, group, batch
        self.send, self.recv, self.send_sem, self.recv_sem = send, recv, send_sem, recv_sem

    def all_copies(self, b):
        slot = lax.rem(b, SLOTS)
        others = pl.ds(0, self.group - 1)
        return pltpu.make_async_remote_copy(
            self.send.at[slot, others], self.recv.at[b, others], self.send_sem.at[slot], self.recv_sem.at[b],
            device_id={'lat': lax.rem(self.me + 1, self.group)}, device_id_type=MESH)

    def reserve(self, b):
        @pl.when(b >= SLOTS)
        def _():
            self.all_copies(b - SLOTS).wait_send()

    def start(self, b):
        slot = lax.rem(b, SLOTS)
        self.recv[b, self.me] = self.send[slot, self.me]

        @pl.loop(1, self.group)
        def _(step):
            target = lax.rem(self.me + step, self.group)
            pltpu.make_async_remote_copy(
                self.send.at[slot, target], self.recv.at[b, self.me], self.send_sem.at[slot], self.recv_sem.at[b],
                device_id={'lat': target}, device_id_type=MESH).start()

    def arrive(self, b):
        self.all_copies(b).wait_recv()

    def drain(self):
        for b in range(max(0, self.batch - SLOTS), self.batch):
            self.all_copies(b).wait_send()


class BridgedExchange:
    def __init__(self, me, group, batch, bufs, sems):
        self.me, self.group, self.batch = me, group, batch
        self.send, self.recv, self.bridge_send, self.bridge_recv, self.relay_send, self.flipped_far = bufs
        self.send_sem, self.recv_sem, self.bridge_send_sem, self.bridge_recv_sem, self.relay_send_sem, self.relay_recv_sem = sems
        self.half_size = group // 2
        self.half = me // self.half_size
        self.place = lax.rem(me, self.half_size)
        self.twin = self.half_size + me - 2 * self.half_size * self.half
        self.rows = self.send.shape[2]
        self.late_rows = self.relay_send.shape[2]
        self.early_rows = self.rows - self.late_rows
        self.tile = self.late_rows // self.flipped_far.shape[0]
        self.direct = self.early_rows // self.tile

    def copy(self, source, target, send_sem, recv_sem, device):
        return pltpu.make_async_remote_copy(source, target, send_sem, recv_sem, device_id={'lat': device},
                                            device_id_type=MESH)

    def all_direct(self, b):
        slot = lax.rem(b, SLOTS)
        count = (self.half_size - 1) * self.rows + self.half_size * self.early_rows
        span = pl.ds(0, count // self.rows)
        return self.copy(self.send.at[slot, span], self.recv.at[b, span], self.send_sem.at[slot], self.recv_sem.at[b], self.twin)

    def all_relayed(self, b):
        slot = lax.rem(b, SLOTS)
        span, part = pl.ds(0, self.half_size - 1), pl.ds(0, self.late_rows)
        return self.copy(self.relay_send.at[slot, span], self.recv.at[b, span, part], self.relay_send_sem.at[slot],
                         self.relay_recv_sem.at[b], self.twin)

    def bridge(self, b):
        slot = lax.rem(b, SLOTS)
        return self.copy(self.bridge_send.at[slot], self.bridge_recv.at[b], self.bridge_send_sem.at[slot],
                         self.bridge_recv_sem.at[b], self.twin)

    def reserve(self, b):
        @pl.when(b >= SLOTS)
        def _():
            self.all_direct(b - SLOTS).wait_send()
            self.bridge(b - SLOTS).wait_send()

    def start(self, b):
        slot = lax.rem(b, SLOTS)
        self.bridge(b).start()
        early = pl.ds(0, self.early_rows)

        @pl.loop(0, self.half_size)
        def _(step):
            target = (1 - self.half) * self.half_size + lax.rem(self.place + step, self.half_size)
            self.copy(self.send.at[slot, target, early], self.recv.at[b, self.me, early], self.send_sem.at[slot],
                      self.recv_sem.at[b], target).start()

        @pl.loop(1, self.half_size)
        def _(step):
            target = self.half * self.half_size + lax.rem(self.place + step, self.half_size)
            self.copy(self.send.at[slot, target], self.recv.at[b, self.me], self.send_sem.at[slot], self.recv_sem.at[b],
                      target).start()

        self.recv[b, self.me] = self.send[slot, self.me]

    def relay(self, b):
        slot = lax.rem(b, SLOTS)

        @pl.when(b >= SLOTS)
        def _():
            self.all_relayed(b - SLOTS).wait_send()

        self.bridge(b).wait_recv()
        lats, degrees = self.flipped_far.shape[1:]
        own = pl.ds(pl.multiple_of(self.half * (lats // 2), lats // 2), lats // 2)
        at = 0
        for late in range(self.flipped_far.shape[0]):
            first = (self.direct + late) * self.group
            count = degrees - first
            parts = []
            for part in range(2):
                rows = self.bridge_recv[b, part, pl.ds(at, count), :]
                parts.append(jnp.concatenate([jnp.zeros((first, rows.shape[1]), BF16), rows], axis=0))
            at += count
            res = dot(self.flipped_far[late, own, :], jnp.concatenate(parts, axis=1), NN)
            lanes = res.shape[1] // 2
            blocks = [res[:, part * lanes:(part + 1) * lanes].reshape(self.half_size, self.tile // 2, lanes) for part in range(2)]
            self.relay_send[slot, :, pl.ds(late * self.tile, self.tile), :] = jnp.concatenate(blocks, axis=1).astype(BF16)
        late_at = pl.ds(self.early_rows, self.late_rows)

        @pl.loop(1, self.half_size)
        def _(step):
            place = lax.rem(self.place + step, self.half_size)
            self.copy(self.relay_send.at[slot, place], self.recv.at[b, self.twin, late_at], self.relay_send_sem.at[slot],
                      self.relay_recv_sem.at[b], self.half * self.half_size + place).start()

        self.recv[b, self.twin, late_at] = self.relay_send[slot, self.place]

    def arrive(self, b):
        self.all_direct(b).wait_recv()
        self.all_relayed(b).wait_recv()

    def drain(self):
        for b in range(max(0, self.batch - SLOTS), self.batch):
            self.all_direct(b).wait_send()
            self.bridge(b).wait_send()
            self.all_relayed(b).wait_send()


class Share:
    def __init__(self, me, group, batch, send, message, out, sems):
        self.batch, self.send, self.message, self.out = batch, send, message, out
        self.send_sem, self.recv_sem, self.local_sem = sems
        self.size = group // 2
        self.base = me // self.size * self.size
        self.place = lax.rem(me, self.size)

    def rank(self, place):
        return place // 4 + 2 * (lax.rem(place, 4) // 2) + 4 * lax.rem(place, 2)

    def copy(self, slot, source, b, target, place):
        return pltpu.make_async_remote_copy(
            self.send.at[slot, source], self.out.at[b, target], self.send_sem.at[slot], self.recv_sem.at[b],
            device_id={'lat': self.base + place}, device_id_type=MESH)

    def every(self, b):
        span = pl.ds(0, self.size - 1)
        return self.copy(lax.rem(b, SLOTS), span, b, span, lax.rem(self.place + 1, self.size))

    def keep(self, b):
        slot = lax.rem(b, SLOTS)
        return pltpu.make_async_copy(self.send.at[slot, self.rank(self.place)], self.out.at[b, self.place],
                                     self.local_sem.at[slot])

    def give(self, b, coef):
        slot_b = lax.rem(b, SLOTS)

        @pl.when(b >= SLOTS)
        def _():
            self.every(b - SLOTS).wait_send()
            self.keep(b - SLOTS).wait()

        size = self.size
        m_local = size
        tile = 2 * size

        def rows(part, slot, rank, first, count):
            return coef[part, pl.ds((first * size + rank) * m_local + slot, count, stride=size * m_local), :]

        for rank in range(size):
            for part in range(2):
                for pair in range(m_local // 2):
                    block = rows(part, pair, rank, 0, tile)
                    if pair:
                        block = block + rows(part, m_local - pair, rank, 2 * (m_local - pair), tile)
                    self.message[rank, pl.ds((part * (m_local // 2) + pair) * tile, tile), :] = block
                self.message[rank, pl.ds(m_local * tile + part * size, size), :] = rows(part, m_local // 2, rank, size, size)
        for rank in range(size):
            self.send[slot_b, rank] = self.message[rank].astype(BF16)
        self.keep(b).start()

        @pl.loop(1, size)
        def _(step):
            place = lax.rem(self.place + step, size)
            self.copy(slot_b, self.rank(place), b, self.place, place).start()

    def drain(self):
        for b in range(max(0, self.batch - SLOTS), self.batch):
            self.every(b).wait_send()
            self.keep(b).wait()

        @pl.loop(0, self.batch)
        def _(b):
            self.every(b).wait_recv()


def clear_after(coef, degrees_rows):
    slots, parts, rows, lanes = coef.shape
    for slot in range(slots):
        for part in range(parts):
            coef[slot, part, pl.ds(degrees_rows, rows - degrees_rows), :] = jnp.zeros((rows - degrees_rows, lanes), F32)


def enter(me, group):
    barrier = pltpu.get_barrier_semaphore()

    @pl.loop(1, group)
    def _(step):
        pl.semaphore_signal(barrier, inc=1, device_id={'lat': lax.rem(me + step, group)}, device_id_type=MESH)

    pl.semaphore_wait(barrier, group - 1)


def load_legendre(me, group, table_hbm, stage, sem):
    m_local = stage.shape[0]
    copies = [pltpu.make_async_copy(table_hbm.at[slot * group + me], stage.at[slot], sem) for slot in range(m_local)]
    for copy in copies:
        copy.start()
    pltpu.make_async_copy(table_hbm.at[pl.ds(0, m_local)], stage, sem).wait()


def expand_rows(stage, expanded, rows_local):
    m_local, degrees, lats = stage.shape
    row = lax.broadcasted_iota(jnp.int32, (lats, 2 * lats), 0)
    col = lax.broadcasted_iota(jnp.int32, (lats, 2 * lats), 1)
    source = col // (2 * rows_local)
    inner = col % (2 * rows_local)
    for part in range(2):
        pick = (row == source * rows_local + inner - part * rows_local) & (inner // rows_local == part)
        pick = pick.astype(F32).astype(BF16)
        for slot in range(m_local):
            expanded[slot, pl.ds(part * degrees, degrees), :] = dot(stage[slot].astype(BF16), pick, NN).astype(BF16)


def flip_far(swap, table_hbm, stage, sem):
    late = swap.flipped_far.shape[0]
    copies = [pltpu.make_async_copy(table_hbm.at[(swap.direct + n) * swap.group + swap.twin], stage.at[n], sem) for n in range(late)]
    for copy in copies:
        copy.start()
    pltpu.make_async_copy(table_hbm.at[pl.ds(0, late)], stage.at[pl.ds(0, late)], sem).wait()
    for n in range(late):
        swap.flipped_far[n] = stage[n].T.astype(BF16)


def flip_rows(stage, flipped):
    for slot in range(stage.shape[0]):
        flipped[slot] = stage[slot].T.astype(BF16)


def analyse(values_at, table, turn, rows_local):
    modes = table.shape[1]
    for t in range(0, rows_local, 2):
        pair = jnp.concatenate([values_at(t), values_at(t + 1)], axis=0)
        high, low = split_halves(pair)
        out = dot(table[0], high, NT) + dot(table[0], low, NT) + dot(table[1], high, NT)
        channels = out.shape[1] // 2
        turn[pl.ds(t, modes, stride=rows_local), :] = out[:, :channels]
        turn[pl.ds(t + 1, modes, stride=rows_local), :] = out[:, channels:]


def pack_blocks(turn, send, slot):
    group, rows, lanes = send.shape[1:]
    for d in range(group):
        send[slot, d] = turn[pl.ds(d * rows, rows), :].astype(BF16)


def unpack_blocks(recv, b, turn):
    group, rows, lanes = recv.shape[1:]
    for d in range(group):
        turn[pl.ds(d * rows, rows), :] = recv[b, d].astype(F32)


def synthesise(turn, t, table, rows_local):
    modes = table.shape[1]
    spec = turn[pl.ds(t, modes, stride=rows_local), :].astype(BF16)
    return dot(spec, table[0], TN) + dot(spec, table[1], TN)


def legendre_forward(recv, b, expanded, out, rows_local):
    m_local = expanded.shape[0]
    degrees = expanded.shape[1] // 2
    group, _, lanes = recv.shape[1:]
    tile = 2 * rows_local
    for slot in range(m_local):
        rows = recv[b, :, pl.ds(slot * tile, tile), :].reshape(group * tile, lanes)
        res = dot(expanded[slot], rows, NN)
        for part in range(2):
            out[part, pl.ds(slot, degrees, stride=m_local), :] = res[part * degrees:(part + 1) * degrees]


def legendre_inverse(coef, flipped, swap, slot_out, rows_local):
    m_local, lats, degrees = flipped.shape
    send = swap.send
    at = 0
    group = lats // rows_local
    tile = 2 * rows_local
    for slot in range(m_local):
        parts = [coef.at[part][pl.ds(slot, degrees, stride=m_local), :].astype(BF16) for part in range(2)]
        if slot >= swap.direct:
            first = slot * group
            for part in range(2):
                swap.bridge_send[slot_out, part, pl.ds(at, degrees - first), :] = parts[part][first:]
            at += degrees - first
        res = dot(flipped[slot], jnp.concatenate(parts, axis=1), NN)
        lanes = res.shape[1] // 2
        blocks = [res[:, part * lanes:(part + 1) * lanes].reshape(group, rows_local, lanes) for part in range(2)]
        send[slot_out, :, pl.ds(slot * tile, tile), :] = jnp.concatenate(blocks, axis=1).astype(BF16)


def gelu_slope(values):
    cumulative = 0.5 * (1.0 + lax.erf(values * math.sqrt(0.5)))
    density = jnp.exp(-0.5 * values * values) * (1.0 / math.sqrt(2.0 * math.pi))
    return cumulative + values * density


def mix_block(w_block):
    half = w_block.shape[0] // 2
    w_real = w_block[pl.ds(0, half, stride=2), :]
    w_imag = w_block[pl.ds(1, half, stride=2), :]
    top = jnp.concatenate([w_real, -w_imag], axis=1)
    bottom = jnp.concatenate([w_imag, w_real], axis=1)
    return jnp.concatenate([top, bottom], axis=0).astype(BF16)


def rows_of_degree(block, inner, m_local):
    batch = block.shape[0]
    lanes = block.shape[-1]
    parts = [block[:, part, pl.ds(inner * m_local, m_local), :].reshape(batch * m_local, lanes) for part in range(2)]
    return jnp.concatenate(parts, axis=1).astype(BF16)


def first_kernel(group, rows_local, field, table, p_fwd, coef_out, shared, field_buf, stage, expanded, turn, send, recv,
                 coef_buf, share_bufs, in_sem, out_sem, p_sem, send_sem, recv_sem, share_sems):
    me = lax.axis_index('lat')
    batch = field.shape[0]
    channels = field.shape[1] // rows_local

    def fetch(b):
        return Halves(field, b, field_buf, lax.rem(b, 2), in_sem)

    def put(b):
        whole = pl.ds(0, coef_out.shape[2])
        return pltpu.make_async_copy(coef_buf.at[lax.rem(b, 2), :, whole], coef_out.at[b], out_sem.at[lax.rem(b, 2)])

    fetch(0).start()
    enter(me, group)
    share = Share(me, group, batch, *share_bufs, shared, share_sems)
    clear_after(coef_buf, coef_out.shape[2])
    swap = Exchange(me, group, batch, send, recv, send_sem, recv_sem)
    lag = 2

    def body(i, carry):
        @pl.when(i < batch)
        def _():
            @pl.when(i + 1 < batch)
            def _():
                fetch(i + 1).start()

            fetch(i).wait()
            half = lax.rem(i, 2)
            analyse(lambda t: read_row(field_buf, half, t, channels, rows_local), table, turn, rows_local)
            swap.reserve(i)
            pack_blocks(turn, send, lax.rem(i, SLOTS))
            swap.start(i)

        @pl.when(i == 0)
        def _():
            load_legendre(me, group, p_fwd, stage, p_sem)
            expand_rows(stage, expanded, rows_local)

        @pl.when(i >= lag)
        def _():
            b = i - lag
            swap.arrive(b)

            @pl.when(b >= 2)
            def _():
                put(b - 2).wait()

            legendre_forward(recv, b, expanded, coef_buf.at[lax.rem(b, 2)], rows_local)
            put(b).start()
            share.give(b, coef_buf.at[lax.rem(b, 2)])

        return carry

    lax.fori_loop(0, batch + lag, body, 0)
    swap.drain()
    share.drain()
    put(batch - 2).wait()
    put(batch - 1).wait()


def mix_loop(w_hbm, in_hbms, bufs, w_buf, w_sem, in_sems, blocks, step):
    per = w_buf.shape[1]

    def copies(k):
        slot = lax.rem(k, 2)
        out = [pltpu.make_async_copy(w_hbm.at[pl.ds(k * per, per)], w_buf.at[slot], w_sem.at[slot])]
        for src, buf, sem in zip(in_hbms, bufs, in_sems):
            rows = buf.shape[3]
            out.append(pltpu.make_async_copy(src.at[:, :, pl.ds(k * rows, rows), :], buf.at[slot], sem.at[slot]))
        return out

    for copy in copies(0):
        copy.start()

    def body(k, carry):
        @pl.when(k + 1 < blocks)
        def _():
            for copy in copies(k + 1):
                copy.start()

        for copy in copies(k):
            copy.wait()
        step(k, lax.rem(k, 2))
        return carry

    lax.fori_loop(0, blocks, body, 0)


def second_kernel(group, rows_local, coef, w_mix, p_inv, table, grad, mixed_out, shared, w_buf, coef_blk, mixed, stage,
                  flipped, expanded, turn, grad_buf, out_buf, bridged, send_b, recv_b, share_bufs, w_sem, c_sem, in_sem, out_sem,
                  p_sem, bridged_sems, send_b_sem, recv_b_sem, share_sems):
    me = lax.axis_index('lat')
    batch = grad.shape[0]
    channels = grad.shape[1] // rows_local
    m_local = stage.shape[0]
    per = w_buf.shape[1]
    degrees = stage.shape[1]

    def fetch(b):
        return Halves(grad, b, grad_buf, lax.rem(b, 2), in_sem)

    def put(b):
        whole = pl.ds(0, mixed_out.shape[2])
        return pltpu.make_async_copy(out_buf.at[lax.rem(b, 2), :, whole], mixed_out.at[b], out_sem.at[lax.rem(b, 2)])

    fetch(0).start()
    swap_a = BridgedExchange(me, group, batch, bridged, bridged_sems)
    load_legendre(me, group, p_inv, stage, p_sem)
    flip_rows(stage, flipped)
    expand_rows(stage, expanded, rows_local)
    flip_far(swap_a, p_inv, stage, p_sem)
    share = Share(me, group, batch, *share_bufs, shared, share_sems)
    clear_after(out_buf, mixed_out.shape[2])

    def mix(k, slot):
        for inner in range(per):
            rows = rows_of_degree(coef_blk.at[slot], inner, m_local)
            res = dot(rows, mix_block(w_buf.at[slot, inner]), NT)
            at = pl.ds(pl.multiple_of((k * per + inner) * m_local, m_local), m_local)
            for part in range(2):
                lanes = res.shape[1] // 2
                mixed[:, part, at, :] = res[:, part * lanes:(part + 1) * lanes].reshape(batch, m_local, lanes)

    mix_loop(w_mix, [coef], [coef_blk], w_buf, w_sem, [c_sem], degrees // per, mix)

    enter(me, group)
    swap_b = Exchange(me, group, batch, send_b, recv_b, send_b_sem, recv_b_sem)
    lag, lag_b = 2, 2

    def body(i, carry):
        @pl.when(i < batch)
        def _():
            swap_a.reserve(i)
            legendre_inverse(mixed.at[i], flipped, swap_a, lax.rem(i, SLOTS), rows_local)
            swap_a.start(i)

        @pl.when((i >= 1) & (i < batch + 1))
        def _():
            swap_a.relay(i - 1)

        @pl.when((i >= lag) & (i < batch + lag))
        def _():
            b = i - lag
            half = lax.rem(b, 2)

            @pl.when(b + 1 < batch)
            def _():
                fetch(b + 1).start()

            fetch(b).wait()
            swap_a.arrive(b)
            unpack_blocks(swap_a.recv, b, turn)
            for t in range(rows_local):
                slope = gelu_slope(synthesise(turn, t, table, rows_local))
                given = read_row(grad_buf, half, t, channels, rows_local)
                write_row(grad_buf, half, t, channels, rows_local, given * slope)
            analyse(lambda t: read_row(grad_buf, half, t, channels, rows_local), table, turn, rows_local)
            swap_b.reserve(b)
            pack_blocks(turn, send_b, lax.rem(b, SLOTS))
            swap_b.start(b)

        @pl.when(i >= lag + lag_b)
        def _():
            b = i - lag - lag_b
            swap_b.arrive(b)

            @pl.when(b >= 2)
            def _():
                put(b - 2).wait()

            legendre_forward(recv_b, b, expanded, out_buf.at[lax.rem(b, 2)], rows_local)
            put(b).start()
            share.give(b, out_buf.at[lax.rem(b, 2)])

        return carry

    lax.fori_loop(0, batch + lag + lag_b, body, 0)
    swap_a.drain()
    swap_b.drain()
    share.drain()
    put(batch - 2).wait()
    put(batch - 1).wait()


class WeightSum:
    def __init__(self, me, group, sums, got, out, sems):
        self.me, self.sums, self.got, self.out, self.sems = me, sums, got, out, sems
        self.core, self.y = lax.rem(me, 2), lax.rem(me // 2, 2)
        self.near, self.far = lax.rem(me // 4, 2), me // (group // 2)
        self.rank = self.near + 2 * self.y + 4 * self.core

    def peer(self, phase):
        step = (1, 2, 4, 8)[phase]
        bit = (self.core, self.y, self.near, self.far)[phase]
        return {'lat': self.me + step - 2 * step * bit}

    def remote(self, phase, k, source, target, stage):
        return pltpu.make_async_remote_copy(source, target, self.sems.at[0, stage, k], self.sems.at[1, stage, k],
                                            device_id=self.peer(phase), device_id_type=MESH)

    def halving(self, k):
        return self.remote(3, k, self.sums.at[2 * k + 1 - self.far], self.got.at[k], 4)

    def settle(self, k):
        mine = 2 * k + self.far
        return pltpu.make_async_copy(self.sums.at[mine], self.out.at[mine, self.rank], self.sems.at[0, 5, k])

    def doubling(self, phase, k):
        if phase == 3:
            mine = 2 * k + self.far
            return self.remote(3, k, self.sums.at[mine], self.out.at[mine, self.rank], 3)
        width = (4, 2, 1)[phase]
        first = (4 * self.core, 4 * self.core + 2 * self.y, self.rank)[phase]
        span = self.out.at[pl.ds(2 * k, 2), pl.ds(first, width)]
        return self.remote(phase, k, span, span, phase)

    def reduce_step(self, k):
        self.halving(k).wait()
        mine = 2 * k + self.far
        self.sums[mine] = self.sums[mine] + self.got[k]
        self.settle(k).start()
        self.doubling(3, k).start()

    def gather_step(self, phase, k):
        if phase == 2:
            self.settle(k).wait()
        self.doubling(phase + 1, k).wait()
        if phase >= 0:
            self.doubling(phase, k).start()


def shared_place(part, slot, step, m_local):
    tile = 2 * m_local
    if slot == m_local // 2:
        return m_local * tile + part * m_local + step - m_local
    pair = min(slot, m_local - slot) if slot else 0
    shift = 0 if slot < m_local // 2 else 2 * slot
    return (part * (m_local // 2) + pair) * tile + step - shift


def weigh(shared, batch_rows, sums, m_local):
    block_rows = shared.shape[1] // batch_rows

    @pl.loop(0, sums.shape[0])
    def _(step):
        sides = []
        for which in range(2):
            slots = []
            for slot in range(m_local):
                used = step >= 2 * slot
                parts = []
                for part in range(2):
                    place = jnp.where(used, shared_place(part, slot, step, m_local), 0)
                    rows = shared[which, pl.ds(place, batch_rows, stride=block_rows), :]
                    parts.append(jnp.where(used, rows, 0.0))
                slots.append(jnp.concatenate(parts, axis=1))
            sides.append(jnp.concatenate(slots, axis=0).astype(BF16))
        big = dot(sides[0], sides[1], TN)
        half = big.shape[0] // 2
        sums[step, pl.ds(0, half, stride=2), :] = big[:half, :half] + big[half:, half:]
        sums[step, pl.ds(1, half, stride=2), :] = big[half:, :half] - big[:half, half:]


def third_kernel(group, rows_local, mixed, shared_mixed, shared_coef, w_mix, p_fwd, table, grad, field_out, grad_w, w_buf,
                 mixed_blk, shared_half, shared, sums, got, back, stage, flipped, turn, grad_buf, bridged, w_sem, m_sem, s_sem,
                 gw_sem, in_sem, out_sem, p_sem, bridged_sems):
    me = lax.axis_index('lat')
    batch = grad.shape[0]
    channels = grad.shape[1] // rows_local
    depth = grad_buf.shape[0]
    per = w_buf.shape[1]
    degrees = w_mix.shape[0]
    m_local = stage.shape[0]
    sources = shared_mixed.shape[1]

    def fetch(b):
        return Halves(grad, b, grad_buf, lax.rem(b, depth), in_sem)

    def put(b):
        return Halves(field_out, b, grad_buf, lax.rem(b, depth), out_sem, outward=True)

    def fetch_shared(which, b):
        return pltpu.make_async_copy((shared_mixed, shared_coef)[which].at[b], shared_half.at[which, b], s_sem.at[which, b])

    for which in range(2):
        @pl.loop(0, batch)
        def _(b):
            fetch_shared(which, b).start()

    enter(me, group)
    total = WeightSum(me, group, sums, got, grad_w, gw_sem)
    swap = BridgedExchange(me, group, batch, bridged, bridged_sems)

    for which in range(2):
        @pl.loop(0, batch)
        def _(b):
            fetch_shared(which, b).wait()
            rows = shared_half.shape[3]
            for source in range(sources):
                at = pl.multiple_of((b * sources + source) * rows, 8)
                shared[which, pl.ds(at, rows), :] = shared_half[which, b, source].astype(F32)

    weigh(shared, batch * sources, sums, m_local)
    chunks = sums.shape[0] // 2
    for k in range(chunks):
        total.halving(k).start()

    def unmix(k, slot):
        for inner in range(per):
            rows = rows_of_degree(mixed_blk.at[slot], inner, m_local)
            res = dot(rows, mix_block(w_buf.at[slot, inner]), NN)
            at = pl.ds(pl.multiple_of((k * per + inner) * m_local, m_local), m_local)
            half = res.shape[1] // 2
            for part in range(2):
                back[:, part, at, :] = res[:, part * half:(part + 1) * half].reshape(batch, m_local, half)

    mix_loop(w_mix, [mixed], [mixed_blk], w_buf, w_sem, [m_sem], degrees // per, unmix)
    fetch(0).start()
    load_legendre(me, group, p_fwd, stage, p_sem)
    flip_rows(stage, flipped)
    flip_far(swap, p_fwd, stage, p_sem)
    lag = 2

    def body(i, carry):
        @pl.when(i < batch)
        def _():
            swap.reserve(i)
            legendre_inverse(back.at[i], flipped, swap, lax.rem(i, SLOTS), rows_local)
            swap.start(i)

        @pl.when((i >= 1) & (i < batch + 1))
        def _():
            swap.relay(i - 1)

        steps = [total.reduce_step] + [functools.partial(total.gather_step, p) for p in (2, 1, 0, -1)]
        for late, step in enumerate(steps):
            k = i - late

            @pl.when((k >= 0) & (k < chunks))
            def _():
                step(k)

        @pl.when((i >= lag) & (i < batch + lag))
        def _():
            b = i - lag
            half = lax.rem(b, depth)

            @pl.when(b >= depth - 1)
            def _():
                put(b - depth + 1).wait()

            @pl.when(b + 1 < batch)
            def _():
                fetch(b + 1).start()

            fetch(b).wait()
            swap.arrive(b)
            unpack_blocks(swap.recv, b, turn)
            for t in range(rows_local):
                added = synthesise(turn, t, table, rows_local)
                given = read_row(grad_buf, half, t, channels, rows_local)
                write_row(grad_buf, half, t, channels, rows_local, given + added)
            put(b).start()

        return carry

    lax.fori_loop(0, max(batch + lag, chunks + 4), body, 0)
    swap.drain()
    for b in range(batch - depth + 1, batch):
        put(b).wait()


def any_specs(n):
    return [pl.BlockSpec(memory_space=pl.ANY)] * n


def params(collective_id=None):
    if collective_id is None:
        return pltpu.CompilerParams(vmem_limit_bytes=VMEM_LIMIT)
    return pltpu.CompilerParams(collective_id=collective_id, has_side_effects=True, vmem_limit_bytes=VMEM_LIMIT)


def solution(mesh):
    group = mesh.shape['lat']
    field_spec = P('member', None, 'lat', None)

    def local_step(field_loc, grad_loc, p_fwd, p_inv, w_mix):
        batch, channels, rows_local, lon_count = field_loc.shape
        degrees, lats = p_fwd.shape[1:]
        m_local = p_fwd.shape[0] // group
        modes = group * m_local * 2
        base, gained = (two_halves(table) for table in dft_tables(group, m_local, lon_count))
        field = field_loc.reshape(batch, channels * rows_local, lon_count)
        grad = grad_loc.reshape(batch, channels * rows_local, lon_count)
        w_rows = jnp.swapaxes(w_mix, 2, 3).reshape(degrees, channels * 2, channels)
        dma, vmem = pltpu.SemaphoreType.DMA, pltpu.VMEM
        block_rows = m_local * 2 * rows_local
        coef_shape = (batch, 2, degrees * m_local, channels)
        send_t = vmem((SLOTS, group, block_rows, channels), BF16)
        recv_t = vmem((batch, group, block_rows, channels), BF16)
        turn_t = vmem((modes * rows_local, channels), F32)
        stage_t = vmem((m_local, degrees, lats), F32)
        expanded_t = vmem((m_local, 2 * degrees, 2 * lats), BF16)
        flipped_t = vmem((m_local, lats, degrees), BF16)
        pair_t = vmem((2, 2, degrees * m_local, channels), F32)
        field_t = vmem((2, lon_count // LANES, channels * rows_local, LANES), F32)
        table_spec = pl.BlockSpec(memory_space=pltpu.VMEM)
        any_spec = pl.BlockSpec(memory_space=pl.ANY)
        per = 8
        late = sum(degrees - slot * group < lats // 2 for slot in range(m_local))
        far_rows = sum(degrees - slot * group for slot in range(m_local - late, m_local))
        late_rows = late * 2 * rows_local
        bridged_t = (send_t, recv_t, vmem((SLOTS, 2, far_rows, channels), BF16), vmem((batch, 2, far_rows, channels), BF16),
                     vmem((SLOTS, group // 2, late_rows, channels), BF16), vmem((late, lats, degrees), BF16))
        bridged_sems = (dma((SLOTS,)), dma((batch,))) * 3

        ranks = group // 2
        share_rows = (m_local + 1) * 2 * ranks
        share_out = jax.ShapeDtypeStruct((batch, ranks, share_rows, channels), BF16)
        share_t = (vmem((SLOTS, ranks, share_rows, channels), BF16), vmem((ranks, share_rows, channels), F32))
        share_sems = (dma((SLOTS,)), dma((batch,)), dma((SLOTS,)))
        padded_t = vmem((2, 2, 2 * degrees * m_local, channels), F32)

        coef, shared_coef = pl.pallas_call(
            functools.partial(first_kernel, group, rows_local), name='first',
            out_shape=[jax.ShapeDtypeStruct(coef_shape, F32), share_out],
            in_specs=[any_spec, table_spec, any_spec], out_specs=[any_spec] * 2,
            scratch_shapes=[field_t, stage_t, expanded_t, turn_t, send_t, recv_t, padded_t, share_t, dma((2, 2)), dma((2,)),
                            dma(()), dma((SLOTS,)), dma((batch,)), share_sems],
            compiler_params=params(0))(field, base, p_fwd)

        blk_t = vmem((2, batch, 2, per * m_local, channels), F32)
        w_t = vmem((2, per, channels * 2, channels), F32)
        mixed, shared_mixed = pl.pallas_call(
            functools.partial(second_kernel, group, rows_local), name='second',
            out_shape=[jax.ShapeDtypeStruct(coef_shape, F32), share_out],
            in_specs=[any_spec, any_spec, any_spec, table_spec, any_spec], out_specs=[any_spec] * 2,
            scratch_shapes=[w_t, blk_t, vmem(coef_shape, F32), stage_t, flipped_t, expanded_t, turn_t, field_t, padded_t,
                            bridged_t, send_t, recv_t, share_t, dma((2,)), dma((2,)), dma((2, 2)), dma((2,)), dma(()),
                            bridged_sems, dma((SLOTS,)), dma((batch,)), share_sems],
            compiler_params=params(1))(coef, w_rows, p_inv, gained, grad)

        steps = degrees // ranks
        w_rect = (channels * 2, channels)
        field_out, gw_total = pl.pallas_call(
            functools.partial(third_kernel, group, rows_local), name='third',
            out_shape=[jax.ShapeDtypeStruct(grad.shape, F32), jax.ShapeDtypeStruct((steps, ranks) + w_rect, F32)],
            in_specs=[any_spec] * 5 + [table_spec, any_spec], out_specs=[any_spec] * 2,
            scratch_shapes=[w_t, blk_t, vmem((2, batch, ranks, share_rows, channels), BF16),
                            vmem((2, batch * ranks * share_rows, channels), F32), vmem((steps,) + w_rect, F32),
                            vmem((steps // 2,) + w_rect, F32), vmem(coef_shape, F32), stage_t, flipped_t, turn_t,
                            vmem((3, lon_count // LANES, channels * rows_local, LANES), F32), bridged_t,
                            dma((2,)), dma((2,)), dma((2, batch)), dma((2, 6, steps // 2)), dma((3, 2)), dma((3, 2)), dma(()),
                            bridged_sems],
            compiler_params=params(2))(mixed, shared_mixed, shared_coef, w_rows, p_fwd, base, grad)

        grad_wmix = jnp.swapaxes(gw_total.reshape(degrees, channels, 2, channels), 2, 3)
        return field_out.reshape(grad_loc.shape), grad_wmix

    return jax.shard_map(local_step, mesh=mesh, in_specs=(field_spec, field_spec, P(), P(), P()),
                         out_specs=(field_spec, P('member', None, None, None)), check_vma=False)
```

```python
import functools
import math

import jax
import jax.numpy as jnp
import numpy as np
from jax import lax
from jax.experimental import pallas as pl
from jax.experimental.pallas import tpu as pltpu
from jax.sharding import PartitionSpec as P

MESH = pl.DeviceIdType.MESH
LANES = 128
SLOTS = 3
DEPTH = 4
VMEM_LIMIT = 60 * 1024 * 1024
F32 = jnp.float32
BF16 = jnp.bfloat16

NN = (((1,), (0,)), ((), ()))
NT = (((1,), (1,)), ((), ()))
TN = (((0,), (0,)), ((), ()))


def dot(lhs, rhs, dims):
    return lax.dot_general(lhs, rhs, dims, preferred_element_type=F32)


def split_halves(values):
    high = values.astype(BF16)
    low = (values - high.astype(F32)).astype(BF16)
    return high, low


def dft_tables(group, m_local, lon_count):
    owner, slot, part = np.meshgrid(np.arange(group), np.arange(m_local), np.arange(2), indexing='ij')
    wave = (slot * group + owner).reshape(-1)
    part = part.reshape(-1)
    phase = 2.0 * np.pi * ((wave[:, None] * np.arange(lon_count)[None, :]) % lon_count) / lon_count
    base = np.where(part[:, None] == 0, np.cos(phase), -np.sin(phase)) / math.sqrt(lon_count)
    gains = np.where(wave == 0, 1.0, 2.0)[:, None]
    return base.astype(np.float32), (base * gains).astype(np.float32)


def two_halves(table):
    high = jnp.asarray(table).astype(BF16)
    low = (jnp.asarray(table) - high.astype(F32)).astype(BF16)
    return jnp.stack([high, low])


class Halves:
    def __init__(self, whole, b, halves, slot, sem, outward=False):
        self.copies = []
        for half in range(halves.shape[1]):
            ends = whole.at[b, :, pl.ds(half * LANES, LANES)], halves.at[slot, half]
            source, target = ends[::-1] if outward else ends
            self.copies.append(pltpu.make_async_copy(source, target, sem.at[slot, half]))

    def start(self):
        for copy in self.copies:
            copy.start()

    def wait(self):
        for copy in self.copies:
            copy.wait()


def read_row(halves, slot, t, channels, rows_local):
    at = pl.ds(t, channels, stride=rows_local)
    return jnp.concatenate([halves[slot, half, at, :] for half in range(halves.shape[1])], axis=1)


def write_row(halves, slot, t, channels, rows_local, values):
    at = pl.ds(t, channels, stride=rows_local)
    for half in range(halves.shape[1]):
        halves[slot, half, at, :] = values[:, half * LANES:(half + 1) * LANES]


class Exchange:
    def __init__(self, me, group, batch, send, recv, send_sem, recv_sem):
        self.me, self.group, self.batch = me, group, batch
        self.send, self.recv, self.send_sem, self.recv_sem = send, recv, send_sem, recv_sem

    def all_copies(self, b):
        slot = lax.rem(b, SLOTS)
        others = pl.ds(0, self.group - 1)
        return pltpu.make_async_remote_copy(
            self.send.at[slot, others], self.recv.at[b, others], self.send_sem.at[slot], self.recv_sem.at[b],
            device_id={'lat': lax.rem(self.me + 1, self.group)}, device_id_type=MESH)

    def reserve(self, b):
        @pl.when(b >= SLOTS)
        def _():
            self.all_copies(b - SLOTS).wait_send()

    def start(self, b):
        slot = lax.rem(b, SLOTS)
        self.recv[b, self.me] = self.send[slot, self.me]

        @pl.loop(1, self.group)
        def _(step):
            target = lax.rem(self.me + step, self.group)
            pltpu.make_async_remote_copy(
                self.send.at[slot, target], self.recv.at[b, self.me], self.send_sem.at[slot], self.recv_sem.at[b],
                device_id={'lat': target}, device_id_type=MESH).start()

    def arrive(self, b):
        self.all_copies(b).wait_recv()

    def drain(self):
        for b in range(max(0, self.batch - SLOTS), self.batch):
            self.all_copies(b).wait_send()


class BridgedExchange:
    def __init__(self, me, group, batch, bufs, sems):
        self.me, self.group, self.batch = me, group, batch
        self.send, self.recv, self.bridge_send, self.bridge_recv, self.relay_send, self.flipped_far = bufs
        self.send_sem, self.recv_sem, self.bridge_send_sem, self.bridge_recv_sem, self.relay_send_sem, self.relay_recv_sem = sems
        self.half_size = group // 2
        self.half = me // self.half_size
        self.place = lax.rem(me, self.half_size)
        self.twin = self.half_size + me - 2 * self.half_size * self.half
        self.rows = self.send.shape[2]
        self.late_rows = self.relay_send.shape[2]
        self.early_rows = self.rows - self.late_rows
        self.tile = self.late_rows // self.flipped_far.shape[0]
        self.direct = self.early_rows // self.tile

    def copy(self, source, target, send_sem, recv_sem, device):
        return pltpu.make_async_remote_copy(source, target, send_sem, recv_sem, device_id={'lat': device},
                                            device_id_type=MESH)

    def all_direct(self, b):
        slot = lax.rem(b, SLOTS)
        count = (self.half_size - 1) * self.rows + self.half_size * self.early_rows
        span = pl.ds(0, count // self.rows)
        return self.copy(self.send.at[slot, span], self.recv.at[b, span], self.send_sem.at[slot], self.recv_sem.at[b], self.twin)

    def all_relayed(self, b):
        slot = lax.rem(b, SLOTS)
        span, part = pl.ds(0, self.half_size - 1), pl.ds(0, self.late_rows)
        return self.copy(self.relay_send.at[slot, span], self.recv.at[b, span, part], self.relay_send_sem.at[slot],
                         self.relay_recv_sem.at[b], self.twin)

    def bridge(self, b):
        slot = lax.rem(b, SLOTS)
        return self.copy(self.bridge_send.at[slot], self.bridge_recv.at[b], self.bridge_send_sem.at[slot],
                         self.bridge_recv_sem.at[b], self.twin)

    def reserve(self, b):
        @pl.when(b >= SLOTS)
        def _():
            self.all_direct(b - SLOTS).wait_send()
            self.bridge(b - SLOTS).wait_send()

    def start(self, b):
        slot = lax.rem(b, SLOTS)
        self.bridge(b).start()
        early = pl.ds(0, self.early_rows)

        @pl.loop(0, self.half_size)
        def _(step):
            target = (1 - self.half) * self.half_size + lax.rem(self.place + step, self.half_size)
            self.copy(self.send.at[slot, target, early], self.recv.at[b, self.me, early], self.send_sem.at[slot],
                      self.recv_sem.at[b], target).start()

        @pl.loop(1, self.half_size)
        def _(step):
            target = self.half * self.half_size + lax.rem(self.place + step, self.half_size)
            self.copy(self.send.at[slot, target], self.recv.at[b, self.me], self.send_sem.at[slot], self.recv_sem.at[b],
                      target).start()

        self.recv[b, self.me] = self.send[slot, self.me]

    def relay(self, b):
        slot = lax.rem(b, SLOTS)

        @pl.when(b >= SLOTS)
        def _():
            self.all_relayed(b - SLOTS).wait_send()

        self.bridge(b).wait_recv()
        lats, degrees = self.flipped_far.shape[1:]
        own = pl.ds(pl.multiple_of(self.half * (lats // 2), lats // 2), lats // 2)
        at = 0
        for late in range(self.flipped_far.shape[0]):
            first = (self.direct + late) * self.group
            count = degrees - first
            parts = []
            for part in range(2):
                rows = self.bridge_recv[b, part, pl.ds(at, count), :]
                parts.append(jnp.concatenate([jnp.zeros((first, rows.shape[1]), BF16), rows], axis=0))
            at += count
            res = dot(self.flipped_far[late, own, :], jnp.concatenate(parts, axis=1), NN)
            lanes = res.shape[1] // 2
            blocks = [res[:, part * lanes:(part + 1) * lanes].reshape(self.half_size, self.tile // 2, lanes) for part in range(2)]
            self.relay_send[slot, :, pl.ds(late * self.tile, self.tile), :] = jnp.concatenate(blocks, axis=1).astype(BF16)
        late_at = pl.ds(self.early_rows, self.late_rows)

        @pl.loop(1, self.half_size)
        def _(step):
            place = lax.rem(self.place + step, self.half_size)
            self.copy(self.relay_send.at[slot, place], self.recv.at[b, self.twin, late_at], self.relay_send_sem.at[slot],
                      self.relay_recv_sem.at[b], self.half * self.half_size + place).start()

        self.recv[b, self.twin, late_at] = self.relay_send[slot, self.place]

    def arrive(self, b):
        self.all_direct(b).wait_recv()
        self.all_relayed(b).wait_recv()

    def drain(self):
        for b in range(max(0, self.batch - SLOTS), self.batch):
            self.all_direct(b).wait_send()
            self.bridge(b).wait_send()
            self.all_relayed(b).wait_send()


class Share:
    def __init__(self, me, group, batch, send, message, out, sems, resident=False):
        self.batch, self.send, self.message, self.out, self.resident = batch, send, message, out, resident
        self.send_sem, self.recv_sem, self.local_sem = sems
        self.size = group // 2
        self.base = me // self.size * self.size
        self.place = lax.rem(me, self.size)

    def rank(self, place):
        return place // 4 + 2 * (lax.rem(place, 4) // 2) + 4 * lax.rem(place, 2)

    def copy(self, slot, source, b, target, place):
        return pltpu.make_async_remote_copy(
            self.send.at[slot, source], self.out.at[b, target], self.send_sem.at[slot], self.recv_sem.at[b],
            device_id={'lat': self.base + place}, device_id_type=MESH)

    def every(self, b):
        span = pl.ds(0, self.size - 1)
        return self.copy(lax.rem(b, SLOTS), span, b, span, lax.rem(self.place + 1, self.size))

    def keep(self, b):
        slot = lax.rem(b, SLOTS)
        return pltpu.make_async_copy(self.send.at[slot, self.rank(self.place)], self.out.at[b, self.place],
                                     self.local_sem.at[slot])

    def give(self, b, coef):
        slot_b = lax.rem(b, SLOTS)

        @pl.when(b >= SLOTS)
        def _():
            self.every(b - SLOTS).wait_send()
            if not self.resident:
                self.keep(b - SLOTS).wait()

        size = self.size
        m_local = size
        tile = 2 * size

        def rows(part, slot, rank, first, count):
            return coef[part, pl.ds((first * size + rank) * m_local + slot, count, stride=size * m_local), :]

        for rank in range(size):
            for part in range(2):
                for pair in range(m_local // 2):
                    block = rows(part, pair, rank, 0, tile)
                    if pair:
                        block = block + rows(part, m_local - pair, rank, 2 * (m_local - pair), tile)
                    self.message[rank, pl.ds((part * (m_local // 2) + pair) * tile, tile), :] = block
                self.message[rank, pl.ds(m_local * tile + part * size, size), :] = rows(part, m_local // 2, rank, size, size)
        for rank in range(size):
            self.send[slot_b, rank] = self.message[rank].astype(BF16)
        if self.resident:
            self.out[b, self.place] = self.send[slot_b, self.rank(self.place)]
        else:
            self.keep(b).start()

        @pl.loop(1, size)
        def _(step):
            place = lax.rem(self.place + step, size)
            self.copy(slot_b, self.rank(place), b, self.place, place).start()

    def drain(self):
        for b in range(max(0, self.batch - SLOTS), self.batch):
            self.every(b).wait_send()
            if not self.resident:
                self.keep(b).wait()
        if not self.resident:
            @pl.loop(0, self.batch)
            def _(b):
                self.every(b).wait_recv()

    def arrive(self, b):
        self.every(b).wait_recv()


def clear_after(coef, degrees_rows):
    slots, parts, rows, lanes = coef.shape
    for slot in range(slots):
        for part in range(parts):
            coef[slot, part, pl.ds(degrees_rows, rows - degrees_rows), :] = jnp.zeros((rows - degrees_rows, lanes), F32)


def greet(me, group):
    barrier = pltpu.get_barrier_semaphore()

    @pl.loop(1, group)
    def _(step):
        pl.semaphore_signal(barrier, inc=1, device_id={'lat': lax.rem(me + step, group)}, device_id_type=MESH)


def meet(group):
    pl.semaphore_wait(pltpu.get_barrier_semaphore(), group - 1)


def load_legendre(me, group, table_hbm, stage, sem):
    m_local = stage.shape[0]
    for slot in range(m_local):
        pltpu.make_async_copy(table_hbm.at[slot * group + me], stage.at[slot], sem).start()
    return pltpu.make_async_copy(table_hbm.at[pl.ds(0, m_local)], stage, sem)


def expand_rows(stage, expanded, rows_local):
    m_local, degrees, lats = stage.shape
    row = lax.broadcasted_iota(jnp.int32, (lats, 2 * lats), 0)
    col = lax.broadcasted_iota(jnp.int32, (lats, 2 * lats), 1)
    source = col // (2 * rows_local)
    inner = col % (2 * rows_local)
    for part in range(2):
        pick = (row == source * rows_local + inner - part * rows_local) & (inner // rows_local == part)
        pick = pick.astype(F32).astype(BF16)
        for slot in range(m_local):
            expanded[slot, pl.ds(part * degrees, degrees), :] = dot(stage[slot].astype(BF16), pick, NN).astype(BF16)


def load_far(swap, table_hbm, stage, sem):
    late = stage.shape[0]
    for n in range(late):
        pltpu.make_async_copy(table_hbm.at[(swap.direct + n) * swap.group + swap.twin], stage.at[n], sem).start()
    return pltpu.make_async_copy(table_hbm.at[pl.ds(0, late)], stage, sem)


def flip_rows(stage, flipped):
    for slot in range(stage.shape[0]):
        flipped[slot] = stage[slot].T.astype(BF16)


def analyse(values_at, table, turn, rows_local):
    modes = table.shape[1]
    for t in range(0, rows_local, 2):
        pair = jnp.concatenate([values_at(t), values_at(t + 1)], axis=0)
        high, low = split_halves(pair)
        out = dot(table[0], high, NT) + dot(table[0], low, NT) + dot(table[1], high, NT)
        channels = out.shape[1] // 2
        turn[pl.ds(t, modes, stride=rows_local), :] = out[:, :channels]
        turn[pl.ds(t + 1, modes, stride=rows_local), :] = out[:, channels:]


def pack_blocks(turn, send, slot):
    group, rows, lanes = send.shape[1:]
    for d in range(group):
        send[slot, d] = turn[pl.ds(d * rows, rows), :].astype(BF16)


def unpack_blocks(recv, b, turn):
    group, rows, lanes = recv.shape[1:]
    for d in range(group):
        turn[pl.ds(d * rows, rows), :] = recv[b, d].astype(F32)


def synthesise(turn, t, table, rows_local):
    modes = table.shape[1]
    spec = turn[pl.ds(t, modes, stride=rows_local), :].astype(BF16)
    return dot(spec, table[0], TN) + dot(spec, table[1], TN)


def legendre_forward(recv, b, expanded, out, rows_local):
    m_local = expanded.shape[0]
    degrees = expanded.shape[1] // 2
    group, _, lanes = recv.shape[1:]
    tile = 2 * rows_local
    for slot in range(m_local):
        rows = recv[b, :, pl.ds(slot * tile, tile), :].reshape(group * tile, lanes)
        res = dot(expanded[slot], rows, NN)
        for part in range(2):
            out[part, pl.ds(slot, degrees, stride=m_local), :] = res[part * degrees:(part + 1) * degrees]


def legendre_inverse(coef, flipped, swap, slot_out, rows_local):
    m_local, lats, degrees = flipped.shape
    send = swap.send
    at = 0
    group = lats // rows_local
    tile = 2 * rows_local
    for slot in range(m_local):
        parts = [coef.at[part][pl.ds(slot, degrees, stride=m_local), :].astype(BF16) for part in range(2)]
        if slot >= swap.direct:
            first = slot * group
            for part in range(2):
                swap.bridge_send[slot_out, part, pl.ds(at, degrees - first), :] = parts[part][first:]
            at += degrees - first
        res = dot(flipped[slot], jnp.concatenate(parts, axis=1), NN)
        lanes = res.shape[1] // 2
        blocks = [res[:, part * lanes:(part + 1) * lanes].reshape(group, rows_local, lanes) for part in range(2)]
        send[slot_out, :, pl.ds(slot * tile, tile), :] = jnp.concatenate(blocks, axis=1).astype(BF16)


def gelu_slope(values):
    cumulative = 0.5 * (1.0 + lax.erf(values * math.sqrt(0.5)))
    density = jnp.exp(-0.5 * values * values) * (1.0 / math.sqrt(2.0 * math.pi))
    return cumulative + values * density


def mix_block(w_block):
    half = w_block.shape[0] // 2
    w_real = w_block[pl.ds(0, half, stride=2), :]
    w_imag = w_block[pl.ds(1, half, stride=2), :]
    top = jnp.concatenate([w_real, -w_imag], axis=1)
    bottom = jnp.concatenate([w_imag, w_real], axis=1)
    return jnp.concatenate([top, bottom], axis=0).astype(BF16)


def rows_of_degree(block, inner, m_local):
    batch = block.shape[0]
    lanes = block.shape[-1]
    parts = [block[:, part, pl.ds(inner * m_local, m_local), :].reshape(batch * m_local, lanes) for part in range(2)]
    return jnp.concatenate(parts, axis=1).astype(BF16)


def first_kernel(group, rows_local, field, table, p_fwd, w_mix, coef_out, shared, w_big, field_buf, stage, expanded, turn, send,
                 recv, coef_buf, share_bufs, w_in, w_out, in_sem, out_sem, p_sem, send_sem, recv_sem, share_sems, w_in_sem,
                 w_out_sem):
    me = lax.axis_index('lat')
    batch = field.shape[0]
    channels = field.shape[1] // rows_local

    def fetch(b):
        return Halves(field, b, field_buf, lax.rem(b, 2), in_sem)

    def put(b):
        whole = pl.ds(0, coef_out.shape[2])
        return pltpu.make_async_copy(coef_buf.at[lax.rem(b, 2), :, whole], coef_out.at[b], out_sem.at[lax.rem(b, 2)])

    per = w_in.shape[1]
    blocks = w_mix.shape[0] // per

    def fetch_w(k):
        return pltpu.make_async_copy(w_mix.at[pl.ds(k * per, per)], w_in.at[lax.rem(k, 2)], w_in_sem.at[lax.rem(k, 2)])

    def put_w(k):
        return pltpu.make_async_copy(w_out.at[lax.rem(k, 2)], w_big.at[pl.ds(k * per, per)], w_out_sem.at[lax.rem(k, 2)])

    fetch(0).start()
    loading = load_legendre(me, group, p_fwd, stage, p_sem)
    fetch_w(0).start()
    greet(me, group)
    share = Share(me, group, batch, *share_bufs, shared, share_sems)
    clear_after(coef_buf, coef_out.shape[2])
    swap = Exchange(me, group, batch, send, recv, send_sem, recv_sem)
    lag = 2
    meet(group)

    def body(i, carry):
        @pl.when(i < batch)
        def _():
            @pl.when(i + 1 < batch)
            def _():
                fetch(i + 1).start()

            fetch(i).wait()
            half = lax.rem(i, 2)
            analyse(lambda t: read_row(field_buf, half, t, channels, rows_local), table, turn, rows_local)
            swap.reserve(i)
            pack_blocks(turn, send, lax.rem(i, SLOTS))
            swap.start(i)

        @pl.when(i == 0)
        def _():
            loading.wait()
            expand_rows(stage, expanded, rows_local)

        @pl.when(i < blocks)
        def _():
            fetch_w(i).wait()

            @pl.when(i + 1 < blocks)
            def _():
                fetch_w(i + 1).start()

            @pl.when(i >= 2)
            def _():
                put_w(i - 2).wait()

            half = lax.rem(i, 2)

            @pl.loop(0, per)
            def _(inner):
                w_out[half, inner] = mix_block(w_in.at[half, inner])

            put_w(i).start()

        @pl.when(i >= lag)
        def _():
            b = i - lag
            swap.arrive(b)

            @pl.when(b >= 2)
            def _():
                put(b - 2).wait()

            legendre_forward(recv, b, expanded, coef_buf.at[lax.rem(b, 2)], rows_local)
            put(b).start()
            share.give(b, coef_buf.at[lax.rem(b, 2)])

        return carry

    lax.fori_loop(0, batch + lag, body, 0)
    swap.drain()
    share.drain()
    put(batch - 2).wait()
    put(batch - 1).wait()
    put_w(blocks - 2).wait()
    put_w(blocks - 1).wait()


def mix_loop(w_hbm, in_hbms, bufs, w_buf, w_sem, in_sems, blocks, step, meanwhile):
    depth, per = w_buf.shape[:2]

    def copies(k):
        slot = lax.rem(k, depth)
        out = [pltpu.make_async_copy(w_hbm.at[pl.ds(k * per, per)], w_buf.at[slot], w_sem.at[slot])]
        for src, buf, sem in zip(in_hbms, bufs, in_sems):
            rows = buf.shape[3]
            out.append(pltpu.make_async_copy(src.at[:, :, pl.ds(k * rows, rows), :], buf.at[slot], sem.at[slot]))
        return out

    for k in range(depth - 1):
        for copy in copies(k):
            copy.start()
    meanwhile()

    def body(k, carry):
        @pl.when(k + depth - 1 < blocks)
        def _():
            for copy in copies(k + depth - 1):
                copy.start()

        for copy in copies(k):
            copy.wait()
        step(k, lax.rem(k, depth))
        return carry

    lax.fori_loop(0, blocks, body, 0)


def second_kernel(group, rows_local, coef, shared_coef, w_mix, p_inv, table, grad, mixed_out, sums_out, w_buf, coef_blk, mixed,
                  stage, flipped, expanded, turn, grad_buf, out_buf, bridged, send_b, recv_b, share_bufs, shared_recv, shared_half,
                  shared, sums, w_sem, c_sem, in_sem, out_sem, p_sem, bridged_sems, send_b_sem, recv_b_sem, share_sems, s_sem,
                  stage_far, far_sem):
    me = lax.axis_index('lat')
    batch = grad.shape[0]
    channels = grad.shape[1] // rows_local
    m_local = stage.shape[0]
    per = w_buf.shape[1]
    degrees = stage.shape[1]

    def fetch(b):
        return Halves(grad, b, grad_buf, lax.rem(b, 2), in_sem)

    def put(b):
        whole = pl.ds(0, mixed_out.shape[2])
        return pltpu.make_async_copy(out_buf.at[lax.rem(b, 2), :, whole], mixed_out.at[b], out_sem.at[lax.rem(b, 2)])

    greet(me, group)
    fetch(0).start()
    swap_a = BridgedExchange(me, group, batch, bridged, bridged_sems)
    loading = load_legendre(me, group, p_inv, stage, p_sem)
    loading_far = load_far(swap_a, p_inv, stage_far, far_sem)

    def prepare():
        sums[...] = jnp.zeros_like(sums)
        loading.wait()
        flip_rows(stage, flipped)
        expand_rows(stage, expanded, rows_local)
        loading_far.wait()
        flip_rows(stage_far, swap_a.flipped_far)

    share = Share(me, group, batch, *share_bufs, shared_recv, share_sems, resident=True)
    clear_after(out_buf, mixed_out.shape[2])
    sources, share_rows = shared_recv.shape[1:3]
    def fetch_shared(b):
        return pltpu.make_async_copy(shared_coef.at[b], shared_half.at[lax.rem(b, 3)], s_sem.at[lax.rem(b, 3)])

    def weigh_sample(b):
        fetch_shared(b).wait()
        share.arrive(b)
        for source in range(sources):
            at = pl.ds(source * (shared.shape[1] // sources), share_rows)
            shared[0, at, :] = shared_recv[b, source].astype(F32)
            shared[1, at, :] = shared_half[lax.rem(b, 3), source].astype(F32)
        weigh(shared, sources, sums, m_local)

    def mix(k, slot):
        for inner in range(per):
            rows = rows_of_degree(coef_blk.at[slot], inner, m_local)
            res = dot(rows, w_buf[slot, inner], NT)
            at = pl.ds(pl.multiple_of((k * per + inner) * m_local, m_local), m_local)
            for part in range(2):
                lanes = res.shape[1] // 2
                mixed[:, part, at, :] = res[:, part * lanes:(part + 1) * lanes].reshape(batch, m_local, lanes)

    mix_loop(w_mix, [coef], [coef_blk], w_buf, w_sem, [c_sem], degrees // per, mix, prepare)

    meet(group)
    swap_b = Exchange(me, group, batch, send_b, recv_b, send_b_sem, recv_b_sem)
    lag, lag_b = 2, 2

    def body(i, carry):
        @pl.when(i < batch)
        def _():
            swap_a.reserve(i)
            legendre_inverse(mixed.at[i], flipped, swap_a, lax.rem(i, SLOTS), rows_local)
            swap_a.start(i)

        @pl.when((i >= 1) & (i < batch + 1))
        def _():
            swap_a.relay(i - 1)

        @pl.when((i >= lag) & (i < batch + lag))
        def _():
            b = i - lag
            half = lax.rem(b, 2)

            @pl.when(b + 1 < batch)
            def _():
                fetch(b + 1).start()

            fetch(b).wait()
            swap_a.arrive(b)
            unpack_blocks(swap_a.recv, b, turn)
            for t in range(rows_local):
                slope = gelu_slope(synthesise(turn, t, table, rows_local))
                given = read_row(grad_buf, half, t, channels, rows_local)
                write_row(grad_buf, half, t, channels, rows_local, given * slope)
            analyse(lambda t: read_row(grad_buf, half, t, channels, rows_local), table, turn, rows_local)
            swap_b.reserve(b)
            pack_blocks(turn, send_b, lax.rem(b, SLOTS))
            swap_b.start(b)

        @pl.when(i >= lag + lag_b)
        def _():
            b = i - lag - lag_b

            @pl.when(b >= 2)
            def _():
                weigh_sample(b - 2)

            swap_b.arrive(b)

            @pl.when(b >= 2)
            def _():
                put(b - 2).wait()

            legendre_forward(recv_b, b, expanded, out_buf.at[lax.rem(b, 2)], rows_local)
            put(b).start()
            share.give(b, out_buf.at[lax.rem(b, 2)])
            fetch_shared(b).start()

        return carry

    lax.fori_loop(0, batch + lag + lag_b, body, 0)
    weigh_sample(batch - 2)
    weigh_sample(batch - 1)
    total = pltpu.make_async_copy(sums, sums_out, p_sem)
    total.start()
    swap_a.drain()
    swap_b.drain()
    share.drain()
    total.wait()
    put(batch - 2).wait()
    put(batch - 1).wait()


class WeightSum:
    def __init__(self, me, group, sums, got, out, sems):
        self.me, self.sums, self.got, self.out, self.sems = me, sums, got, out, sems
        self.core, self.y = lax.rem(me, 2), lax.rem(me // 2, 2)
        self.near, self.far = lax.rem(me // 4, 2), me // (group // 2)
        self.rank = self.near + 2 * self.y + 4 * self.core

    def peer(self, phase):
        step = (1, 2, 4, 8)[phase]
        bit = (self.core, self.y, self.near, self.far)[phase]
        return {'lat': self.me + step - 2 * step * bit}

    def remote(self, phase, k, source, target, stage):
        return pltpu.make_async_remote_copy(source, target, self.sems.at[0, stage, k], self.sems.at[1, stage, k],
                                            device_id=self.peer(phase), device_id_type=MESH)

    def halving(self, k):
        return self.remote(3, k, self.sums.at[2 * k + 1 - self.far], self.got.at[k], 4)

    def settle(self, k):
        mine = 2 * k + self.far
        return pltpu.make_async_copy(self.sums.at[mine], self.out.at[mine, self.rank], self.sems.at[0, 5, k])

    def doubling(self, phase, k):
        if phase == 3:
            mine = 2 * k + self.far
            return self.remote(3, k, self.sums.at[mine], self.out.at[mine, self.rank], 3)
        width = (4, 2, 1)[phase]
        first = (4 * self.core, 4 * self.core + 2 * self.y, self.rank)[phase]
        span = self.out.at[pl.ds(2 * k, 2), pl.ds(first, width)]
        return self.remote(phase, k, span, span, phase)

    def reduce_step(self, k):
        self.halving(k).wait()
        mine = 2 * k + self.far
        self.sums[mine] = self.sums[mine] + self.got[k]
        self.settle(k).start()
        self.doubling(3, k).start()

    def gather_step(self, phase, k):
        if phase == 2:
            self.settle(k).wait()
        self.doubling(phase + 1, k).wait()
        if phase >= 0:
            self.doubling(phase, k).start()


def shared_place(part, slot, step, m_local):
    tile = 2 * m_local
    if slot == m_local // 2:
        return m_local * tile + part * m_local + step - m_local
    pair = min(slot, m_local - slot) if slot else 0
    shift = 0 if slot < m_local // 2 else 2 * slot
    return (part * (m_local // 2) + pair) * tile + step - shift


def weigh(shared, sources, sums, m_local):
    stride = shared.shape[1] // sources

    @pl.loop(0, sums.shape[0])
    def _(step):
        sides = []
        for which in range(2):
            slots = []
            for slot in range(m_local):
                used = step >= 2 * slot
                parts = []
                for part in range(2):
                    place = jnp.where(used, shared_place(part, slot, step, m_local), 0)
                    rows = shared[which, pl.ds(place, sources, stride=stride), :]
                    parts.append(jnp.where(used, rows, 0.0))
                slots.append(jnp.concatenate(parts, axis=1))
            sides.append(jnp.concatenate(slots, axis=0).astype(BF16))
        big = dot(sides[0], sides[1], TN)
        half = big.shape[0] // 2
        real, imag = pl.ds(0, half, stride=2), pl.ds(1, half, stride=2)
        sums[step, real, :] = sums[step, real, :] + (big[:half, :half] + big[half:, half:])
        sums[step, imag, :] = sums[step, imag, :] + (big[half:, :half] - big[:half, half:])


def third_kernel(group, rows_local, mixed, part_sums, w_mix, p_fwd, table, grad, field_out, grad_w, w_buf, mixed_blk, sums, got,
                 back, stage, flipped, turn, grad_buf, bridged, w_sem, m_sem, s_sem, gw_sem, in_sem, out_sem, p_sem, bridged_sems,
                 stage_far, far_sem):
    me = lax.axis_index('lat')
    batch = grad.shape[0]
    channels = grad.shape[1] // rows_local
    depth = grad_buf.shape[0]
    per = w_buf.shape[1]
    degrees = w_mix.shape[0]
    m_local = stage.shape[0]

    def fetch(b):
        return Halves(grad, b, grad_buf, lax.rem(b, depth), in_sem)

    def put(b):
        return Halves(field_out, b, grad_buf, lax.rem(b, depth), out_sem, outward=True)

    load_sums = pltpu.make_async_copy(part_sums, sums, s_sem)
    load_sums.start()
    greet(me, group)
    total = WeightSum(me, group, sums, got, grad_w, gw_sem)
    swap = BridgedExchange(me, group, batch, bridged, bridged_sems)
    loading = load_legendre(me, group, p_fwd, stage, p_sem)
    loading_far = load_far(swap, p_fwd, stage_far, far_sem)
    load_sums.wait()
    meet(group)
    chunks = sums.shape[0] // 2
    for k in range(chunks):
        total.halving(k).start()

    def unmix(k, slot):
        for inner in range(per):
            rows = rows_of_degree(mixed_blk.at[slot], inner, m_local)
            res = dot(rows, w_buf[slot, inner], NN)
            at = pl.ds(pl.multiple_of((k * per + inner) * m_local, m_local), m_local)
            half = res.shape[1] // 2
            for part in range(2):
                back[:, part, at, :] = res[:, part * half:(part + 1) * half].reshape(batch, m_local, half)

    def prepare():
        loading.wait()
        flip_rows(stage, flipped)
        loading_far.wait()
        flip_rows(stage_far, swap.flipped_far)

    mix_loop(w_mix, [mixed], [mixed_blk], w_buf, w_sem, [m_sem], degrees // per, unmix, prepare)
    fetch(0).start()
    lag = 2

    def body(i, carry):
        @pl.when(i < batch)
        def _():
            swap.reserve(i)
            legendre_inverse(back.at[i], flipped, swap, lax.rem(i, SLOTS), rows_local)
            swap.start(i)

        @pl.when((i >= 1) & (i < batch + 1))
        def _():
            swap.relay(i - 1)

        steps = [total.reduce_step] + [functools.partial(total.gather_step, p) for p in (2, 1, 0, -1)]
        for late, step in reversed(list(enumerate(steps))):
            k = i - late

            @pl.when((k >= 0) & (k < chunks))
            def _():
                step(k)

        @pl.when((i >= lag) & (i < batch + lag))
        def _():
            b = i - lag
            half = lax.rem(b, depth)

            @pl.when(b >= depth - 1)
            def _():
                put(b - depth + 1).wait()

            @pl.when(b + 1 < batch)
            def _():
                fetch(b + 1).start()

            fetch(b).wait()
            swap.arrive(b)
            unpack_blocks(swap.recv, b, turn)
            for t in range(rows_local):
                added = synthesise(turn, t, table, rows_local)
                given = read_row(grad_buf, half, t, channels, rows_local)
                write_row(grad_buf, half, t, channels, rows_local, given + added)
            put(b).start()

        return carry

    lax.fori_loop(0, max(batch + lag, chunks + 4), body, 0)
    swap.drain()
    for b in range(batch - depth + 1, batch):
        put(b).wait()


def any_specs(n):
    return [pl.BlockSpec(memory_space=pl.ANY)] * n


def params(collective_id=None):
    if collective_id is None:
        return pltpu.CompilerParams(vmem_limit_bytes=VMEM_LIMIT)
    return pltpu.CompilerParams(collective_id=collective_id, has_side_effects=True, vmem_limit_bytes=VMEM_LIMIT)


def solution(mesh):
    group = mesh.shape['lat']
    field_spec = P('member', None, 'lat', None)

    def local_step(field_loc, grad_loc, p_fwd, p_inv, w_mix):
        batch, channels, rows_local, lon_count = field_loc.shape
        degrees, lats = p_fwd.shape[1:]
        m_local = p_fwd.shape[0] // group
        modes = group * m_local * 2
        base, gained = (two_halves(table) for table in dft_tables(group, m_local, lon_count))
        field = field_loc.reshape(batch, channels * rows_local, lon_count)
        grad = grad_loc.reshape(batch, channels * rows_local, lon_count)
        w_rows = jnp.swapaxes(w_mix, 2, 3).reshape(degrees, channels * 2, channels)
        dma, vmem = pltpu.SemaphoreType.DMA, pltpu.VMEM
        block_rows = m_local * 2 * rows_local
        coef_shape = (batch, 2, degrees * m_local, channels)
        send_t = vmem((SLOTS, group, block_rows, channels), BF16)
        recv_t = vmem((batch, group, block_rows, channels), BF16)
        turn_t = vmem((modes * rows_local, channels), F32)
        stage_t = vmem((m_local, degrees, lats), F32)
        expanded_t = vmem((m_local, 2 * degrees, 2 * lats), BF16)
        flipped_t = vmem((m_local, lats, degrees), BF16)
        pair_t = vmem((2, 2, degrees * m_local, channels), F32)
        field_t = vmem((2, lon_count // LANES, channels * rows_local, LANES), F32)
        table_spec = pl.BlockSpec(memory_space=pltpu.VMEM)
        any_spec = pl.BlockSpec(memory_space=pl.ANY)
        per = 8
        late = sum(degrees - slot * group < lats // 2 for slot in range(m_local))
        far_rows = sum(degrees - slot * group for slot in range(m_local - late, m_local))
        late_rows = late * 2 * rows_local
        bridged_t = (send_t, recv_t, vmem((SLOTS, 2, far_rows, channels), BF16), vmem((batch, 2, far_rows, channels), BF16),
                     vmem((SLOTS, group // 2, late_rows, channels), BF16), vmem((late, lats, degrees), BF16))
        bridged_sems = (dma((SLOTS,)), dma((batch,))) * 3

        ranks = group // 2
        share_rows = (m_local + 1) * 2 * ranks
        share_out = jax.ShapeDtypeStruct((batch, ranks, share_rows, channels), BF16)
        share_t = (vmem((SLOTS, ranks, share_rows, channels), BF16), vmem((ranks, share_rows, channels), F32))
        share_sems = (dma((SLOTS,)), dma((batch,)), dma((SLOTS,)))
        padded_t = vmem((2, 2, 2 * degrees * m_local, channels), F32)

        w_wide = 16
        big_shape = (2 * channels, 2 * channels)
        far_stage_t = vmem((late, degrees, lats), F32)
        coef, shared_coef, w_big = pl.pallas_call(
            functools.partial(first_kernel, group, rows_local), name='first',
            out_shape=[jax.ShapeDtypeStruct(coef_shape, F32), share_out, jax.ShapeDtypeStruct((degrees,) + big_shape, BF16)],
            in_specs=[any_spec, table_spec, any_spec, any_spec], out_specs=[any_spec] * 3,
            scratch_shapes=[field_t, stage_t, expanded_t, turn_t, send_t, recv_t, padded_t, share_t,
                            vmem((2, w_wide, 2 * channels, channels), F32), vmem((2, w_wide) + big_shape, BF16),
                            dma((2, 2)), dma((2,)), dma(()), dma((SLOTS,)), dma((batch,)), share_sems, dma((2,)), dma((2,))],
            compiler_params=params(0))(field, base, p_fwd, w_rows)

        blk_t = vmem((DEPTH, batch, 2, per * m_local, channels), F32)
        w_t = vmem((DEPTH, per) + big_shape, BF16)
        steps = degrees // ranks
        sums_shape = (steps, channels * 2, channels)
        mixed, sums = pl.pallas_call(
            functools.partial(second_kernel, group, rows_local), name='second',
            out_shape=[jax.ShapeDtypeStruct(coef_shape, F32), jax.ShapeDtypeStruct(sums_shape, F32)],
            in_specs=[any_spec] * 4 + [table_spec, any_spec], out_specs=[any_spec] * 2,
            scratch_shapes=[w_t, blk_t, vmem(coef_shape, F32), stage_t, flipped_t, expanded_t, turn_t, field_t, padded_t,
                            bridged_t, send_t, recv_t, share_t, vmem(share_out.shape, BF16), vmem((3,) + share_out.shape[1:], BF16),
                            vmem((2, ranks * (share_rows + 8), channels), F32), vmem(sums_shape, F32),
                            dma((DEPTH,)), dma((DEPTH,)), dma((2, 2)), dma((2,)), dma(()),
                            bridged_sems, dma((SLOTS,)), dma((batch,)), share_sems, dma((3,)), far_stage_t, dma(())],
            compiler_params=params(1))(coef, shared_coef, w_big, p_inv, gained, grad)

        w_rect = (channels * 2, channels)
        field_out, gw_total = pl.pallas_call(
            functools.partial(third_kernel, group, rows_local), name='third',
            out_shape=[jax.ShapeDtypeStruct(grad.shape, F32), jax.ShapeDtypeStruct((steps, ranks) + w_rect, F32)],
            in_specs=[any_spec] * 4 + [table_spec, any_spec], out_specs=[any_spec] * 2,
            scratch_shapes=[w_t, blk_t, vmem(sums_shape, F32), vmem((steps // 2,) + w_rect, F32), vmem(coef_shape, F32), stage_t, flipped_t, turn_t,
                            vmem((3, lon_count // LANES, channels * rows_local, LANES), F32), bridged_t,
                            dma((DEPTH,)), dma((DEPTH,)), dma(()), dma((2, 6, steps // 2)), dma((3, 2)), dma((3, 2)), dma(()),
                            bridged_sems, far_stage_t, dma(())],
            compiler_params=params(2))(mixed, sums, w_big, p_fwd, base, grad)

        grad_wmix = jnp.swapaxes(gw_total.reshape(degrees, channels, 2, channels), 2, 3)
        return field_out.reshape(grad_loc.shape), grad_wmix

    return jax.shard_map(local_step, mesh=mesh, in_specs=(field_spec, field_spec, P(), P(), P()),
                         out_specs=(field_spec, P('member', None, None, None)), check_vma=False)
```

```python
import functools
import math

import jax
import jax.numpy as jnp
import numpy as np
from jax import lax
from jax.experimental import pallas as pl
from jax.experimental.pallas import tpu as pltpu
from jax.sharding import PartitionSpec as P

MESH = pl.DeviceIdType.MESH
LANES = 128
SLOTS = 3
DEPTH = 4
BUNCH = 3
VMEM_LIMIT = 60 * 1024 * 1024
F32 = jnp.float32
BF16 = jnp.bfloat16

NN = (((1,), (0,)), ((), ()))
NT = (((1,), (1,)), ((), ()))
TN = (((0,), (0,)), ((), ()))


def dot(lhs, rhs, dims):
    return lax.dot_general(lhs, rhs, dims, preferred_element_type=F32)


def split_halves(values):
    high = values.astype(BF16)
    low = (values - high.astype(F32)).astype(BF16)
    return high, low


def dft_tables(group, m_local, lon_count):
    owner, slot, part = np.meshgrid(np.arange(group), np.arange(m_local), np.arange(2), indexing='ij')
    wave = (slot * group + owner).reshape(-1)
    part = part.reshape(-1)
    phase = 2.0 * np.pi * ((wave[:, None] * np.arange(lon_count)[None, :]) % lon_count) / lon_count
    base = np.where(part[:, None] == 0, np.cos(phase), -np.sin(phase)) / math.sqrt(lon_count)
    gains = np.where(wave == 0, 1.0, 2.0)[:, None]
    return base.astype(np.float32), (base * gains).astype(np.float32)


def two_halves(table):
    high = jnp.asarray(table).astype(BF16)
    low = (jnp.asarray(table) - high.astype(F32)).astype(BF16)
    return jnp.stack([high, low])


class Halves:
    def __init__(self, whole, b, halves, slot, sem, outward=False):
        self.copies = []
        for half in range(halves.shape[1]):
            ends = whole.at[b, :, pl.ds(half * LANES, LANES)], halves.at[slot, half]
            source, target = ends[::-1] if outward else ends
            self.copies.append(pltpu.make_async_copy(source, target, sem.at[slot, half]))

    def start(self):
        for copy in self.copies:
            copy.start()

    def wait(self):
        for copy in self.copies:
            copy.wait()


def read_row(halves, slot, t, channels, rows_local):
    at = pl.ds(t, channels, stride=rows_local)
    return jnp.concatenate([halves[slot, half, at, :] for half in range(halves.shape[1])], axis=1)


def write_row(halves, slot, t, channels, rows_local, values):
    at = pl.ds(t, channels, stride=rows_local)
    for half in range(halves.shape[1]):
        halves[slot, half, at, :] = values[:, half * LANES:(half + 1) * LANES]


class Exchange:
    def __init__(self, me, group, batch, send, recv, send_sem, recv_sem):
        self.me, self.group, self.batch = me, group, batch
        self.send, self.recv, self.send_sem, self.recv_sem = send, recv, send_sem, recv_sem

    def all_copies(self, b):
        slot = lax.rem(b, SLOTS)
        others = pl.ds(0, self.group - 1)
        return pltpu.make_async_remote_copy(
            self.send.at[slot, others], self.recv.at[b, others], self.send_sem.at[slot], self.recv_sem.at[b],
            device_id={'lat': lax.rem(self.me + 1, self.group)}, device_id_type=MESH)

    def reserve(self, b):
        @pl.when(b >= SLOTS)
        def _():
            self.all_copies(b - SLOTS).wait_send()

    def start(self, b):
        slot = lax.rem(b, SLOTS)
        self.recv[b, self.me] = self.send[slot, self.me]

        @pl.loop(1, self.group)
        def _(step):
            target = lax.rem(self.me + step, self.group)
            pltpu.make_async_remote_copy(
                self.send.at[slot, target], self.recv.at[b, self.me], self.send_sem.at[slot], self.recv_sem.at[b],
                device_id={'lat': target}, device_id_type=MESH).start()

    def arrive(self, b):
        self.all_copies(b).wait_recv()

    def drain(self):
        for b in range(max(0, self.batch - SLOTS), self.batch):
            self.all_copies(b).wait_send()


class BridgedExchange:
    def __init__(self, me, group, batch, bufs, sems):
        self.me, self.group, self.batch = me, group, batch
        self.send, self.recv, self.bridge_send, self.bridge_recv, self.relay_send, self.flipped_far = bufs
        self.send_sem, self.recv_sem, self.bridge_send_sem, self.bridge_recv_sem, self.relay_send_sem, self.relay_recv_sem = sems
        self.half_size = group // 2
        self.half = me // self.half_size
        self.place = lax.rem(me, self.half_size)
        self.twin = self.half_size + me - 2 * self.half_size * self.half
        self.rows = self.send.shape[2]
        self.late_rows = self.relay_send.shape[2]
        self.early_rows = self.rows - self.late_rows
        self.tile = self.late_rows // self.flipped_far.shape[0]
        self.direct = self.early_rows // self.tile

    def copy(self, source, target, send_sem, recv_sem, device):
        return pltpu.make_async_remote_copy(source, target, send_sem, recv_sem, device_id={'lat': device},
                                            device_id_type=MESH)

    def all_direct(self, b):
        slot = lax.rem(b, SLOTS)
        count = (self.half_size - 1) * self.rows + self.half_size * self.early_rows
        span = pl.ds(0, count // self.rows)
        return self.copy(self.send.at[slot, span], self.recv.at[b, span], self.send_sem.at[slot], self.recv_sem.at[b], self.twin)

    def all_relayed(self, b):
        slot = lax.rem(b, SLOTS)
        span, part = pl.ds(0, self.half_size - 1), pl.ds(0, self.late_rows)
        return self.copy(self.relay_send.at[slot, span], self.recv.at[b, span, part], self.relay_send_sem.at[slot],
                         self.relay_recv_sem.at[b], self.twin)

    def bridge(self, b):
        slot = lax.rem(b, SLOTS)
        return self.copy(self.bridge_send.at[slot], self.bridge_recv.at[b], self.bridge_send_sem.at[slot],
                         self.bridge_recv_sem.at[b], self.twin)

    def reserve(self, b):
        @pl.when(b >= SLOTS)
        def _():
            self.all_direct(b - SLOTS).wait_send()
            self.bridge(b - SLOTS).wait_send()

    def start(self, b):
        slot = lax.rem(b, SLOTS)
        self.bridge(b).start()
        early = pl.ds(0, self.early_rows)

        @pl.loop(0, self.half_size)
        def _(step):
            target = (1 - self.half) * self.half_size + lax.rem(self.place + step, self.half_size)
            self.copy(self.send.at[slot, target, early], self.recv.at[b, self.me, early], self.send_sem.at[slot],
                      self.recv_sem.at[b], target).start()

        @pl.loop(1, self.half_size)
        def _(step):
            target = self.half * self.half_size + lax.rem(self.place + step, self.half_size)
            self.copy(self.send.at[slot, target], self.recv.at[b, self.me], self.send_sem.at[slot], self.recv_sem.at[b],
                      target).start()

        self.recv[b, self.me] = self.send[slot, self.me]

    def relay(self, b):
        slot = lax.rem(b, SLOTS)

        @pl.when(b >= SLOTS)
        def _():
            self.all_relayed(b - SLOTS).wait_send()

        self.bridge(b).wait_recv()
        lats, degrees = self.flipped_far.shape[1:]
        own = pl.ds(pl.multiple_of(self.half * (lats // 2), lats // 2), lats // 2)
        at = 0
        for late in range(self.flipped_far.shape[0]):
            first = (self.direct + late) * self.group
            count = degrees - first
            parts = []
            for part in range(2):
                rows = self.bridge_recv[b, part, pl.ds(at, count), :]
                parts.append(jnp.concatenate([jnp.zeros((first, rows.shape[1]), BF16), rows], axis=0))
            at += count
            res = dot(self.flipped_far[late, own, :], jnp.concatenate(parts, axis=1), NN)
            lanes = res.shape[1] // 2
            blocks = [res[:, part * lanes:(part + 1) * lanes].reshape(self.half_size, self.tile // 2, lanes) for part in range(2)]
            self.relay_send[slot, :, pl.ds(late * self.tile, self.tile), :] = jnp.concatenate(blocks, axis=1).astype(BF16)
        late_at = pl.ds(self.early_rows, self.late_rows)

        @pl.loop(1, self.half_size)
        def _(step):
            place = lax.rem(self.place + step, self.half_size)
            self.copy(self.relay_send.at[slot, place], self.recv.at[b, self.twin, late_at], self.relay_send_sem.at[slot],
                      self.relay_recv_sem.at[b], self.half * self.half_size + place).start()

        self.recv[b, self.twin, late_at] = self.relay_send[slot, self.place]

    def arrive(self, b):
        self.all_direct(b).wait_recv()
        self.all_relayed(b).wait_recv()

    def drain(self):
        for b in range(max(0, self.batch - SLOTS), self.batch):
            self.all_direct(b).wait_send()
            self.bridge(b).wait_send()
            self.all_relayed(b).wait_send()


class Share:
    def __init__(self, me, group, batch, send, message, out, sems):
        self.batch, self.send, self.message, self.out = batch, send, message, out
        self.send_sem, self.recv_sem, self.local_sem = sems
        self.size = group // 2
        self.base = me // self.size * self.size
        self.place = lax.rem(me, self.size)

    def rank(self, place):
        return place // 4 + 2 * (lax.rem(place, 4) // 2) + 4 * lax.rem(place, 2)

    def copy(self, slot, source, b, target, place):
        return pltpu.make_async_remote_copy(
            self.send.at[slot, source], self.out.at[b, target], self.send_sem.at[slot], self.recv_sem.at[b],
            device_id={'lat': self.base + place}, device_id_type=MESH)

    def every(self, b):
        span = pl.ds(0, self.size - 1)
        return self.copy(lax.rem(b, SLOTS), span, b, span, lax.rem(self.place + 1, self.size))

    def keep(self, b):
        slot = lax.rem(b, SLOTS)
        return pltpu.make_async_copy(self.send.at[slot, self.rank(self.place)], self.out.at[b, self.place],
                                     self.local_sem.at[slot])

    def give(self, b, coef):
        slot_b = lax.rem(b, SLOTS)

        @pl.when(b >= SLOTS)
        def _():
            self.every(b - SLOTS).wait_send()

        size = self.size
        m_local = size
        tile = 2 * size

        def rows(part, slot, rank, first, count):
            return coef[part, pl.ds((first * size + rank) * m_local + slot, count, stride=size * m_local), :]

        for rank in range(size):
            for part in range(2):
                for pair in range(m_local // 2):
                    block = rows(part, pair, rank, 0, tile)
                    if pair:
                        block = block + rows(part, m_local - pair, rank, 2 * (m_local - pair), tile)
                    self.message[rank, pl.ds((part * (m_local // 2) + pair) * tile, tile), :] = block
                self.message[rank, pl.ds(m_local * tile + part * size, size), :] = rows(part, m_local // 2, rank, size, size)
        for rank in range(size):
            self.send[slot_b, rank] = self.message[rank].astype(BF16)
        self.keep(b).start()

        @pl.loop(1, size)
        def _(step):
            place = lax.rem(self.place + step, size)
            self.copy(slot_b, self.rank(place), b, self.place, place).start()

        self.keep(b).wait()

    def drain(self):
        for b in range(max(0, self.batch - SLOTS), self.batch):
            self.every(b).wait_send()

    def arrive(self, b):
        self.every(b).wait_recv()


def clear_after(coef, used):
    for part in range(coef.shape[0]):
        coef[part, pl.ds(used, coef.shape[1] - used), :] = jnp.zeros((coef.shape[1] - used, coef.shape[2]), F32)


def greet(me, group):
    barrier = pltpu.get_barrier_semaphore()

    @pl.loop(1, group)
    def _(step):
        pl.semaphore_signal(barrier, inc=1, device_id={'lat': lax.rem(me + step, group)}, device_id_type=MESH)


def meet(group):
    pl.semaphore_wait(pltpu.get_barrier_semaphore(), group - 1)


class Tables:
    def __init__(self, waves, whole, stage, sem):
        self.waves, self.whole, self.stage, self.sem = waves, whole, stage, sem

    def start(self):
        for n, wave in enumerate(self.waves):
            pltpu.make_async_copy(self.whole.at[wave], self.stage.at[n], self.sem).start()

    def wait(self):
        pltpu.make_async_copy(self.whole.at[pl.ds(0, len(self.waves))], self.stage, self.sem).wait()


def own_tables(me, group, whole, stage, sem):
    return Tables([slot * group + me for slot in range(stage.shape[0])], whole, stage, sem)


def far_tables(swap, whole, stage, sem):
    return Tables([(swap.direct + n) * swap.group + swap.twin for n in range(stage.shape[0])], whole, stage, sem)


def expand_rows(stage, expanded, rows_local):
    m_local, degrees, lats = stage.shape
    row = lax.broadcasted_iota(jnp.int32, (lats, 2 * lats), 0)
    col = lax.broadcasted_iota(jnp.int32, (lats, 2 * lats), 1)
    source = col // (2 * rows_local)
    inner = col % (2 * rows_local)
    for part in range(2):
        pick = (row == source * rows_local + inner - part * rows_local) & (inner // rows_local == part)
        pick = pick.astype(F32).astype(BF16)
        for slot in range(m_local):
            expanded[slot, pl.ds(part * degrees, degrees), :] = dot(stage[slot].astype(BF16), pick, NN).astype(BF16)


def flip_rows(stage, flipped):
    for slot in range(stage.shape[0]):
        flipped[slot] = stage[slot].T.astype(BF16)


def analyse(values_at, table, turn, rows_local):
    modes = table.shape[1]
    for t in range(0, rows_local, 2):
        pair = jnp.concatenate([values_at(t), values_at(t + 1)], axis=0)
        high, low = split_halves(pair)
        out = dot(table[0], high, NT) + dot(table[0], low, NT) + dot(table[1], high, NT)
        channels = out.shape[1] // 2
        turn[pl.ds(t, modes, stride=rows_local), :] = out[:, :channels]
        turn[pl.ds(t + 1, modes, stride=rows_local), :] = out[:, channels:]


def pack_blocks(turn, send, slot):
    group, rows, lanes = send.shape[1:]
    for d in range(group):
        send[slot, d] = turn[pl.ds(d * rows, rows), :].astype(BF16)


def unpack_blocks(recv, b, turn):
    group, rows, lanes = recv.shape[1:]
    for d in range(group):
        turn[pl.ds(d * rows, rows), :] = recv[b, d].astype(F32)


def synthesise(turn, t, table, rows_local):
    modes = table.shape[1]
    spec = turn[pl.ds(t, modes, stride=rows_local), :].astype(BF16)
    return dot(spec, table[0], TN) + dot(spec, table[1], TN)


def legendre_forward(recv, b, expanded, out, rows_local):
    m_local = expanded.shape[0]
    degrees = expanded.shape[1] // 2
    group, _, lanes = recv.shape[1:]
    tile = 2 * rows_local
    for slot in range(m_local):
        rows = recv[b, :, pl.ds(slot * tile, tile), :].reshape(group * tile, lanes)
        res = dot(expanded[slot], rows, NN)
        for part in range(2):
            out[part, pl.ds(slot, degrees, stride=m_local), :] = res[part * degrees:(part + 1) * degrees]


def legendre_inverse(coef, flipped, swap, slot_out, rows_local):
    m_local, lats, degrees = flipped.shape
    send = swap.send
    at = 0
    group = lats // rows_local
    tile = 2 * rows_local
    for slot in range(m_local):
        parts = [coef.at[part][pl.ds(slot, degrees, stride=m_local), :].astype(BF16) for part in range(2)]
        if slot >= swap.direct:
            first = slot * group
            for part in range(2):
                swap.bridge_send[slot_out, part, pl.ds(at, degrees - first), :] = parts[part][first:]
            at += degrees - first
        res = dot(flipped[slot], jnp.concatenate(parts, axis=1), NN)
        lanes = res.shape[1] // 2
        blocks = [res[:, part * lanes:(part + 1) * lanes].reshape(group, rows_local, lanes) for part in range(2)]
        send[slot_out, :, pl.ds(slot * tile, tile), :] = jnp.concatenate(blocks, axis=1).astype(BF16)


def gelu_slope(values):
    cumulative = 0.5 * (1.0 + lax.erf(values * math.sqrt(0.5)))
    density = jnp.exp(-0.5 * values * values) * (1.0 / math.sqrt(2.0 * math.pi))
    return cumulative + values * density


def mix_block(planes):
    real, imag = planes[0], planes[1]
    return jnp.concatenate([jnp.concatenate([real, -imag], axis=1), jnp.concatenate([imag, real], axis=1)], axis=0)


def rows_of_degree(block, inner, m_local):
    batch = block.shape[0]
    lanes = block.shape[-1]
    parts = [block[:, part, pl.ds(inner * m_local, m_local), :].reshape(batch * m_local, lanes) for part in range(2)]
    return jnp.concatenate(parts, axis=1).astype(BF16)


def front_kernel(group, rows_local, field, grad, base, gained, p_fwd, p_inv, w_mix, mixed_out, sums_out, planes_out, coef_shared,
                 mixed_shared, field_buf, grad_buf, turn, stage, stage_far, expanded_fwd, expanded_inv, flipped, send_f, recv_f,
                 padded, coef, mixed, w_in, planes, bridged, send_d, recv_d, message, share_send_a, share_send_d, halves,
                 shared, sums, out_buf, field_sem, grad_sem, p_sem, far_sem, send_f_sem, recv_f_sem, w_sem, planes_sem,
                 bridged_sems, send_d_sem, recv_d_sem, share_a_sems, share_d_sems, half_sem, out_sem, sums_sem):
    me = lax.axis_index('lat')
    batch = field.shape[0]
    channels = field.shape[1] // rows_local
    m_local, degrees = stage.shape[:2]
    used = degrees * m_local
    bunch = coef.shape[0]
    sources, share_rows = coef_shared.shape[1:3]

    def fetch_field(b):
        return Halves(field, b, field_buf, lax.rem(b, 2), field_sem)

    def fetch_grad(b):
        return Halves(grad, b, grad_buf, lax.rem(b, 2), grad_sem)

    def put(b):
        return pltpu.make_async_copy(out_buf.at[lax.rem(b, 2)], mixed_out.at[b], out_sem.at[lax.rem(b, 2)])

    def put_planes():
        return pltpu.make_async_copy(planes, planes_out, planes_sem)

    def fetch_shares(b):
        slot = lax.rem(b, 2)
        return [pltpu.make_async_copy(whole.at[b], halves.at[slot, which], half_sem.at[slot, which])
                for which, whole in enumerate((mixed_shared, coef_shared))]

    greet(me, group)
    fetch_field(0).start()
    fetch_grad(0).start()
    loading = own_tables(me, group, p_fwd, stage, p_sem)
    loading_inv = own_tables(me, group, p_inv, stage, p_sem)
    loading.start()
    swap_f = Exchange(me, group, batch, send_f, recv_f, send_f_sem, recv_f_sem)
    swap_g = BridgedExchange(me, group, batch, bridged, bridged_sems)
    swap_d = Exchange(me, group, batch, send_d, recv_d, send_d_sem, recv_d_sem)
    share_a = Share(me, group, batch, share_send_a, message, coef_shared, share_a_sems)
    share_d = Share(me, group, batch, share_send_d, message, mixed_shared, share_d_sems)
    loading_far = far_tables(swap_g, p_inv, stage_far, far_sem)
    loading_far.start()
    clear_after(padded, used)
    meet(group)

    def build_planes():
        depth, per = w_in.shape[:2]
        blocks = degrees // per
        half = w_in.shape[2] // 2

        def fetch(k):
            return pltpu.make_async_copy(w_mix.at[pl.ds(k * per, per)], w_in.at[lax.rem(k, depth)], w_sem.at[lax.rem(k, depth)])

        for k in range(depth - 1):
            fetch(k).start()

        @pl.loop(0, blocks)
        def _(k):
            @pl.when(k + depth - 1 < blocks)
            def _():
                fetch(k + depth - 1).start()

            fetch(k).wait()
            for inner in range(per):
                rows = w_in.at[lax.rem(k, depth), inner]
                for part in range(2):
                    planes[k * per + inner, part] = rows[pl.ds(part, half, stride=2), :].astype(BF16)

        put_planes().start()

    def mix_bunch():
        @pl.loop(0, degrees // 8)
        def _(k):
            for inner in range(8):
                at = pl.ds(pl.multiple_of((k * 8 + inner) * m_local, m_local), m_local)
                rows = [coef[:, part, at, :].reshape(bunch * m_local, channels) for part in range(2)]
                res = dot(jnp.concatenate(rows, axis=1).astype(BF16), mix_block(planes[k * 8 + inner]), NT)
                for part in range(2):
                    mixed[:, part, at, :] = res[:, part * channels:(part + 1) * channels].reshape(bunch, m_local, channels)

    def weigh_sample(b):
        for copy in fetch_shares(b):
            copy.wait()
        for which in range(2):
            for source in range(sources):
                at = pl.ds(source * (shared.shape[1] // sources), share_rows)
                shared[which, at, :] = halves[lax.rem(b, 2), which, source].astype(F32)
        weigh(shared, sources, sums, m_local)

    def collect(b):
        share_a.arrive(b)
        share_d.arrive(b)
        for copy in fetch_shares(b):
            copy.start()

    lag_a, lag_b, lag_c, lag_d = 2, 4, 6, 8

    def body(i, carry):
        @pl.when(i < batch)
        def _():
            @pl.when(i + 1 < batch)
            def _():
                fetch_field(i + 1).start()

            fetch_field(i).wait()
            half = lax.rem(i, 2)
            analyse(lambda t: read_row(field_buf, half, t, channels, rows_local), base, turn, rows_local)
            swap_f.reserve(i)
            pack_blocks(turn, send_f, lax.rem(i, SLOTS))
            swap_f.start(i)

        @pl.when(i == 0)
        def _():
            loading.wait()
            expand_rows(stage, expanded_fwd, rows_local)
            loading_inv.start()
            loading_far.wait()
            flip_rows(stage_far, swap_g.flipped_far)

        @pl.when(i == 1)
        def _():
            build_planes()
            loading_inv.wait()
            expand_rows(stage, expanded_inv, rows_local)
            flip_rows(stage, flipped)
            sums[...] = jnp.zeros_like(sums)

        @pl.when((i >= lag_a) & (i < batch + lag_a))
        def _():
            b = i - lag_a
            swap_f.arrive(b)
            legendre_forward(recv_f, b, expanded_fwd, padded, rows_local)
            coef[lax.rem(b, bunch)] = padded[:, pl.ds(0, used), :]
            share_a.give(b, padded)

            @pl.when(lax.rem(b, bunch) == bunch - 1)
            def _():
                mix_bunch()

        @pl.when((i >= lag_b) & (i < batch + lag_b))
        def _():
            b = i - lag_b
            swap_g.reserve(b)
            legendre_inverse(mixed.at[lax.rem(b, bunch)], flipped, swap_g, lax.rem(b, SLOTS), rows_local)
            swap_g.start(b)

        @pl.when((i >= lag_b + 1) & (i < batch + lag_b + 1))
        def _():
            swap_g.relay(i - lag_b - 1)

        @pl.when((i >= lag_c) & (i < batch + lag_c))
        def _():
            b = i - lag_c
            half = lax.rem(b, 2)

            @pl.when(b + 1 < batch)
            def _():
                fetch_grad(b + 1).start()

            fetch_grad(b).wait()
            swap_g.arrive(b)
            unpack_blocks(swap_g.recv, b, turn)
            for t in range(rows_local):
                slope = gelu_slope(synthesise(turn, t, gained, rows_local))
                given = read_row(grad_buf, half, t, channels, rows_local)
                write_row(grad_buf, half, t, channels, rows_local, given * slope)
            analyse(lambda t: read_row(grad_buf, half, t, channels, rows_local), gained, turn, rows_local)
            swap_d.reserve(b)
            pack_blocks(turn, send_d, lax.rem(b, SLOTS))
            swap_d.start(b)

        @pl.when(i >= lag_d)
        def _():
            b = i - lag_d

            @pl.when(b >= 2)
            def _():
                weigh_sample(b - 2)

            @pl.when(b >= 1)
            def _():
                collect(b - 1)

            swap_d.arrive(b)

            @pl.when(b >= 2)
            def _():
                put(b - 2).wait()

            legendre_forward(recv_d, b, expanded_inv, padded, rows_local)
            out_buf[lax.rem(b, 2)] = padded[:, pl.ds(0, used), :]
            put(b).start()
            share_d.give(b, padded)

        return carry

    lax.fori_loop(0, batch + lag_d, body, 0)
    weigh_sample(batch - 2)
    collect(batch - 1)
    weigh_sample(batch - 1)
    total = pltpu.make_async_copy(sums, sums_out, sums_sem)
    total.start()
    for swap in (swap_f, swap_g, swap_d, share_a, share_d):
        swap.drain()
    put_planes().wait()
    put(batch - 2).wait()
    put(batch - 1).wait()
    total.wait()


def mix_loop(w_hbm, in_hbms, bufs, w_buf, w_sem, in_sems, blocks, step, meanwhile):
    depth, per = w_buf.shape[:2]

    def copies(k):
        slot = lax.rem(k, depth)
        out = [pltpu.make_async_copy(w_hbm.at[pl.ds(k * per, per)], w_buf.at[slot], w_sem.at[slot])]
        for src, buf, sem in zip(in_hbms, bufs, in_sems):
            rows = buf.shape[3]
            out.append(pltpu.make_async_copy(src.at[:, :, pl.ds(k * rows, rows), :], buf.at[slot], sem.at[slot]))
        return out

    for k in range(depth - 1):
        for copy in copies(k):
            copy.start()
    meanwhile()

    def body(k, carry):
        @pl.when(k + depth - 1 < blocks)
        def _():
            for copy in copies(k + depth - 1):
                copy.start()

        for copy in copies(k):
            copy.wait()
        step(k, lax.rem(k, depth))
        return carry

    lax.fori_loop(0, blocks, body, 0)


class WeightSum:
    def __init__(self, me, group, sums, got, out, sems):
        self.me, self.sums, self.got, self.out, self.sems = me, sums, got, out, sems
        self.core, self.y = lax.rem(me, 2), lax.rem(me // 2, 2)
        self.near, self.far = lax.rem(me // 4, 2), me // (group // 2)
        self.rank = self.near + 2 * self.y + 4 * self.core

    def peer(self, phase):
        step = (1, 2, 4, 8)[phase]
        bit = (self.core, self.y, self.near, self.far)[phase]
        return {'lat': self.me + step - 2 * step * bit}

    def remote(self, phase, k, source, target, stage):
        return pltpu.make_async_remote_copy(source, target, self.sems.at[0, stage, k], self.sems.at[1, stage, k],
                                            device_id=self.peer(phase), device_id_type=MESH)

    def halving(self, k):
        return self.remote(3, k, self.sums.at[2 * k + 1 - self.far], self.got.at[k], 4)

    def settle(self, k):
        mine = 2 * k + self.far
        return pltpu.make_async_copy(self.sums.at[mine], self.out.at[mine, self.rank], self.sems.at[0, 5, k])

    def doubling(self, phase, k):
        if phase == 3:
            mine = 2 * k + self.far
            return self.remote(3, k, self.sums.at[mine], self.out.at[mine, self.rank], 3)
        width = (4, 2, 1)[phase]
        first = (4 * self.core, 4 * self.core + 2 * self.y, self.rank)[phase]
        span = self.out.at[pl.ds(2 * k, 2), pl.ds(first, width)]
        return self.remote(phase, k, span, span, phase)

    def reduce_step(self, k):
        self.halving(k).wait()
        mine = 2 * k + self.far
        self.sums[mine] = self.sums[mine] + self.got[k]
        self.settle(k).start()
        self.doubling(3, k).start()

    def gather_step(self, phase, k):
        if phase == 2:
            self.settle(k).wait()
        self.doubling(phase + 1, k).wait()
        if phase >= 0:
            self.doubling(phase, k).start()


def shared_place(part, slot, step, m_local):
    tile = 2 * m_local
    if slot == m_local // 2:
        return m_local * tile + part * m_local + step - m_local
    pair = min(slot, m_local - slot) if slot else 0
    shift = 0 if slot < m_local // 2 else 2 * slot
    return (part * (m_local // 2) + pair) * tile + step - shift


def weigh(shared, sources, sums, m_local):
    stride = shared.shape[1] // sources

    @pl.loop(0, sums.shape[0])
    def _(step):
        sides = []
        for which in range(2):
            slots = []
            for slot in range(m_local):
                used = step >= 2 * slot
                parts = []
                for part in range(2):
                    place = jnp.where(used, shared_place(part, slot, step, m_local), 0)
                    rows = shared[which, pl.ds(place, sources, stride=stride), :]
                    parts.append(jnp.where(used, rows, 0.0))
                slots.append(jnp.concatenate(parts, axis=1))
            sides.append(jnp.concatenate(slots, axis=0).astype(BF16))
        big = dot(sides[0], sides[1], TN)
        half = big.shape[0] // 2
        real, imag = pl.ds(0, half, stride=2), pl.ds(1, half, stride=2)
        sums[step, real, :] = sums[step, real, :] + (big[:half, :half] + big[half:, half:])
        sums[step, imag, :] = sums[step, imag, :] + (big[half:, :half] - big[:half, half:])


def third_kernel(group, rows_local, mixed, part_sums, w_mix, p_fwd, table, grad, field_out, grad_w, w_buf, mixed_blk, sums, got,
                 back, stage, flipped, turn, grad_buf, bridged, w_sem, m_sem, s_sem, gw_sem, in_sem, out_sem, p_sem, bridged_sems,
                 stage_far, far_sem):
    me = lax.axis_index('lat')
    batch = grad.shape[0]
    channels = grad.shape[1] // rows_local
    depth = grad_buf.shape[0]
    per = w_buf.shape[1]
    degrees = w_mix.shape[0]
    m_local = stage.shape[0]

    def fetch(b):
        return Halves(grad, b, grad_buf, lax.rem(b, depth), in_sem)

    def put(b):
        return Halves(field_out, b, grad_buf, lax.rem(b, depth), out_sem, outward=True)

    load_sums = pltpu.make_async_copy(part_sums, sums, s_sem)
    load_sums.start()
    greet(me, group)
    total = WeightSum(me, group, sums, got, grad_w, gw_sem)
    swap = BridgedExchange(me, group, batch, bridged, bridged_sems)
    loading = own_tables(me, group, p_fwd, stage, p_sem)
    loading_far = far_tables(swap, p_fwd, stage_far, far_sem)
    loading.start()
    loading_far.start()
    load_sums.wait()
    meet(group)
    chunks = sums.shape[0] // 2
    for k in range(2):
        total.halving(k).start()

    def unmix(k, slot):
        for inner in range(per):
            rows = rows_of_degree(mixed_blk.at[slot], inner, m_local)
            res = dot(rows, mix_block(w_buf[slot, inner]), NN)
            at = pl.ds(pl.multiple_of((k * per + inner) * m_local, m_local), m_local)
            half = res.shape[1] // 2
            for part in range(2):
                back[:, part, at, :] = res[:, part * half:(part + 1) * half].reshape(batch, m_local, half)

    def prepare():
        loading.wait()
        flip_rows(stage, flipped)
        loading_far.wait()
        flip_rows(stage_far, swap.flipped_far)

    mix_loop(w_mix, [mixed], [mixed_blk], w_buf, w_sem, [m_sem], degrees // per, unmix, prepare)
    fetch(0).start()
    lag = 2

    def body(i, carry):
        @pl.when(i < batch)
        def _():
            swap.reserve(i)
            legendre_inverse(back.at[i], flipped, swap, lax.rem(i, SLOTS), rows_local)
            swap.start(i)

        @pl.when((i >= 1) & (i < batch + 1))
        def _():
            swap.relay(i - 1)

        steps = [total.reduce_step] + [functools.partial(total.gather_step, p) for p in (2, 1, 0, -1)]
        @pl.when((i >= lag) & (i < batch + lag))
        def _():
            b = i - lag
            half = lax.rem(b, depth)

            @pl.when(b >= depth - 1)
            def _():
                put(b - depth + 1).wait()

            @pl.when(b + 1 < batch)
            def _():
                fetch(b + 1).start()

            fetch(b).wait()
            swap.arrive(b)
            unpack_blocks(swap.recv, b, turn)
            for t in range(rows_local):
                added = synthesise(turn, t, table, rows_local)
                given = read_row(grad_buf, half, t, channels, rows_local)
                write_row(grad_buf, half, t, channels, rows_local, given + added)
            put(b).start()

        @pl.when(i + 2 < chunks)
        def _():
            total.halving(i + 2).start()

        for late, step in reversed(list(enumerate(steps))):
            k = i - late

            @pl.when((k >= 0) & (k < chunks))
            def _():
                step(k)

        return carry

    lax.fori_loop(0, max(batch + lag, chunks + 4), body, 0)
    swap.drain()
    for b in range(batch - depth + 1, batch):
        put(b).wait()


def any_specs(n):
    return [pl.BlockSpec(memory_space=pl.ANY)] * n


def params(collective_id=None):
    if collective_id is None:
        return pltpu.CompilerParams(vmem_limit_bytes=VMEM_LIMIT)
    return pltpu.CompilerParams(collective_id=collective_id, has_side_effects=True, vmem_limit_bytes=VMEM_LIMIT)


def solution(mesh):
    group = mesh.shape['lat']
    field_spec = P('member', None, 'lat', None)

    def local_step(field_loc, grad_loc, p_fwd, p_inv, w_mix):
        batch, channels, rows_local, lon_count = field_loc.shape
        degrees, lats = p_fwd.shape[1:]
        m_local = p_fwd.shape[0] // group
        modes = group * m_local * 2
        base, gained = (two_halves(table) for table in dft_tables(group, m_local, lon_count))
        field = field_loc.reshape(batch, channels * rows_local, lon_count)
        grad = grad_loc.reshape(batch, channels * rows_local, lon_count)
        w_rows = jnp.swapaxes(w_mix, 2, 3).reshape(degrees, channels * 2, channels)
        dma, vmem = pltpu.SemaphoreType.DMA, pltpu.VMEM
        block_rows = m_local * 2 * rows_local
        coef_shape = (batch, 2, degrees * m_local, channels)
        send_t = vmem((SLOTS, group, block_rows, channels), BF16)
        recv_t = vmem((batch, group, block_rows, channels), BF16)
        turn_t = vmem((modes * rows_local, channels), F32)
        stage_t = vmem((m_local, degrees, lats), F32)
        expanded_t = vmem((m_local, 2 * degrees, 2 * lats), BF16)
        flipped_t = vmem((m_local, lats, degrees), BF16)
        field_t = vmem((2, lon_count // LANES, channels * rows_local, LANES), F32)
        table_spec = pl.BlockSpec(memory_space=pltpu.VMEM)
        any_spec = pl.BlockSpec(memory_space=pl.ANY)
        per = 8
        late = sum(degrees - slot * group < lats // 2 for slot in range(m_local))
        far_rows = sum(degrees - slot * group for slot in range(m_local - late, m_local))
        late_rows = late * 2 * rows_local
        bridged_t = (send_t, recv_t, vmem((SLOTS, 2, far_rows, channels), BF16), vmem((batch, 2, far_rows, channels), BF16),
                     vmem((SLOTS, group // 2, late_rows, channels), BF16), vmem((late, lats, degrees), BF16))
        bridged_sems = (dma((SLOTS,)), dma((batch,))) * 3

        ranks = group // 2
        share_rows = (m_local + 1) * 2 * ranks
        share_out = jax.ShapeDtypeStruct((batch, ranks, share_rows, channels), BF16)
        share_sems = (dma((SLOTS,)), dma((batch,)), dma((SLOTS,)))

        blk_t = vmem((DEPTH, batch, 2, per * m_local, channels), F32)
        w_t = vmem((DEPTH, per, 2, channels, channels), BF16)
        far_stage_t = vmem((late, degrees, lats), F32)
        steps = degrees // ranks
        sums_shape = (steps, channels * 2, channels)
        planes_shape = (degrees, 2, channels, channels)
        single_t = vmem((BUNCH,) + coef_shape[1:], F32)
        share_send_t = vmem((SLOTS, ranks, share_rows, channels), BF16)
        swap_sems = (dma((SLOTS,)), dma((batch,)))
        mixed, sums, planes, _, _ = pl.pallas_call(
            functools.partial(front_kernel, group, rows_local), name='front',
            out_shape=[jax.ShapeDtypeStruct(coef_shape, F32), jax.ShapeDtypeStruct(sums_shape, F32),
                       jax.ShapeDtypeStruct(planes_shape, BF16), share_out, share_out],
            in_specs=[any_spec, any_spec, table_spec, table_spec, any_spec, any_spec, any_spec], out_specs=[any_spec] * 5,
            scratch_shapes=[field_t, field_t, turn_t, stage_t, far_stage_t, expanded_t, expanded_t, flipped_t, send_t, recv_t,
                            vmem((2, 2 * degrees * m_local, channels), F32), single_t, single_t,
                            vmem((4, 4, channels * 2, channels), F32), vmem(planes_shape, BF16), bridged_t, send_t, recv_t,
                            vmem((ranks, share_rows, channels), F32), share_send_t, share_send_t,
                            vmem((2, 2) + share_out.shape[1:], BF16), vmem((2, ranks * (share_rows + 8), channels), F32),
                            vmem(sums_shape, F32), vmem((2,) + coef_shape[1:], F32),
                            dma((2, 2)), dma((2, 2)), dma(()), dma(()), *swap_sems, dma((4,)), dma(()), bridged_sems, *swap_sems,
                            share_sems, share_sems, dma((2, 2)), dma((2,)), dma(())],
            compiler_params=params(0))(field, grad, base, gained, p_fwd, p_inv, w_rows)

        w_rect = (channels * 2, channels)
        field_out, gw_total = pl.pallas_call(
            functools.partial(third_kernel, group, rows_local), name='third',
            out_shape=[jax.ShapeDtypeStruct(grad.shape, F32), jax.ShapeDtypeStruct((steps, ranks) + w_rect, F32)],
            in_specs=[any_spec] * 4 + [table_spec, any_spec], out_specs=[any_spec] * 2,
            scratch_shapes=[w_t, blk_t, vmem(sums_shape, F32), vmem((steps // 2,) + w_rect, F32), vmem(coef_shape, F32), stage_t, flipped_t, turn_t,
                            vmem((3, lon_count // LANES, channels * rows_local, LANES), F32), bridged_t,
                            dma((DEPTH,)), dma((DEPTH,)), dma(()), dma((2, 6, steps // 2)), dma((3, 2)), dma((3, 2)), dma(()),
                            bridged_sems, far_stage_t, dma(())],
            compiler_params=params(2))(mixed, sums, planes, p_fwd, base, grad)

        grad_wmix = jnp.swapaxes(gw_total.reshape(degrees, channels, 2, channels), 2, 3)
        return field_out.reshape(grad_loc.shape), grad_wmix

    return jax.shard_map(local_step, mesh=mesh, in_specs=(field_spec, field_spec, P(), P(), P()),
                         out_specs=(field_spec, P('member', None, None, None)), check_vma=False)
```

```python
import functools
import math

import jax
import jax.numpy as jnp
import numpy as np
from jax import lax
from jax.experimental import pallas as pl
from jax.experimental.pallas import tpu as pltpu
from jax.sharding import PartitionSpec as P

MESH = pl.DeviceIdType.MESH
LANES = 128
SLOTS = 3
DEPTH = 4
BUNCH = 3
PIECES = 2
RING = 6
VMEM_LIMIT = 60 * 1024 * 1024
F32 = jnp.float32
BF16 = jnp.bfloat16

NN = (((1,), (0,)), ((), ()))
NT = (((1,), (1,)), ((), ()))
TN = (((0,), (0,)), ((), ()))


def dot(lhs, rhs, dims):
    return lax.dot_general(lhs, rhs, dims, preferred_element_type=F32)


def split_halves(values):
    high = values.astype(BF16)
    low = (values - high.astype(F32)).astype(BF16)
    return high, low


def dft_tables(group, m_local, lon_count):
    owner, slot, part = np.meshgrid(np.arange(group), np.arange(m_local), np.arange(2), indexing='ij')
    wave = (slot * group + owner).reshape(-1)
    part = part.reshape(-1)
    phase = 2.0 * np.pi * ((wave[:, None] * np.arange(lon_count)[None, :]) % lon_count) / lon_count
    base = np.where(part[:, None] == 0, np.cos(phase), -np.sin(phase)) / math.sqrt(lon_count)
    gains = np.where(wave == 0, 1.0, 2.0)[:, None]
    return base.astype(np.float32), (base * gains).astype(np.float32)


def two_halves(table):
    high = jnp.asarray(table).astype(BF16)
    low = (jnp.asarray(table) - high.astype(F32)).astype(BF16)
    return jnp.stack([high, low])


class Halves:
    def __init__(self, whole, b, halves, slot, sem, outward=False):
        self.copies = []
        for half in range(halves.shape[1]):
            ends = whole.at[b, :, pl.ds(half * LANES, LANES)], halves.at[slot, half]
            source, target = ends[::-1] if outward else ends
            self.copies.append(pltpu.make_async_copy(source, target, sem.at[slot, half]))

    def start(self):
        for copy in self.copies:
            copy.start()

    def wait(self):
        for copy in self.copies:
            copy.wait()


def read_row(halves, slot, t, channels, rows_local):
    at = pl.ds(t, channels, stride=rows_local)
    return jnp.concatenate([halves[slot, half, at, :] for half in range(halves.shape[1])], axis=1)


def write_row(halves, slot, t, channels, rows_local, values):
    at = pl.ds(t, channels, stride=rows_local)
    for half in range(halves.shape[1]):
        halves[slot, half, at, :] = values[:, half * LANES:(half + 1) * LANES]


class Exchange:
    def __init__(self, me, group, batch, send, recv, send_sem, recv_sem):
        self.me, self.group, self.batch = me, group, batch
        self.send, self.recv, self.send_sem, self.recv_sem = send, recv, send_sem, recv_sem

    def all_copies(self, b):
        slot = lax.rem(b, SLOTS)
        others = pl.ds(0, self.group - 1)
        return pltpu.make_async_remote_copy(
            self.send.at[slot, others], self.recv.at[b, others], self.send_sem.at[slot], self.recv_sem.at[b],
            device_id={'lat': lax.rem(self.me + 1, self.group)}, device_id_type=MESH)

    def reserve(self, b):
        @pl.when(b >= SLOTS)
        def _():
            self.all_copies(b - SLOTS).wait_send()

    def start(self, b):
        slot = lax.rem(b, SLOTS)
        self.recv[b, self.me] = self.send[slot, self.me]

        @pl.loop(1, self.group)
        def _(step):
            target = jnp.bitwise_xor(self.me, self.group - step)
            pltpu.make_async_remote_copy(
                self.send.at[slot, target], self.recv.at[b, self.me], self.send_sem.at[slot], self.recv_sem.at[b],
                device_id={'lat': target}, device_id_type=MESH).start()

    def arrive(self, b):
        self.all_copies(b).wait_recv()

    def drain(self):
        for b in range(max(0, self.batch - SLOTS), self.batch):
            self.all_copies(b).wait_send()


class BridgedExchange:
    def __init__(self, me, group, batch, bufs, sems):
        self.me, self.group, self.batch = me, group, batch
        self.send, self.recv, self.bridge_send, self.bridge_recv, self.relay_send, self.flipped_far = bufs
        self.send_sem, self.recv_sem, self.bridge_send_sem, self.bridge_recv_sem, self.relay_send_sem, self.relay_recv_sem = sems
        self.half_size = group // 2
        self.half = me // self.half_size
        self.place = lax.rem(me, self.half_size)
        self.twin = self.half_size + me - 2 * self.half_size * self.half
        self.rows = self.send.shape[2]
        self.late_rows = self.relay_send.shape[2]
        self.early_rows = self.rows - self.late_rows
        self.tile = self.late_rows // self.flipped_far.shape[0]
        self.direct = self.early_rows // self.tile

    def copy(self, source, target, send_sem, recv_sem, device):
        return pltpu.make_async_remote_copy(source, target, send_sem, recv_sem, device_id={'lat': device},
                                            device_id_type=MESH)

    def all_direct(self, b):
        slot = lax.rem(b, SLOTS)
        count = (self.half_size - 1) * self.rows + self.half_size * self.early_rows
        span = pl.ds(0, count // self.rows)
        return self.copy(self.send.at[slot, span], self.recv.at[b, span], self.send_sem.at[slot], self.recv_sem.at[b], self.twin)

    def all_relayed(self, b):
        slot = lax.rem(b, SLOTS)
        span, part = pl.ds(0, self.half_size - 1), pl.ds(0, self.late_rows)
        return self.copy(self.relay_send.at[slot, span], self.recv.at[b, span, part], self.relay_send_sem.at[slot],
                         self.relay_recv_sem.at[b], self.twin)

    def bridge(self, b):
        slot = lax.rem(b, SLOTS)
        return self.copy(self.bridge_send.at[slot], self.bridge_recv.at[b], self.bridge_send_sem.at[slot],
                         self.bridge_recv_sem.at[b], self.twin)

    def reserve(self, b):
        @pl.when(b >= SLOTS)
        def _():
            self.all_direct(b - SLOTS).wait_send()
            self.bridge(b - SLOTS).wait_send()

    def start(self, b):
        slot = lax.rem(b, SLOTS)
        self.bridge(b).start()
        early = pl.ds(0, self.early_rows)

        @pl.loop(0, self.half_size)
        def _(step):
            target = jnp.bitwise_xor(self.me, 2 * self.half_size - 1 - step)
            self.copy(self.send.at[slot, target, early], self.recv.at[b, self.me, early], self.send_sem.at[slot],
                      self.recv_sem.at[b], target).start()

        @pl.loop(1, self.half_size)
        def _(step):
            target = jnp.bitwise_xor(self.me, self.half_size - step)
            self.copy(self.send.at[slot, target], self.recv.at[b, self.me], self.send_sem.at[slot], self.recv_sem.at[b],
                      target).start()

        self.recv[b, self.me] = self.send[slot, self.me]

    def relay(self, b):
        slot = lax.rem(b, SLOTS)

        @pl.when(b >= SLOTS)
        def _():
            self.all_relayed(b - SLOTS).wait_send()

        self.bridge(b).wait_recv()
        lats, degrees = self.flipped_far.shape[1:]
        own = pl.ds(pl.multiple_of(self.half * (lats // 2), lats // 2), lats // 2)
        at = 0
        for late in range(self.flipped_far.shape[0]):
            first = (self.direct + late) * self.group
            count = degrees - first
            parts = []
            for part in range(2):
                rows = self.bridge_recv[b, part, pl.ds(at, count), :]
                parts.append(jnp.concatenate([jnp.zeros((first, rows.shape[1]), BF16), rows], axis=0))
            at += count
            res = dot(self.flipped_far[late, own, :], jnp.concatenate(parts, axis=1), NN)
            lanes = res.shape[1] // 2
            blocks = [res[:, part * lanes:(part + 1) * lanes].reshape(self.half_size, self.tile // 2, lanes) for part in range(2)]
            self.relay_send[slot, :, pl.ds(late * self.tile, self.tile), :] = jnp.concatenate(blocks, axis=1).astype(BF16)
        late_at = pl.ds(self.early_rows, self.late_rows)

        @pl.loop(1, self.half_size)
        def _(step):
            place = jnp.bitwise_xor(self.place, self.half_size - step)
            self.copy(self.relay_send.at[slot, place], self.recv.at[b, self.twin, late_at], self.relay_send_sem.at[slot],
                      self.relay_recv_sem.at[b], self.half * self.half_size + place).start()

        self.recv[b, self.twin, late_at] = self.relay_send[slot, self.place]

    def arrive(self, b):
        self.all_direct(b).wait_recv()
        self.all_relayed(b).wait_recv()

    def drain(self):
        for b in range(max(0, self.batch - SLOTS), self.batch):
            self.all_direct(b).wait_send()
            self.bridge(b).wait_send()
            self.all_relayed(b).wait_send()


class Share:
    def __init__(self, me, group, batch, send, message, out, sems):
        self.batch, self.send, self.message, self.out = batch, send, message, out
        self.send_sem, self.recv_sem, self.local_sem = sems
        self.size = group // 2
        self.base = me // self.size * self.size
        self.place = lax.rem(me, self.size)

    def rank(self, place):
        return place // 4 + 2 * (lax.rem(place, 4) // 2) + 4 * lax.rem(place, 2)

    def copy(self, slot, source, b, target, place):
        return pltpu.make_async_remote_copy(
            self.send.at[slot, source], self.out.at[b, target], self.send_sem.at[slot], self.recv_sem.at[b],
            device_id={'lat': self.base + place}, device_id_type=MESH)

    def every(self, b):
        span = pl.ds(0, self.size - 1)
        return self.copy(lax.rem(b, SLOTS), span, b, span, lax.rem(self.place + 1, self.size))

    def keep(self, b):
        slot = lax.rem(b, SLOTS)
        return pltpu.make_async_copy(self.send.at[slot, self.rank(self.place)], self.out.at[b, self.place],
                                     self.local_sem.at[slot])

    def give(self, b, coef):
        slot_b = lax.rem(b, SLOTS)

        @pl.when(b >= SLOTS)
        def _():
            self.every(b - SLOTS).wait_send()

        size = self.size
        m_local = size
        tile = 2 * size

        def rows(part, slot, rank, first, count):
            return coef[part, pl.ds((first * size + rank) * m_local + slot, count, stride=size * m_local), :]

        for rank in range(size):
            for part in range(2):
                for pair in range(m_local // 2):
                    block = rows(part, pair, rank, 0, tile)
                    if pair:
                        block = block + rows(part, m_local - pair, rank, 2 * (m_local - pair), tile)
                    self.message[rank, pl.ds((part * (m_local // 2) + pair) * tile, tile), :] = block
                self.message[rank, pl.ds(m_local * tile + part * size, size), :] = rows(part, m_local // 2, rank, size, size)
        for rank in range(size):
            self.send[slot_b, rank] = self.message[rank].astype(BF16)
        self.keep(b).start()

        @pl.loop(1, size)
        def _(step):
            place = jnp.bitwise_xor(self.place, size - step)
            self.copy(slot_b, self.rank(place), b, self.place, place).start()

        self.keep(b).wait()

    def drain(self):
        for b in range(max(0, self.batch - SLOTS), self.batch):
            self.every(b).wait_send()

    def arrive(self, b):
        self.every(b).wait_recv()


def clear_after(coef, used):
    for part in range(coef.shape[0]):
        coef[part, pl.ds(used, coef.shape[1] - used), :] = jnp.zeros((coef.shape[1] - used, coef.shape[2]), F32)


def greet(me, group):
    barrier = pltpu.get_barrier_semaphore()

    @pl.loop(1, group)
    def _(step):
        pl.semaphore_signal(barrier, inc=1, device_id={'lat': lax.rem(me + step, group)}, device_id_type=MESH)


def meet(group):
    pl.semaphore_wait(pltpu.get_barrier_semaphore(), group - 1)


class Tables:
    def __init__(self, waves, whole, stage, sem):
        self.waves, self.whole, self.stage, self.sem = waves, whole, stage, sem

    def start(self):
        for n, wave in enumerate(self.waves):
            pltpu.make_async_copy(self.whole.at[wave], self.stage.at[n], self.sem).start()

    def wait(self):
        pltpu.make_async_copy(self.whole.at[pl.ds(0, len(self.waves))], self.stage, self.sem).wait()


def own_tables(me, group, whole, stage, sem):
    return Tables([slot * group + me for slot in range(stage.shape[0])], whole, stage, sem)


def far_tables(swap, whole, stage, sem):
    return Tables([(swap.direct + n) * swap.group + swap.twin for n in range(stage.shape[0])], whole, stage, sem)


def expand_rows(stage, expanded, rows_local):
    m_local, degrees, lats = stage.shape
    row = lax.broadcasted_iota(jnp.int32, (lats, 2 * lats), 0)
    col = lax.broadcasted_iota(jnp.int32, (lats, 2 * lats), 1)
    source = col // (2 * rows_local)
    inner = col % (2 * rows_local)
    for part in range(2):
        pick = (row == source * rows_local + inner - part * rows_local) & (inner // rows_local == part)
        pick = pick.astype(F32).astype(BF16)
        for slot in range(m_local):
            expanded[slot, pl.ds(part * degrees, degrees), :] = dot(stage[slot].astype(BF16), pick, NN).astype(BF16)


def flip_rows(stage, flipped):
    for slot in range(stage.shape[0]):
        flipped[slot] = stage[slot].T.astype(BF16)


def analyse(values_at, table, turn, rows_local):
    modes = table.shape[1]
    for t in range(0, rows_local, 2):
        pair = jnp.concatenate([values_at(t), values_at(t + 1)], axis=0)
        high, low = split_halves(pair)
        out = dot(table[0], high, NT) + dot(table[0], low, NT) + dot(table[1], high, NT)
        channels = out.shape[1] // 2
        turn[pl.ds(t, modes, stride=rows_local), :] = out[:, :channels]
        turn[pl.ds(t + 1, modes, stride=rows_local), :] = out[:, channels:]


def pack_blocks(turn, send, slot):
    group, rows, lanes = send.shape[1:]
    for d in range(group):
        send[slot, d] = turn[pl.ds(d * rows, rows), :].astype(BF16)


def unpack_blocks(recv, b, turn):
    group, rows, lanes = recv.shape[1:]
    for d in range(group):
        turn[pl.ds(d * rows, rows), :] = recv[b, d].astype(F32)


def synthesise(turn, t, table, rows_local):
    modes = table.shape[1]
    spec = turn[pl.ds(t, modes, stride=rows_local), :].astype(BF16)
    return dot(spec, table[0], TN) + dot(spec, table[1], TN)


def legendre_forward(recv, b, expanded, out, rows_local):
    m_local = expanded.shape[0]
    degrees = expanded.shape[1] // 2
    group, _, lanes = recv.shape[1:]
    tile = 2 * rows_local
    for slot in range(m_local):
        rows = recv[b, :, pl.ds(slot * tile, tile), :].reshape(group * tile, lanes)
        res = dot(expanded[slot], rows, NN)
        for part in range(2):
            out[part, pl.ds(slot, degrees, stride=m_local), :] = res[part * degrees:(part + 1) * degrees]


def legendre_inverse(coef, flipped, swap, slot_out, rows_local):
    m_local, lats, degrees = flipped.shape
    send = swap.send
    at = 0
    group = lats // rows_local
    tile = 2 * rows_local
    for slot in range(m_local):
        parts = [coef.at[part][pl.ds(slot, degrees, stride=m_local), :].astype(BF16) for part in range(2)]
        if slot >= swap.direct:
            first = slot * group
            for part in range(2):
                swap.bridge_send[slot_out, part, pl.ds(at, degrees - first), :] = parts[part][first:]
            at += degrees - first
        res = dot(flipped[slot], jnp.concatenate(parts, axis=1), NN)
        lanes = res.shape[1] // 2
        blocks = [res[:, part * lanes:(part + 1) * lanes].reshape(group, rows_local, lanes) for part in range(2)]
        send[slot_out, :, pl.ds(slot * tile, tile), :] = jnp.concatenate(blocks, axis=1).astype(BF16)


def gelu_slope(values):
    cumulative = 0.5 * (1.0 + lax.erf(values * math.sqrt(0.5)))
    density = jnp.exp(-0.5 * values * values) * (1.0 / math.sqrt(2.0 * math.pi))
    return cumulative + values * density


def mix_block(planes):
    real, imag = planes[0], planes[1]
    return jnp.concatenate([jnp.concatenate([real, -imag], axis=1), jnp.concatenate([imag, real], axis=1)], axis=0)


def rows_of_degree(block, inner, m_local):
    batch = block.shape[0]
    lanes = block.shape[-1]
    parts = [block[:, part, pl.ds(inner * m_local, m_local), :].reshape(batch * m_local, lanes) for part in range(2)]
    return jnp.concatenate(parts, axis=1).astype(BF16)


def front_kernel(group, rows_local, field, grad, base, gained, p_fwd, p_inv, w_mix, mixed_out, sums_out, planes_out, coef_shared,
                 mixed_shared, field_buf, grad_buf, turn, stage, stage_far, expanded_fwd, expanded_inv, flipped, send_f, recv_f,
                 padded, coef, mixed, w_in, planes, bridged, send_d, recv_d, message, share_send_a, share_send_d, halves,
                 shared, sums, out_buf, field_sem, grad_sem, p_sem, far_sem, send_f_sem, recv_f_sem, w_sem, planes_sem,
                 bridged_sems, send_d_sem, recv_d_sem, share_a_sems, share_d_sems, half_sem, out_sem, sums_sem):
    me = lax.axis_index('lat')
    batch = field.shape[0]
    channels = field.shape[1] // rows_local
    m_local, degrees = stage.shape[:2]
    used = degrees * m_local
    bunch = coef.shape[0]
    sources, share_rows = coef_shared.shape[1:3]

    def fetch_field(b):
        return Halves(field, b, field_buf, lax.rem(b, 2), field_sem)

    def fetch_grad(b):
        return Halves(grad, b, grad_buf, lax.rem(b, 2), grad_sem)

    def put(b):
        return pltpu.make_async_copy(out_buf.at[lax.rem(b, 2)], mixed_out.at[b], out_sem.at[lax.rem(b, 2)])

    def put_planes():
        return pltpu.make_async_copy(planes, planes_out, planes_sem)

    def fetch_shares(b):
        slot = lax.rem(b, 2)
        return [pltpu.make_async_copy(whole.at[b], halves.at[slot, which], half_sem.at[slot, which])
                for which, whole in enumerate((mixed_shared, coef_shared))]

    greet(me, group)
    fetch_field(0).start()
    fetch_grad(0).start()
    loading = own_tables(me, group, p_fwd, stage, p_sem)
    loading_inv = own_tables(me, group, p_inv, stage, p_sem)
    loading.start()
    swap_f = Exchange(me, group, batch, send_f, recv_f, send_f_sem, recv_f_sem)
    swap_g = BridgedExchange(me, group, batch, bridged, bridged_sems)
    swap_d = Exchange(me, group, batch, send_d, recv_d, send_d_sem, recv_d_sem)
    share_a = Share(me, group, batch, share_send_a, message, coef_shared, share_a_sems)
    share_d = Share(me, group, batch, share_send_d, message, mixed_shared, share_d_sems)
    loading_far = far_tables(swap_g, p_inv, stage_far, far_sem)
    loading_far.start()
    clear_after(padded, used)
    meet(group)

    def build_planes():
        depth, per = w_in.shape[:2]
        blocks = degrees // per
        half = w_in.shape[2] // 2

        def fetch(k):
            return pltpu.make_async_copy(w_mix.at[pl.ds(k * per, per)], w_in.at[lax.rem(k, depth)], w_sem.at[lax.rem(k, depth)])

        for k in range(depth - 1):
            fetch(k).start()

        @pl.loop(0, blocks)
        def _(k):
            @pl.when(k + depth - 1 < blocks)
            def _():
                fetch(k + depth - 1).start()

            fetch(k).wait()
            for inner in range(per):
                rows = w_in.at[lax.rem(k, depth), inner]
                for part in range(2):
                    planes[k * per + inner, part] = rows[pl.ds(part, half, stride=2), :].astype(BF16)

        put_planes().start()

    def mix_bunch():
        @pl.loop(0, degrees // 8)
        def _(k):
            for inner in range(8):
                at = pl.ds(pl.multiple_of((k * 8 + inner) * m_local, m_local), m_local)
                rows = [coef[:, part, at, :].reshape(bunch * m_local, channels) for part in range(2)]
                res = dot(jnp.concatenate(rows, axis=1).astype(BF16), mix_block(planes[k * 8 + inner]), NT)
                for part in range(2):
                    mixed[:, part, at, :] = res[:, part * channels:(part + 1) * channels].reshape(bunch, m_local, channels)

    def weigh_sample(b):
        for copy in fetch_shares(b):
            copy.wait()
        for which in range(2):
            for source in range(sources):
                at = pl.ds(source * (shared.shape[1] // sources), share_rows)
                shared[which, at, :] = halves[lax.rem(b, 2), which, source].astype(F32)
        weigh(shared, sources, sums, m_local)

    def collect(b):
        share_a.arrive(b)
        share_d.arrive(b)
        for copy in fetch_shares(b):
            copy.start()

    lag_a, lag_b, lag_c, lag_d = 2, 4, 6, 8

    def body(i, carry):
        @pl.when(i < batch)
        def _():
            @pl.when(i + 1 < batch)
            def _():
                fetch_field(i + 1).start()

            fetch_field(i).wait()
            half = lax.rem(i, 2)
            analyse(lambda t: read_row(field_buf, half, t, channels, rows_local), base, turn, rows_local)
            swap_f.reserve(i)
            pack_blocks(turn, send_f, lax.rem(i, SLOTS))
            swap_f.start(i)

        @pl.when(i == 0)
        def _():
            loading.wait()
            expand_rows(stage, expanded_fwd, rows_local)
            loading_inv.start()
            loading_far.wait()
            flip_rows(stage_far, swap_g.flipped_far)

        @pl.when(i == 1)
        def _():
            build_planes()
            loading_inv.wait()
            expand_rows(stage, expanded_inv, rows_local)
            flip_rows(stage, flipped)
            sums[...] = jnp.zeros_like(sums)

        @pl.when((i >= lag_a) & (i < batch + lag_a))
        def _():
            b = i - lag_a
            swap_f.arrive(b)
            legendre_forward(recv_f, b, expanded_fwd, padded, rows_local)
            coef[lax.rem(b, bunch)] = padded[:, pl.ds(0, used), :]
            share_a.give(b, padded)

            @pl.when(lax.rem(b, bunch) == bunch - 1)
            def _():
                mix_bunch()

        @pl.when((i >= lag_b) & (i < batch + lag_b))
        def _():
            b = i - lag_b
            swap_g.reserve(b)
            legendre_inverse(mixed.at[lax.rem(b, bunch)], flipped, swap_g, lax.rem(b, SLOTS), rows_local)
            swap_g.start(b)

        @pl.when((i >= lag_b + 1) & (i < batch + lag_b + 1))
        def _():
            swap_g.relay(i - lag_b - 1)

        @pl.when((i >= lag_c) & (i < batch + lag_c))
        def _():
            b = i - lag_c
            half = lax.rem(b, 2)

            @pl.when(b + 1 < batch)
            def _():
                fetch_grad(b + 1).start()

            fetch_grad(b).wait()
            swap_g.arrive(b)
            unpack_blocks(swap_g.recv, b, turn)
            for t in range(rows_local):
                slope = gelu_slope(synthesise(turn, t, gained, rows_local))
                given = read_row(grad_buf, half, t, channels, rows_local)
                write_row(grad_buf, half, t, channels, rows_local, given * slope)
            analyse(lambda t: read_row(grad_buf, half, t, channels, rows_local), gained, turn, rows_local)
            swap_d.reserve(b)
            pack_blocks(turn, send_d, lax.rem(b, SLOTS))
            swap_d.start(b)

        @pl.when(i >= lag_d)
        def _():
            b = i - lag_d

            @pl.when(b >= 2)
            def _():
                weigh_sample(b - 2)

            @pl.when(b >= 1)
            def _():
                collect(b - 1)

            swap_d.arrive(b)

            @pl.when(b >= 2)
            def _():
                put(b - 2).wait()

            legendre_forward(recv_d, b, expanded_inv, padded, rows_local)
            out_buf[lax.rem(b, 2)] = padded[:, pl.ds(0, used), :]
            put(b).start()
            share_d.give(b, padded)

        return carry

    lax.fori_loop(0, batch + lag_d, body, 0)
    weigh_sample(batch - 2)
    collect(batch - 1)
    weigh_sample(batch - 1)
    total = pltpu.make_async_copy(sums, sums_out, sums_sem)
    total.start()
    for swap in (swap_f, swap_g, swap_d, share_a, share_d):
        swap.drain()
    put_planes().wait()
    put(batch - 2).wait()
    put(batch - 1).wait()
    total.wait()


def mix_loop(w_hbm, in_hbms, bufs, w_buf, w_sem, in_sems, blocks, step, meanwhile):
    depth, per = w_buf.shape[:2]

    def copies(k):
        slot = lax.rem(k, depth)
        out = [pltpu.make_async_copy(w_hbm.at[pl.ds(k * per, per)], w_buf.at[slot], w_sem.at[slot])]
        for src, buf, sem in zip(in_hbms, bufs, in_sems):
            rows = buf.shape[3]
            out.append(pltpu.make_async_copy(src.at[:, :, pl.ds(k * rows, rows), :], buf.at[slot], sem.at[slot]))
        return out

    for k in range(depth - 1):
        for copy in copies(k):
            copy.start()
    meanwhile()

    def body(k, carry):
        @pl.when(k + depth - 1 < blocks)
        def _():
            for copy in copies(k + depth - 1):
                copy.start()

        for copy in copies(k):
            copy.wait()
        step(k, lax.rem(k, depth))
        return carry

    lax.fori_loop(0, blocks, body, 0)


class WeightSum:
    def __init__(self, me, group, sums, got, out, sems):
        self.me, self.sums, self.got, self.out, self.sems = me, sums, got, out, sems
        self.core, self.y = lax.rem(me, 2), lax.rem(me // 2, 2)
        self.near, self.far = lax.rem(me // 4, 2), me // (group // 2)
        self.rank = self.near + 2 * self.y + 4 * self.core

    def peer(self, phase):
        step = (1, 2, 4, 8)[phase]
        bit = (self.core, self.y, self.near, self.far)[phase]
        return {'lat': self.me + step - 2 * step * bit}

    def remote(self, phase, k, source, target, stage):
        return pltpu.make_async_remote_copy(source, target, self.sems.at[0, stage, k], self.sems.at[1, stage, k],
                                            device_id=self.peer(phase), device_id_type=MESH)

    def halving(self, k):
        pair, at = self.piece(k)
        return self.remote(3, k, self.sums.at[2 * pair + 1 - self.far, at], self.got.at[k], 4)

    def piece(self, k):
        rows = self.got.shape[1]
        pieces = self.sums.shape[1] // rows
        return k // pieces, pl.ds(pl.multiple_of(lax.rem(k, pieces) * rows, rows), rows)

    def settle(self, k):
        pair, at = self.piece(k)
        mine = 2 * pair + self.far
        return pltpu.make_async_copy(self.sums.at[mine, at], self.out.at[mine, self.rank, at], self.sems.at[0, 5, k])

    def doubling(self, phase, k):
        pair, at = self.piece(k)
        if phase == 3:
            mine = 2 * pair + self.far
            return self.remote(3, k, self.sums.at[mine, at], self.out.at[mine, self.rank, at], 3)
        width = (4, 2, 1)[phase]
        first = (4 * self.core, 4 * self.core + 2 * self.y, self.rank)[phase]
        span = self.out.at[pl.ds(2 * pair, 2), pl.ds(first, width), at]
        return self.remote(phase, k, span, span, phase)

    def reduce_step(self, k):
        self.halving(k).wait()
        pair, at = self.piece(k)
        mine = 2 * pair + self.far
        self.sums[mine, at] = self.sums[mine, at] + self.got[k]
        self.settle(k).start()
        self.doubling(3, k).start()

    def gather_step(self, phase, k):
        if phase == 2:
            self.settle(k).wait()
        self.doubling(phase + 1, k).wait()
        if phase >= 0:
            self.doubling(phase, k).start()


def shared_place(part, slot, step, m_local):
    tile = 2 * m_local
    if slot == m_local // 2:
        return m_local * tile + part * m_local + step - m_local
    pair = min(slot, m_local - slot) if slot else 0
    shift = 0 if slot < m_local // 2 else 2 * slot
    return (part * (m_local // 2) + pair) * tile + step - shift


def weigh(shared, sources, sums, m_local):
    stride = shared.shape[1] // sources

    @pl.loop(0, sums.shape[0])
    def _(step):
        sides = []
        for which in range(2):
            slots = []
            for slot in range(m_local):
                used = step >= 2 * slot
                parts = []
                for part in range(2):
                    place = jnp.where(used, shared_place(part, slot, step, m_local), 0)
                    rows = shared[which, pl.ds(place, sources, stride=stride), :]
                    parts.append(jnp.where(used, rows, 0.0))
                slots.append(jnp.concatenate(parts, axis=1))
            sides.append(jnp.concatenate(slots, axis=0).astype(BF16))
        big = dot(sides[0], sides[1], TN)
        half = big.shape[0] // 2
        real, imag = pl.ds(0, half, stride=2), pl.ds(1, half, stride=2)
        sums[step, real, :] = sums[step, real, :] + (big[:half, :half] + big[half:, half:])
        sums[step, imag, :] = sums[step, imag, :] + (big[half:, :half] - big[:half, half:])


def third_kernel(group, rows_local, mixed, part_sums, w_mix, p_fwd, table, grad, field_out, grad_w, w_buf, mixed_blk, sums, got,
                 back, stage, flipped, turn, grad_buf, bridged, w_sem, m_sem, s_sem, gw_sem, in_sem, out_sem, p_sem, bridged_sems,
                 stage_far, far_sem):
    me = lax.axis_index('lat')
    batch = grad.shape[0]
    channels = grad.shape[1] // rows_local
    depth = grad_buf.shape[0]
    per = w_buf.shape[1]
    degrees = w_mix.shape[0]
    m_local = stage.shape[0]

    def fetch(b):
        return Halves(grad, b, grad_buf, lax.rem(b, depth), in_sem)

    def put(b):
        return Halves(field_out, b, grad_buf, lax.rem(b, depth), out_sem, outward=True)

    load_sums = pltpu.make_async_copy(part_sums, sums, s_sem)
    load_sums.start()
    greet(me, group)
    total = WeightSum(me, group, sums, got, grad_w, gw_sem)
    swap = BridgedExchange(me, group, batch, bridged, bridged_sems)
    loading = own_tables(me, group, p_fwd, stage, p_sem)
    loading_far = far_tables(swap, p_fwd, stage_far, far_sem)
    loading.start()
    loading_far.start()
    load_sums.wait()
    meet(group)
    chunks = got.shape[0]
    for k in range(4):
        total.halving(k).start()

    def unmix(k, slot):
        for inner in range(per):
            rows = rows_of_degree(mixed_blk.at[slot], inner, m_local)
            res = dot(rows, mix_block(w_buf[slot, inner]), NN)
            at = pl.ds(pl.multiple_of((k * per + inner) * m_local, m_local), m_local)
            half = res.shape[1] // 2
            for part in range(2):
                back[:, part, at, :] = res[:, part * half:(part + 1) * half].reshape(batch, m_local, half)

    def prepare():
        loading.wait()
        flip_rows(stage, flipped)
        loading_far.wait()
        flip_rows(stage_far, swap.flipped_far)

    mix_loop(w_mix, [mixed], [mixed_blk], w_buf, w_sem, [m_sem], degrees // per, unmix, prepare)
    fetch(0).start()
    lag = 2

    def body(i, carry):
        steps = [total.reduce_step] + [functools.partial(total.gather_step, p) for p in (2, 1, 0, -1)]
        steps = [total.reduce_step] + [functools.partial(total.gather_step, p) for p in (2, 1, 0, -1)]
        def advance(sub):
            @pl.when(i * 2 + sub + 4 < chunks)
            def _():
                total.halving(i * 2 + sub + 4).start()

            for late, step in reversed(list(enumerate(steps))):
                k = (i - late) * 2 + sub

                @pl.when((k >= 0) & (k < chunks))
                def _():
                    step(k)

        advance(0)

        @pl.when(i < batch)
        def _():
            swap.reserve(i)
            legendre_inverse(back.at[i], flipped, swap, lax.rem(i, SLOTS), rows_local)
            swap.start(i)

        @pl.when((i >= 1) & (i < batch + 1))
        def _():
            swap.relay(i - 1)


        @pl.when((i >= lag) & (i < batch + lag))
        def _():
            b = i - lag
            half = lax.rem(b, depth)

            @pl.when(b >= depth - 1)
            def _():
                put(b - depth + 1).wait()

            @pl.when(b + 1 < batch)
            def _():
                fetch(b + 1).start()

            fetch(b).wait()
            swap.arrive(b)
            unpack_blocks(swap.recv, b, turn)
            for t in range(rows_local):
                added = synthesise(turn, t, table, rows_local)
                given = read_row(grad_buf, half, t, channels, rows_local)
                write_row(grad_buf, half, t, channels, rows_local, given + added)
            put(b).start()

        advance(1)
        return carry

    lax.fori_loop(0, max(batch + lag, chunks // 2 + 4), body, 0)
    swap.drain()
    for b in range(batch - depth + 1, batch):
        put(b).wait()


def finish_kernel(first, second, first_out, second_out, first_ring, second_ring, in_sem, out_sem):
    depth = first_ring.shape[0]
    pieces = []
    for side, (source, target, ring) in enumerate(((first, first_out, first_ring), (second, second_out, second_ring))):
        for n in range(source.shape[0]):
            slot = n % depth
            take = pltpu.make_async_copy(source.at[n], ring.at[slot], in_sem.at[side, slot])
            give = pltpu.make_async_copy(ring.at[slot], target.at[n], out_sem.at[side, slot])
            pieces.append(((n, side), (side, n), take, give))
    pieces.sort(key=lambda piece: piece[0])
    given = {piece[1]: piece[3] for piece in pieces}
    waited = set()
    for k in range(len(pieces) + depth):
        if k < len(pieces):
            _, (side, n), take, _ = pieces[k]
            if n >= depth:
                given[side, n - depth].wait()
                waited.add((side, n - depth))
            take.start()
        if k >= depth:
            pieces[k - depth][2].wait()
            pieces[k - depth][3].start()
    for _, place, _, give in pieces:
        if place not in waited:
            give.wait()


def any_specs(n):
    return [pl.BlockSpec(memory_space=pl.ANY)] * n


def params(collective_id=None):
    if collective_id is None:
        return pltpu.CompilerParams(vmem_limit_bytes=VMEM_LIMIT)
    return pltpu.CompilerParams(collective_id=collective_id, has_side_effects=True, vmem_limit_bytes=VMEM_LIMIT)


def solution(mesh):
    group = mesh.shape['lat']
    field_spec = P('member', None, 'lat', None)

    def local_step(field_loc, grad_loc, p_fwd, p_inv, w_mix):
        batch, channels, rows_local, lon_count = field_loc.shape
        degrees, lats = p_fwd.shape[1:]
        m_local = p_fwd.shape[0] // group
        modes = group * m_local * 2
        base, gained = (two_halves(table) for table in dft_tables(group, m_local, lon_count))
        field = field_loc.reshape(batch, channels * rows_local, lon_count)
        grad = grad_loc.reshape(batch, channels * rows_local, lon_count)
        w_rows = jnp.swapaxes(w_mix, 2, 3).reshape(degrees, channels * 2, channels)
        dma, vmem = pltpu.SemaphoreType.DMA, pltpu.VMEM
        block_rows = m_local * 2 * rows_local
        coef_shape = (batch, 2, degrees * m_local, channels)
        send_t = vmem((SLOTS, group, block_rows, channels), BF16)
        recv_t = vmem((batch, group, block_rows, channels), BF16)
        turn_t = vmem((modes * rows_local, channels), F32)
        stage_t = vmem((m_local, degrees, lats), F32)
        expanded_t = vmem((m_local, 2 * degrees, 2 * lats), BF16)
        flipped_t = vmem((m_local, lats, degrees), BF16)
        field_t = vmem((2, lon_count // LANES, channels * rows_local, LANES), F32)
        table_spec = pl.BlockSpec(memory_space=pltpu.VMEM)
        any_spec = pl.BlockSpec(memory_space=pl.ANY)
        per = 8
        late = sum(degrees - slot * group < lats // 2 for slot in range(m_local))
        far_rows = sum(degrees - slot * group for slot in range(m_local - late, m_local))
        late_rows = late * 2 * rows_local
        bridged_t = (send_t, recv_t, vmem((SLOTS, 2, far_rows, channels), BF16), vmem((batch, 2, far_rows, channels), BF16),
                     vmem((SLOTS, group // 2, late_rows, channels), BF16), vmem((late, lats, degrees), BF16))
        bridged_sems = (dma((SLOTS,)), dma((batch,))) * 3

        ranks = group // 2
        share_rows = (m_local + 1) * 2 * ranks
        share_out = jax.ShapeDtypeStruct((batch, ranks, share_rows, channels), BF16)
        share_sems = (dma((SLOTS,)), dma((batch,)), dma((SLOTS,)))

        blk_t = vmem((DEPTH, batch, 2, per * m_local, channels), F32)
        w_t = vmem((DEPTH, per, 2, channels, channels), BF16)
        far_stage_t = vmem((late, degrees, lats), F32)
        steps = degrees // ranks
        sums_shape = (steps, channels * 2, channels)
        planes_shape = (degrees, 2, channels, channels)
        single_t = vmem((BUNCH,) + coef_shape[1:], F32)
        share_send_t = vmem((SLOTS, ranks, share_rows, channels), BF16)
        swap_sems = (dma((SLOTS,)), dma((batch,)))
        mixed, sums, planes, _, _ = pl.pallas_call(
            functools.partial(front_kernel, group, rows_local), name='front',
            out_shape=[jax.ShapeDtypeStruct(coef_shape, F32), jax.ShapeDtypeStruct(sums_shape, F32),
                       jax.ShapeDtypeStruct(planes_shape, BF16), share_out, share_out],
            in_specs=[any_spec, any_spec, table_spec, table_spec, any_spec, any_spec, any_spec], out_specs=[any_spec] * 5,
            scratch_shapes=[field_t, field_t, turn_t, stage_t, far_stage_t, expanded_t, expanded_t, flipped_t, send_t, recv_t,
                            vmem((2, 2 * degrees * m_local, channels), F32), single_t, single_t,
                            vmem((4, 4, channels * 2, channels), F32), vmem(planes_shape, BF16), bridged_t, send_t, recv_t,
                            vmem((ranks, share_rows, channels), F32), share_send_t, share_send_t,
                            vmem((2, 2) + share_out.shape[1:], BF16), vmem((2, ranks * (share_rows + 8), channels), F32),
                            vmem(sums_shape, F32), vmem((2,) + coef_shape[1:], F32),
                            dma((2, 2)), dma((2, 2)), dma(()), dma(()), *swap_sems, dma((4,)), dma(()), bridged_sems, *swap_sems,
                            share_sems, share_sems, dma((2, 2)), dma((2,)), dma(())],
            compiler_params=params(0))(field, grad, base, gained, p_fwd, p_inv, w_rows)

        w_rect = (channels * 2, channels)
        field_out, gw_total = pl.pallas_call(
            functools.partial(third_kernel, group, rows_local), name='third',
            out_shape=[jax.ShapeDtypeStruct(grad.shape, F32), jax.ShapeDtypeStruct((steps, ranks) + w_rect, F32)],
            in_specs=[any_spec] * 4 + [table_spec, any_spec], out_specs=[any_spec] * 2,
            scratch_shapes=[w_t, blk_t, vmem(sums_shape, F32), vmem((PIECES * steps // 2, channels * 2 // PIECES, channels), F32), vmem(coef_shape, F32), stage_t, flipped_t, turn_t,
                            vmem((3, lon_count // LANES, channels * rows_local, LANES), F32), bridged_t,
                            dma((DEPTH,)), dma((DEPTH,)), dma(()), dma((2, 6, PIECES * steps // 2)), dma((3, 2)), dma((3, 2)), dma(()),
                            bridged_sems, far_stage_t, dma(())],
            compiler_params=params(2))(mixed, sums, planes, p_fwd, base, grad)

        gw_total = gw_total.reshape(steps, ranks * channels * 2, channels)
        results = [jax.ShapeDtypeStruct(whole.shape, F32) for whole in (field_out, gw_total)]
        field_out, gw_total = pl.pallas_call(
            finish_kernel, name='finish', out_shape=results, in_specs=[any_spec] * 2, out_specs=[any_spec] * 2,
            scratch_shapes=[vmem((RING,) + whole.shape[1:], F32) for whole in results] + [dma((2, RING)), dma((2, RING))],
            compiler_params=params())(field_out, gw_total)

        grad_wmix = jnp.swapaxes(gw_total.reshape(degrees, channels, 2, channels), 2, 3)
        return field_out.reshape(grad_loc.shape), grad_wmix

    return jax.shard_map(local_step, mesh=mesh, in_specs=(field_spec, field_spec, P(), P(), P()),
                         out_specs=(field_spec, P('member', None, None, None)), check_vma=False)
```

```python
import functools
import math

import jax
import jax.numpy as jnp
import numpy as np
from jax import lax
from jax.experimental import pallas as pl
from jax.experimental.pallas import tpu as pltpu
from jax.sharding import PartitionSpec as P

MESH = pl.DeviceIdType.MESH
LANES = 128
SLOTS = 3
BUNCH = 3
PIECES = 2
RING = 6
VMEM_LIMIT = 67043328
F32 = jnp.float32
BF16 = jnp.bfloat16

NN = (((1,), (0,)), ((), ()))
NT = (((1,), (1,)), ((), ()))
TN = (((0,), (0,)), ((), ()))


def dot(lhs, rhs, dims):
    return lax.dot_general(lhs, rhs, dims, preferred_element_type=F32)


def split_halves(values):
    high = values.astype(BF16)
    low = (values - high.astype(F32)).astype(BF16)
    return high, low


def dft_tables(group, m_local, lon_count):
    owner, slot, part = np.meshgrid(np.arange(group), np.arange(m_local), np.arange(2), indexing='ij')
    wave = (slot * group + owner).reshape(-1)
    part = part.reshape(-1)
    phase = 2.0 * np.pi * ((wave[:, None] * np.arange(lon_count)[None, :]) % lon_count) / lon_count
    base = np.where(part[:, None] == 0, np.cos(phase), -np.sin(phase)) / math.sqrt(lon_count)
    gains = np.where(wave == 0, 1.0, 2.0)[:, None]
    return base.astype(np.float32), (base * gains).astype(np.float32)


def two_halves(table):
    high = jnp.asarray(table).astype(BF16)
    low = (jnp.asarray(table) - high.astype(F32)).astype(BF16)
    return jnp.stack([high, low])


class Halves:
    def __init__(self, whole, b, halves, slot, sem, outward=False):
        self.copies = []
        for half in range(halves.shape[1]):
            ends = whole.at[b, :, pl.ds(half * LANES, LANES)], halves.at[slot, half]
            source, target = ends[::-1] if outward else ends
            self.copies.append(pltpu.make_async_copy(source, target, sem.at[slot, half]))

    def start(self):
        for copy in self.copies:
            copy.start()

    def wait(self):
        for copy in self.copies:
            copy.wait()


def read_row(halves, slot, t, channels, rows_local):
    at = pl.ds(t, channels, stride=rows_local)
    return jnp.concatenate([halves[slot, half, at, :] for half in range(halves.shape[1])], axis=1)


def write_row(halves, slot, t, channels, rows_local, values):
    at = pl.ds(t, channels, stride=rows_local)
    for half in range(halves.shape[1]):
        halves[slot, half, at, :] = values[:, half * LANES:(half + 1) * LANES]


class Exchange:
    def __init__(self, me, group, batch, send, recv, send_sem, recv_sem):
        self.me, self.group, self.batch = me, group, batch
        self.send, self.recv, self.send_sem, self.recv_sem = send, recv, send_sem, recv_sem

    def all_copies(self, b):
        slot = lax.rem(b, SLOTS)
        others = pl.ds(0, self.group - 1)
        return pltpu.make_async_remote_copy(
            self.send.at[slot, others], self.recv.at[b, others], self.send_sem.at[slot], self.recv_sem.at[b],
            device_id={'lat': lax.rem(self.me + 1, self.group)}, device_id_type=MESH)

    def reserve(self, b):
        @pl.when(b >= SLOTS)
        def _():
            self.all_copies(b - SLOTS).wait_send()

    def start(self, b):
        slot = lax.rem(b, SLOTS)
        self.recv[b, self.me] = self.send[slot, self.me]

        @pl.loop(1, self.group)
        def _(step):
            target = jnp.bitwise_xor(self.me, self.group - step)
            pltpu.make_async_remote_copy(
                self.send.at[slot, target], self.recv.at[b, self.me], self.send_sem.at[slot], self.recv_sem.at[b],
                device_id={'lat': target}, device_id_type=MESH).start()

    def arrive(self, b):
        self.all_copies(b).wait_recv()

    def drain(self):
        for b in range(max(0, self.batch - SLOTS), self.batch):
            self.all_copies(b).wait_send()


class BridgedExchange:
    def __init__(self, me, group, batch, bufs, sems):
        self.me, self.group, self.batch = me, group, batch
        self.send, self.recv, self.bridge_send, self.bridge_recv, self.relay_send, self.flipped_far = bufs
        self.send_sem, self.recv_sem, self.bridge_send_sem, self.bridge_recv_sem, self.relay_send_sem, self.relay_recv_sem = sems
        self.half_size = group // 2
        self.half = me // self.half_size
        self.place = lax.rem(me, self.half_size)
        self.twin = self.half_size + me - 2 * self.half_size * self.half
        self.rows = self.send.shape[2]
        self.late_rows = self.relay_send.shape[2]
        self.early_rows = self.rows - self.late_rows
        self.tile = self.late_rows // self.flipped_far.shape[0]
        self.direct = self.early_rows // self.tile

    def copy(self, source, target, send_sem, recv_sem, device):
        return pltpu.make_async_remote_copy(source, target, send_sem, recv_sem, device_id={'lat': device},
                                            device_id_type=MESH)

    def all_direct(self, b):
        slot = lax.rem(b, SLOTS)
        count = (self.half_size - 1) * self.rows + self.half_size * self.early_rows
        span = pl.ds(0, count // self.rows)
        return self.copy(self.send.at[slot, span], self.recv.at[b, span], self.send_sem.at[slot], self.recv_sem.at[b], self.twin)

    def all_relayed(self, b):
        slot = lax.rem(b, SLOTS)
        span, part = pl.ds(0, self.half_size - 1), pl.ds(0, self.late_rows)
        return self.copy(self.relay_send.at[slot, span], self.recv.at[b, span, part], self.relay_send_sem.at[slot],
                         self.relay_recv_sem.at[b], self.twin)

    def bridge(self, b):
        slot = lax.rem(b, SLOTS)
        return self.copy(self.bridge_send.at[slot], self.bridge_recv.at[b], self.bridge_send_sem.at[slot],
                         self.bridge_recv_sem.at[b], self.twin)

    def reserve(self, b):
        @pl.when(b >= SLOTS)
        def _():
            self.all_direct(b - SLOTS).wait_send()
            self.bridge(b - SLOTS).wait_send()

    def start(self, b):
        slot = lax.rem(b, SLOTS)
        self.bridge(b).start()
        early = pl.ds(0, self.early_rows)

        @pl.loop(0, self.half_size)
        def _(step):
            target = jnp.bitwise_xor(self.me, 2 * self.half_size - 1 - step)
            self.copy(self.send.at[slot, target, early], self.recv.at[b, self.me, early], self.send_sem.at[slot],
                      self.recv_sem.at[b], target).start()

        @pl.loop(1, self.half_size)
        def _(step):
            target = jnp.bitwise_xor(self.me, self.half_size - step)
            self.copy(self.send.at[slot, target], self.recv.at[b, self.me], self.send_sem.at[slot], self.recv_sem.at[b],
                      target).start()

        self.recv[b, self.me] = self.send[slot, self.me]

    def relay(self, b):
        slot = lax.rem(b, SLOTS)

        @pl.when(b >= SLOTS)
        def _():
            self.all_relayed(b - SLOTS).wait_send()

        self.bridge(b).wait_recv()
        lats, degrees = self.flipped_far.shape[1:]
        own = pl.ds(pl.multiple_of(self.half * (lats // 2), lats // 2), lats // 2)
        at = 0
        for late in range(self.flipped_far.shape[0]):
            first = (self.direct + late) * self.group
            count = degrees - first
            parts = []
            for part in range(2):
                rows = self.bridge_recv[b, part, pl.ds(at, count), :]
                parts.append(jnp.concatenate([jnp.zeros((first, rows.shape[1]), BF16), rows], axis=0))
            at += count
            res = dot(self.flipped_far[late, own, :], jnp.concatenate(parts, axis=1), NN)
            lanes = res.shape[1] // 2
            blocks = [res[:, part * lanes:(part + 1) * lanes].reshape(self.half_size, self.tile // 2, lanes) for part in range(2)]
            self.relay_send[slot, :, pl.ds(late * self.tile, self.tile), :] = jnp.concatenate(blocks, axis=1).astype(BF16)
        late_at = pl.ds(self.early_rows, self.late_rows)

        @pl.loop(1, self.half_size)
        def _(step):
            place = jnp.bitwise_xor(self.place, self.half_size - step)
            self.copy(self.relay_send.at[slot, place], self.recv.at[b, self.twin, late_at], self.relay_send_sem.at[slot],
                      self.relay_recv_sem.at[b], self.half * self.half_size + place).start()

        self.recv[b, self.twin, late_at] = self.relay_send[slot, self.place]

    def arrive(self, b):
        self.all_direct(b).wait_recv()
        self.all_relayed(b).wait_recv()

    def drain(self):
        for b in range(max(0, self.batch - SLOTS), self.batch):
            self.all_direct(b).wait_send()
            self.bridge(b).wait_send()
            self.all_relayed(b).wait_send()


class Share:
    def __init__(self, me, group, batch, send, message, out, sems):
        self.batch, self.send, self.message, self.out = batch, send, message, out
        self.send_sem, self.recv_sem, self.local_sem = sems
        self.size = group // 2
        self.base = me // self.size * self.size
        self.place = lax.rem(me, self.size)

    def rank(self, place):
        return place // 4 + 2 * (lax.rem(place, 4) // 2) + 4 * lax.rem(place, 2)

    def copy(self, slot, source, b, target, place):
        return pltpu.make_async_remote_copy(
            self.send.at[slot, source], self.out.at[b, target], self.send_sem.at[slot], self.recv_sem.at[b],
            device_id={'lat': self.base + place}, device_id_type=MESH)

    def every(self, b):
        span = pl.ds(0, self.size - 1)
        return self.copy(lax.rem(b, SLOTS), span, b, span, lax.rem(self.place + 1, self.size))

    def keep(self, b):
        slot = lax.rem(b, SLOTS)
        return pltpu.make_async_copy(self.send.at[slot, self.rank(self.place)], self.out.at[b, self.place],
                                     self.local_sem.at[slot])

    def give(self, b, coef):
        slot_b = lax.rem(b, SLOTS)

        @pl.when(b >= SLOTS)
        def _():
            self.every(b - SLOTS).wait_send()

        size = self.size
        m_local = size
        tile = 2 * size

        def rows(part, slot, rank, first, count):
            return coef[part, pl.ds((first * size + rank) * m_local + slot, count, stride=size * m_local), :]

        for rank in range(size):
            for part in range(2):
                for pair in range(m_local // 2):
                    block = rows(part, pair, rank, 0, tile)
                    if pair:
                        block = block + rows(part, m_local - pair, rank, 2 * (m_local - pair), tile)
                    self.message[rank, pl.ds((part * (m_local // 2) + pair) * tile, tile), :] = block
                self.message[rank, pl.ds(m_local * tile + part * size, size), :] = rows(part, m_local // 2, rank, size, size)
        for rank in range(size):
            self.send[slot_b, rank] = self.message[rank].astype(BF16)
        self.keep(b).start()

        @pl.loop(1, size)
        def _(step):
            place = jnp.bitwise_xor(self.place, size - step)
            self.copy(slot_b, self.rank(place), b, self.place, place).start()

        self.keep(b).wait()

    def drain(self):
        for b in range(max(0, self.batch - SLOTS), self.batch):
            self.every(b).wait_send()

    def arrive(self, b):
        self.every(b).wait_recv()


def clear_after(coef, used):
    for part in range(coef.shape[0]):
        coef[part, pl.ds(used, coef.shape[1] - used), :] = jnp.zeros((coef.shape[1] - used, coef.shape[2]), F32)


def greet(me, group):
    barrier = pltpu.get_barrier_semaphore()

    @pl.loop(1, group)
    def _(step):
        pl.semaphore_signal(barrier, inc=1, device_id={'lat': lax.rem(me + step, group)}, device_id_type=MESH)


def meet(group):
    pl.semaphore_wait(pltpu.get_barrier_semaphore(), group - 1)


class Tables:
    def __init__(self, waves, whole, stage, sem):
        self.waves, self.whole, self.stage, self.sem = waves, whole, stage, sem

    def start(self):
        for n, wave in enumerate(self.waves):
            pltpu.make_async_copy(self.whole.at[wave], self.stage.at[n], self.sem).start()

    def wait(self):
        pltpu.make_async_copy(self.whole.at[pl.ds(0, len(self.waves))], self.stage, self.sem).wait()


def own_tables(me, group, whole, stage, sem):
    return Tables([slot * group + me for slot in range(stage.shape[0])], whole, stage, sem)


def far_tables(swap, whole, stage, sem):
    return Tables([(swap.direct + n) * swap.group + swap.twin for n in range(stage.shape[0])], whole, stage, sem)


def expand_rows(stage, expanded, rows_local):
    m_local, degrees, lats = stage.shape
    row = lax.broadcasted_iota(jnp.int32, (lats, 2 * lats), 0)
    col = lax.broadcasted_iota(jnp.int32, (lats, 2 * lats), 1)
    source = col // (2 * rows_local)
    inner = col % (2 * rows_local)
    for part in range(2):
        pick = (row == source * rows_local + inner - part * rows_local) & (inner // rows_local == part)
        pick = pick.astype(F32).astype(BF16)
        for slot in range(m_local):
            expanded[slot, pl.ds(part * degrees, degrees), :] = dot(stage[slot].astype(BF16), pick, NN).astype(BF16)


def flip_rows(stage, flipped):
    for slot in range(stage.shape[0]):
        flipped[slot] = stage[slot].T.astype(BF16)


def analyse(values_at, table, turn, rows_local):
    modes = table.shape[1]
    for t in range(0, rows_local, 2):
        pair = jnp.concatenate([values_at(t), values_at(t + 1)], axis=0)
        high, low = split_halves(pair)
        out = dot(table[0], high, NT) + dot(table[0], low, NT) + dot(table[1], high, NT)
        channels = out.shape[1] // 2
        turn[pl.ds(t, modes, stride=rows_local), :] = out[:, :channels]
        turn[pl.ds(t + 1, modes, stride=rows_local), :] = out[:, channels:]


def pack_blocks(turn, send, slot):
    group, rows, lanes = send.shape[1:]
    for d in range(group):
        send[slot, d] = turn[pl.ds(d * rows, rows), :].astype(BF16)


def unpack_blocks(recv, b, turn):
    group, rows, lanes = recv.shape[1:]
    for d in range(group):
        turn[pl.ds(d * rows, rows), :] = recv[b, d].astype(F32)


def synthesise(turn, t, table, rows_local):
    modes = table.shape[1]
    spec = turn[pl.ds(t, modes, stride=rows_local), :].astype(BF16)
    return dot(spec, table[0], TN) + dot(spec, table[1], TN)


def legendre_forward(recv, b, expanded, out, rows_local):
    m_local = expanded.shape[0]
    degrees = expanded.shape[1] // 2
    group, _, lanes = recv.shape[1:]
    tile = 2 * rows_local
    for slot in range(m_local):
        rows = recv[b, :, pl.ds(slot * tile, tile), :].reshape(group * tile, lanes)
        res = dot(expanded[slot], rows, NN)
        for part in range(2):
            out[part, pl.ds(slot, degrees, stride=m_local), :] = res[part * degrees:(part + 1) * degrees]


def legendre_inverse(coef, flipped, swap, slot_out, rows_local):
    m_local, lats, degrees = flipped.shape
    send = swap.send
    at = 0
    group = lats // rows_local
    tile = 2 * rows_local
    for slot in range(m_local):
        parts = [coef.at[part][pl.ds(slot, degrees, stride=m_local), :].astype(BF16) for part in range(2)]
        if slot >= swap.direct:
            first = slot * group
            for part in range(2):
                swap.bridge_send[slot_out, part, pl.ds(at, degrees - first), :] = parts[part][first:]
            at += degrees - first
        res = dot(flipped[slot], jnp.concatenate(parts, axis=1), NN)
        lanes = res.shape[1] // 2
        blocks = [res[:, part * lanes:(part + 1) * lanes].reshape(group, rows_local, lanes) for part in range(2)]
        send[slot_out, :, pl.ds(slot * tile, tile), :] = jnp.concatenate(blocks, axis=1).astype(BF16)


def gelu_slope(values):
    cumulative = 0.5 * (1.0 + lax.erf(values * math.sqrt(0.5)))
    density = jnp.exp(-0.5 * values * values) * (1.0 / math.sqrt(2.0 * math.pi))
    return cumulative + values * density


def mix_block(planes):
    real, imag = planes[0], planes[1]
    return jnp.concatenate([jnp.concatenate([real, -imag], axis=1), jnp.concatenate([imag, real], axis=1)], axis=0)


class WeightSum:
    def __init__(self, me, group, sums, got, out, sems):
        self.me, self.sums, self.got, self.out, self.sems = me, sums, got, out, sems
        self.core, self.y = lax.rem(me, 2), lax.rem(me // 2, 2)
        self.near, self.far = lax.rem(me // 4, 2), me // (group // 2)
        self.rank = self.near + 2 * self.y + 4 * self.core

    def peer(self, phase):
        step = (1, 2, 4, 8)[phase]
        bit = (self.core, self.y, self.near, self.far)[phase]
        return {'lat': self.me + step - 2 * step * bit}

    def remote(self, phase, k, source, target, stage):
        return pltpu.make_async_remote_copy(source, target, self.sems.at[0, stage, k], self.sems.at[1, stage, k],
                                            device_id=self.peer(phase), device_id_type=MESH)

    def halving(self, k):
        pair, at = self.piece(k)
        return self.remote(3, k, self.sums.at[2 * pair + 1 - self.far, at], self.got.at[k], 4)

    def piece(self, k):
        rows = self.got.shape[1]
        pieces = self.sums.shape[1] // rows
        return k // pieces, pl.ds(pl.multiple_of(lax.rem(k, pieces) * rows, rows), rows)

    def settle(self, k):
        pair, at = self.piece(k)
        mine = 2 * pair + self.far
        return pltpu.make_async_copy(self.sums.at[mine, at], self.out.at[mine, self.rank, at], self.sems.at[0, 5, k])

    def doubling(self, phase, k):
        pair, at = self.piece(k)
        if phase == 3:
            mine = 2 * pair + self.far
            return self.remote(3, k, self.sums.at[mine, at], self.out.at[mine, self.rank, at], 3)
        width = (4, 2, 1)[phase]
        first = (4 * self.core, 4 * self.core + 2 * self.y, self.rank)[phase]
        span = self.out.at[pl.ds(2 * pair, 2), pl.ds(first, width), at]
        return self.remote(phase, k, span, span, phase)

    def reduce_step(self, k):
        self.halving(k).wait()
        pair, at = self.piece(k)
        mine = 2 * pair + self.far
        self.sums[mine, at] = self.sums[mine, at] + self.got[k]
        self.settle(k).start()
        self.doubling(3, k).start()

    def gather_step(self, phase, k):
        if phase == 2:
            self.settle(k).wait()
        self.doubling(phase + 1, k).wait()
        if phase >= 0:
            self.doubling(phase, k).start()


def shared_place(part, slot, step, m_local):
    tile = 2 * m_local
    if slot == m_local // 2:
        return m_local * tile + part * m_local + step - m_local
    pair = min(slot, m_local - slot) if slot else 0
    shift = 0 if slot < m_local // 2 else 2 * slot
    return (part * (m_local // 2) + pair) * tile + step - shift


def weigh(shared, sources, sums, m_local):
    stride = shared.shape[1] // sources

    @pl.loop(0, sums.shape[0])
    def _(step):
        sides = []
        for which in range(2):
            slots = []
            for slot in range(m_local):
                used = step >= 2 * slot
                parts = []
                for part in range(2):
                    place = jnp.where(used, shared_place(part, slot, step, m_local), 0)
                    rows = shared[which, pl.ds(place, sources, stride=stride), :]
                    parts.append(jnp.where(used, rows, 0.0))
                slots.append(jnp.concatenate(parts, axis=1))
            sides.append(jnp.concatenate(slots, axis=0).astype(BF16))
        big = dot(sides[0], sides[1], TN)
        half = big.shape[0] // 2
        real, imag = pl.ds(0, half, stride=2), pl.ds(1, half, stride=2)
        sums[step, real, :] = sums[step, real, :] + (big[:half, :half] + big[half:, half:])
        sums[step, imag, :] = sums[step, imag, :] + (big[half:, :half] - big[:half, half:])


def whole_kernel(group, rows_local, field, grad, base, gained, p_fwd, p_inv, w_mix, field_out, grad_w, back_out, coef_shared,
                 mixed_shared, field_buf, grad_buf, turn, stage, stage_far, expanded_fwd, expanded_inv, flipped, send_f, recv_f,
                 padded, coef, mixed, w_in, planes, bridged, send_d, recv_d, message, share_send_a, share_send_d, halves,
                 shared, sums, back, got, field_sem, grad_sem, p_sem, far_sem, send_f_sem, recv_f_sem, w_sem, bridged_sems,
                 send_d_sem, recv_d_sem, share_a_sems, share_d_sems, half_sem, out_sem, gw_sem, again_sems, back_sem, last_sem):
    me = lax.axis_index('lat')
    batch = field.shape[0]
    channels = field.shape[1] // rows_local
    m_local, degrees = stage.shape[:2]
    used = degrees * m_local
    bunch = coef.shape[0]
    sources, share_rows = coef_shared.shape[1:3]

    def fetch_field(b):
        return Halves(field, b, field_buf, lax.rem(b, 2), field_sem)

    def fetch_grad(b):
        return Halves(grad, b, grad_buf, lax.rem(b, 2), grad_sem)

    def put(b):
        return pltpu.make_async_copy(back.at[lax.rem(b, bunch)], back_out.at[b], out_sem.at[lax.rem(b, bunch)])

    def fetch_back(b):
        return pltpu.make_async_copy(back_out.at[b], coef.at[lax.rem(b, 2)], back_sem.at[lax.rem(b, 2)])

    def fetch_last(b):
        return Halves(grad, b, field_buf, lax.rem(b, 2), field_sem)

    def put_last(b):
        return Halves(field_out, b, field_buf, lax.rem(b, 2), last_sem, outward=True)

    def fetch_shares(b):
        slot = lax.rem(b, 2)
        return [pltpu.make_async_copy(whole.at[b], halves.at[slot, which], half_sem.at[slot, which])
                for which, whole in enumerate((mixed_shared, coef_shared))]

    greet(me, group)
    fetch_field(0).start()
    fetch_grad(0).start()
    loading = own_tables(me, group, p_fwd, stage, p_sem)
    loading_inv = own_tables(me, group, p_inv, stage, p_sem)
    loading.start()
    swap_f = Exchange(me, group, batch, send_f, recv_f, send_f_sem, recv_f_sem)
    swap_g = BridgedExchange(me, group, batch, bridged, bridged_sems)
    swap_h = BridgedExchange(me, group, batch, bridged, again_sems)
    total = WeightSum(me, group, sums, got, grad_w, gw_sem)
    swap_d = Exchange(me, group, batch, send_d, recv_d, send_d_sem, recv_d_sem)
    share_a = Share(me, group, batch, share_send_a, message, coef_shared, share_a_sems)
    share_d = Share(me, group, batch, share_send_d, message, mixed_shared, share_d_sems)
    loading_far = far_tables(swap_g, p_inv, stage_far, far_sem)
    loading_far.start()
    loading_fwd = own_tables(me, group, p_fwd, stage, p_sem)
    loading_far_fwd = far_tables(swap_h, p_fwd, stage_far, far_sem)
    chunks = got.shape[0]
    clear_after(padded, used)
    meet(group)

    def build_planes():
        depth, per = w_in.shape[:2]
        blocks = degrees // per
        half = w_in.shape[2] // 2

        def fetch(k):
            return pltpu.make_async_copy(w_mix.at[pl.ds(k * per, per)], w_in.at[lax.rem(k, depth)], w_sem.at[lax.rem(k, depth)])

        for k in range(depth - 1):
            fetch(k).start()

        @pl.loop(0, blocks)
        def _(k):
            @pl.when(k + depth - 1 < blocks)
            def _():
                fetch(k + depth - 1).start()

            fetch(k).wait()
            for inner in range(per):
                rows = w_in.at[lax.rem(k, depth), inner]
                for part in range(2):
                    planes[k * per + inner, part] = rows[pl.ds(part, half, stride=2), :].astype(BF16)

    def unmix_bunch():
        @pl.loop(0, degrees // 8)
        def _(k):
            for inner in range(8):
                at = pl.ds(pl.multiple_of((k * 8 + inner) * m_local, m_local), m_local)
                rows = [back[:, part, at, :].reshape(bunch * m_local, channels) for part in range(2)]
                res = dot(jnp.concatenate(rows, axis=1).astype(BF16), mix_block(planes[k * 8 + inner]), NN)
                for part in range(2):
                    back[:, part, at, :] = res[:, part * channels:(part + 1) * channels].reshape(bunch, m_local, channels)

    def mix_bunch():
        @pl.loop(0, degrees // 8)
        def _(k):
            for inner in range(8):
                at = pl.ds(pl.multiple_of((k * 8 + inner) * m_local, m_local), m_local)
                rows = [coef[:, part, at, :].reshape(bunch * m_local, channels) for part in range(2)]
                res = dot(jnp.concatenate(rows, axis=1).astype(BF16), mix_block(planes[k * 8 + inner]), NT)
                for part in range(2):
                    mixed[:, part, at, :] = res[:, part * channels:(part + 1) * channels].reshape(bunch, m_local, channels)

    def weigh_sample(b):
        for copy in fetch_shares(b):
            copy.wait()
        for which in range(2):
            for source in range(sources):
                at = pl.ds(source * (shared.shape[1] // sources), share_rows)
                shared[which, at, :] = halves[lax.rem(b, 2), which, source].astype(F32)
        weigh(shared, sources, sums, m_local)

    def collect(b):
        share_a.arrive(b)
        share_d.arrive(b)
        for copy in fetch_shares(b):
            copy.start()

    lag_a, lag_b, lag_c, lag_d = 2, 4, 6, 8
    lag_e = batch + lag_c
    close = batch + lag_d
    steps = [total.reduce_step] + [functools.partial(total.gather_step, p) for p in (2, 1, 0, -1)]

    def advance(n, sub):
        @pl.when((n >= 0) & (n * 2 + sub + 4 < chunks))
        def _():
            total.halving(n * 2 + sub + 4).start()

        for late, step in reversed(list(enumerate(steps))):
            k = (n - late) * 2 + sub

            @pl.when((k >= 0) & (k < chunks))
            def _():
                step(k)

    def body(i, carry):
        @pl.when((i >= lag_e) & (i < batch + lag_e))
        def _():
            b = i - lag_e

            @pl.when(b + 1 < batch)
            def _():
                fetch_back(b + 1).start()

            fetch_back(b).wait()
            swap_h.reserve(b)
            legendre_inverse(coef.at[lax.rem(b, 2)], flipped, swap_h, lax.rem(b, SLOTS), rows_local)
            swap_h.start(b)

        @pl.when(i < batch)
        def _():
            @pl.when(i + 1 < batch)
            def _():
                fetch_field(i + 1).start()

            fetch_field(i).wait()
            half = lax.rem(i, 2)
            analyse(lambda t: read_row(field_buf, half, t, channels, rows_local), base, turn, rows_local)
            swap_f.reserve(i)
            pack_blocks(turn, send_f, lax.rem(i, SLOTS))
            swap_f.start(i)

        @pl.when(i == 0)
        def _():
            loading.wait()
            expand_rows(stage, expanded_fwd, rows_local)
            loading_inv.start()
            loading_far.wait()
            flip_rows(stage_far, swap_g.flipped_far)

        @pl.when(i == 1)
        def _():
            build_planes()
            loading_inv.wait()
            expand_rows(stage, expanded_inv, rows_local)
            flip_rows(stage, flipped)
            sums[...] = jnp.zeros_like(sums)

        @pl.when((i >= lag_a) & (i < batch + lag_a))
        def _():
            b = i - lag_a
            swap_f.arrive(b)
            legendre_forward(recv_f, b, expanded_fwd, padded, rows_local)
            coef[lax.rem(b, bunch)] = padded[:, pl.ds(0, used), :]
            share_a.give(b, padded)

            @pl.when(lax.rem(b, bunch) == bunch - 1)
            def _():
                mix_bunch()

        @pl.when((i >= lag_b) & (i < batch + lag_b))
        def _():
            b = i - lag_b
            swap_g.reserve(b)
            legendre_inverse(mixed.at[lax.rem(b, bunch)], flipped, swap_g, lax.rem(b, SLOTS), rows_local)
            swap_g.start(b)

        @pl.when((i >= lag_b + 1) & (i < batch + lag_b + 1))
        def _():
            swap_g.relay(i - lag_b - 1)

        @pl.when((i >= lag_c) & (i < batch + lag_c))
        def _():
            b = i - lag_c
            half = lax.rem(b, 2)

            @pl.when(b + 1 < batch)
            def _():
                fetch_grad(b + 1).start()

            fetch_grad(b).wait()
            swap_g.arrive(b)
            unpack_blocks(swap_g.recv, b, turn)
            for t in range(rows_local):
                slope = gelu_slope(synthesise(turn, t, gained, rows_local))
                given = read_row(grad_buf, half, t, channels, rows_local)
                write_row(grad_buf, half, t, channels, rows_local, given * slope)
            analyse(lambda t: read_row(grad_buf, half, t, channels, rows_local), gained, turn, rows_local)
            swap_d.reserve(b)
            pack_blocks(turn, send_d, lax.rem(b, SLOTS))
            swap_d.start(b)

        @pl.when(i == lag_e - 2)
        def _():
            loading_fwd.start()
            loading_far_fwd.start()

        @pl.when(i == lag_e - 1)
        def _():
            loading_fwd.wait()
            flip_rows(stage, flipped)
            loading_far_fwd.wait()
            flip_rows(stage_far, swap_h.flipped_far)
            swap_g.drain()
            fetch_back(0).start()

        @pl.when((i >= lag_d) & (i < batch + lag_d))
        def _():
            b = i - lag_d

            @pl.when((b >= bunch) & (lax.rem(b, bunch) == 0))
            def _():
                unmix_bunch()
                for n in range(bunch):
                    put(b - bunch + n).start()

            @pl.when(b >= 2)
            def _():
                weigh_sample(b - 2)

            @pl.when(b >= 1)
            def _():
                collect(b - 1)

            swap_d.arrive(b)
            legendre_forward(recv_d, b, expanded_inv, padded, rows_local)
            share_d.give(b, padded)

            @pl.when(b >= bunch)
            def _():
                put(b - bunch).wait()

            back[lax.rem(b, bunch)] = padded[:, pl.ds(0, used), :]

        @pl.when(i == close)
        def _():
            fetch_last(0).start()
            weigh_sample(batch - 2)
            collect(batch - 1)
            weigh_sample(batch - 1)
            for k in range(4):
                total.halving(k).start()

        advance(i - close, 0)

        @pl.when((i >= lag_e + 1) & (i < batch + lag_e + 1))
        def _():
            swap_h.relay(i - lag_e - 1)

        @pl.when((i >= close) & (i < batch + close))
        def _():
            b = i - close
            half = lax.rem(b, 2)

            @pl.when(b >= 1)
            def _():
                put_last(b - 1).wait()

            @pl.when(b + 1 < batch)
            def _():
                fetch_last(b + 1).start()

            fetch_last(b).wait()
            swap_h.arrive(b)
            unpack_blocks(swap_h.recv, b, turn)
            for t in range(rows_local):
                added = synthesise(turn, t, base, rows_local)
                given = read_row(field_buf, half, t, channels, rows_local)
                write_row(field_buf, half, t, channels, rows_local, given + added)
            put_last(b).start()

        @pl.when(i == close + 1)
        def _():
            unmix_bunch()
            for n in range(bunch):
                put(batch - bunch + n).start()

        @pl.when(i == close + 3)
        def _():
            for n in range(bunch):
                put(batch - bunch + n).wait()

        advance(i - close, 1)
        return carry

    lax.fori_loop(0, close + max(batch, chunks // 2 + 4), body, 0)
    for swap in (swap_f, swap_h, swap_d, share_a, share_d):
        swap.drain()
    put_last(batch - 1).wait()


def finish_kernel(first, second, first_out, second_out, first_ring, second_ring, in_sem, out_sem):
    depth = first_ring.shape[0]
    pieces = []
    for side, (source, target, ring) in enumerate(((first, first_out, first_ring), (second, second_out, second_ring))):
        for n in range(source.shape[0]):
            slot = n % depth
            take = pltpu.make_async_copy(source.at[n], ring.at[slot], in_sem.at[side, slot])
            give = pltpu.make_async_copy(ring.at[slot], target.at[n], out_sem.at[side, slot])
            pieces.append(((n, side), (side, n), take, give))
    pieces.sort(key=lambda piece: piece[0])
    given = {piece[1]: piece[3] for piece in pieces}
    waited = set()
    for k in range(len(pieces) + depth):
        if k < len(pieces):
            _, (side, n), take, _ = pieces[k]
            if n >= depth:
                given[side, n - depth].wait()
                waited.add((side, n - depth))
            take.start()
        if k >= depth:
            pieces[k - depth][2].wait()
            pieces[k - depth][3].start()
    for _, place, _, give in pieces:
        if place not in waited:
            give.wait()


def any_specs(n):
    return [pl.BlockSpec(memory_space=pl.ANY)] * n


def params(collective_id=None):
    if collective_id is None:
        return pltpu.CompilerParams(vmem_limit_bytes=VMEM_LIMIT)
    return pltpu.CompilerParams(collective_id=collective_id, has_side_effects=True, vmem_limit_bytes=VMEM_LIMIT)


def solution(mesh):
    group = mesh.shape['lat']
    field_spec = P('member', None, 'lat', None)

    def local_step(field_loc, grad_loc, p_fwd, p_inv, w_mix):
        batch, channels, rows_local, lon_count = field_loc.shape
        degrees, lats = p_fwd.shape[1:]
        m_local = p_fwd.shape[0] // group
        modes = group * m_local * 2
        base, gained = (two_halves(table) for table in dft_tables(group, m_local, lon_count))
        field = field_loc.reshape(batch, channels * rows_local, lon_count)
        grad = grad_loc.reshape(batch, channels * rows_local, lon_count)
        w_rows = jnp.swapaxes(w_mix, 2, 3).reshape(degrees, channels * 2, channels)
        dma, vmem = pltpu.SemaphoreType.DMA, pltpu.VMEM
        block_rows = m_local * 2 * rows_local
        coef_shape = (batch, 2, degrees * m_local, channels)
        send_t = vmem((SLOTS, group, block_rows, channels), BF16)
        recv_t = vmem((batch, group, block_rows, channels), BF16)
        turn_t = vmem((modes * rows_local, channels), F32)
        stage_t = vmem((m_local, degrees, lats), F32)
        expanded_t = vmem((m_local, 2 * degrees, 2 * lats), BF16)
        flipped_t = vmem((m_local, lats, degrees), BF16)
        field_t = vmem((2, lon_count // LANES, channels * rows_local, LANES), F32)
        table_spec = pl.BlockSpec(memory_space=pltpu.VMEM)
        any_spec = pl.BlockSpec(memory_space=pl.ANY)
        late = sum(degrees - slot * group < lats // 2 for slot in range(m_local))
        far_rows = sum(degrees - slot * group for slot in range(m_local - late, m_local))
        late_rows = late * 2 * rows_local
        bridged_t = (send_t, recv_t, vmem((SLOTS, 2, far_rows, channels), BF16), vmem((batch, 2, far_rows, channels), BF16),
                     vmem((SLOTS, group // 2, late_rows, channels), BF16), vmem((late, lats, degrees), BF16))
        bridged_sems = (dma((SLOTS,)), dma((batch,))) * 3

        ranks = group // 2
        share_rows = (m_local + 1) * 2 * ranks
        share_out = jax.ShapeDtypeStruct((batch, ranks, share_rows, channels), BF16)
        share_sems = (dma((SLOTS,)), dma((batch,)), dma((SLOTS,)))

        far_stage_t = vmem((late, degrees, lats), F32)
        steps = degrees // ranks
        sums_shape = (steps, channels * 2, channels)
        planes_shape = (degrees, 2, channels, channels)
        single_t = vmem((BUNCH,) + coef_shape[1:], F32)
        share_send_t = vmem((SLOTS, ranks, share_rows, channels), BF16)
        swap_sems = (dma((SLOTS,)), dma((batch,)))
        field_out, gw_total, _, _, _ = pl.pallas_call(
            functools.partial(whole_kernel, group, rows_local), name='whole',
            out_shape=[jax.ShapeDtypeStruct(grad.shape, F32),
                       jax.ShapeDtypeStruct((steps, ranks, channels * 2, channels), F32),
                       jax.ShapeDtypeStruct(coef_shape, F32), share_out, share_out],
            in_specs=[any_spec, any_spec, table_spec, table_spec, any_spec, any_spec, any_spec], out_specs=[any_spec] * 5,
            scratch_shapes=[field_t, field_t, turn_t, stage_t, far_stage_t, expanded_t, expanded_t, flipped_t, send_t, recv_t,
                            vmem((2, 2 * degrees * m_local, channels), F32), single_t, single_t,
                            vmem((4, 4, channels * 2, channels), F32), vmem(planes_shape, BF16), bridged_t, send_t, recv_t,
                            vmem((ranks, share_rows, channels), F32), share_send_t, share_send_t,
                            vmem((2, 2) + share_out.shape[1:], BF16), vmem((2, ranks * (share_rows + 8), channels), F32),
                            vmem(sums_shape, F32), single_t, vmem((PIECES * steps // 2, channels * 2 // PIECES, channels), F32),
                            dma((2, 2)), dma((2, 2)), dma(()), dma(()), *swap_sems, dma((4,)), bridged_sems, *swap_sems,
                            share_sems, share_sems, dma((2, 2)), dma((BUNCH,)), dma((2, 6, PIECES * steps // 2)), bridged_sems,
                            dma((2,)), dma((2, 2))],
            compiler_params=params(0))(field, grad, base, gained, p_fwd, p_inv, w_rows)

        gw_total = gw_total.reshape(steps, ranks * channels * 2, channels)
        results = [jax.ShapeDtypeStruct(whole.shape, F32) for whole in (field_out, gw_total)]
        field_out, gw_total = pl.pallas_call(
            finish_kernel, name='finish', out_shape=results, in_specs=[any_spec] * 2, out_specs=[any_spec] * 2,
            scratch_shapes=[vmem((RING,) + whole.shape[1:], F32) for whole in results] + [dma((2, RING)), dma((2, RING))],
            compiler_params=params())(field_out, gw_total)

        grad_wmix = jnp.swapaxes(gw_total.reshape(degrees, channels, 2, channels), 2, 3)
        return field_out.reshape(grad_loc.shape), grad_wmix

    return jax.shard_map(local_step, mesh=mesh, in_specs=(field_spec, field_spec, P(), P(), P()),
                         out_specs=(field_spec, P('member', None, None, None)), check_vma=False)
```

```python
import functools
import math

import jax
import jax.numpy as jnp
import numpy as np
from jax import lax
from jax.experimental import pallas as pl
from jax.experimental.pallas import tpu as pltpu
from jax.sharding import PartitionSpec as P

MESH = pl.DeviceIdType.MESH
LANES = 128
SLOTS = 3
BUNCH = 3
PIECES = 2
RING = 6
VMEM_LIMIT = 67043328
F32 = jnp.float32
BF16 = jnp.bfloat16

NN = (((1,), (0,)), ((), ()))
NT = (((1,), (1,)), ((), ()))
TN = (((0,), (0,)), ((), ()))


def dot(lhs, rhs, dims):
    return lax.dot_general(lhs, rhs, dims, preferred_element_type=F32)


def split_halves(values):
    high = values.astype(BF16)
    low = (values - high.astype(F32)).astype(BF16)
    return high, low


def dft_tables(group, m_local, lon_count):
    owner, slot, part = np.meshgrid(np.arange(group), np.arange(m_local), np.arange(2), indexing='ij')
    wave = (slot * group + owner).reshape(-1)
    part = part.reshape(-1)
    phase = 2.0 * np.pi * ((wave[:, None] * np.arange(lon_count)[None, :]) % lon_count) / lon_count
    base = np.where(part[:, None] == 0, np.cos(phase), -np.sin(phase)) / math.sqrt(lon_count)
    gains = np.where(wave == 0, 1.0, 2.0)[:, None]
    return base.astype(np.float32), (base * gains).astype(np.float32)


def two_halves(table):
    high = jnp.asarray(table).astype(BF16)
    low = (jnp.asarray(table) - high.astype(F32)).astype(BF16)
    return jnp.stack([high, low])


class Halves:
    def __init__(self, whole, b, halves, slot, sem, outward=False):
        self.copies = []
        for half in range(halves.shape[1]):
            ends = whole.at[b, :, pl.ds(half * LANES, LANES)], halves.at[slot, half]
            source, target = ends[::-1] if outward else ends
            self.copies.append(pltpu.make_async_copy(source, target, sem.at[slot, half]))

    def start(self):
        for copy in self.copies:
            copy.start()

    def wait(self):
        for copy in self.copies:
            copy.wait()


def read_row(halves, slot, t, channels, rows_local):
    at = pl.ds(t, channels, stride=rows_local)
    return jnp.concatenate([halves[slot, half, at, :] for half in range(halves.shape[1])], axis=1)


def write_row(halves, slot, t, channels, rows_local, values):
    at = pl.ds(t, channels, stride=rows_local)
    for half in range(halves.shape[1]):
        halves[slot, half, at, :] = values[:, half * LANES:(half + 1) * LANES]


class Exchange:
    def __init__(self, me, group, batch, send, recv, send_sem, recv_sem):
        self.me, self.group, self.batch = me, group, batch
        self.send, self.recv, self.send_sem, self.recv_sem = send, recv, send_sem, recv_sem

    def all_copies(self, b):
        slot = lax.rem(b, SLOTS)
        others = pl.ds(0, self.group - 1)
        return pltpu.make_async_remote_copy(
            self.send.at[slot, others], self.recv.at[b, others], self.send_sem.at[slot], self.recv_sem.at[b],
            device_id={'lat': lax.rem(self.me + 1, self.group)}, device_id_type=MESH)

    def reserve(self, b):
        @pl.when(b >= SLOTS)
        def _():
            self.all_copies(b - SLOTS).wait_send()

    def start(self, b):
        slot = lax.rem(b, SLOTS)
        self.recv[b, self.me] = self.send[slot, self.me]

        @pl.loop(1, self.group)
        def _(step):
            target = jnp.bitwise_xor(self.me, self.group - step)
            pltpu.make_async_remote_copy(
                self.send.at[slot, target], self.recv.at[b, self.me], self.send_sem.at[slot], self.recv_sem.at[b],
                device_id={'lat': target}, device_id_type=MESH).start()

    def arrive(self, b):
        self.all_copies(b).wait_recv()

    def drain(self):
        for b in range(max(0, self.batch - SLOTS), self.batch):
            self.all_copies(b).wait_send()


class BridgedExchange:
    def __init__(self, me, group, batch, bufs, sems):
        self.me, self.group, self.batch = me, group, batch
        self.send, self.recv, self.bridge_send, self.bridge_recv, self.relay_send, self.flipped_far = bufs
        self.send_sem, self.recv_sem, self.bridge_send_sem, self.bridge_recv_sem, self.relay_send_sem, self.relay_recv_sem = sems
        self.half_size = group // 2
        self.half = me // self.half_size
        self.place = lax.rem(me, self.half_size)
        self.twin = self.half_size + me - 2 * self.half_size * self.half
        self.rows = self.send.shape[2]
        self.late_rows = self.relay_send.shape[2]
        self.early_rows = self.rows - self.late_rows
        self.tile = self.late_rows // self.flipped_far.shape[0]
        self.direct = self.early_rows // self.tile

    def copy(self, source, target, send_sem, recv_sem, device):
        return pltpu.make_async_remote_copy(source, target, send_sem, recv_sem, device_id={'lat': device},
                                            device_id_type=MESH)

    def all_direct(self, b):
        slot = lax.rem(b, SLOTS)
        count = (self.half_size - 1) * self.rows + self.half_size * self.early_rows
        span = pl.ds(0, count // self.rows)
        return self.copy(self.send.at[slot, span], self.recv.at[b, span], self.send_sem.at[slot], self.recv_sem.at[b], self.twin)

    def all_relayed(self, b):
        slot = lax.rem(b, SLOTS)
        span, part = pl.ds(0, self.half_size - 1), pl.ds(0, self.late_rows)
        return self.copy(self.relay_send.at[slot, span], self.recv.at[b, span, part], self.relay_send_sem.at[slot],
                         self.relay_recv_sem.at[b], self.twin)

    def bridge(self, b):
        slot = lax.rem(b, SLOTS)
        return self.copy(self.bridge_send.at[slot], self.bridge_recv.at[b], self.bridge_send_sem.at[slot],
                         self.bridge_recv_sem.at[b], self.twin)

    def reserve(self, b):
        @pl.when(b >= SLOTS)
        def _():
            self.all_direct(b - SLOTS).wait_send()
            self.bridge(b - SLOTS).wait_send()

    def start(self, b):
        slot = lax.rem(b, SLOTS)
        self.bridge(b).start()
        early = pl.ds(0, self.early_rows)

        @pl.loop(0, self.half_size)
        def _(step):
            target = jnp.bitwise_xor(self.me, 2 * self.half_size - 1 - step)
            self.copy(self.send.at[slot, target, early], self.recv.at[b, self.me, early], self.send_sem.at[slot],
                      self.recv_sem.at[b], target).start()

        @pl.loop(1, self.half_size)
        def _(step):
            target = jnp.bitwise_xor(self.me, self.half_size - step)
            self.copy(self.send.at[slot, target], self.recv.at[b, self.me], self.send_sem.at[slot], self.recv_sem.at[b],
                      target).start()

        self.recv[b, self.me] = self.send[slot, self.me]

    def relay(self, b):
        slot = lax.rem(b, SLOTS)

        @pl.when(b >= SLOTS)
        def _():
            self.all_relayed(b - SLOTS).wait_send()

        self.bridge(b).wait_recv()
        lats, degrees = self.flipped_far.shape[1:]
        own = pl.ds(pl.multiple_of(self.half * (lats // 2), lats // 2), lats // 2)
        at = 0
        for late in range(self.flipped_far.shape[0]):
            first = (self.direct + late) * self.group
            count = degrees - first
            parts = []
            for part in range(2):
                rows = self.bridge_recv[b, part, pl.ds(at, count), :]
                parts.append(jnp.concatenate([jnp.zeros((first, rows.shape[1]), BF16), rows], axis=0))
            at += count
            res = dot(self.flipped_far[late, own, :], jnp.concatenate(parts, axis=1), NN)
            lanes = res.shape[1] // 2
            blocks = [res[:, part * lanes:(part + 1) * lanes].reshape(self.half_size, self.tile // 2, lanes) for part in range(2)]
            self.relay_send[slot, :, pl.ds(late * self.tile, self.tile), :] = jnp.concatenate(blocks, axis=1).astype(BF16)
        late_at = pl.ds(self.early_rows, self.late_rows)

        @pl.loop(1, self.half_size)
        def _(step):
            place = jnp.bitwise_xor(self.place, self.half_size - step)
            self.copy(self.relay_send.at[slot, place], self.recv.at[b, self.twin, late_at], self.relay_send_sem.at[slot],
                      self.relay_recv_sem.at[b], self.half * self.half_size + place).start()

        self.recv[b, self.twin, late_at] = self.relay_send[slot, self.place]

    def arrive(self, b):
        self.all_direct(b).wait_recv()
        self.all_relayed(b).wait_recv()

    def drain(self):
        for b in range(max(0, self.batch - SLOTS), self.batch):
            self.all_direct(b).wait_send()
            self.bridge(b).wait_send()
            self.all_relayed(b).wait_send()


class Share:
    def __init__(self, me, group, batch, send, message, out, sems):
        self.batch, self.send, self.message, self.out = batch, send, message, out
        self.send_sem, self.recv_sem, self.local_sem = sems
        self.size = group // 2
        self.base = me // self.size * self.size
        self.place = lax.rem(me, self.size)

    def rank(self, place):
        return place // 4 + 2 * (lax.rem(place, 4) // 2) + 4 * lax.rem(place, 2)

    def copy(self, slot, source, b, target, place):
        return pltpu.make_async_remote_copy(
            self.send.at[slot, source], self.out.at[b, target], self.send_sem.at[slot], self.recv_sem.at[b],
            device_id={'lat': self.base + place}, device_id_type=MESH)

    def every(self, b):
        span = pl.ds(0, self.size - 1)
        return self.copy(lax.rem(b, SLOTS), span, b, span, lax.rem(self.place + 1, self.size))

    def keep(self, b):
        slot = lax.rem(b, SLOTS)
        return pltpu.make_async_copy(self.send.at[slot, self.rank(self.place)], self.out.at[b, self.place],
                                     self.local_sem.at[slot])

    def give(self, b, coef):
        slot_b = lax.rem(b, SLOTS)

        @pl.when(b >= SLOTS)
        def _():
            self.every(b - SLOTS).wait_send()

        size = self.size
        m_local = size
        tile = 2 * size

        def rows(part, slot, rank, first, count):
            return coef[part, pl.ds((first * size + rank) * m_local + slot, count, stride=size * m_local), :]

        for rank in range(size):
            for part in range(2):
                for pair in range(m_local // 2):
                    block = rows(part, pair, rank, 0, tile)
                    if pair:
                        block = block + rows(part, m_local - pair, rank, 2 * (m_local - pair), tile)
                    self.message[rank, pl.ds((part * (m_local // 2) + pair) * tile, tile), :] = block
                self.message[rank, pl.ds(m_local * tile + part * size, size), :] = rows(part, m_local // 2, rank, size, size)
        for rank in range(size):
            self.send[slot_b, rank] = self.message[rank].astype(BF16)
        self.keep(b).start()

        @pl.loop(1, size)
        def _(step):
            place = jnp.bitwise_xor(self.place, size - step)
            self.copy(slot_b, self.rank(place), b, self.place, place).start()

        self.keep(b).wait()

    def drain(self):
        for b in range(max(0, self.batch - SLOTS), self.batch):
            self.every(b).wait_send()

    def arrive(self, b):
        self.every(b).wait_recv()


def clear_after(coef, used):
    for part in range(coef.shape[0]):
        coef[part, pl.ds(used, coef.shape[1] - used), :] = jnp.zeros((coef.shape[1] - used, coef.shape[2]), F32)


def greet(me, group):
    barrier = pltpu.get_barrier_semaphore()

    @pl.loop(1, group)
    def _(step):
        pl.semaphore_signal(barrier, inc=1, device_id={'lat': lax.rem(me + step, group)}, device_id_type=MESH)


def meet(group):
    pl.semaphore_wait(pltpu.get_barrier_semaphore(), group - 1)


class Tables:
    def __init__(self, waves, whole, stage, sem):
        self.waves, self.whole, self.stage, self.sem = waves, whole, stage, sem

    def start(self):
        for n, wave in enumerate(self.waves):
            pltpu.make_async_copy(self.whole.at[wave], self.stage.at[n], self.sem).start()

    def wait(self):
        pltpu.make_async_copy(self.whole.at[pl.ds(0, len(self.waves))], self.stage, self.sem).wait()


def own_tables(me, group, whole, stage, sem):
    return Tables([slot * group + me for slot in range(stage.shape[0])], whole, stage, sem)


def far_tables(swap, whole, stage, sem):
    return Tables([(swap.direct + n) * swap.group + swap.twin for n in range(stage.shape[0])], whole, stage, sem)


def expand_rows(stage, expanded, rows_local):
    m_local, degrees, lats = stage.shape
    row = lax.broadcasted_iota(jnp.int32, (lats, 2 * lats), 0)
    col = lax.broadcasted_iota(jnp.int32, (lats, 2 * lats), 1)
    source = col // (2 * rows_local)
    inner = col % (2 * rows_local)
    for part in range(2):
        pick = (row == source * rows_local + inner - part * rows_local) & (inner // rows_local == part)
        pick = pick.astype(F32).astype(BF16)
        for slot in range(m_local):
            expanded[slot, pl.ds(part * degrees, degrees), :] = dot(stage[slot].astype(BF16), pick, NN).astype(BF16)


def flip_rows(stage, flipped):
    for slot in range(stage.shape[0]):
        flipped[slot] = stage[slot].T.astype(BF16)


def analyse(values_at, table, turn, rows_local):
    modes = table.shape[1]
    for t in range(0, rows_local, 2):
        pair = jnp.concatenate([values_at(t), values_at(t + 1)], axis=0)
        high, low = split_halves(pair * 0.5)
        out = 2.0 * (dot(table[0], high, NT) + dot(table[0], low, NT) + dot(table[1], high, NT))
        channels = out.shape[1] // 2
        turn[pl.ds(t, modes, stride=rows_local), :] = out[:, :channels]
        turn[pl.ds(t + 1, modes, stride=rows_local), :] = out[:, channels:]


def pack_blocks(turn, send, slot):
    group, rows, lanes = send.shape[1:]
    for d in range(group):
        send[slot, d] = turn[pl.ds(d * rows, rows), :].astype(BF16)


def unpack_blocks(recv, b, turn):
    group, rows, lanes = recv.shape[1:]
    for d in range(group):
        turn[pl.ds(d * rows, rows), :] = recv[b, d].astype(F32)


def synthesise(turn, t, table, rows_local):
    modes = table.shape[1]
    spec = turn[pl.ds(t, modes, stride=rows_local), :].astype(BF16)
    return dot(spec, table[0], TN) + dot(spec, table[1], TN)


def legendre_forward(recv, b, expanded, out, rows_local):
    m_local = expanded.shape[0]
    degrees = expanded.shape[1] // 2
    group, _, lanes = recv.shape[1:]
    tile = 2 * rows_local
    for slot in range(m_local):
        rows = recv[b, :, pl.ds(slot * tile, tile), :].reshape(group * tile, lanes)
        res = dot(expanded[slot], rows, NN)
        for part in range(2):
            out[part, pl.ds(slot, degrees, stride=m_local), :] = res[part * degrees:(part + 1) * degrees]


def legendre_inverse(coef, flipped, swap, slot_out, rows_local):
    m_local, lats, degrees = flipped.shape
    send = swap.send
    at = 0
    group = lats // rows_local
    tile = 2 * rows_local
    for slot in range(m_local):
        parts = [coef.at[part][pl.ds(slot, degrees, stride=m_local), :].astype(BF16) for part in range(2)]
        if slot >= swap.direct:
            first = slot * group
            for part in range(2):
                swap.bridge_send[slot_out, part, pl.ds(at, degrees - first), :] = parts[part][first:]
            at += degrees - first
        res = dot(flipped[slot], jnp.concatenate(parts, axis=1), NN)
        lanes = res.shape[1] // 2
        blocks = [res[:, part * lanes:(part + 1) * lanes].reshape(group, rows_local, lanes) for part in range(2)]
        send[slot_out, :, pl.ds(slot * tile, tile), :] = jnp.concatenate(blocks, axis=1).astype(BF16)


def gelu_slope(values):
    cumulative = 0.5 * (1.0 + lax.erf(values * math.sqrt(0.5)))
    density = jnp.exp(-0.5 * values * values) * (1.0 / math.sqrt(2.0 * math.pi))
    return cumulative + values * density


def mix_block(planes):
    real, imag = planes[0], planes[1]
    return jnp.concatenate([jnp.concatenate([real, -imag], axis=1), jnp.concatenate([imag, real], axis=1)], axis=0)


class WeightSum:
    def __init__(self, me, group, sums, got, out, sems):
        self.me, self.sums, self.got, self.out, self.sems = me, sums, got, out, sems
        self.core, self.y = lax.rem(me, 2), lax.rem(me // 2, 2)
        self.near, self.far = lax.rem(me // 4, 2), me // (group // 2)
        self.rank = self.near + 2 * self.y + 4 * self.core

    def peer(self, phase):
        step = (1, 2, 4, 8)[phase]
        bit = (self.core, self.y, self.near, self.far)[phase]
        return {'lat': self.me + step - 2 * step * bit}

    def remote(self, phase, k, source, target, stage):
        return pltpu.make_async_remote_copy(source, target, self.sems.at[0, stage, k], self.sems.at[1, stage, k],
                                            device_id=self.peer(phase), device_id_type=MESH)

    def halving(self, k):
        pair, at = self.piece(k)
        return self.remote(3, k, self.sums.at[2 * pair + 1 - self.far, at], self.got.at[k], 4)

    def piece(self, k):
        rows = self.got.shape[1]
        pieces = self.sums.shape[1] // rows
        return k // pieces, pl.ds(pl.multiple_of(lax.rem(k, pieces) * rows, rows), rows)

    def settle(self, k):
        pair, at = self.piece(k)
        mine = 2 * pair + self.far
        return pltpu.make_async_copy(self.sums.at[mine, at], self.out.at[mine, self.rank, at], self.sems.at[0, 5, k])

    def doubling(self, phase, k):
        pair, at = self.piece(k)
        if phase == 3:
            mine = 2 * pair + self.far
            return self.remote(3, k, self.sums.at[mine, at], self.out.at[mine, self.rank, at], 3)
        width = (4, 2, 1)[phase]
        first = (4 * self.core, 4 * self.core + 2 * self.y, self.rank)[phase]
        span = self.out.at[pl.ds(2 * pair, 2), pl.ds(first, width), at]
        return self.remote(phase, k, span, span, phase)

    def reduce_step(self, k):
        self.halving(k).wait()
        pair, at = self.piece(k)
        mine = 2 * pair + self.far
        self.sums[mine, at] = self.sums[mine, at] + self.got[k]
        self.settle(k).start()
        self.doubling(3, k).start()

    def gather_step(self, phase, k):
        if phase == 2:
            self.settle(k).wait()
        self.doubling(phase + 1, k).wait()
        if phase >= 0:
            self.doubling(phase, k).start()


def shared_place(part, slot, step, m_local):
    tile = 2 * m_local
    if slot == m_local // 2:
        return m_local * tile + part * m_local + step - m_local
    pair = min(slot, m_local - slot) if slot else 0
    shift = 0 if slot < m_local // 2 else 2 * slot
    return (part * (m_local // 2) + pair) * tile + step - shift


def weigh(shared, sources, sums, m_local):
    stride = shared.shape[1] // sources

    @pl.loop(0, sums.shape[0])
    def _(step):
        sides = []
        for which in range(2):
            slots = []
            for slot in range(m_local):
                used = step >= 2 * slot
                parts = []
                for part in range(2):
                    place = jnp.where(used, shared_place(part, slot, step, m_local), 0)
                    rows = shared[which, pl.ds(place, sources, stride=stride), :]
                    parts.append(jnp.where(used, rows, 0.0))
                slots.append(jnp.concatenate(parts, axis=1))
            sides.append(jnp.concatenate(slots, axis=0).astype(BF16))
        big = dot(sides[0], sides[1], TN)
        half = big.shape[0] // 2
        real, imag = pl.ds(0, half, stride=2), pl.ds(1, half, stride=2)
        sums[step, real, :] = sums[step, real, :] + (big[:half, :half] + big[half:, half:])
        sums[step, imag, :] = sums[step, imag, :] + (big[half:, :half] - big[:half, half:])


def whole_kernel(group, rows_local, field, grad, base, gained, p_fwd, p_inv, w_mix, field_out, grad_w, back_out, coef_shared,
                 mixed_shared, field_buf, grad_buf, turn, stage, stage_far, expanded_fwd, expanded_inv, flipped, send_f, recv_f,
                 padded, coef, mixed, w_in, planes, bridged, send_d, recv_d, message, share_send_a, share_send_d, halves,
                 shared, sums, back, got, field_sem, grad_sem, p_sem, far_sem, send_f_sem, recv_f_sem, w_sem, bridged_sems,
                 send_d_sem, recv_d_sem, share_a_sems, share_d_sems, half_sem, out_sem, gw_sem, again_sems, back_sem, last_sem):
    me = lax.axis_index('lat')
    batch = field.shape[0]
    channels = field.shape[1] // rows_local
    m_local, degrees = stage.shape[:2]
    used = degrees * m_local
    bunch = coef.shape[0]
    sources, share_rows = coef_shared.shape[1:3]

    def fetch_field(b):
        return Halves(field, b, field_buf, lax.rem(b, 2), field_sem)

    def fetch_grad(b):
        return Halves(grad, b, grad_buf, lax.rem(b, 2), grad_sem)

    def put(b):
        return pltpu.make_async_copy(back.at[lax.rem(b, bunch)], back_out.at[b], out_sem.at[lax.rem(b, bunch)])

    def fetch_back(b):
        return pltpu.make_async_copy(back_out.at[b], coef.at[lax.rem(b, 2)], back_sem.at[lax.rem(b, 2)])

    def fetch_last(b):
        return Halves(grad, b, field_buf, lax.rem(b, 2), field_sem)

    def put_last(b):
        return Halves(field_out, b, field_buf, lax.rem(b, 2), last_sem, outward=True)

    def fetch_shares(b):
        slot = lax.rem(b, 2)
        return [pltpu.make_async_copy(whole.at[b], halves.at[slot, which], half_sem.at[slot, which])
                for which, whole in enumerate((mixed_shared, coef_shared))]

    greet(me, group)
    fetch_field(0).start()
    fetch_grad(0).start()
    loading = own_tables(me, group, p_fwd, stage, p_sem)
    loading_inv = own_tables(me, group, p_inv, stage, p_sem)
    loading.start()
    swap_f = Exchange(me, group, batch, send_f, recv_f, send_f_sem, recv_f_sem)
    swap_g = BridgedExchange(me, group, batch, bridged, bridged_sems)
    swap_h = BridgedExchange(me, group, batch, bridged, again_sems)
    total = WeightSum(me, group, sums, got, grad_w, gw_sem)
    swap_d = Exchange(me, group, batch, send_d, recv_d, send_d_sem, recv_d_sem)
    share_a = Share(me, group, batch, share_send_a, message, coef_shared, share_a_sems)
    share_d = Share(me, group, batch, share_send_d, message, mixed_shared, share_d_sems)
    loading_far = far_tables(swap_g, p_inv, stage_far, far_sem)
    loading_far.start()
    loading_fwd = own_tables(me, group, p_fwd, stage, p_sem)
    loading_far_fwd = far_tables(swap_h, p_fwd, stage_far, far_sem)
    chunks = got.shape[0]
    clear_after(padded, used)
    meet(group)

    def build_planes():
        depth, per = w_in.shape[:2]
        blocks = degrees // per
        half = w_in.shape[2] // 2

        def fetch(k):
            return pltpu.make_async_copy(w_mix.at[pl.ds(k * per, per)], w_in.at[lax.rem(k, depth)], w_sem.at[lax.rem(k, depth)])

        for k in range(depth - 1):
            fetch(k).start()

        @pl.loop(0, blocks)
        def _(k):
            @pl.when(k + depth - 1 < blocks)
            def _():
                fetch(k + depth - 1).start()

            fetch(k).wait()
            for inner in range(per):
                rows = w_in.at[lax.rem(k, depth), inner]
                for part in range(2):
                    planes[k * per + inner, part] = rows[pl.ds(part, half, stride=2), :].astype(BF16)

    def unmix_bunch():
        @pl.loop(0, degrees // 8)
        def _(k):
            for inner in range(8):
                at = pl.ds(pl.multiple_of((k * 8 + inner) * m_local, m_local), m_local)
                rows = [back[:, part, at, :].reshape(bunch * m_local, channels) for part in range(2)]
                res = dot(jnp.concatenate(rows, axis=1).astype(BF16), mix_block(planes[k * 8 + inner]), NN)
                for part in range(2):
                    back[:, part, at, :] = res[:, part * channels:(part + 1) * channels].reshape(bunch, m_local, channels)

    def mix_bunch():
        @pl.loop(0, degrees // 8)
        def _(k):
            for inner in range(8):
                at = pl.ds(pl.multiple_of((k * 8 + inner) * m_local, m_local), m_local)
                rows = [coef[:, part, at, :].reshape(bunch * m_local, channels) for part in range(2)]
                res = dot(jnp.concatenate(rows, axis=1).astype(BF16), mix_block(planes[k * 8 + inner]), NT)
                for part in range(2):
                    mixed[:, part, at, :] = res[:, part * channels:(part + 1) * channels].reshape(bunch, m_local, channels)

    def weigh_sample(b):
        for copy in fetch_shares(b):
            copy.wait()
        for which in range(2):
            for source in range(sources):
                at = pl.ds(source * (shared.shape[1] // sources), share_rows)
                shared[which, at, :] = halves[lax.rem(b, 2), which, source].astype(F32)
        weigh(shared, sources, sums, m_local)

    def collect(b):
        share_a.arrive(b)
        share_d.arrive(b)
        for copy in fetch_shares(b):
            copy.start()

    lag_a, lag_b, lag_c, lag_d = 2, 4, 6, 8
    lag_e = batch + lag_c
    close = batch + lag_d
    steps = [total.reduce_step] + [functools.partial(total.gather_step, p) for p in (2, 1, 0, -1)]

    def advance(n, sub):
        @pl.when((n >= 0) & (n * 2 + sub + 2 < chunks))
        def _():
            total.halving(n * 2 + sub + 2).start()

        for late, step in reversed(list(enumerate(steps))):
            k = (n - late) * 2 + sub

            @pl.when((k >= 0) & (k < chunks))
            def _():
                step(k)

    def body(i, carry):
        @pl.when((i >= lag_e) & (i < batch + lag_e))
        def _():
            b = i - lag_e

            @pl.when(b + 1 < batch)
            def _():
                fetch_back(b + 1).start()

            fetch_back(b).wait()
            swap_h.reserve(b)
            legendre_inverse(coef.at[lax.rem(b, 2)], flipped, swap_h, lax.rem(b, SLOTS), rows_local)
            swap_h.start(b)

        @pl.when(i < batch)
        def _():
            @pl.when(i + 1 < batch)
            def _():
                fetch_field(i + 1).start()

            fetch_field(i).wait()
            half = lax.rem(i, 2)
            analyse(lambda t: read_row(field_buf, half, t, channels, rows_local), base, turn, rows_local)
            swap_f.reserve(i)
            pack_blocks(turn, send_f, lax.rem(i, SLOTS))
            swap_f.start(i)

        @pl.when(i == 0)
        def _():
            loading.wait()
            expand_rows(stage, expanded_fwd, rows_local)
            loading_inv.start()
            loading_far.wait()
            flip_rows(stage_far, swap_g.flipped_far)

        @pl.when(i == 1)
        def _():
            build_planes()
            loading_inv.wait()
            expand_rows(stage, expanded_inv, rows_local)
            flip_rows(stage, flipped)
            sums[...] = jnp.zeros_like(sums)

        @pl.when((i >= lag_a) & (i < batch + lag_a))
        def _():
            b = i - lag_a
            swap_f.arrive(b)
            legendre_forward(recv_f, b, expanded_fwd, padded, rows_local)
            coef[lax.rem(b, bunch)] = padded[:, pl.ds(0, used), :]
            share_a.give(b, padded)

            @pl.when(lax.rem(b, bunch) == bunch - 1)
            def _():
                mix_bunch()

        @pl.when((i >= lag_b) & (i < batch + lag_b))
        def _():
            b = i - lag_b
            swap_g.reserve(b)
            legendre_inverse(mixed.at[lax.rem(b, bunch)], flipped, swap_g, lax.rem(b, SLOTS), rows_local)
            swap_g.start(b)

        @pl.when((i >= lag_b + 1) & (i < batch + lag_b + 1))
        def _():
            swap_g.relay(i - lag_b - 1)

        @pl.when((i >= lag_c) & (i < batch + lag_c))
        def _():
            b = i - lag_c
            half = lax.rem(b, 2)

            @pl.when(b + 1 < batch)
            def _():
                fetch_grad(b + 1).start()

            fetch_grad(b).wait()
            swap_g.arrive(b)
            unpack_blocks(swap_g.recv, b, turn)
            for t in range(rows_local):
                slope = gelu_slope(synthesise(turn, t, gained, rows_local))
                given = read_row(grad_buf, half, t, channels, rows_local)
                write_row(grad_buf, half, t, channels, rows_local, given * slope)
            analyse(lambda t: read_row(grad_buf, half, t, channels, rows_local), gained, turn, rows_local)
            swap_d.reserve(b)
            pack_blocks(turn, send_d, lax.rem(b, SLOTS))
            swap_d.start(b)

        @pl.when(i == lag_e - 2)
        def _():
            loading_fwd.start()
            loading_far_fwd.start()

        @pl.when(i == lag_e - 1)
        def _():
            loading_fwd.wait()
            flip_rows(stage, flipped)
            loading_far_fwd.wait()
            flip_rows(stage_far, swap_h.flipped_far)
            swap_g.drain()
            fetch_back(0).start()

        @pl.when((i >= lag_d) & (i < batch + lag_d))
        def _():
            b = i - lag_d

            @pl.when((b >= bunch) & (lax.rem(b, bunch) == 0))
            def _():
                unmix_bunch()
                for n in range(bunch):
                    put(b - bunch + n).start()

            @pl.when(b >= 2)
            def _():
                weigh_sample(b - 2)

            @pl.when(b >= 1)
            def _():
                collect(b - 1)

            swap_d.arrive(b)
            legendre_forward(recv_d, b, expanded_inv, padded, rows_local)
            share_d.give(b, padded)

            @pl.when(b >= bunch)
            def _():
                put(b - bunch).wait()

            back[lax.rem(b, bunch)] = padded[:, pl.ds(0, used), :]

        @pl.when(i == close)
        def _():
            fetch_last(0).start()
            weigh_sample(batch - 2)
            collect(batch - 1)
            weigh_sample(batch - 1)
            for k in range(2):
                total.halving(k).start()

        advance(i - close, 0)

        @pl.when((i >= lag_e + 1) & (i < batch + lag_e + 1))
        def _():
            swap_h.relay(i - lag_e - 1)

        @pl.when((i >= close) & (i < batch + close))
        def _():
            b = i - close
            half = lax.rem(b, 2)

            @pl.when(b >= 1)
            def _():
                put_last(b - 1).wait()

            @pl.when(b + 1 < batch)
            def _():
                fetch_last(b + 1).start()

            fetch_last(b).wait()
            swap_h.arrive(b)
            unpack_blocks(swap_h.recv, b, turn)
            for t in range(rows_local):
                added = synthesise(turn, t, base, rows_local)
                given = read_row(field_buf, half, t, channels, rows_local)
                write_row(field_buf, half, t, channels, rows_local, given + added)
            put_last(b).start()

        @pl.when(i == close + 1)
        def _():
            unmix_bunch()
            for n in range(bunch):
                put(batch - bunch + n).start()

        @pl.when(i == close + 3)
        def _():
            for n in range(bunch):
                put(batch - bunch + n).wait()

        advance(i - close, 1)
        return carry

    lax.fori_loop(0, close + max(batch, chunks // 2 + 4), body, 0)
    for swap in (swap_f, swap_h, swap_d, share_a, share_d):
        swap.drain()
    put_last(batch - 1).wait()


def finish_kernel(first, second, first_out, second_out, first_ring, second_ring, in_sem, out_sem):
    depth = first_ring.shape[0]
    pieces = []
    for side, (source, target, ring) in enumerate(((first, first_out, first_ring), (second, second_out, second_ring))):
        for n in range(source.shape[0]):
            slot = n % depth
            take = pltpu.make_async_copy(source.at[n], ring.at[slot], in_sem.at[side, slot])
            give = pltpu.make_async_copy(ring.at[slot], target.at[n], out_sem.at[side, slot])
            pieces.append(((n, side), (side, n), take, give))
    pieces.sort(key=lambda piece: piece[0])
    given = {piece[1]: piece[3] for piece in pieces}
    waited = set()
    for k in range(len(pieces) + depth):
        if k < len(pieces):
            _, (side, n), take, _ = pieces[k]
            if n >= depth:
                given[side, n - depth].wait()
                waited.add((side, n - depth))
            take.start()
        if k >= depth:
            pieces[k - depth][2].wait()
            pieces[k - depth][3].start()
    for _, place, _, give in pieces:
        if place not in waited:
            give.wait()


def any_specs(n):
    return [pl.BlockSpec(memory_space=pl.ANY)] * n


def params(collective_id=None):
    if collective_id is None:
        return pltpu.CompilerParams(vmem_limit_bytes=VMEM_LIMIT)
    return pltpu.CompilerParams(collective_id=collective_id, has_side_effects=True, vmem_limit_bytes=VMEM_LIMIT)


def solution(mesh):
    group = mesh.shape['lat']
    field_spec = P('member', None, 'lat', None)

    def local_step(field_loc, grad_loc, p_fwd, p_inv, w_mix):
        batch, channels, rows_local, lon_count = field_loc.shape
        degrees, lats = p_fwd.shape[1:]
        m_local = p_fwd.shape[0] // group
        modes = group * m_local * 2
        base, gained = (two_halves(table) for table in dft_tables(group, m_local, lon_count))
        field = field_loc.reshape(batch, channels * rows_local, lon_count)
        grad = grad_loc.reshape(batch, channels * rows_local, lon_count)
        w_rows = jnp.swapaxes(w_mix, 2, 3).reshape(degrees, channels * 2, channels)
        dma, vmem = pltpu.SemaphoreType.DMA, pltpu.VMEM
        block_rows = m_local * 2 * rows_local
        coef_shape = (batch, 2, degrees * m_local, channels)
        send_t = vmem((SLOTS, group, block_rows, channels), BF16)
        recv_t = vmem((batch, group, block_rows, channels), BF16)
        turn_t = vmem((modes * rows_local, channels), F32)
        stage_t = vmem((m_local, degrees, lats), F32)
        expanded_t = vmem((m_local, 2 * degrees, 2 * lats), BF16)
        flipped_t = vmem((m_local, lats, degrees), BF16)
        field_t = vmem((2, lon_count // LANES, channels * rows_local, LANES), F32)
        table_spec = pl.BlockSpec(memory_space=pltpu.VMEM)
        any_spec = pl.BlockSpec(memory_space=pl.ANY)
        late = sum(degrees - slot * group < lats // 2 for slot in range(m_local))
        far_rows = sum(degrees - slot * group for slot in range(m_local - late, m_local))
        late_rows = late * 2 * rows_local
        bridged_t = (send_t, recv_t, vmem((SLOTS, 2, far_rows, channels), BF16), vmem((batch, 2, far_rows, channels), BF16),
                     vmem((SLOTS, group // 2, late_rows, channels), BF16), vmem((late, lats, degrees), BF16))
        bridged_sems = (dma((SLOTS,)), dma((batch,))) * 3

        ranks = group // 2
        share_rows = (m_local + 1) * 2 * ranks
        share_out = jax.ShapeDtypeStruct((batch, ranks, share_rows, channels), BF16)
        share_sems = (dma((SLOTS,)), dma((batch,)), dma((SLOTS,)))

        far_stage_t = vmem((late, degrees, lats), F32)
        steps = degrees // ranks
        sums_shape = (steps, channels * 2, channels)
        planes_shape = (degrees, 2, channels, channels)
        single_t = vmem((BUNCH,) + coef_shape[1:], F32)
        share_send_t = vmem((SLOTS, ranks, share_rows, channels), BF16)
        swap_sems = (dma((SLOTS,)), dma((batch,)))
        field_out, gw_total, _, _, _ = pl.pallas_call(
            functools.partial(whole_kernel, group, rows_local), name='whole',
            out_shape=[jax.ShapeDtypeStruct(grad.shape, F32),
                       jax.ShapeDtypeStruct((steps, ranks, channels * 2, channels), F32),
                       jax.ShapeDtypeStruct(coef_shape, F32), share_out, share_out],
            in_specs=[any_spec, any_spec, table_spec, table_spec, any_spec, any_spec, any_spec], out_specs=[any_spec] * 5,
            scratch_shapes=[field_t, field_t, turn_t, stage_t, far_stage_t, expanded_t, expanded_t, flipped_t, send_t, recv_t,
                            vmem((2, 2 * degrees * m_local, channels), F32), single_t, single_t,
                            vmem((4, 4, channels * 2, channels), F32), vmem(planes_shape, BF16), bridged_t, send_t, recv_t,
                            vmem((ranks, share_rows, channels), F32), share_send_t, share_send_t,
                            vmem((2, 2) + share_out.shape[1:], BF16), vmem((2, ranks * (share_rows + 8), channels), F32),
                            vmem(sums_shape, F32), single_t, vmem((PIECES * steps // 2, channels * 2 // PIECES, channels), F32),
                            dma((2, 2)), dma((2, 2)), dma(()), dma(()), *swap_sems, dma((4,)), bridged_sems, *swap_sems,
                            share_sems, share_sems, dma((2, 2)), dma((BUNCH,)), dma((2, 6, PIECES * steps // 2)), bridged_sems,
                            dma((2,)), dma((2, 2))],
            compiler_params=params(0))(field, grad, base, gained, p_fwd, p_inv, w_rows)

        gw_total = gw_total.reshape(steps, ranks * channels * 2, channels)
        results = [jax.ShapeDtypeStruct(whole.shape, F32) for whole in (field_out, gw_total)]
        field_out, gw_total = pl.pallas_call(
            finish_kernel, name='finish', out_shape=results, in_specs=[any_spec] * 2, out_specs=[any_spec] * 2,
            scratch_shapes=[vmem((RING,) + whole.shape[1:], F32) for whole in results] + [dma((2, RING)), dma((2, RING))],
            compiler_params=params())(field_out, gw_total)

        grad_wmix = jnp.swapaxes(gw_total.reshape(degrees, channels, 2, channels), 2, 3)
        return field_out.reshape(grad_loc.shape), grad_wmix

    return jax.shard_map(local_step, mesh=mesh, in_specs=(field_spec, field_spec, P(), P(), P()),
                         out_specs=(field_spec, P('member', None, None, None)), check_vma=False)
```

```python
import functools
import math

import jax
import jax.numpy as jnp
import numpy as np
from jax import lax
from jax.experimental import pallas as pl
from jax.experimental.pallas import tpu as pltpu
from jax.sharding import PartitionSpec as P

MESH = pl.DeviceIdType.MESH
LANES = 128
SLOTS = 3
BUNCH = 3
PIECES = 2
RING = 6
VMEM_LIMIT = 67043328
F32 = jnp.float32
BF16 = jnp.bfloat16

NN = (((1,), (0,)), ((), ()))
NT = (((1,), (1,)), ((), ()))
TN = (((0,), (0,)), ((), ()))


def dot(lhs, rhs, dims):
    return lax.dot_general(lhs, rhs, dims, preferred_element_type=F32)


def split_halves(values):
    high = values.astype(BF16)
    low = (values - high.astype(F32)).astype(BF16)
    return high, low


def dft_tables(group, m_local, lon_count):
    owner, slot, part = np.meshgrid(np.arange(group), np.arange(m_local), np.arange(2), indexing='ij')
    wave = (slot * group + owner).reshape(-1)
    part = part.reshape(-1)
    phase = 2.0 * np.pi * ((wave[:, None] * np.arange(lon_count)[None, :]) % lon_count) / lon_count
    base = np.where(part[:, None] == 0, np.cos(phase), -np.sin(phase)) / math.sqrt(lon_count)
    gains = np.where(wave == 0, 1.0, 2.0)[:, None]
    return base.astype(np.float32), (base * gains).astype(np.float32)


def two_halves(table):
    high = jnp.asarray(table).astype(BF16)
    low = (jnp.asarray(table) - high.astype(F32)).astype(BF16)
    return jnp.stack([high, low])


class Halves:
    def __init__(self, whole, b, halves, slot, sem, outward=False):
        self.copies = []
        for half in range(halves.shape[1]):
            ends = whole.at[b, :, pl.ds(half * LANES, LANES)], halves.at[slot, half]
            source, target = ends[::-1] if outward else ends
            self.copies.append(pltpu.make_async_copy(source, target, sem.at[slot, half]))

    def start(self):
        for copy in self.copies:
            copy.start()

    def wait(self):
        for copy in self.copies:
            copy.wait()


def read_row(halves, slot, t, channels, rows_local):
    at = pl.ds(t, channels, stride=rows_local)
    return jnp.concatenate([halves[slot, half, at, :] for half in range(halves.shape[1])], axis=1)


def write_row(halves, slot, t, channels, rows_local, values):
    at = pl.ds(t, channels, stride=rows_local)
    for half in range(halves.shape[1]):
        halves[slot, half, at, :] = values[:, half * LANES:(half + 1) * LANES]


class Exchange:
    def __init__(self, me, group, batch, send, recv, send_sem, recv_sem):
        self.me, self.group, self.batch = me, group, batch
        self.send, self.recv, self.send_sem, self.recv_sem = send, recv, send_sem, recv_sem

    def all_copies(self, b):
        slot = lax.rem(b, SLOTS)
        others = pl.ds(0, self.group - 1)
        return pltpu.make_async_remote_copy(
            self.send.at[slot, others], self.recv.at[b, others], self.send_sem.at[slot], self.recv_sem.at[b],
            device_id={'lat': lax.rem(self.me + 1, self.group)}, device_id_type=MESH)

    def reserve(self, b):
        @pl.when(b >= SLOTS)
        def _():
            self.all_copies(b - SLOTS).wait_send()

    def start(self, b):
        slot = lax.rem(b, SLOTS)
        self.recv[b, self.me] = self.send[slot, self.me]

        @pl.loop(1, self.group)
        def _(step):
            target = jnp.bitwise_xor(self.me, self.group - step)
            pltpu.make_async_remote_copy(
                self.send.at[slot, target], self.recv.at[b, self.me], self.send_sem.at[slot], self.recv_sem.at[b],
                device_id={'lat': target}, device_id_type=MESH).start()

    def arrive(self, b):
        self.all_copies(b).wait_recv()

    def drain(self):
        for b in range(max(0, self.batch - SLOTS), self.batch):
            self.all_copies(b).wait_send()


class BridgedExchange:
    def __init__(self, me, group, batch, bufs, sems):
        self.me, self.group, self.batch = me, group, batch
        self.send, self.recv, self.bridge_send, self.bridge_recv, self.relay_send, self.flipped_far = bufs
        self.send_sem, self.recv_sem, self.bridge_send_sem, self.bridge_recv_sem, self.relay_send_sem, self.relay_recv_sem = sems
        self.half_size = group // 2
        self.half = me // self.half_size
        self.place = lax.rem(me, self.half_size)
        self.twin = self.half_size + me - 2 * self.half_size * self.half
        self.rows = self.send.shape[2]
        self.late_rows = self.relay_send.shape[2]
        self.early_rows = self.rows - self.late_rows
        self.tile = self.late_rows // self.flipped_far.shape[0]
        self.direct = self.early_rows // self.tile

    def copy(self, source, target, send_sem, recv_sem, device):
        return pltpu.make_async_remote_copy(source, target, send_sem, recv_sem, device_id={'lat': device},
                                            device_id_type=MESH)

    def all_direct(self, b):
        slot = lax.rem(b, SLOTS)
        count = (self.half_size - 1) * self.rows + self.half_size * self.early_rows
        span = pl.ds(0, count // self.rows)
        return self.copy(self.send.at[slot, span], self.recv.at[b, span], self.send_sem.at[slot], self.recv_sem.at[b], self.twin)

    def all_relayed(self, b):
        slot = lax.rem(b, SLOTS)
        span, part = pl.ds(0, self.half_size - 1), pl.ds(0, self.late_rows)
        return self.copy(self.relay_send.at[slot, span], self.recv.at[b, span, part], self.relay_send_sem.at[slot],
                         self.relay_recv_sem.at[b], self.twin)

    def bridge(self, b):
        slot = lax.rem(b, SLOTS)
        return self.copy(self.bridge_send.at[slot], self.bridge_recv.at[b], self.bridge_send_sem.at[slot],
                         self.bridge_recv_sem.at[b], self.twin)

    def reserve(self, b):
        @pl.when(b >= SLOTS)
        def _():
            self.all_direct(b - SLOTS).wait_send()
            self.bridge(b - SLOTS).wait_send()

    def start(self, b):
        slot = lax.rem(b, SLOTS)
        self.bridge(b).start()
        early = pl.ds(0, self.early_rows)

        @pl.loop(0, self.half_size)
        def _(step):
            target = jnp.bitwise_xor(self.me, 2 * self.half_size - 1 - step)
            self.copy(self.send.at[slot, target, early], self.recv.at[b, self.me, early], self.send_sem.at[slot],
                      self.recv_sem.at[b], target).start()

        @pl.loop(1, self.half_size)
        def _(step):
            target = jnp.bitwise_xor(self.me, self.half_size - step)
            self.copy(self.send.at[slot, target], self.recv.at[b, self.me], self.send_sem.at[slot], self.recv_sem.at[b],
                      target).start()

        self.recv[b, self.me] = self.send[slot, self.me]

    def relay(self, b):
        slot = lax.rem(b, SLOTS)

        @pl.when(b >= SLOTS)
        def _():
            self.all_relayed(b - SLOTS).wait_send()

        self.bridge(b).wait_recv()
        lats, degrees = self.flipped_far.shape[1:]
        own = pl.ds(pl.multiple_of(self.half * (lats // 2), lats // 2), lats // 2)
        at = 0
        for late in range(self.flipped_far.shape[0]):
            first = (self.direct + late) * self.group
            count = degrees - first
            parts = []
            for part in range(2):
                rows = self.bridge_recv[b, part, pl.ds(at, count), :]
                parts.append(jnp.concatenate([jnp.zeros((first, rows.shape[1]), BF16), rows], axis=0))
            at += count
            res = dot(self.flipped_far[late, own, :], jnp.concatenate(parts, axis=1), NN)
            lanes = res.shape[1] // 2
            blocks = [res[:, part * lanes:(part + 1) * lanes].reshape(self.half_size, self.tile // 2, lanes) for part in range(2)]
            self.relay_send[slot, :, pl.ds(late * self.tile, self.tile), :] = jnp.concatenate(blocks, axis=1).astype(BF16)
        late_at = pl.ds(self.early_rows, self.late_rows)

        @pl.loop(1, self.half_size)
        def _(step):
            place = jnp.bitwise_xor(self.place, self.half_size - step)
            self.copy(self.relay_send.at[slot, place], self.recv.at[b, self.twin, late_at], self.relay_send_sem.at[slot],
                      self.relay_recv_sem.at[b], self.half * self.half_size + place).start()

        self.recv[b, self.twin, late_at] = self.relay_send[slot, self.place]

    def arrive(self, b):
        self.all_direct(b).wait_recv()
        self.all_relayed(b).wait_recv()

    def drain(self):
        for b in range(max(0, self.batch - SLOTS), self.batch):
            self.all_direct(b).wait_send()
            self.bridge(b).wait_send()
            self.all_relayed(b).wait_send()


class Share:
    def __init__(self, me, group, batch, send, message, out, sems):
        self.batch, self.send, self.message, self.out = batch, send, message, out
        self.send_sem, self.recv_sem, self.local_sem = sems
        self.size = group // 2
        self.base = me // self.size * self.size
        self.place = lax.rem(me, self.size)

    def rank(self, place):
        return place // 4 + 2 * (lax.rem(place, 4) // 2) + 4 * lax.rem(place, 2)

    def copy(self, slot, source, b, target, place):
        return pltpu.make_async_remote_copy(
            self.send.at[slot, source], self.out.at[b, target], self.send_sem.at[slot], self.recv_sem.at[b],
            device_id={'lat': self.base + place}, device_id_type=MESH)

    def every(self, b):
        span = pl.ds(0, self.size - 1)
        return self.copy(lax.rem(b, SLOTS), span, b, span, lax.rem(self.place + 1, self.size))

    def keep(self, b):
        slot = lax.rem(b, SLOTS)
        return pltpu.make_async_copy(self.send.at[slot, self.rank(self.place)], self.out.at[b, self.place],
                                     self.local_sem.at[slot])

    def give(self, b, coef):
        slot_b = lax.rem(b, SLOTS)

        @pl.when(b >= SLOTS)
        def _():
            self.every(b - SLOTS).wait_send()

        size = self.size
        m_local = size
        tile = 2 * size

        def rows(part, slot, rank, first, count):
            return coef[part, pl.ds((first * size + rank) * m_local + slot, count, stride=size * m_local), :]

        for rank in range(size):
            for part in range(2):
                for pair in range(m_local // 2):
                    block = rows(part, pair, rank, 0, tile)
                    if pair:
                        block = block + rows(part, m_local - pair, rank, 2 * (m_local - pair), tile)
                    self.message[rank, pl.ds((part * (m_local // 2) + pair) * tile, tile), :] = block
                self.message[rank, pl.ds(m_local * tile + part * size, size), :] = rows(part, m_local // 2, rank, size, size)
        for rank in range(size):
            self.send[slot_b, rank] = self.message[rank].astype(BF16)
        self.keep(b).start()

        @pl.loop(1, size)
        def _(step):
            place = jnp.bitwise_xor(self.place, size - step)
            self.copy(slot_b, self.rank(place), b, self.place, place).start()

        self.keep(b).wait()

    def drain(self):
        for b in range(max(0, self.batch - SLOTS), self.batch):
            self.every(b).wait_send()

    def arrive(self, b):
        self.every(b).wait_recv()


def clear_after(coef, used):
    for part in range(coef.shape[0]):
        coef[part, pl.ds(used, coef.shape[1] - used), :] = jnp.zeros((coef.shape[1] - used, coef.shape[2]), F32)


def greet(me, group):
    barrier = pltpu.get_barrier_semaphore()

    @pl.loop(1, group)
    def _(step):
        pl.semaphore_signal(barrier, inc=1, device_id={'lat': lax.rem(me + step, group)}, device_id_type=MESH)


def meet(group):
    pl.semaphore_wait(pltpu.get_barrier_semaphore(), group - 1)


class Tables:
    def __init__(self, waves, whole, stage, sem):
        self.waves, self.whole, self.stage, self.sem = waves, whole, stage, sem

    def start(self):
        for n, wave in enumerate(self.waves):
            pltpu.make_async_copy(self.whole.at[wave], self.stage.at[n], self.sem).start()

    def wait(self):
        pltpu.make_async_copy(self.whole.at[pl.ds(0, len(self.waves))], self.stage, self.sem).wait()


def own_tables(me, group, whole, stage, sem):
    return Tables([slot * group + me for slot in range(stage.shape[0])], whole, stage, sem)


def far_tables(swap, whole, stage, sem):
    return Tables([(swap.direct + n) * swap.group + swap.twin for n in range(stage.shape[0])], whole, stage, sem)


def expand_rows(stage, expanded, rows_local):
    m_local, degrees, lats = stage.shape
    row = lax.broadcasted_iota(jnp.int32, (lats, 2 * lats), 0)
    col = lax.broadcasted_iota(jnp.int32, (lats, 2 * lats), 1)
    source = col // (2 * rows_local)
    inner = col % (2 * rows_local)
    for part in range(2):
        pick = (row == source * rows_local + inner - part * rows_local) & (inner // rows_local == part)
        pick = pick.astype(F32).astype(BF16)
        for slot in range(m_local):
            expanded[slot, pl.ds(part * degrees, degrees), :] = dot(stage[slot].astype(BF16), pick, NN).astype(BF16)


def flip_rows(stage, flipped):
    for slot in range(stage.shape[0]):
        flipped[slot] = stage[slot].T.astype(BF16)


def analyse(values_at, table, turn, rows_local):
    modes = table.shape[1]
    for t in range(0, rows_local, 2):
        pair = jnp.concatenate([values_at(t), values_at(t + 1)], axis=0)
        high, low = split_halves(pair * 0.5)
        out = 2.0 * (dot(table[0], high, NT) + dot(table[0], low, NT) + dot(table[1], high, NT))
        channels = out.shape[1] // 2
        turn[pl.ds(t, modes, stride=rows_local), :] = out[:, :channels]
        turn[pl.ds(t + 1, modes, stride=rows_local), :] = out[:, channels:]


def pack_blocks(turn, send, slot):
    group, rows, lanes = send.shape[1:]
    for d in range(group):
        send[slot, d] = turn[pl.ds(d * rows, rows), :].astype(BF16)


def unpack_blocks(recv, b, turn):
    group, rows, lanes = recv.shape[1:]
    for d in range(group):
        turn[pl.ds(d * rows, rows), :] = recv[b, d].astype(F32)


def synthesise(turn, t, table, rows_local):
    modes = table.shape[1]
    spec = turn[pl.ds(t, modes, stride=rows_local), :].astype(BF16)
    return dot(spec, table[0], TN) + dot(spec, table[1], TN)


def legendre_forward(recv, b, expanded, out, rows_local):
    m_local = expanded.shape[0]
    degrees = expanded.shape[1] // 2
    group, _, lanes = recv.shape[1:]
    tile = 2 * rows_local
    for slot in range(m_local):
        rows = recv[b, :, pl.ds(slot * tile, tile), :].reshape(group * tile, lanes)
        res = dot(expanded[slot], rows, NN)
        for part in range(2):
            out[part, pl.ds(slot, degrees, stride=m_local), :] = res[part * degrees:(part + 1) * degrees]


def legendre_inverse(coef, flipped, swap, slot_out, rows_local):
    m_local, lats, degrees = flipped.shape
    send = swap.send
    at = 0
    group = lats // rows_local
    tile = 2 * rows_local
    for slot in range(m_local):
        parts = [coef.at[part][pl.ds(slot, degrees, stride=m_local), :].astype(BF16) for part in range(2)]
        if slot >= swap.direct:
            first = slot * group
            for part in range(2):
                swap.bridge_send[slot_out, part, pl.ds(at, degrees - first), :] = parts[part][first:]
            at += degrees - first
        res = dot(flipped[slot], jnp.concatenate(parts, axis=1), NN)
        lanes = res.shape[1] // 2
        blocks = [res[:, part * lanes:(part + 1) * lanes].reshape(group, rows_local, lanes) for part in range(2)]
        send[slot_out, :, pl.ds(slot * tile, tile), :] = jnp.concatenate(blocks, axis=1).astype(BF16)


def gelu_slope(values):
    cumulative = 0.5 * (1.0 + lax.erf(values * math.sqrt(0.5)))
    density = jnp.exp(-0.5 * values * values) * (1.0 / math.sqrt(2.0 * math.pi))
    return cumulative + values * density


def mix_block(planes):
    real, imag = planes[0], planes[1]
    return jnp.concatenate([jnp.concatenate([real, -imag], axis=1), jnp.concatenate([imag, real], axis=1)], axis=0)


class WeightSum:
    def __init__(self, me, group, sums, got, out, sems):
        self.me, self.sums, self.got, self.out, self.sems = me, sums, got, out, sems
        self.core, self.y = lax.rem(me, 2), lax.rem(me // 2, 2)
        self.near, self.far = lax.rem(me // 4, 2), me // (group // 2)
        self.rank = self.near + 2 * self.y + 4 * self.core

    def peer(self, phase):
        step = (1, 2, 4, 8)[phase]
        bit = (self.core, self.y, self.near, self.far)[phase]
        return {'lat': self.me + step - 2 * step * bit}

    def remote(self, phase, k, source, target, stage):
        return pltpu.make_async_remote_copy(source, target, self.sems.at[0, stage, k], self.sems.at[1, stage, k],
                                            device_id=self.peer(phase), device_id_type=MESH)

    def halving(self, k):
        pair, at = self.piece(k)
        return self.remote(3, k, self.sums.at[2 * pair + 1 - self.far, at], self.got.at[k], 4)

    def piece(self, k):
        rows = self.got.shape[1]
        pieces = self.sums.shape[1] // rows
        return k // pieces, pl.ds(pl.multiple_of(lax.rem(k, pieces) * rows, rows), rows)

    def settle(self, k):
        pair, at = self.piece(k)
        mine = 2 * pair + self.far
        return pltpu.make_async_copy(self.sums.at[mine, at], self.out.at[mine, self.rank, at], self.sems.at[0, 5, k])

    def doubling(self, phase, k):
        pair, at = self.piece(k)
        if phase == 3:
            mine = 2 * pair + self.far
            return self.remote(3, k, self.sums.at[mine, at], self.out.at[mine, self.rank, at], 3)
        width = (4, 2, 1)[phase]
        first = (4 * self.core, 4 * self.core + 2 * self.y, self.rank)[phase]
        span = self.out.at[pl.ds(2 * pair, 2), pl.ds(first, width), at]
        return self.remote(phase, k, span, span, phase)

    def reduce_step(self, k):
        self.halving(k).wait()
        pair, at = self.piece(k)
        mine = 2 * pair + self.far
        self.sums[mine, at] = self.sums[mine, at] + self.got[k]
        self.settle(k).start()
        self.doubling(3, k).start()

    def gather_step(self, phase, k):
        if phase == 2:
            self.settle(k).wait()
        self.doubling(phase + 1, k).wait()
        if phase >= 0:
            self.doubling(phase, k).start()


def shared_place(part, slot, step, m_local):
    tile = 2 * m_local
    if slot == m_local // 2:
        return m_local * tile + part * m_local + step - m_local
    pair = min(slot, m_local - slot) if slot else 0
    shift = 0 if slot < m_local // 2 else 2 * slot
    return (part * (m_local // 2) + pair) * tile + step - shift


def weigh(shared, sources, sums, m_local):
    stride = shared.shape[1] // sources

    @pl.loop(0, sums.shape[0])
    def _(step):
        sides = []
        for which in range(2):
            slots = []
            for slot in range(m_local):
                used = step >= 2 * slot
                parts = []
                for part in range(2):
                    place = jnp.where(used, shared_place(part, slot, step, m_local), 0)
                    rows = shared[which, pl.ds(place, sources, stride=stride), :]
                    parts.append(jnp.where(used, rows, 0.0))
                slots.append(jnp.concatenate(parts, axis=1))
            sides.append(jnp.concatenate(slots, axis=0).astype(BF16))
        big = dot(sides[0], sides[1], TN)
        half = big.shape[0] // 2
        real, imag = pl.ds(0, half, stride=2), pl.ds(1, half, stride=2)
        sums[step, real, :] = sums[step, real, :] + (big[:half, :half] + big[half:, half:])
        sums[step, imag, :] = sums[step, imag, :] + (big[half:, :half] - big[:half, half:])


def whole_kernel(group, rows_local, field, grad, base_hbm, gained_hbm, p_fwd, p_inv, w_mix, field_out, grad_w, back_out, coef_shared,
                 mixed_shared, field_buf, grad_buf, turn, stage, stage_far, expanded_fwd, expanded_inv, flipped, send_f, recv_f,
                 padded, coef, mixed, w_in, planes, bridged, send_d, recv_d, message, share_send_a, share_send_d, halves,
                 shared, sums, back, got, field_sem, grad_sem, p_sem, far_sem, send_f_sem, recv_f_sem, w_sem, bridged_sems,
                 send_d_sem, recv_d_sem, share_a_sems, share_d_sems, half_sem, out_sem, gw_sem, again_sems, back_sem, last_sem, base, gained,
                 table_sem):
    me = lax.axis_index('lat')
    batch = field.shape[0]
    channels = field.shape[1] // rows_local
    m_local, degrees = stage.shape[:2]
    used = degrees * m_local
    bunch = coef.shape[0]
    sources, share_rows = coef_shared.shape[1:3]

    def fetch_field(b):
        return Halves(field, b, field_buf, lax.rem(b, 2), field_sem)

    def fetch_grad(b):
        return Halves(grad, b, grad_buf, lax.rem(b, 2), grad_sem)

    def put(b):
        return pltpu.make_async_copy(back.at[lax.rem(b, bunch)], back_out.at[b], out_sem.at[lax.rem(b, bunch)])

    def fetch_back(b):
        return pltpu.make_async_copy(back_out.at[b], coef.at[lax.rem(b, 2)], back_sem.at[lax.rem(b, 2)])

    def fetch_last(b):
        return Halves(grad, b, field_buf, lax.rem(b, 2), field_sem)

    def put_last(b):
        return Halves(field_out, b, field_buf, lax.rem(b, 2), last_sem, outward=True)

    def fetch_shares(b):
        slot = lax.rem(b, 2)
        return [pltpu.make_async_copy(whole.at[b], halves.at[slot, which], half_sem.at[slot, which])
                for which, whole in enumerate((mixed_shared, coef_shared))]

    load_base = pltpu.make_async_copy(base_hbm, base, table_sem.at[0])
    load_gained = pltpu.make_async_copy(gained_hbm, gained, table_sem.at[1])
    fetch_field(0).start()
    load_base.start()
    greet(me, group)
    load_gained.start()
    fetch_grad(0).start()
    loading = own_tables(me, group, p_fwd, stage, p_sem)
    loading_inv = own_tables(me, group, p_inv, stage, p_sem)
    loading.start()
    swap_f = Exchange(me, group, batch, send_f, recv_f, send_f_sem, recv_f_sem)
    swap_g = BridgedExchange(me, group, batch, bridged, bridged_sems)
    swap_h = BridgedExchange(me, group, batch, bridged, again_sems)
    total = WeightSum(me, group, sums, got, grad_w, gw_sem)
    swap_d = Exchange(me, group, batch, send_d, recv_d, send_d_sem, recv_d_sem)
    share_a = Share(me, group, batch, share_send_a, message, coef_shared, share_a_sems)
    share_d = Share(me, group, batch, share_send_d, message, mixed_shared, share_d_sems)
    loading_far = far_tables(swap_g, p_inv, stage_far, far_sem)
    loading_far.start()
    loading_fwd = own_tables(me, group, p_fwd, stage, p_sem)
    loading_far_fwd = far_tables(swap_h, p_fwd, stage_far, far_sem)
    chunks = got.shape[0]

    def build_planes():
        depth, per = w_in.shape[:2]
        blocks = degrees // per
        half = w_in.shape[2] // 2

        def fetch(k):
            return pltpu.make_async_copy(w_mix.at[pl.ds(k * per, per)], w_in.at[lax.rem(k, depth)], w_sem.at[lax.rem(k, depth)])

        for k in range(depth - 1):
            fetch(k).start()

        @pl.loop(0, blocks)
        def _(k):
            @pl.when(k + depth - 1 < blocks)
            def _():
                fetch(k + depth - 1).start()

            fetch(k).wait()
            for inner in range(per):
                rows = w_in.at[lax.rem(k, depth), inner]
                for part in range(2):
                    planes[k * per + inner, part] = rows[pl.ds(part, half, stride=2), :].astype(BF16)

    def unmix_bunch():
        @pl.loop(0, degrees // 8)
        def _(k):
            for inner in range(8):
                at = pl.ds(pl.multiple_of((k * 8 + inner) * m_local, m_local), m_local)
                rows = [back[:, part, at, :].reshape(bunch * m_local, channels) for part in range(2)]
                res = dot(jnp.concatenate(rows, axis=1).astype(BF16), mix_block(planes[k * 8 + inner]), NN)
                for part in range(2):
                    back[:, part, at, :] = res[:, part * channels:(part + 1) * channels].reshape(bunch, m_local, channels)

    def mix_bunch():
        @pl.loop(0, degrees // 8)
        def _(k):
            for inner in range(8):
                at = pl.ds(pl.multiple_of((k * 8 + inner) * m_local, m_local), m_local)
                rows = [coef[:, part, at, :].reshape(bunch * m_local, channels) for part in range(2)]
                res = dot(jnp.concatenate(rows, axis=1).astype(BF16), mix_block(planes[k * 8 + inner]), NT)
                for part in range(2):
                    mixed[:, part, at, :] = res[:, part * channels:(part + 1) * channels].reshape(bunch, m_local, channels)

    def weigh_sample(b):
        for copy in fetch_shares(b):
            copy.wait()
        for which in range(2):
            for source in range(sources):
                at = pl.ds(source * (shared.shape[1] // sources), share_rows)
                shared[which, at, :] = halves[lax.rem(b, 2), which, source].astype(F32)
        weigh(shared, sources, sums, m_local)

    def collect(b):
        share_a.arrive(b)
        share_d.arrive(b)
        for copy in fetch_shares(b):
            copy.start()

    lag_a, lag_b, lag_c, lag_d = 2, 4, 6, 8
    lag_e = batch + lag_c
    close = batch + lag_d
    steps = [total.reduce_step] + [functools.partial(total.gather_step, p) for p in (2, 1, 0, -1)]

    def advance(n, sub):
        @pl.when((n >= 0) & (n * 2 + sub + 2 < chunks))
        def _():
            total.halving(n * 2 + sub + 2).start()

        for late, step in reversed(list(enumerate(steps))):
            k = (n - late) * 2 + sub

            @pl.when((k >= 0) & (k < chunks))
            def _():
                step(k)

    def take_modes(b):
        @pl.when(b + 1 < batch)
        def _():
            fetch_field(b + 1).start()

        fetch_field(b).wait()
        half = lax.rem(b, 2)
        analyse(lambda t: read_row(field_buf, half, t, channels, rows_local), base, turn, rows_local)
        swap_f.reserve(b)
        pack_blocks(turn, send_f, lax.rem(b, SLOTS))

    load_base.wait()
    take_modes(0)
    meet(group)

    def body(i, carry):
        @pl.when((i >= lag_e) & (i < batch + lag_e))
        def _():
            b = i - lag_e

            @pl.when(b + 1 < batch)
            def _():
                fetch_back(b + 1).start()

            fetch_back(b).wait()
            swap_h.reserve(b)
            legendre_inverse(coef.at[lax.rem(b, 2)], flipped, swap_h, lax.rem(b, SLOTS), rows_local)
            swap_h.start(b)

        @pl.when((i >= 1) & (i < batch))
        def _():
            take_modes(i)

        @pl.when(i < batch)
        def _():
            swap_f.start(i)

        @pl.when(i == 0)
        def _():
            clear_after(padded, used)
            load_gained.wait()
            loading.wait()
            expand_rows(stage, expanded_fwd, rows_local)
            loading_inv.start()
            loading_far.wait()
            flip_rows(stage_far, swap_g.flipped_far)

        @pl.when(i == 1)
        def _():
            build_planes()
            loading_inv.wait()
            expand_rows(stage, expanded_inv, rows_local)
            flip_rows(stage, flipped)
            sums[...] = jnp.zeros_like(sums)

        @pl.when((i >= lag_a) & (i < batch + lag_a))
        def _():
            b = i - lag_a
            swap_f.arrive(b)
            legendre_forward(recv_f, b, expanded_fwd, padded, rows_local)
            coef[lax.rem(b, bunch)] = padded[:, pl.ds(0, used), :]
            share_a.give(b, padded)

            @pl.when(lax.rem(b, bunch) == bunch - 1)
            def _():
                mix_bunch()

        @pl.when((i >= lag_b) & (i < batch + lag_b))
        def _():
            b = i - lag_b
            swap_g.reserve(b)
            legendre_inverse(mixed.at[lax.rem(b, bunch)], flipped, swap_g, lax.rem(b, SLOTS), rows_local)
            swap_g.start(b)

        @pl.when((i >= lag_b + 1) & (i < batch + lag_b + 1))
        def _():
            swap_g.relay(i - lag_b - 1)

        @pl.when((i >= lag_c) & (i < batch + lag_c))
        def _():
            b = i - lag_c
            half = lax.rem(b, 2)

            @pl.when(b + 1 < batch)
            def _():
                fetch_grad(b + 1).start()

            fetch_grad(b).wait()
            swap_g.arrive(b)
            unpack_blocks(swap_g.recv, b, turn)
            for t in range(rows_local):
                slope = gelu_slope(synthesise(turn, t, gained, rows_local))
                given = read_row(grad_buf, half, t, channels, rows_local)
                write_row(grad_buf, half, t, channels, rows_local, given * slope)
            analyse(lambda t: read_row(grad_buf, half, t, channels, rows_local), gained, turn, rows_local)
            swap_d.reserve(b)
            pack_blocks(turn, send_d, lax.rem(b, SLOTS))
            swap_d.start(b)

        @pl.when(i == lag_e - 2)
        def _():
            loading_fwd.start()
            loading_far_fwd.start()

        @pl.when(i == lag_e - 1)
        def _():
            loading_fwd.wait()
            flip_rows(stage, flipped)
            loading_far_fwd.wait()
            flip_rows(stage_far, swap_h.flipped_far)
            swap_g.drain()
            fetch_back(0).start()

        @pl.when((i >= lag_d) & (i < batch + lag_d))
        def _():
            b = i - lag_d

            @pl.when((b >= bunch) & (lax.rem(b, bunch) == 0))
            def _():
                unmix_bunch()
                for n in range(bunch):
                    put(b - bunch + n).start()

            @pl.when(b >= 2)
            def _():
                weigh_sample(b - 2)

            @pl.when(b >= 1)
            def _():
                collect(b - 1)

            swap_d.arrive(b)
            legendre_forward(recv_d, b, expanded_inv, padded, rows_local)
            share_d.give(b, padded)

            @pl.when(b >= bunch)
            def _():
                put(b - bunch).wait()

            back[lax.rem(b, bunch)] = padded[:, pl.ds(0, used), :]

        @pl.when(i == close)
        def _():
            fetch_last(0).start()
            weigh_sample(batch - 2)
            collect(batch - 1)
            weigh_sample(batch - 1)
            for k in range(2):
                total.halving(k).start()

        advance(i - close, 0)

        @pl.when((i >= lag_e + 1) & (i < batch + lag_e + 1))
        def _():
            swap_h.relay(i - lag_e - 1)

        @pl.when((i >= close) & (i < batch + close))
        def _():
            b = i - close
            half = lax.rem(b, 2)

            @pl.when(b >= 1)
            def _():
                put_last(b - 1).wait()

            @pl.when(b + 1 < batch)
            def _():
                fetch_last(b + 1).start()

            fetch_last(b).wait()
            swap_h.arrive(b)
            unpack_blocks(swap_h.recv, b, turn)
            for t in range(rows_local):
                added = synthesise(turn, t, base, rows_local)
                given = read_row(field_buf, half, t, channels, rows_local)
                write_row(field_buf, half, t, channels, rows_local, given + added)
            put_last(b).start()

        @pl.when(i == close + 1)
        def _():
            unmix_bunch()
            for n in range(bunch):
                put(batch - bunch + n).start()

        @pl.when(i == close + 3)
        def _():
            for n in range(bunch):
                put(batch - bunch + n).wait()

        advance(i - close, 1)
        return carry

    lax.fori_loop(0, close + max(batch, chunks // 2 + 4), body, 0)
    for swap in (swap_f, swap_h, swap_d, share_a, share_d):
        swap.drain()
    put_last(batch - 1).wait()


def finish_kernel(first, second, first_out, second_out, first_ring, second_ring, in_sem, out_sem):
    depth = first_ring.shape[0]
    pieces = []
    for side, (source, target, ring) in enumerate(((first, first_out, first_ring), (second, second_out, second_ring))):
        for n in range(source.shape[0]):
            slot = n % depth
            take = pltpu.make_async_copy(source.at[n], ring.at[slot], in_sem.at[side, slot])
            give = pltpu.make_async_copy(ring.at[slot], target.at[n], out_sem.at[side, slot])
            pieces.append(((n, side), (side, n), take, give))
    pieces.sort(key=lambda piece: piece[0])
    given = {piece[1]: piece[3] for piece in pieces}
    waited = set()
    for k in range(len(pieces) + depth):
        if k < len(pieces):
            _, (side, n), take, _ = pieces[k]
            if n >= depth:
                given[side, n - depth].wait()
                waited.add((side, n - depth))
            take.start()
        if k >= depth:
            pieces[k - depth][2].wait()
            pieces[k - depth][3].start()
    for _, place, _, give in pieces:
        if place not in waited:
            give.wait()


def any_specs(n):
    return [pl.BlockSpec(memory_space=pl.ANY)] * n


def params(collective_id=None):
    if collective_id is None:
        return pltpu.CompilerParams(vmem_limit_bytes=VMEM_LIMIT)
    return pltpu.CompilerParams(collective_id=collective_id, has_side_effects=True, vmem_limit_bytes=VMEM_LIMIT)


def solution(mesh):
    group = mesh.shape['lat']
    field_spec = P('member', None, 'lat', None)

    def local_step(field_loc, grad_loc, p_fwd, p_inv, w_mix):
        batch, channels, rows_local, lon_count = field_loc.shape
        degrees, lats = p_fwd.shape[1:]
        m_local = p_fwd.shape[0] // group
        modes = group * m_local * 2
        base, gained = (two_halves(table) for table in dft_tables(group, m_local, lon_count))
        field = field_loc.reshape(batch, channels * rows_local, lon_count)
        grad = grad_loc.reshape(batch, channels * rows_local, lon_count)
        w_rows = jnp.swapaxes(w_mix, 2, 3).reshape(degrees, channels * 2, channels)
        dma, vmem = pltpu.SemaphoreType.DMA, pltpu.VMEM
        block_rows = m_local * 2 * rows_local
        coef_shape = (batch, 2, degrees * m_local, channels)
        send_t = vmem((SLOTS, group, block_rows, channels), BF16)
        recv_t = vmem((batch, group, block_rows, channels), BF16)
        turn_t = vmem((modes * rows_local, channels), F32)
        stage_t = vmem((m_local, degrees, lats), F32)
        expanded_t = vmem((m_local, 2 * degrees, 2 * lats), BF16)
        flipped_t = vmem((m_local, lats, degrees), BF16)
        field_t = vmem((2, lon_count // LANES, channels * rows_local, LANES), F32)
        any_spec = pl.BlockSpec(memory_space=pl.ANY)
        late = sum(degrees - slot * group < lats // 2 for slot in range(m_local))
        far_rows = sum(degrees - slot * group for slot in range(m_local - late, m_local))
        late_rows = late * 2 * rows_local
        bridged_t = (send_t, recv_t, vmem((SLOTS, 2, far_rows, channels), BF16), vmem((batch, 2, far_rows, channels), BF16),
                     vmem((SLOTS, group // 2, late_rows, channels), BF16), vmem((late, lats, degrees), BF16))
        bridged_sems = (dma((SLOTS,)), dma((batch,))) * 3

        ranks = group // 2
        share_rows = (m_local + 1) * 2 * ranks
        share_out = jax.ShapeDtypeStruct((batch, ranks, share_rows, channels), BF16)
        share_sems = (dma((SLOTS,)), dma((batch,)), dma((SLOTS,)))

        far_stage_t = vmem((late, degrees, lats), F32)
        steps = degrees // ranks
        sums_shape = (steps, channels * 2, channels)
        planes_shape = (degrees, 2, channels, channels)
        single_t = vmem((BUNCH,) + coef_shape[1:], F32)
        share_send_t = vmem((SLOTS, ranks, share_rows, channels), BF16)
        swap_sems = (dma((SLOTS,)), dma((batch,)))
        field_out, gw_total, _, _, _ = pl.pallas_call(
            functools.partial(whole_kernel, group, rows_local), name='whole',
            out_shape=[jax.ShapeDtypeStruct(grad.shape, F32),
                       jax.ShapeDtypeStruct((steps, ranks, channels * 2, channels), F32),
                       jax.ShapeDtypeStruct(coef_shape, F32), share_out, share_out],
            in_specs=[any_spec] * 7, out_specs=[any_spec] * 5,
            scratch_shapes=[field_t, field_t, turn_t, stage_t, far_stage_t, expanded_t, expanded_t, flipped_t, send_t, recv_t,
                            vmem((2, 2 * degrees * m_local, channels), F32), single_t, single_t,
                            vmem((4, 4, channels * 2, channels), F32), vmem(planes_shape, BF16), bridged_t, send_t, recv_t,
                            vmem((ranks, share_rows, channels), F32), share_send_t, share_send_t,
                            vmem((2, 2) + share_out.shape[1:], BF16), vmem((2, ranks * (share_rows + 8), channels), F32),
                            vmem(sums_shape, F32), single_t, vmem((PIECES * steps // 2, channels * 2 // PIECES, channels), F32),
                            dma((2, 2)), dma((2, 2)), dma(()), dma(()), *swap_sems, dma((4,)), bridged_sems, *swap_sems,
                            share_sems, share_sems, dma((2, 2)), dma((BUNCH,)), dma((2, 6, PIECES * steps // 2)), bridged_sems,
                            dma((2,)), dma((2, 2)), vmem(base.shape, BF16), vmem(base.shape, BF16), dma((2,))],
            compiler_params=params(0))(field, grad, base, gained, p_fwd, p_inv, w_rows)

        gw_total = gw_total.reshape(steps, ranks * channels * 2, channels)
        results = [jax.ShapeDtypeStruct(whole.shape, F32) for whole in (field_out, gw_total)]
        field_out, gw_total = pl.pallas_call(
            finish_kernel, name='finish', out_shape=results, in_specs=[any_spec] * 2, out_specs=[any_spec] * 2,
            scratch_shapes=[vmem((RING,) + whole.shape[1:], F32) for whole in results] + [dma((2, RING)), dma((2, RING))],
            compiler_params=params())(field_out, gw_total)

        grad_wmix = jnp.swapaxes(gw_total.reshape(degrees, channels, 2, channels), 2, 3)
        return field_out.reshape(grad_loc.shape), grad_wmix

    return jax.shard_map(local_step, mesh=mesh, in_specs=(field_spec, field_spec, P(), P(), P()),
                         out_specs=(field_spec, P('member', None, None, None)), check_vma=False)
```

```python
import functools
import math

import jax
import jax.numpy as jnp
import numpy as np
from jax import lax
from jax.experimental import pallas as pl
from jax.experimental.pallas import tpu as pltpu
from jax.sharding import PartitionSpec as P

MESH = pl.DeviceIdType.MESH
LANES = 128
SLOTS = 3
BUNCH = 3
PIECES = 2
RING = 6
VMEM_LIMIT = 67043328
F32 = jnp.float32
BF16 = jnp.bfloat16

NN = (((1,), (0,)), ((), ()))
NT = (((1,), (1,)), ((), ()))
TN = (((0,), (0,)), ((), ()))


def dot(lhs, rhs, dims):
    return lax.dot_general(lhs, rhs, dims, preferred_element_type=F32)


def split_halves(values):
    high = values.astype(BF16)
    low = (values - high.astype(F32)).astype(BF16)
    return high, low


def dft_tables(group, m_local, lon_count):
    owner, slot, part = np.meshgrid(np.arange(group), np.arange(m_local), np.arange(2), indexing='ij')
    wave = (slot * group + owner).reshape(-1)
    part = part.reshape(-1)
    phase = 2.0 * np.pi * ((wave[:, None] * np.arange(lon_count)[None, :]) % lon_count) / lon_count
    base = np.where(part[:, None] == 0, np.cos(phase), -np.sin(phase)) / math.sqrt(lon_count)
    gains = np.where(wave == 0, 1.0, 2.0)[:, None]
    return base.astype(np.float32), (base * gains).astype(np.float32)


def two_halves(table):
    high = jnp.asarray(table).astype(BF16)
    low = (jnp.asarray(table) - high.astype(F32)).astype(BF16)
    return jnp.stack([high, low])


class Halves:
    def __init__(self, whole, b, halves, slot, sem, outward=False):
        self.copies = []
        for half in range(halves.shape[1]):
            ends = whole.at[b, :, pl.ds(half * LANES, LANES)], halves.at[slot, half]
            source, target = ends[::-1] if outward else ends
            self.copies.append(pltpu.make_async_copy(source, target, sem.at[slot, half]))

    def start(self):
        for copy in self.copies:
            copy.start()

    def wait(self):
        for copy in self.copies:
            copy.wait()


def read_row(halves, slot, t, channels, rows_local):
    at = pl.ds(t, channels, stride=rows_local)
    return jnp.concatenate([halves[slot, half, at, :] for half in range(halves.shape[1])], axis=1)


def write_row(halves, slot, t, channels, rows_local, values):
    at = pl.ds(t, channels, stride=rows_local)
    for half in range(halves.shape[1]):
        halves[slot, half, at, :] = values[:, half * LANES:(half + 1) * LANES]


class Exchange:
    def __init__(self, me, group, batch, send, recv, send_sem, recv_sem):
        self.me, self.group, self.batch = me, group, batch
        self.send, self.recv, self.send_sem, self.recv_sem = send, recv, send_sem, recv_sem

    def all_copies(self, b):
        slot = lax.rem(b, SLOTS)
        others = pl.ds(0, self.group - 1)
        return pltpu.make_async_remote_copy(
            self.send.at[slot, others], self.recv.at[b, others], self.send_sem.at[slot], self.recv_sem.at[b],
            device_id={'lat': lax.rem(self.me + 1, self.group)}, device_id_type=MESH)

    def reserve(self, b):
        @pl.when(b >= SLOTS)
        def _():
            self.all_copies(b - SLOTS).wait_send()

    def start(self, b):
        slot = lax.rem(b, SLOTS)
        self.recv[b, self.me] = self.send[slot, self.me]

        @pl.loop(1, self.group)
        def _(step):
            target = jnp.bitwise_xor(self.me, jnp.where(step <= 8, 16 - step, step - 8))
            pltpu.make_async_remote_copy(
                self.send.at[slot, target], self.recv.at[b, self.me], self.send_sem.at[slot], self.recv_sem.at[b],
                device_id={'lat': target}, device_id_type=MESH).start()

    def arrive(self, b):
        self.all_copies(b).wait_recv()

    def drain(self):
        for b in range(max(0, self.batch - SLOTS), self.batch):
            self.all_copies(b).wait_send()


class BridgedExchange:
    def __init__(self, me, group, batch, bufs, sems):
        self.me, self.group, self.batch = me, group, batch
        self.send, self.recv, self.bridge_send, self.bridge_recv, self.relay_send, self.flipped_far = bufs
        self.send_sem, self.recv_sem, self.bridge_send_sem, self.bridge_recv_sem, self.relay_send_sem, self.relay_recv_sem = sems
        self.half_size = group // 2
        self.half = me // self.half_size
        self.place = lax.rem(me, self.half_size)
        self.twin = self.half_size + me - 2 * self.half_size * self.half
        self.rows = self.send.shape[2]
        self.late_rows = self.relay_send.shape[2]
        self.early_rows = self.rows - self.late_rows
        self.tile = self.late_rows // self.flipped_far.shape[0]
        self.direct = self.early_rows // self.tile

    def copy(self, source, target, send_sem, recv_sem, device):
        return pltpu.make_async_remote_copy(source, target, send_sem, recv_sem, device_id={'lat': device},
                                            device_id_type=MESH)

    def all_direct(self, b):
        slot = lax.rem(b, SLOTS)
        count = (self.half_size - 1) * self.rows + self.half_size * self.early_rows
        span = pl.ds(0, count // self.rows)
        return self.copy(self.send.at[slot, span], self.recv.at[b, span], self.send_sem.at[slot], self.recv_sem.at[b], self.twin)

    def all_relayed(self, b):
        slot = lax.rem(b, SLOTS)
        span, part = pl.ds(0, self.half_size - 1), pl.ds(0, self.late_rows)
        return self.copy(self.relay_send.at[slot, span], self.recv.at[b, span, part], self.relay_send_sem.at[slot],
                         self.relay_recv_sem.at[b], self.twin)

    def bridge(self, b):
        slot = lax.rem(b, SLOTS)
        return self.copy(self.bridge_send.at[slot], self.bridge_recv.at[b], self.bridge_send_sem.at[slot],
                         self.bridge_recv_sem.at[b], self.twin)

    def reserve(self, b):
        @pl.when(b >= SLOTS)
        def _():
            self.all_direct(b - SLOTS).wait_send()
            self.bridge(b - SLOTS).wait_send()

    def start(self, b):
        slot = lax.rem(b, SLOTS)
        self.bridge(b).start()
        early = pl.ds(0, self.early_rows)

        @pl.loop(0, self.half_size)
        def _(step):
            target = jnp.bitwise_xor(self.me, 2 * self.half_size - 1 - step)
            self.copy(self.send.at[slot, target, early], self.recv.at[b, self.me, early], self.send_sem.at[slot],
                      self.recv_sem.at[b], target).start()

        @pl.loop(1, self.half_size)
        def _(step):
            target = jnp.bitwise_xor(self.me, self.half_size - step)
            self.copy(self.send.at[slot, target], self.recv.at[b, self.me], self.send_sem.at[slot], self.recv_sem.at[b],
                      target).start()

        self.recv[b, self.me] = self.send[slot, self.me]

    def relay(self, b):
        slot = lax.rem(b, SLOTS)

        @pl.when(b >= SLOTS)
        def _():
            self.all_relayed(b - SLOTS).wait_send()

        self.bridge(b).wait_recv()
        lats, degrees = self.flipped_far.shape[1:]
        own = pl.ds(pl.multiple_of(self.half * (lats // 2), lats // 2), lats // 2)
        at = 0
        for late in range(self.flipped_far.shape[0]):
            first = (self.direct + late) * self.group
            count = degrees - first
            parts = []
            for part in range(2):
                rows = self.bridge_recv[b, part, pl.ds(at, count), :]
                parts.append(jnp.concatenate([jnp.zeros((first, rows.shape[1]), BF16), rows], axis=0))
            at += count
            res = dot(self.flipped_far[late, own, :], jnp.concatenate(parts, axis=1), NN)
            lanes = res.shape[1] // 2
            blocks = [res[:, part * lanes:(part + 1) * lanes].reshape(self.half_size, self.tile // 2, lanes) for part in range(2)]
            self.relay_send[slot, :, pl.ds(late * self.tile, self.tile), :] = jnp.concatenate(blocks, axis=1).astype(BF16)
        late_at = pl.ds(self.early_rows, self.late_rows)

        @pl.loop(1, self.half_size)
        def _(step):
            place = jnp.bitwise_xor(self.place, self.half_size - step)
            self.copy(self.relay_send.at[slot, place], self.recv.at[b, self.twin, late_at], self.relay_send_sem.at[slot],
                      self.relay_recv_sem.at[b], self.half * self.half_size + place).start()

        self.recv[b, self.twin, late_at] = self.relay_send[slot, self.place]

    def arrive(self, b):
        self.all_direct(b).wait_recv()
        self.all_relayed(b).wait_recv()

    def drain(self):
        for b in range(max(0, self.batch - SLOTS), self.batch):
            self.all_direct(b).wait_send()
            self.bridge(b).wait_send()
            self.all_relayed(b).wait_send()


class Share:
    def __init__(self, me, group, batch, send, message, out, sems):
        self.batch, self.send, self.message, self.out = batch, send, message, out
        self.send_sem, self.recv_sem, self.local_sem = sems
        self.size = group // 2
        self.base = me // self.size * self.size
        self.place = lax.rem(me, self.size)

    def rank(self, place):
        return place // 4 + 2 * (lax.rem(place, 4) // 2) + 4 * lax.rem(place, 2)

    def copy(self, slot, source, b, target, place):
        return pltpu.make_async_remote_copy(
            self.send.at[slot, source], self.out.at[b, target], self.send_sem.at[slot], self.recv_sem.at[b],
            device_id={'lat': self.base + place}, device_id_type=MESH)

    def every(self, b):
        span = pl.ds(0, self.size - 1)
        return self.copy(lax.rem(b, SLOTS), span, b, span, lax.rem(self.place + 1, self.size))

    def keep(self, b):
        slot = lax.rem(b, SLOTS)
        return pltpu.make_async_copy(self.send.at[slot, self.rank(self.place)], self.out.at[b, self.place],
                                     self.local_sem.at[slot])

    def give(self, b, coef):
        slot_b = lax.rem(b, SLOTS)

        @pl.when(b >= SLOTS)
        def _():
            self.every(b - SLOTS).wait_send()

        size = self.size
        m_local = size
        tile = 2 * size

        def rows(part, slot, rank, first, count):
            return coef[part, pl.ds((first * size + rank) * m_local + slot, count, stride=size * m_local), :]

        for rank in range(size):
            for part in range(2):
                for pair in range(m_local // 2):
                    block = rows(part, pair, rank, 0, tile)
                    if pair:
                        block = block + rows(part, m_local - pair, rank, 2 * (m_local - pair), tile)
                    self.message[rank, pl.ds((part * (m_local // 2) + pair) * tile, tile), :] = block
                self.message[rank, pl.ds(m_local * tile + part * size, size), :] = rows(part, m_local // 2, rank, size, size)
        for rank in range(size):
            self.send[slot_b, rank] = self.message[rank].astype(BF16)
        self.keep(b).start()

        @pl.loop(1, size)
        def _(step):
            place = jnp.bitwise_xor(self.place, size - step)
            self.copy(slot_b, self.rank(place), b, self.place, place).start()

        self.keep(b).wait()

    def drain(self):
        for b in range(max(0, self.batch - SLOTS), self.batch):
            self.every(b).wait_send()

    def arrive(self, b):
        self.every(b).wait_recv()


def clear_after(coef, used):
    for part in range(coef.shape[0]):
        coef[part, pl.ds(used, coef.shape[1] - used), :] = jnp.zeros((coef.shape[1] - used, coef.shape[2]), F32)


def greet(me, group):
    barrier = pltpu.get_barrier_semaphore()

    @pl.loop(1, group)
    def _(step):
        pl.semaphore_signal(barrier, inc=1, device_id={'lat': lax.rem(me + step, group)}, device_id_type=MESH)


def meet(group):
    pl.semaphore_wait(pltpu.get_barrier_semaphore(), group - 1)


class Tables:
    def __init__(self, waves, whole, stage, sem):
        self.waves, self.whole, self.stage, self.sem = waves, whole, stage, sem

    def start(self):
        for n, wave in enumerate(self.waves):
            pltpu.make_async_copy(self.whole.at[wave], self.stage.at[n], self.sem).start()

    def wait(self):
        pltpu.make_async_copy(self.whole.at[pl.ds(0, len(self.waves))], self.stage, self.sem).wait()


def own_tables(me, group, whole, stage, sem):
    return Tables([slot * group + me for slot in range(stage.shape[0])], whole, stage, sem)


def far_tables(swap, whole, stage, sem):
    return Tables([(swap.direct + n) * swap.group + swap.twin for n in range(stage.shape[0])], whole, stage, sem)


def expand_rows(stage, expanded, rows_local):
    m_local, degrees, lats = stage.shape
    row = lax.broadcasted_iota(jnp.int32, (lats, 2 * lats), 0)
    col = lax.broadcasted_iota(jnp.int32, (lats, 2 * lats), 1)
    source = col // (2 * rows_local)
    inner = col % (2 * rows_local)
    for part in range(2):
        pick = (row == source * rows_local + inner - part * rows_local) & (inner // rows_local == part)
        pick = pick.astype(F32).astype(BF16)
        for slot in range(m_local):
            expanded[slot, pl.ds(part * degrees, degrees), :] = dot(stage[slot].astype(BF16), pick, NN).astype(BF16)


def flip_rows(stage, flipped):
    for slot in range(stage.shape[0]):
        flipped[slot] = stage[slot].T.astype(BF16)


def analyse(values_at, table, turn, rows_local):
    modes = table.shape[1]
    for t in range(0, rows_local, 2):
        pair = jnp.concatenate([values_at(t), values_at(t + 1)], axis=0)
        high, low = split_halves(pair * 0.5)
        out = 2.0 * (dot(table[0], high, NT) + dot(table[0], low, NT) + dot(table[1], high, NT))
        channels = out.shape[1] // 2
        turn[pl.ds(t, modes, stride=rows_local), :] = out[:, :channels]
        turn[pl.ds(t + 1, modes, stride=rows_local), :] = out[:, channels:]


def pack_blocks(turn, send, slot):
    group, rows, lanes = send.shape[1:]
    for d in range(group):
        send[slot, d] = turn[pl.ds(d * rows, rows), :].astype(BF16)


def unpack_blocks(recv, b, turn):
    group, rows, lanes = recv.shape[1:]
    for d in range(group):
        turn[pl.ds(d * rows, rows), :] = recv[b, d].astype(F32)


def synthesise(turn, t, table, rows_local):
    modes = table.shape[1]
    spec = turn[pl.ds(t, modes, stride=rows_local), :].astype(BF16)
    return dot(spec, table[0], TN) + dot(spec, table[1], TN)


def legendre_forward(recv, b, expanded, out, rows_local):
    m_local = expanded.shape[0]
    degrees = expanded.shape[1] // 2
    group, _, lanes = recv.shape[1:]
    tile = 2 * rows_local
    for slot in range(m_local):
        rows = recv[b, :, pl.ds(slot * tile, tile), :].reshape(group * tile, lanes)
        res = dot(expanded[slot], rows, NN)
        for part in range(2):
            out[part, pl.ds(slot, degrees, stride=m_local), :] = res[part * degrees:(part + 1) * degrees]


def legendre_inverse(coef, flipped, swap, slot_out, rows_local):
    m_local, lats, degrees = flipped.shape
    send = swap.send
    at = 0
    group = lats // rows_local
    tile = 2 * rows_local
    for slot in range(m_local):
        parts = [coef.at[part][pl.ds(slot, degrees, stride=m_local), :].astype(BF16) for part in range(2)]
        if slot >= swap.direct:
            first = slot * group
            for part in range(2):
                swap.bridge_send[slot_out, part, pl.ds(at, degrees - first), :] = parts[part][first:]
            at += degrees - first
        res = dot(flipped[slot], jnp.concatenate(parts, axis=1), NN)
        lanes = res.shape[1] // 2
        blocks = [res[:, part * lanes:(part + 1) * lanes].reshape(group, rows_local, lanes) for part in range(2)]
        send[slot_out, :, pl.ds(slot * tile, tile), :] = jnp.concatenate(blocks, axis=1).astype(BF16)


def gelu_slope(values):
    cumulative = 0.5 * (1.0 + lax.erf(values * math.sqrt(0.5)))
    density = jnp.exp(-0.5 * values * values) * (1.0 / math.sqrt(2.0 * math.pi))
    return cumulative + values * density


def mix_block(planes):
    real, imag = planes[0], planes[1]
    return jnp.concatenate([jnp.concatenate([real, -imag], axis=1), jnp.concatenate([imag, real], axis=1)], axis=0)


class WeightSum:
    def __init__(self, me, group, sums, got, out, sems):
        self.me, self.sums, self.got, self.out, self.sems = me, sums, got, out, sems
        self.core, self.y = lax.rem(me, 2), lax.rem(me // 2, 2)
        self.near, self.far = lax.rem(me // 4, 2), me // (group // 2)
        self.rank = self.near + 2 * self.y + 4 * self.core

    def peer(self, phase):
        step = (1, 2, 4, 8)[phase]
        bit = (self.core, self.y, self.near, self.far)[phase]
        return {'lat': self.me + step - 2 * step * bit}

    def remote(self, phase, k, source, target, stage):
        return pltpu.make_async_remote_copy(source, target, self.sems.at[0, stage, k], self.sems.at[1, stage, k],
                                            device_id=self.peer(phase), device_id_type=MESH)

    def halving(self, k):
        pair, at = self.piece(k)
        return self.remote(3, k, self.sums.at[2 * pair + 1 - self.far, at], self.got.at[k], 4)

    def piece(self, k):
        rows = self.got.shape[1]
        pieces = self.sums.shape[1] // rows
        return k // pieces, pl.ds(pl.multiple_of(lax.rem(k, pieces) * rows, rows), rows)

    def settle(self, k):
        pair, at = self.piece(k)
        mine = 2 * pair + self.far
        return pltpu.make_async_copy(self.sums.at[mine, at], self.out.at[mine, self.rank, at], self.sems.at[0, 5, k])

    def doubling(self, phase, k):
        pair, at = self.piece(k)
        if phase == 3:
            mine = 2 * pair + self.far
            return self.remote(3, k, self.sums.at[mine, at], self.out.at[mine, self.rank, at], 3)
        width = (4, 2, 1)[phase]
        first = (4 * self.core, 4 * self.core + 2 * self.y, self.rank)[phase]
        span = self.out.at[pl.ds(2 * pair, 2), pl.ds(first, width), at]
        return self.remote(phase, k, span, span, phase)

    def reduce_step(self, k):
        self.halving(k).wait()
        pair, at = self.piece(k)
        mine = 2 * pair + self.far
        self.sums[mine, at] = self.sums[mine, at] + self.got[k]
        self.settle(k).start()
        self.doubling(3, k).start()

    def gather_step(self, phase, k):
        if phase == 2:
            self.settle(k).wait()
        self.doubling(phase + 1, k).wait()
        if phase >= 0:
            self.doubling(phase, k).start()


def shared_place(part, slot, step, m_local):
    tile = 2 * m_local
    if slot == m_local // 2:
        return m_local * tile + part * m_local + step - m_local
    pair = min(slot, m_local - slot) if slot else 0
    shift = 0 if slot < m_local // 2 else 2 * slot
    return (part * (m_local // 2) + pair) * tile + step - shift


def weigh(shared, sources, sums, m_local):
    stride = shared.shape[1] // sources

    @pl.loop(0, sums.shape[0])
    def _(step):
        sides = []
        for which in range(2):
            slots = []
            for slot in range(m_local):
                used = step >= 2 * slot
                parts = []
                for part in range(2):
                    place = jnp.where(used, shared_place(part, slot, step, m_local), 0)
                    rows = shared[which, pl.ds(place, sources, stride=stride), :]
                    parts.append(jnp.where(used, rows, 0.0))
                slots.append(jnp.concatenate(parts, axis=1))
            sides.append(jnp.concatenate(slots, axis=0).astype(BF16))
        big = dot(sides[0], sides[1], TN)
        half = big.shape[0] // 2
        real, imag = pl.ds(0, half, stride=2), pl.ds(1, half, stride=2)
        sums[step, real, :] = sums[step, real, :] + (big[:half, :half] + big[half:, half:])
        sums[step, imag, :] = sums[step, imag, :] + (big[half:, :half] - big[:half, half:])


def whole_kernel(group, rows_local, field, grad, base_hbm, gained_hbm, p_fwd, p_inv, w_mix, field_out, grad_w, back_out, coef_shared,
                 mixed_shared, field_buf, grad_buf, turn, stage, stage_far, expanded_fwd, expanded_inv, flipped, send_f, recv_f,
                 padded, coef, mixed, w_in, planes, bridged, send_d, recv_d, message, share_send_a, share_send_d, halves,
                 shared, sums, back, got, field_sem, grad_sem, p_sem, far_sem, send_f_sem, recv_f_sem, w_sem, bridged_sems,
                 send_d_sem, recv_d_sem, share_a_sems, share_d_sems, half_sem, out_sem, gw_sem, again_sems, back_sem, last_sem, base, gained,
                 table_sem):
    me = lax.axis_index('lat')
    batch = field.shape[0]
    channels = field.shape[1] // rows_local
    m_local, degrees = stage.shape[:2]
    used = degrees * m_local
    bunch = coef.shape[0]
    sources, share_rows = coef_shared.shape[1:3]

    def fetch_field(b):
        return Halves(field, b, field_buf, lax.rem(b, 2), field_sem)

    def fetch_grad(b):
        return Halves(grad, b, grad_buf, lax.rem(b, 2), grad_sem)

    def put(b):
        return pltpu.make_async_copy(back.at[lax.rem(b, bunch)], back_out.at[b], out_sem.at[lax.rem(b, bunch)])

    def fetch_back(b):
        return pltpu.make_async_copy(back_out.at[b], coef.at[lax.rem(b, 2)], back_sem.at[lax.rem(b, 2)])

    def fetch_last(b):
        return Halves(grad, b, field_buf, lax.rem(b, 2), field_sem)

    def put_last(b):
        return Halves(field_out, b, field_buf, lax.rem(b, 2), last_sem, outward=True)

    def fetch_shares(b):
        slot = lax.rem(b, 2)
        return [pltpu.make_async_copy(whole.at[b], halves.at[slot, which], half_sem.at[slot, which])
                for which, whole in enumerate((mixed_shared, coef_shared))]

    load_base = pltpu.make_async_copy(base_hbm, base, table_sem.at[0])
    load_gained = pltpu.make_async_copy(gained_hbm, gained, table_sem.at[1])
    fetch_field(0).start()
    load_base.start()
    greet(me, group)
    load_gained.start()
    fetch_grad(0).start()
    loading = own_tables(me, group, p_fwd, stage, p_sem)
    loading_inv = own_tables(me, group, p_inv, stage, p_sem)
    loading.start()
    swap_f = Exchange(me, group, batch, send_f, recv_f, send_f_sem, recv_f_sem)
    swap_g = BridgedExchange(me, group, batch, bridged, bridged_sems)
    swap_h = BridgedExchange(me, group, batch, bridged, again_sems)
    total = WeightSum(me, group, sums, got, grad_w, gw_sem)
    swap_d = Exchange(me, group, batch, send_d, recv_d, send_d_sem, recv_d_sem)
    share_a = Share(me, group, batch, share_send_a, message, coef_shared, share_a_sems)
    share_d = Share(me, group, batch, share_send_d, message, mixed_shared, share_d_sems)
    loading_far = far_tables(swap_g, p_inv, stage_far, far_sem)
    loading_far.start()
    loading_fwd = own_tables(me, group, p_fwd, stage, p_sem)
    loading_far_fwd = far_tables(swap_h, p_fwd, stage_far, far_sem)
    chunks = got.shape[0]

    def build_planes():
        depth, per = w_in.shape[:2]
        blocks = degrees // per
        half = w_in.shape[2] // 2

        def fetch(k):
            return pltpu.make_async_copy(w_mix.at[pl.ds(k * per, per)], w_in.at[lax.rem(k, depth)], w_sem.at[lax.rem(k, depth)])

        for k in range(depth - 1):
            fetch(k).start()

        @pl.loop(0, blocks)
        def _(k):
            @pl.when(k + depth - 1 < blocks)
            def _():
                fetch(k + depth - 1).start()

            fetch(k).wait()
            for inner in range(per):
                rows = w_in.at[lax.rem(k, depth), inner]
                for part in range(2):
                    planes[k * per + inner, part] = rows[pl.ds(part, half, stride=2), :].astype(BF16)

    def unmix_bunch():
        @pl.loop(0, degrees // 8)
        def _(k):
            for inner in range(8):
                at = pl.ds(pl.multiple_of((k * 8 + inner) * m_local, m_local), m_local)
                rows = [back[:, part, at, :].reshape(bunch * m_local, channels) for part in range(2)]
                res = dot(jnp.concatenate(rows, axis=1).astype(BF16), mix_block(planes[k * 8 + inner]), NN)
                for part in range(2):
                    back[:, part, at, :] = res[:, part * channels:(part + 1) * channels].reshape(bunch, m_local, channels)

    def mix_bunch():
        @pl.loop(0, degrees // 8)
        def _(k):
            for inner in range(8):
                at = pl.ds(pl.multiple_of((k * 8 + inner) * m_local, m_local), m_local)
                rows = [coef[:, part, at, :].reshape(bunch * m_local, channels) for part in range(2)]
                res = dot(jnp.concatenate(rows, axis=1).astype(BF16), mix_block(planes[k * 8 + inner]), NT)
                for part in range(2):
                    mixed[:, part, at, :] = res[:, part * channels:(part + 1) * channels].reshape(bunch, m_local, channels)

    def weigh_sample(b):
        for copy in fetch_shares(b):
            copy.wait()
        for which in range(2):
            for source in range(sources):
                at = pl.ds(source * (shared.shape[1] // sources), share_rows)
                shared[which, at, :] = halves[lax.rem(b, 2), which, source].astype(F32)
        weigh(shared, sources, sums, m_local)

    def collect(b):
        share_a.arrive(b)
        share_d.arrive(b)
        for copy in fetch_shares(b):
            copy.start()

    lag_a, lag_b, lag_c, lag_d = 2, 4, 6, 8
    lag_e = batch + lag_c
    close = batch + lag_d
    steps = [total.reduce_step] + [functools.partial(total.gather_step, p) for p in (2, 1, 0, -1)]

    def advance(n, sub):
        @pl.when((n >= 0) & (n * 2 + sub + 2 < chunks))
        def _():
            total.halving(n * 2 + sub + 2).start()

        for late, step in reversed(list(enumerate(steps))):
            k = (n - late) * 2 + sub

            @pl.when((k >= 0) & (k < chunks))
            def _():
                step(k)

    def take_modes(b):
        @pl.when(b + 1 < batch)
        def _():
            fetch_field(b + 1).start()

        fetch_field(b).wait()
        half = lax.rem(b, 2)
        analyse(lambda t: read_row(field_buf, half, t, channels, rows_local), base, turn, rows_local)
        swap_f.reserve(b)
        pack_blocks(turn, send_f, lax.rem(b, SLOTS))

    load_base.wait()
    take_modes(0)
    meet(group)

    def body(i, carry):
        @pl.when((i >= lag_e) & (i < batch + lag_e))
        def _():
            b = i - lag_e

            @pl.when(b + 1 < batch)
            def _():
                fetch_back(b + 1).start()

            fetch_back(b).wait()
            swap_h.reserve(b)
            legendre_inverse(coef.at[lax.rem(b, 2)], flipped, swap_h, lax.rem(b, SLOTS), rows_local)
            swap_h.start(b)

        @pl.when((i >= 1) & (i < batch))
        def _():
            take_modes(i)

        @pl.when(i < batch)
        def _():
            swap_f.start(i)

        @pl.when(i == 0)
        def _():
            clear_after(padded, used)
            load_gained.wait()
            loading.wait()
            expand_rows(stage, expanded_fwd, rows_local)
            loading_inv.start()
            loading_far.wait()
            flip_rows(stage_far, swap_g.flipped_far)

        @pl.when(i == 1)
        def _():
            build_planes()
            loading_inv.wait()
            expand_rows(stage, expanded_inv, rows_local)
            flip_rows(stage, flipped)
            sums[...] = jnp.zeros_like(sums)

        @pl.when((i >= lag_a) & (i < batch + lag_a))
        def _():
            b = i - lag_a
            swap_f.arrive(b)
            legendre_forward(recv_f, b, expanded_fwd, padded, rows_local)
            coef[lax.rem(b, bunch)] = padded[:, pl.ds(0, used), :]
            share_a.give(b, padded)

            @pl.when(lax.rem(b, bunch) == bunch - 1)
            def _():
                mix_bunch()

        @pl.when((i >= lag_b) & (i < batch + lag_b))
        def _():
            b = i - lag_b
            swap_g.reserve(b)
            legendre_inverse(mixed.at[lax.rem(b, bunch)], flipped, swap_g, lax.rem(b, SLOTS), rows_local)
            swap_g.start(b)

        @pl.when((i >= lag_b + 1) & (i < batch + lag_b + 1))
        def _():
            swap_g.relay(i - lag_b - 1)

        @pl.when((i >= lag_c) & (i < batch + lag_c))
        def _():
            b = i - lag_c
            half = lax.rem(b, 2)

            @pl.when(b + 1 < batch)
            def _():
                fetch_grad(b + 1).start()

            fetch_grad(b).wait()
            swap_g.arrive(b)
            unpack_blocks(swap_g.recv, b, turn)
            for t in range(rows_local):
                slope = gelu_slope(synthesise(turn, t, gained, rows_local))
                given = read_row(grad_buf, half, t, channels, rows_local)
                write_row(grad_buf, half, t, channels, rows_local, given * slope)
            analyse(lambda t: read_row(grad_buf, half, t, channels, rows_local), gained, turn, rows_local)
            swap_d.reserve(b)
            pack_blocks(turn, send_d, lax.rem(b, SLOTS))
            swap_d.start(b)

        @pl.when(i == lag_e - 2)
        def _():
            loading_fwd.start()
            loading_far_fwd.start()

        @pl.when(i == lag_e - 1)
        def _():
            loading_fwd.wait()
            flip_rows(stage, flipped)
            loading_far_fwd.wait()
            flip_rows(stage_far, swap_h.flipped_far)
            swap_g.drain()
            fetch_back(0).start()

        @pl.when((i >= lag_d) & (i < batch + lag_d))
        def _():
            b = i - lag_d

            @pl.when((b >= bunch) & (lax.rem(b, bunch) == 0))
            def _():
                unmix_bunch()
                for n in range(bunch):
                    put(b - bunch + n).start()

            @pl.when(b >= 2)
            def _():
                weigh_sample(b - 2)

            @pl.when(b >= 1)
            def _():
                collect(b - 1)

            swap_d.arrive(b)
            legendre_forward(recv_d, b, expanded_inv, padded, rows_local)
            share_d.give(b, padded)

            @pl.when(b >= bunch)
            def _():
                put(b - bunch).wait()

            back[lax.rem(b, bunch)] = padded[:, pl.ds(0, used), :]

        @pl.when(i == close)
        def _():
            fetch_last(0).start()
            weigh_sample(batch - 2)
            collect(batch - 1)
            weigh_sample(batch - 1)
            for k in range(2):
                total.halving(k).start()

        advance(i - close, 0)

        @pl.when((i >= lag_e + 1) & (i < batch + lag_e + 1))
        def _():
            swap_h.relay(i - lag_e - 1)

        @pl.when((i >= close) & (i < batch + close))
        def _():
            b = i - close
            half = lax.rem(b, 2)

            @pl.when(b >= 1)
            def _():
                put_last(b - 1).wait()

            @pl.when(b + 1 < batch)
            def _():
                fetch_last(b + 1).start()

            fetch_last(b).wait()
            swap_h.arrive(b)
            unpack_blocks(swap_h.recv, b, turn)
            for t in range(rows_local):
                added = synthesise(turn, t, base, rows_local)
                given = read_row(field_buf, half, t, channels, rows_local)
                write_row(field_buf, half, t, channels, rows_local, given + added)
            put_last(b).start()

        @pl.when(i == close + 1)
        def _():
            unmix_bunch()
            for n in range(bunch):
                put(batch - bunch + n).start()

        @pl.when(i == close + 3)
        def _():
            for n in range(bunch):
                put(batch - bunch + n).wait()

        advance(i - close, 1)
        return carry

    lax.fori_loop(0, close + max(batch, chunks // 2 + 4), body, 0)
    for swap in (swap_f, swap_h, swap_d, share_a, share_d):
        swap.drain()
    put_last(batch - 1).wait()


def finish_kernel(first, second, first_out, second_out, first_ring, second_ring, in_sem, out_sem):
    depth = first_ring.shape[0]
    pieces = []
    for side, (source, target, ring) in enumerate(((first, first_out, first_ring), (second, second_out, second_ring))):
        for n in range(source.shape[0]):
            slot = n % depth
            take = pltpu.make_async_copy(source.at[n], ring.at[slot], in_sem.at[side, slot])
            give = pltpu.make_async_copy(ring.at[slot], target.at[n], out_sem.at[side, slot])
            pieces.append(((n, side), (side, n), take, give))
    pieces.sort(key=lambda piece: piece[0])
    given = {piece[1]: piece[3] for piece in pieces}
    waited = set()
    for k in range(len(pieces) + depth):
        if k < len(pieces):
            _, (side, n), take, _ = pieces[k]
            if n >= depth:
                given[side, n - depth].wait()
                waited.add((side, n - depth))
            take.start()
        if k >= depth:
            pieces[k - depth][2].wait()
            pieces[k - depth][3].start()
    for _, place, _, give in pieces:
        if place not in waited:
            give.wait()


def any_specs(n):
    return [pl.BlockSpec(memory_space=pl.ANY)] * n


def params(collective_id=None):
    if collective_id is None:
        return pltpu.CompilerParams(vmem_limit_bytes=VMEM_LIMIT)
    return pltpu.CompilerParams(collective_id=collective_id, has_side_effects=True, vmem_limit_bytes=VMEM_LIMIT)


def solution(mesh):
    group = mesh.shape['lat']
    field_spec = P('member', None, 'lat', None)

    def local_step(field_loc, grad_loc, p_fwd, p_inv, w_mix):
        batch, channels, rows_local, lon_count = field_loc.shape
        degrees, lats = p_fwd.shape[1:]
        m_local = p_fwd.shape[0] // group
        modes = group * m_local * 2
        base, gained = (two_halves(table) for table in dft_tables(group, m_local, lon_count))
        field = field_loc.reshape(batch, channels * rows_local, lon_count)
        grad = grad_loc.reshape(batch, channels * rows_local, lon_count)
        w_rows = jnp.swapaxes(w_mix, 2, 3).reshape(degrees, channels * 2, channels)
        dma, vmem = pltpu.SemaphoreType.DMA, pltpu.VMEM
        block_rows = m_local * 2 * rows_local
        coef_shape = (batch, 2, degrees * m_local, channels)
        send_t = vmem((SLOTS, group, block_rows, channels), BF16)
        recv_t = vmem((batch, group, block_rows, channels), BF16)
        turn_t = vmem((modes * rows_local, channels), F32)
        stage_t = vmem((m_local, degrees, lats), F32)
        expanded_t = vmem((m_local, 2 * degrees, 2 * lats), BF16)
        flipped_t = vmem((m_local, lats, degrees), BF16)
        field_t = vmem((2, lon_count // LANES, channels * rows_local, LANES), F32)
        any_spec = pl.BlockSpec(memory_space=pl.ANY)
        late = sum(degrees - slot * group < lats // 2 for slot in range(m_local))
        far_rows = sum(degrees - slot * group for slot in range(m_local - late, m_local))
        late_rows = late * 2 * rows_local
        bridged_t = (send_t, recv_t, vmem((SLOTS, 2, far_rows, channels), BF16), vmem((batch, 2, far_rows, channels), BF16),
                     vmem((SLOTS, group // 2, late_rows, channels), BF16), vmem((late, lats, degrees), BF16))
        bridged_sems = (dma((SLOTS,)), dma((batch,))) * 3

        ranks = group // 2
        share_rows = (m_local + 1) * 2 * ranks
        share_out = jax.ShapeDtypeStruct((batch, ranks, share_rows, channels), BF16)
        share_sems = (dma((SLOTS,)), dma((batch,)), dma((SLOTS,)))

        far_stage_t = vmem((late, degrees, lats), F32)
        steps = degrees // ranks
        sums_shape = (steps, channels * 2, channels)
        planes_shape = (degrees, 2, channels, channels)
        single_t = vmem((BUNCH,) + coef_shape[1:], F32)
        share_send_t = vmem((SLOTS, ranks, share_rows, channels), BF16)
        swap_sems = (dma((SLOTS,)), dma((batch,)))
        field_out, gw_total, _, _, _ = pl.pallas_call(
            functools.partial(whole_kernel, group, rows_local), name='whole',
            out_shape=[jax.ShapeDtypeStruct(grad.shape, F32),
                       jax.ShapeDtypeStruct((steps, ranks, channels * 2, channels), F32),
                       jax.ShapeDtypeStruct(coef_shape, F32), share_out, share_out],
            in_specs=[any_spec] * 7, out_specs=[any_spec] * 5,
            scratch_shapes=[field_t, field_t, turn_t, stage_t, far_stage_t, expanded_t, expanded_t, flipped_t, send_t, recv_t,
                            vmem((2, 2 * degrees * m_local, channels), F32), single_t, single_t,
                            vmem((4, 4, channels * 2, channels), F32), vmem(planes_shape, BF16), bridged_t, send_t, recv_t,
                            vmem((ranks, share_rows, channels), F32), share_send_t, share_send_t,
                            vmem((2, 2) + share_out.shape[1:], BF16), vmem((2, ranks * (share_rows + 8), channels), F32),
                            vmem(sums_shape, F32), single_t, vmem((PIECES * steps // 2, channels * 2 // PIECES, channels), F32),
                            dma((2, 2)), dma((2, 2)), dma(()), dma(()), *swap_sems, dma((4,)), bridged_sems, *swap_sems,
                            share_sems, share_sems, dma((2, 2)), dma((BUNCH,)), dma((2, 6, PIECES * steps // 2)), bridged_sems,
                            dma((2,)), dma((2, 2)), vmem(base.shape, BF16), vmem(base.shape, BF16), dma((2,))],
            compiler_params=params(0))(field, grad, base, gained, p_fwd, p_inv, w_rows)

        gw_total = gw_total.reshape(steps, ranks * channels * 2, channels)
        results = [jax.ShapeDtypeStruct(whole.shape, F32) for whole in (field_out, gw_total)]
        field_out, gw_total = pl.pallas_call(
            finish_kernel, name='finish', out_shape=results, in_specs=[any_spec] * 2, out_specs=[any_spec] * 2,
            scratch_shapes=[vmem((RING,) + whole.shape[1:], F32) for whole in results] + [dma((2, RING)), dma((2, RING))],
            compiler_params=params())(field_out, gw_total)

        grad_wmix = jnp.swapaxes(gw_total.reshape(degrees, channels, 2, channels), 2, 3)
        return field_out.reshape(grad_loc.shape), grad_wmix

    return jax.shard_map(local_step, mesh=mesh, in_specs=(field_spec, field_spec, P(), P(), P()),
                         out_specs=(field_spec, P('member', None, None, None)), check_vma=False)
```

```python
import functools
import math

import jax
import jax.numpy as jnp
import numpy as np
from jax import lax
from jax.experimental import pallas as pl
from jax.experimental.pallas import tpu as pltpu
from jax.sharding import PartitionSpec as P

MESH = pl.DeviceIdType.MESH
LANES = 128
SLOTS = 3
BUNCH = 2
PIECES = 2
RING = 6
VMEM_LIMIT = 67043328
F32 = jnp.float32
BF16 = jnp.bfloat16

NN = (((1,), (0,)), ((), ()))
NT = (((1,), (1,)), ((), ()))
TN = (((0,), (0,)), ((), ()))


def dot(lhs, rhs, dims):
    return lax.dot_general(lhs, rhs, dims, preferred_element_type=F32)


def split_halves(values):
    high = values.astype(BF16)
    low = (values - high.astype(F32)).astype(BF16)
    return high, low


def dft_tables(group, m_local, lon_count):
    owner, slot, part = np.meshgrid(np.arange(group), np.arange(m_local), np.arange(2), indexing='ij')
    wave = (slot * group + owner).reshape(-1)
    part = part.reshape(-1)
    phase = 2.0 * np.pi * ((wave[:, None] * np.arange(lon_count)[None, :]) % lon_count) / lon_count
    base = np.where(part[:, None] == 0, np.cos(phase), -np.sin(phase)) / math.sqrt(lon_count)
    gains = np.where(wave == 0, 1.0, 2.0)[:, None]
    return base.astype(np.float32), (base * gains).astype(np.float32)


def two_halves(table):
    high = jnp.asarray(table).astype(BF16)
    low = (jnp.asarray(table) - high.astype(F32)).astype(BF16)
    return jnp.stack([high, low])


class Halves:
    def __init__(self, whole, b, halves, slot, sem, outward=False):
        self.copies = []
        for half in range(halves.shape[1]):
            ends = whole.at[b, :, pl.ds(half * LANES, LANES)], halves.at[slot, half]
            source, target = ends[::-1] if outward else ends
            self.copies.append(pltpu.make_async_copy(source, target, sem.at[slot, half]))

    def start(self):
        for copy in self.copies:
            copy.start()

    def wait(self):
        for copy in self.copies:
            copy.wait()


def read_row(halves, slot, t, channels, rows_local):
    at = pl.ds(t, channels, stride=rows_local)
    return jnp.concatenate([halves[slot, half, at, :] for half in range(halves.shape[1])], axis=1)


def write_row(halves, slot, t, channels, rows_local, values):
    at = pl.ds(t, channels, stride=rows_local)
    for half in range(halves.shape[1]):
        halves[slot, half, at, :] = values[:, half * LANES:(half + 1) * LANES]


class Exchange:
    def __init__(self, me, group, batch, send, recv, send_sem, recv_sem):
        self.me, self.group, self.batch = me, group, batch
        self.send, self.recv, self.send_sem, self.recv_sem = send, recv, send_sem, recv_sem

    def all_copies(self, b):
        slot = lax.rem(b, SLOTS)
        others = pl.ds(0, self.group - 1)
        return pltpu.make_async_remote_copy(
            self.send.at[slot, others], self.recv.at[b, others], self.send_sem.at[slot], self.recv_sem.at[b],
            device_id={'lat': lax.rem(self.me + 1, self.group)}, device_id_type=MESH)

    def reserve(self, b):
        @pl.when(b >= SLOTS)
        def _():
            self.all_copies(b - SLOTS).wait_send()

    def start(self, b):
        slot = lax.rem(b, SLOTS)
        self.recv[b, self.me] = self.send[slot, self.me]

        @pl.loop(1, self.group)
        def _(step):
            target = jnp.bitwise_xor(self.me, jnp.where(step <= 8, 16 - step, step - 8))
            pltpu.make_async_remote_copy(
                self.send.at[slot, target], self.recv.at[b, self.me], self.send_sem.at[slot], self.recv_sem.at[b],
                device_id={'lat': target}, device_id_type=MESH).start()

    def arrive(self, b):
        self.all_copies(b).wait_recv()

    def drain(self):
        for b in range(max(0, self.batch - SLOTS), self.batch):
            self.all_copies(b).wait_send()


class BridgedExchange:
    def __init__(self, me, group, batch, bufs, sems):
        self.me, self.group, self.batch = me, group, batch
        self.send, self.recv, self.bridge_send, self.bridge_recv, self.relay_send, self.flipped_far = bufs
        self.send_sem, self.recv_sem, self.bridge_send_sem, self.bridge_recv_sem, self.relay_send_sem, self.relay_recv_sem = sems
        self.half_size = group // 2
        self.half = me // self.half_size
        self.place = lax.rem(me, self.half_size)
        self.twin = self.half_size + me - 2 * self.half_size * self.half
        self.rows = self.send.shape[2]
        self.late_rows = self.relay_send.shape[2]
        self.early_rows = self.rows - self.late_rows
        self.tile = self.late_rows // self.flipped_far.shape[0]
        self.direct = self.early_rows // self.tile

    def copy(self, source, target, send_sem, recv_sem, device):
        return pltpu.make_async_remote_copy(source, target, send_sem, recv_sem, device_id={'lat': device},
                                            device_id_type=MESH)

    def all_direct(self, b):
        slot = lax.rem(b, SLOTS)
        count = (self.half_size - 1) * self.rows + self.half_size * self.early_rows
        span = pl.ds(0, count // self.rows)
        return self.copy(self.send.at[slot, span], self.recv.at[b, span], self.send_sem.at[slot], self.recv_sem.at[b], self.twin)

    def all_relayed(self, b):
        slot = lax.rem(b, SLOTS)
        span, part = pl.ds(0, self.half_size - 1), pl.ds(0, self.late_rows)
        return self.copy(self.relay_send.at[slot, span], self.recv.at[b, span, part], self.relay_send_sem.at[slot],
                         self.relay_recv_sem.at[b], self.twin)

    def bridge(self, b):
        slot = lax.rem(b, SLOTS)
        return self.copy(self.bridge_send.at[slot], self.bridge_recv.at[b], self.bridge_send_sem.at[slot],
                         self.bridge_recv_sem.at[b], self.twin)

    def reserve(self, b):
        @pl.when(b >= SLOTS)
        def _():
            self.all_direct(b - SLOTS).wait_send()
            self.bridge(b - SLOTS).wait_send()

    def start(self, b):
        slot = lax.rem(b, SLOTS)
        self.bridge(b).start()
        early = pl.ds(0, self.early_rows)

        @pl.loop(0, self.half_size)
        def _(step):
            target = jnp.bitwise_xor(self.me, 2 * self.half_size - 1 - step)
            self.copy(self.send.at[slot, target, early], self.recv.at[b, self.me, early], self.send_sem.at[slot],
                      self.recv_sem.at[b], target).start()

        @pl.loop(1, self.half_size)
        def _(step):
            target = jnp.bitwise_xor(self.me, self.half_size - step)
            self.copy(self.send.at[slot, target], self.recv.at[b, self.me], self.send_sem.at[slot], self.recv_sem.at[b],
                      target).start()

        self.recv[b, self.me] = self.send[slot, self.me]

    def relay(self, b):
        slot = lax.rem(b, SLOTS)

        @pl.when(b >= SLOTS)
        def _():
            self.all_relayed(b - SLOTS).wait_send()

        self.bridge(b).wait_recv()
        lats, degrees = self.flipped_far.shape[1:]
        own = pl.ds(pl.multiple_of(self.half * (lats // 2), lats // 2), lats // 2)
        at = 0
        for late in range(self.flipped_far.shape[0]):
            first = (self.direct + late) * self.group
            count = degrees - first
            parts = []
            for part in range(2):
                rows = self.bridge_recv[b, part, pl.ds(at, count), :]
                parts.append(jnp.concatenate([jnp.zeros((first, rows.shape[1]), BF16), rows], axis=0))
            at += count
            res = dot(self.flipped_far[late, own, :], jnp.concatenate(parts, axis=1), NN)
            lanes = res.shape[1] // 2
            blocks = [res[:, part * lanes:(part + 1) * lanes].reshape(self.half_size, self.tile // 2, lanes) for part in range(2)]
            self.relay_send[slot, :, pl.ds(late * self.tile, self.tile), :] = jnp.concatenate(blocks, axis=1).astype(BF16)
        late_at = pl.ds(self.early_rows, self.late_rows)

        @pl.loop(1, self.half_size)
        def _(step):
            place = jnp.bitwise_xor(self.place, self.half_size - step)
            self.copy(self.relay_send.at[slot, place], self.recv.at[b, self.twin, late_at], self.relay_send_sem.at[slot],
                      self.relay_recv_sem.at[b], self.half * self.half_size + place).start()

        self.recv[b, self.twin, late_at] = self.relay_send[slot, self.place]

    def arrive(self, b):
        self.all_direct(b).wait_recv()
        self.all_relayed(b).wait_recv()

    def drain(self):
        for b in range(max(0, self.batch - SLOTS), self.batch):
            self.all_direct(b).wait_send()
            self.bridge(b).wait_send()
            self.all_relayed(b).wait_send()


class Share:
    def __init__(self, me, group, batch, send, message, out, sems):
        self.batch, self.send, self.message, self.out = batch, send, message, out
        self.send_sem, self.recv_sem, self.local_sem = sems
        self.size = group // 2
        self.base = me // self.size * self.size
        self.place = lax.rem(me, self.size)

    def rank(self, place):
        return place // 4 + 2 * (lax.rem(place, 4) // 2) + 4 * lax.rem(place, 2)

    def copy(self, slot, source, b, target, place):
        return pltpu.make_async_remote_copy(
            self.send.at[slot, source], self.out.at[b, target], self.send_sem.at[slot], self.recv_sem.at[b],
            device_id={'lat': self.base + place}, device_id_type=MESH)

    def every(self, b):
        span = pl.ds(0, self.size - 1)
        return self.copy(lax.rem(b, SLOTS), span, b, span, lax.rem(self.place + 1, self.size))

    def keep(self, b):
        slot = lax.rem(b, SLOTS)
        return pltpu.make_async_copy(self.send.at[slot, self.rank(self.place)], self.out.at[b, self.place],
                                     self.local_sem.at[slot])

    def give(self, b, coef):
        slot_b = lax.rem(b, SLOTS)

        @pl.when(b >= SLOTS)
        def _():
            self.every(b - SLOTS).wait_send()

        size = self.size
        m_local = size
        tile = 2 * size

        def rows(part, slot, rank, first, count):
            return coef[part, pl.ds((first * size + rank) * m_local + slot, count, stride=size * m_local), :]

        for rank in range(size):
            for part in range(2):
                for pair in range(m_local // 2):
                    block = rows(part, pair, rank, 0, tile)
                    if pair:
                        block = block + rows(part, m_local - pair, rank, 2 * (m_local - pair), tile)
                    self.message[rank, pl.ds((part * (m_local // 2) + pair) * tile, tile), :] = block
                self.message[rank, pl.ds(m_local * tile + part * size, size), :] = rows(part, m_local // 2, rank, size, size)
        for rank in range(size):
            self.send[slot_b, rank] = self.message[rank].astype(BF16)
        self.keep(b).start()

        @pl.loop(1, size)
        def _(step):
            place = jnp.bitwise_xor(self.place, size - step)
            self.copy(slot_b, self.rank(place), b, self.place, place).start()

        self.keep(b).wait()

    def drain(self):
        for b in range(max(0, self.batch - SLOTS), self.batch):
            self.every(b).wait_send()

    def arrive(self, b):
        self.every(b).wait_recv()


def clear_after(coef, used):
    for part in range(coef.shape[0]):
        coef[part, pl.ds(used, coef.shape[1] - used), :] = jnp.zeros((coef.shape[1] - used, coef.shape[2]), F32)


def greet(me, group):
    barrier = pltpu.get_barrier_semaphore()

    @pl.loop(1, group)
    def _(step):
        pl.semaphore_signal(barrier, inc=1, device_id={'lat': lax.rem(me + step, group)}, device_id_type=MESH)


def meet(group):
    pl.semaphore_wait(pltpu.get_barrier_semaphore(), group - 1)


class Tables:
    def __init__(self, waves, whole, stage, sem):
        self.waves, self.whole, self.stage, self.sem = waves, whole, stage, sem

    def start(self):
        for n, wave in enumerate(self.waves):
            pltpu.make_async_copy(self.whole.at[wave], self.stage.at[n], self.sem).start()

    def wait(self):
        pltpu.make_async_copy(self.whole.at[pl.ds(0, len(self.waves))], self.stage, self.sem).wait()


def own_tables(me, group, whole, stage, sem):
    return Tables([slot * group + me for slot in range(stage.shape[0])], whole, stage, sem)


def far_tables(swap, whole, stage, sem):
    return Tables([(swap.direct + n) * swap.group + swap.twin for n in range(stage.shape[0])], whole, stage, sem)


def expand_rows(stage, expanded, rows_local):
    m_local, degrees, lats = stage.shape
    row = lax.broadcasted_iota(jnp.int32, (lats, 2 * lats), 0)
    col = lax.broadcasted_iota(jnp.int32, (lats, 2 * lats), 1)
    source = col // (2 * rows_local)
    inner = col % (2 * rows_local)
    for part in range(2):
        pick = (row == source * rows_local + inner - part * rows_local) & (inner // rows_local == part)
        pick = pick.astype(F32).astype(BF16)
        for slot in range(m_local):
            expanded[slot, pl.ds(part * degrees, degrees), :] = dot(stage[slot].astype(BF16), pick, NN).astype(BF16)


def flip_rows(stage, flipped):
    for slot in range(stage.shape[0]):
        flipped[slot] = stage[slot].T.astype(BF16)


def analyse(values_at, table, turn, rows_local):
    modes = table.shape[1]
    for t in range(0, rows_local, 2):
        pair = jnp.concatenate([values_at(t), values_at(t + 1)], axis=0)
        high, low = split_halves(pair * 0.5)
        out = 2.0 * (dot(table[0], high, NT) + dot(table[0], low, NT) + dot(table[1], high, NT))
        channels = out.shape[1] // 2
        turn[pl.ds(t, modes, stride=rows_local), :] = out[:, :channels]
        turn[pl.ds(t + 1, modes, stride=rows_local), :] = out[:, channels:]


def pack_blocks(turn, send, slot):
    group, rows, lanes = send.shape[1:]
    for d in range(group):
        send[slot, d] = turn[pl.ds(d * rows, rows), :].astype(BF16)


def unpack_blocks(recv, b, turn):
    group, rows, lanes = recv.shape[1:]
    for d in range(group):
        turn[pl.ds(d * rows, rows), :] = recv[b, d].astype(F32)


def synthesise(turn, t, table, rows_local):
    modes = table.shape[1]
    spec = turn[pl.ds(t, modes, stride=rows_local), :].astype(BF16)
    return dot(spec, table[0], TN) + dot(spec, table[1], TN)


def legendre_forward(recv, b, expanded, out, rows_local):
    m_local = expanded.shape[0]
    degrees = expanded.shape[1] // 2
    group, _, lanes = recv.shape[1:]
    tile = 2 * rows_local
    for slot in range(m_local):
        rows = recv[b, :, pl.ds(slot * tile, tile), :].reshape(group * tile, lanes)
        res = dot(expanded[slot], rows, NN)
        for part in range(2):
            out[part, pl.ds(slot, degrees, stride=m_local), :] = res[part * degrees:(part + 1) * degrees]


def legendre_inverse(coef, flipped, swap, slot_out, rows_local):
    m_local, lats, degrees = flipped.shape
    send = swap.send
    at = 0
    group = lats // rows_local
    tile = 2 * rows_local
    for slot in range(m_local):
        parts = [coef.at[part][pl.ds(slot, degrees, stride=m_local), :].astype(BF16) for part in range(2)]
        if slot >= swap.direct:
            first = slot * group
            for part in range(2):
                swap.bridge_send[slot_out, part, pl.ds(at, degrees - first), :] = parts[part][first:]
            at += degrees - first
        res = dot(flipped[slot], jnp.concatenate(parts, axis=1), NN)
        lanes = res.shape[1] // 2
        blocks = [res[:, part * lanes:(part + 1) * lanes].reshape(group, rows_local, lanes) for part in range(2)]
        send[slot_out, :, pl.ds(slot * tile, tile), :] = jnp.concatenate(blocks, axis=1).astype(BF16)


def gelu_slope(values):
    cumulative = 0.5 * (1.0 + lax.erf(values * math.sqrt(0.5)))
    density = jnp.exp(-0.5 * values * values) * (1.0 / math.sqrt(2.0 * math.pi))
    return cumulative + values * density


def mix_block(planes):
    real, imag = planes[0], planes[1]
    return jnp.concatenate([jnp.concatenate([real, -imag], axis=1), jnp.concatenate([imag, real], axis=1)], axis=0)


class WeightSum:
    def __init__(self, me, group, sums, got, out, sems):
        self.me, self.sums, self.got, self.out, self.sems = me, sums, got, out, sems
        self.core, self.y = lax.rem(me, 2), lax.rem(me // 2, 2)
        self.near, self.far = lax.rem(me // 4, 2), me // (group // 2)
        self.rank = self.near + 2 * self.y + 4 * self.core

    def peer(self, phase):
        step = (1, 2, 4, 8)[phase]
        bit = (self.core, self.y, self.near, self.far)[phase]
        return {'lat': self.me + step - 2 * step * bit}

    def remote(self, phase, k, source, target, stage):
        return pltpu.make_async_remote_copy(source, target, self.sems.at[0, stage, k], self.sems.at[1, stage, k],
                                            device_id=self.peer(phase), device_id_type=MESH)

    def halving(self, k):
        pair, at = self.piece(k)
        return self.remote(3, k, self.sums.at[2 * pair + 1 - self.far, at], self.got.at[k], 4)

    def piece(self, k):
        rows = self.got.shape[1]
        pieces = self.sums.shape[1] // rows
        return k // pieces, pl.ds(pl.multiple_of(lax.rem(k, pieces) * rows, rows), rows)

    def settle(self, k):
        pair, at = self.piece(k)
        mine = 2 * pair + self.far
        return pltpu.make_async_copy(self.sums.at[mine, at], self.out.at[mine, self.rank, at], self.sems.at[0, 5, k])

    def doubling(self, phase, k):
        pair, at = self.piece(k)
        if phase == 3:
            mine = 2 * pair + self.far
            return self.remote(3, k, self.sums.at[mine, at], self.out.at[mine, self.rank, at], 3)
        width = (4, 2, 1)[phase]
        first = (4 * self.core, 4 * self.core + 2 * self.y, self.rank)[phase]
        span = self.out.at[pl.ds(2 * pair, 2), pl.ds(first, width), at]
        return self.remote(phase, k, span, span, phase)

    def reduce_step(self, k):
        self.halving(k).wait()
        pair, at = self.piece(k)
        mine = 2 * pair + self.far
        self.sums[mine, at] = self.sums[mine, at] + self.got[k]
        self.settle(k).start()
        self.doubling(3, k).start()

    def gather_step(self, phase, k):
        if phase == 2:
            self.settle(k).wait()
        self.doubling(phase + 1, k).wait()
        if phase >= 0:
            self.doubling(phase, k).start()


def shared_place(part, slot, step, m_local):
    tile = 2 * m_local
    if slot == m_local // 2:
        return m_local * tile + part * m_local + step - m_local
    pair = min(slot, m_local - slot) if slot else 0
    shift = 0 if slot < m_local // 2 else 2 * slot
    return (part * (m_local // 2) + pair) * tile + step - shift


def weigh(shared, sources, sums, m_local):
    stride = shared.shape[1] // sources

    @pl.loop(0, sums.shape[0])
    def _(step):
        sides = []
        for which in range(2):
            slots = []
            for slot in range(m_local):
                used = step >= 2 * slot
                parts = []
                for part in range(2):
                    place = jnp.where(used, shared_place(part, slot, step, m_local), 0)
                    rows = shared[which, pl.ds(place, sources, stride=stride), :]
                    parts.append(jnp.where(used, rows, 0.0))
                slots.append(jnp.concatenate(parts, axis=1))
            sides.append(jnp.concatenate(slots, axis=0).astype(BF16))
        big = dot(sides[0], sides[1], TN)
        half = big.shape[0] // 2
        real, imag = pl.ds(0, half, stride=2), pl.ds(1, half, stride=2)
        sums[step, real, :] = sums[step, real, :] + (big[:half, :half] + big[half:, half:])
        sums[step, imag, :] = sums[step, imag, :] + (big[half:, :half] - big[:half, half:])


def whole_kernel(group, rows_local, field, grad, base_hbm, gained_hbm, p_fwd, p_inv, w_mix, field_out, grad_w, back_out, coef_shared,
                 mixed_shared, field_buf, grad_buf, turn, stage, stage_far, expanded_fwd, expanded_inv, flipped, send_f, recv_f,
                 padded, coef, mixed, w_in, planes, bridged, send_d, recv_d, message, share_send_a, share_send_d, halves,
                 shared, sums, back, got, field_sem, grad_sem, p_sem, far_sem, send_f_sem, recv_f_sem, w_sem, bridged_sems,
                 send_d_sem, recv_d_sem, share_a_sems, share_d_sems, half_sem, out_sem, gw_sem, again_sems, back_sem, last_sem, base, gained,
                 table_sem):
    me = lax.axis_index('lat')
    batch = field.shape[0]
    channels = field.shape[1] // rows_local
    m_local, degrees = stage.shape[:2]
    used = degrees * m_local
    bunch = coef.shape[0]
    sources, share_rows = coef_shared.shape[1:3]

    def fetch_field(b):
        return Halves(field, b, field_buf, lax.rem(b, 2), field_sem)

    def fetch_grad(b):
        return Halves(grad, b, grad_buf, lax.rem(b, 2), grad_sem)

    def put(b):
        return pltpu.make_async_copy(back.at[lax.rem(b, bunch)], back_out.at[b], out_sem.at[lax.rem(b, bunch)])

    def fetch_back(b):
        return pltpu.make_async_copy(back_out.at[b], coef.at[lax.rem(b, 2)], back_sem.at[lax.rem(b, 2)])

    def fetch_last(b):
        return Halves(grad, b, field_buf, lax.rem(b, 2), field_sem)

    def put_last(b):
        return Halves(field_out, b, field_buf, lax.rem(b, 2), last_sem, outward=True)

    def fetch_shares(b):
        slot = lax.rem(b, 2)
        return [pltpu.make_async_copy(whole.at[b], halves.at[slot, which], half_sem.at[slot, which])
                for which, whole in enumerate((mixed_shared, coef_shared))]

    load_base = pltpu.make_async_copy(base_hbm, base, table_sem.at[0])
    load_gained = pltpu.make_async_copy(gained_hbm, gained, table_sem.at[1])
    fetch_field(0).start()
    load_base.start()
    greet(me, group)
    load_gained.start()
    fetch_grad(0).start()
    loading = own_tables(me, group, p_fwd, stage, p_sem)
    loading_inv = own_tables(me, group, p_inv, stage, p_sem)
    loading.start()
    swap_f = Exchange(me, group, batch, send_f, recv_f, send_f_sem, recv_f_sem)
    swap_g = BridgedExchange(me, group, batch, bridged, bridged_sems)
    swap_h = BridgedExchange(me, group, batch, bridged, again_sems)
    total = WeightSum(me, group, sums, got, grad_w, gw_sem)
    swap_d = Exchange(me, group, batch, send_d, recv_d, send_d_sem, recv_d_sem)
    share_a = Share(me, group, batch, share_send_a, message, coef_shared, share_a_sems)
    share_d = Share(me, group, batch, share_send_d, message, mixed_shared, share_d_sems)
    loading_far = far_tables(swap_g, p_inv, stage_far, far_sem)
    loading_far.start()
    loading_fwd = own_tables(me, group, p_fwd, stage, p_sem)
    loading_far_fwd = far_tables(swap_h, p_fwd, stage_far, far_sem)
    chunks = got.shape[0]

    def build_planes():
        depth, per = w_in.shape[:2]
        blocks = degrees // per
        half = w_in.shape[2] // 2

        def fetch(k):
            return pltpu.make_async_copy(w_mix.at[pl.ds(k * per, per)], w_in.at[lax.rem(k, depth)], w_sem.at[lax.rem(k, depth)])

        for k in range(depth - 1):
            fetch(k).start()

        @pl.loop(0, blocks)
        def _(k):
            @pl.when(k + depth - 1 < blocks)
            def _():
                fetch(k + depth - 1).start()

            fetch(k).wait()
            for inner in range(per):
                rows = w_in.at[lax.rem(k, depth), inner]
                for part in range(2):
                    planes[k * per + inner, part] = rows[pl.ds(part, half, stride=2), :].astype(BF16)

    def unmix_bunch():
        @pl.loop(0, degrees // 8)
        def _(k):
            for inner in range(8):
                at = pl.ds(pl.multiple_of((k * 8 + inner) * m_local, m_local), m_local)
                rows = [back[:, part, at, :].reshape(bunch * m_local, channels) for part in range(2)]
                res = dot(jnp.concatenate(rows, axis=1).astype(BF16), mix_block(planes[k * 8 + inner]), NN)
                for part in range(2):
                    back[:, part, at, :] = res[:, part * channels:(part + 1) * channels].reshape(bunch, m_local, channels)

    def mix_bunch():
        @pl.loop(0, degrees // 8)
        def _(k):
            for inner in range(8):
                at = pl.ds(pl.multiple_of((k * 8 + inner) * m_local, m_local), m_local)
                rows = [coef[:, part, at, :].reshape(bunch * m_local, channels) for part in range(2)]
                res = dot(jnp.concatenate(rows, axis=1).astype(BF16), mix_block(planes[k * 8 + inner]), NT)
                for part in range(2):
                    mixed[:, part, at, :] = res[:, part * channels:(part + 1) * channels].reshape(bunch, m_local, channels)

    def weigh_sample(b):
        for copy in fetch_shares(b):
            copy.wait()
        for which in range(2):
            for source in range(sources):
                at = pl.ds(source * (shared.shape[1] // sources), share_rows)
                shared[which, at, :] = halves[lax.rem(b, 2), which, source].astype(F32)
        weigh(shared, sources, sums, m_local)

    def collect(b):
        share_a.arrive(b)
        share_d.arrive(b)
        for copy in fetch_shares(b):
            copy.start()

    lag_a, lag_b, lag_c, lag_d = 2, 3, 5, 7
    lag_e = batch + lag_c
    close = batch + lag_d
    steps = [total.reduce_step] + [functools.partial(total.gather_step, p) for p in (2, 1, 0, -1)]

    def advance(n, sub):
        @pl.when((n >= 0) & (n * 2 + sub + 2 < chunks))
        def _():
            total.halving(n * 2 + sub + 2).start()

        for late, step in reversed(list(enumerate(steps))):
            k = (n - late) * 2 + sub

            @pl.when((k >= 0) & (k < chunks))
            def _():
                step(k)

    def take_modes(b):
        @pl.when(b + 1 < batch)
        def _():
            fetch_field(b + 1).start()

        fetch_field(b).wait()
        half = lax.rem(b, 2)
        analyse(lambda t: read_row(field_buf, half, t, channels, rows_local), base, turn, rows_local)
        swap_f.reserve(b)
        pack_blocks(turn, send_f, lax.rem(b, SLOTS))

    load_base.wait()
    take_modes(0)
    meet(group)

    def body(i, carry):
        @pl.when((i >= lag_e) & (i < batch + lag_e))
        def _():
            b = i - lag_e

            @pl.when(b + 1 < batch)
            def _():
                fetch_back(b + 1).start()

            fetch_back(b).wait()
            swap_h.reserve(b)
            legendre_inverse(coef.at[lax.rem(b, 2)], flipped, swap_h, lax.rem(b, SLOTS), rows_local)
            swap_h.start(b)

        @pl.when((i >= 1) & (i < batch))
        def _():
            take_modes(i)

        @pl.when(i < batch)
        def _():
            swap_f.start(i)

        @pl.when(i == 0)
        def _():
            clear_after(padded, used)
            load_gained.wait()
            loading.wait()
            expand_rows(stage, expanded_fwd, rows_local)
            loading_inv.start()
            loading_far.wait()
            flip_rows(stage_far, swap_g.flipped_far)

        @pl.when(i == 1)
        def _():
            build_planes()
            loading_inv.wait()
            expand_rows(stage, expanded_inv, rows_local)
            flip_rows(stage, flipped)
            sums[...] = jnp.zeros_like(sums)

        @pl.when((i >= lag_a) & (i < batch + lag_a))
        def _():
            b = i - lag_a
            swap_f.arrive(b)
            legendre_forward(recv_f, b, expanded_fwd, padded, rows_local)
            coef[lax.rem(b, bunch)] = padded[:, pl.ds(0, used), :]
            share_a.give(b, padded)

            @pl.when(lax.rem(b, bunch) == bunch - 1)
            def _():
                mix_bunch()

        @pl.when((i >= lag_b) & (i < batch + lag_b))
        def _():
            b = i - lag_b
            swap_g.reserve(b)
            legendre_inverse(mixed.at[lax.rem(b, bunch)], flipped, swap_g, lax.rem(b, SLOTS), rows_local)
            swap_g.start(b)

        @pl.when((i >= lag_b + 1) & (i < batch + lag_b + 1))
        def _():
            swap_g.relay(i - lag_b - 1)

        @pl.when((i >= lag_c) & (i < batch + lag_c))
        def _():
            b = i - lag_c
            half = lax.rem(b, 2)

            @pl.when(b + 1 < batch)
            def _():
                fetch_grad(b + 1).start()

            fetch_grad(b).wait()
            swap_g.arrive(b)
            unpack_blocks(swap_g.recv, b, turn)
            for t in range(rows_local):
                slope = gelu_slope(synthesise(turn, t, gained, rows_local))
                given = read_row(grad_buf, half, t, channels, rows_local)
                write_row(grad_buf, half, t, channels, rows_local, given * slope)
            analyse(lambda t: read_row(grad_buf, half, t, channels, rows_local), gained, turn, rows_local)
            swap_d.reserve(b)
            pack_blocks(turn, send_d, lax.rem(b, SLOTS))
            swap_d.start(b)

        @pl.when(i == lag_e - 2)
        def _():
            loading_fwd.start()
            loading_far_fwd.start()

        @pl.when(i == lag_e - 1)
        def _():
            loading_fwd.wait()
            flip_rows(stage, flipped)
            loading_far_fwd.wait()
            flip_rows(stage_far, swap_h.flipped_far)
            swap_g.drain()
            fetch_back(0).start()

        @pl.when((i >= lag_d) & (i < batch + lag_d))
        def _():
            b = i - lag_d

            @pl.when((b >= bunch) & (lax.rem(b, bunch) == 0))
            def _():
                unmix_bunch()
                for n in range(bunch):
                    put(b - bunch + n).start()

            @pl.when(b >= 2)
            def _():
                weigh_sample(b - 2)

            @pl.when(b >= 1)
            def _():
                collect(b - 1)

            swap_d.arrive(b)
            legendre_forward(recv_d, b, expanded_inv, padded, rows_local)
            share_d.give(b, padded)

            @pl.when(b >= bunch)
            def _():
                put(b - bunch).wait()

            back[lax.rem(b, bunch)] = padded[:, pl.ds(0, used), :]

        @pl.when(i == close)
        def _():
            fetch_last(0).start()
            weigh_sample(batch - 2)
            collect(batch - 1)
            weigh_sample(batch - 1)
            for k in range(2):
                total.halving(k).start()

        advance(i - close, 0)

        @pl.when((i >= lag_e + 1) & (i < batch + lag_e + 1))
        def _():
            swap_h.relay(i - lag_e - 1)

        @pl.when((i >= close) & (i < batch + close))
        def _():
            b = i - close
            half = lax.rem(b, 2)

            @pl.when(b >= 1)
            def _():
                put_last(b - 1).wait()

            @pl.when(b + 1 < batch)
            def _():
                fetch_last(b + 1).start()

            fetch_last(b).wait()
            swap_h.arrive(b)
            unpack_blocks(swap_h.recv, b, turn)
            for t in range(rows_local):
                added = synthesise(turn, t, base, rows_local)
                given = read_row(field_buf, half, t, channels, rows_local)
                write_row(field_buf, half, t, channels, rows_local, given + added)
            put_last(b).start()

        @pl.when(i == close + 1)
        def _():
            unmix_bunch()
            for n in range(bunch):
                put(batch - bunch + n).start()

        @pl.when(i == close + 3)
        def _():
            for n in range(bunch):
                put(batch - bunch + n).wait()

        advance(i - close, 1)
        return carry

    lax.fori_loop(0, close + max(batch, chunks // 2 + 4), body, 0)
    for swap in (swap_f, swap_h, swap_d, share_a, share_d):
        swap.drain()
    put_last(batch - 1).wait()


def finish_kernel(first, second, first_out, second_out, first_ring, second_ring, in_sem, out_sem):
    depth = first_ring.shape[0]
    pieces = []
    for side, (source, target, ring) in enumerate(((first, first_out, first_ring), (second, second_out, second_ring))):
        for n in range(source.shape[0]):
            slot = n % depth
            take = pltpu.make_async_copy(source.at[n], ring.at[slot], in_sem.at[side, slot])
            give = pltpu.make_async_copy(ring.at[slot], target.at[n], out_sem.at[side, slot])
            pieces.append(((n, side), (side, n), take, give))
    pieces.sort(key=lambda piece: piece[0])
    given = {piece[1]: piece[3] for piece in pieces}
    waited = set()
    for k in range(len(pieces) + depth):
        if k < len(pieces):
            _, (side, n), take, _ = pieces[k]
            if n >= depth:
                given[side, n - depth].wait()
                waited.add((side, n - depth))
            take.start()
        if k >= depth:
            pieces[k - depth][2].wait()
            pieces[k - depth][3].start()
    for _, place, _, give in pieces:
        if place not in waited:
            give.wait()


def any_specs(n):
    return [pl.BlockSpec(memory_space=pl.ANY)] * n


def params(collective_id=None):
    if collective_id is None:
        return pltpu.CompilerParams(vmem_limit_bytes=VMEM_LIMIT)
    return pltpu.CompilerParams(collective_id=collective_id, has_side_effects=True, vmem_limit_bytes=VMEM_LIMIT)


def solution(mesh):
    group = mesh.shape['lat']
    field_spec = P('member', None, 'lat', None)

    def local_step(field_loc, grad_loc, p_fwd, p_inv, w_mix):
        batch, channels, rows_local, lon_count = field_loc.shape
        degrees, lats = p_fwd.shape[1:]
        m_local = p_fwd.shape[0] // group
        modes = group * m_local * 2
        base, gained = (two_halves(table) for table in dft_tables(group, m_local, lon_count))
        field = field_loc.reshape(batch, channels * rows_local, lon_count)
        grad = grad_loc.reshape(batch, channels * rows_local, lon_count)
        w_rows = jnp.swapaxes(w_mix, 2, 3).reshape(degrees, channels * 2, channels)
        dma, vmem = pltpu.SemaphoreType.DMA, pltpu.VMEM
        block_rows = m_local * 2 * rows_local
        coef_shape = (batch, 2, degrees * m_local, channels)
        send_t = vmem((SLOTS, group, block_rows, channels), BF16)
        recv_t = vmem((batch, group, block_rows, channels), BF16)
        turn_t = vmem((modes * rows_local, channels), F32)
        stage_t = vmem((m_local, degrees, lats), F32)
        expanded_t = vmem((m_local, 2 * degrees, 2 * lats), BF16)
        flipped_t = vmem((m_local, lats, degrees), BF16)
        field_t = vmem((2, lon_count // LANES, channels * rows_local, LANES), F32)
        any_spec = pl.BlockSpec(memory_space=pl.ANY)
        late = sum(degrees - slot * group < lats // 2 for slot in range(m_local))
        far_rows = sum(degrees - slot * group for slot in range(m_local - late, m_local))
        late_rows = late * 2 * rows_local
        bridged_t = (send_t, recv_t, vmem((SLOTS, 2, far_rows, channels), BF16), vmem((batch, 2, far_rows, channels), BF16),
                     vmem((SLOTS, group // 2, late_rows, channels), BF16), vmem((late, lats, degrees), BF16))
        bridged_sems = (dma((SLOTS,)), dma((batch,))) * 3

        ranks = group // 2
        share_rows = (m_local + 1) * 2 * ranks
        share_out = jax.ShapeDtypeStruct((batch, ranks, share_rows, channels), BF16)
        share_sems = (dma((SLOTS,)), dma((batch,)), dma((SLOTS,)))

        far_stage_t = vmem((late, degrees, lats), F32)
        steps = degrees // ranks
        sums_shape = (steps, channels * 2, channels)
        planes_shape = (degrees, 2, channels, channels)
        single_t = vmem((BUNCH,) + coef_shape[1:], F32)
        share_send_t = vmem((SLOTS, ranks, share_rows, channels), BF16)
        swap_sems = (dma((SLOTS,)), dma((batch,)))
        field_out, gw_total, _, _, _ = pl.pallas_call(
            functools.partial(whole_kernel, group, rows_local), name='whole',
            out_shape=[jax.ShapeDtypeStruct(grad.shape, F32),
                       jax.ShapeDtypeStruct((steps, ranks, channels * 2, channels), F32),
                       jax.ShapeDtypeStruct(coef_shape, F32), share_out, share_out],
            in_specs=[any_spec] * 7, out_specs=[any_spec] * 5,
            scratch_shapes=[field_t, field_t, turn_t, stage_t, far_stage_t, expanded_t, expanded_t, flipped_t, send_t, recv_t,
                            vmem((2, 2 * degrees * m_local, channels), F32), single_t, single_t,
                            vmem((4, 4, channels * 2, channels), F32), vmem(planes_shape, BF16), bridged_t, send_t, recv_t,
                            vmem((ranks, share_rows, channels), F32), share_send_t, share_send_t,
                            vmem((2, 2) + share_out.shape[1:], BF16), vmem((2, ranks * (share_rows + 8), channels), F32),
                            vmem(sums_shape, F32), single_t, vmem((PIECES * steps // 2, channels * 2 // PIECES, channels), F32),
                            dma((2, 2)), dma((2, 2)), dma(()), dma(()), *swap_sems, dma((4,)), bridged_sems, *swap_sems,
                            share_sems, share_sems, dma((2, 2)), dma((BUNCH,)), dma((2, 6, PIECES * steps // 2)), bridged_sems,
                            dma((2,)), dma((2, 2)), vmem(base.shape, BF16), vmem(base.shape, BF16), dma((2,))],
            compiler_params=params(0))(field, grad, base, gained, p_fwd, p_inv, w_rows)

        gw_total = gw_total.reshape(steps, ranks * channels * 2, channels)
        results = [jax.ShapeDtypeStruct(whole.shape, F32) for whole in (field_out, gw_total)]
        field_out, gw_total = pl.pallas_call(
            finish_kernel, name='finish', out_shape=results, in_specs=[any_spec] * 2, out_specs=[any_spec] * 2,
            scratch_shapes=[vmem((RING,) + whole.shape[1:], F32) for whole in results] + [dma((2, RING)), dma((2, RING))],
            compiler_params=params())(field_out, gw_total)

        grad_wmix = jnp.swapaxes(gw_total.reshape(degrees, channels, 2, channels), 2, 3)
        return field_out.reshape(grad_loc.shape), grad_wmix

    return jax.shard_map(local_step, mesh=mesh, in_specs=(field_spec, field_spec, P(), P(), P()),
                         out_specs=(field_spec, P('member', None, None, None)), check_vma=False)
```
